32 devices in a mesh: dp: 8 (over z, x), tensor: 4 (over y, core).
Axes of the slice: x: 2, y: 2, z: 4, core: 2. Of those that a mesh axis runs over, the one named last changes fastest.
Arguments:
- patches: bfloat16 [16384, 768], P(('dp', 'tensor')), may hold values from -6 to 6
- counts: int32 [8, 3], P('dp'), may hold values from 1 to 2, as said below
- norm_gain: float32 [2, 768], replicated, may hold values from 0.5 to 1.5
- norm_bias: float32 [2, 768], replicated, may hold values from -3 to 3
- w_qkv: bfloat16 [768, 3, 768], P(None, None, 'tensor'), may hold values from -0.21875 to 0.21875
- b_qv: float32 [2, 768], P(None, 'tensor'), may hold values from -3 to 3
- w_out: bfloat16 [768, 768], P('tensor'), may hold values from -0.625 to 0.625
- out_bias: float32 [2, 768], replicated, may hold values from -3 to 3
- w_up: bfloat16 [768, 3072], P(None, 'tensor'), may hold values from -0.21875 to 0.21875
- b_up: float32 [3072], P('tensor'), may hold values from -3 to 3
- w_down: bfloat16 [3072, 768], P('tensor'), may hold values from -0.109375 to 0.109375
- cotangent: bfloat16 [16384, 768], P(('dp', 'tensor')), may hold values from -6 to 6
Outputs:
- encoded: bfloat16 [16384, 768], P(('dp', 'tensor'))
- patches_grad: bfloat16 [16384, 768], P(('dp', 'tensor'))
- norm_gain_grad: float32 [2, 768], replicated
- norm_bias_grad: float32 [2, 768], replicated
- w_qkv_grad: float32 [768, 3, 768], P('dp', None, 'tensor')
- b_qv_grad: float32 [2, 768], replicated
- w_out_grad: float32 [768, 768], P('tensor', 'dp')
- out_bias_grad: float32 [2, 768], replicated
- w_up_grad: float32 [768, 3072], P('dp', 'tensor')
- b_up_grad: float32 [3072], replicated
- w_down_grad: float32 [3072, 768], P('tensor', 'dp')
The draws below stay inside these ranges and needn't reach their ends.
Inputs may be any that keep to these rules, and one draw needn't show every extreme that they name: `counts`: in every column some group has exactly 2 images of that size; every group has at least one image of each size.
All inputs are finite; a program needn't handle non-finite values.
Results may differ from the reference program's by a relative error of at most 0.015.
Values may be sent and summed in bfloat16 or wider, within the bound.
A program may use at most 192 MiB of HBM per device.

```python
import jax
import jax.numpy as jnp
from jax import lax

D = 768
HEADS = 12
HEAD_DIM = 64
FF = 3072
SIDE_S = 12
SIDE_M = 15
SIDE_L = 20
MAX_IMG = 2
TOK_DEV = 2048
GROUPS = 8
TOKENS = 16384


def draw_counts(key, part):
    drawn = jax.random.randint(jax.random.fold_in(key, 11), (GROUPS, 3), 1, MAX_IMG + 1)
    columns = jnp.arange(3, dtype=jnp.int32)
    low_rows = jax.random.randint(jax.random.fold_in(key, 12), (3,), 0, GROUPS)
    drawn = drawn.at[low_rows, columns].set(1)
    top_rows = jax.random.randint(jax.random.fold_in(key, 13), (3,), 0, GROUPS)
    drawn = drawn.at[top_rows, columns].set(MAX_IMG)
    return drawn.astype(jnp.int32)


def strengthened(entries, key, source, target, shards_of, factor):
    def block_of(position):
        return (jnp.arange(entries.shape[position]) // (entries.shape[position] // shards_of)).reshape((-1,) + (1,) * (entries.ndim - 1 - position))

    one_side = jax.random.permutation(key, shards_of)[block_of(target)]
    far = (block_of(target) + shards_of // 2) % shards_of
    return jnp.where((block_of(source) == one_side) | (block_of(source) == far), factor * entries, entries)


def shard_levels(rng, extent, cuts, least, high):
    def one(axis_at, blocks):
        heights = jax.random.uniform(jax.random.fold_in(jax.random.fold_in(rng, 6), axis_at), (blocks,), jnp.float32, least / len(cuts), high / len(cuts))
        return jnp.repeat(jnp.exp(heights), extent[axis_at] // blocks).reshape((-1,) + (1,) * (len(extent) - axis_at - 1))

    level = one(*cuts[0])
    for cut in cuts[1:]:
        level = level * one(*cut)
    return level


def normal_values(stream_key, dims, scale, reach, pieces=(), kind=jnp.bfloat16):
    array = scale * jax.random.normal(stream_key, dims, jnp.float32)
    if pieces:
        array = array * shard_levels(stream_key, dims, pieces, -0.22, 0.18)
    return jnp.clip(array, -reach, reach).astype(kind)


def gaussian_with(stream_key, shape, deviation, most, pieces, heavy, kind=jnp.bfloat16):
    values = deviation * jax.random.normal(stream_key, shape, jnp.float32)
    if pieces:
        values = values * shard_levels(stream_key, shape, pieces, -0.22, 0.18)
    return jnp.clip(strengthened(values, jax.random.fold_in(stream_key, 3), *heavy), -most, most).astype(kind)


def setup_inputs(seed: int = 0) -> dict:
    seeds = jax.random.split(jax.random.key(seed), 13)
    return {
        "patches": gaussian_with(seeds[0], (TOKENS, D), 1.0, 6.0, ((0, 32),), (0, 1, 32, 2.75)),
        "counts": draw_counts(jax.random.fold_in(seeds[12], 71), 0),
        "norm_gain": jnp.clip(1.0 + 0.1 * jax.random.normal(seeds[2], (2, D), jnp.float32), 0.5, 1.5),
        "norm_bias": normal_values(seeds[3], (2, D), 0.5, 3.0, (), jnp.float32),
        "w_qkv": normal_values(seeds[4], (D, 3, D), D ** -0.5, 0.21875, ((2, 4),)),
        "b_qv": normal_values(seeds[5], (2, D), 0.5, 3.0, ((1, 4),), jnp.float32),
        "w_out": normal_values(seeds[6], (D, D), (D // 8) ** -0.5, 0.625, ((0, 4),)),
        "out_bias": normal_values(seeds[7], (2, D), 0.5, 3.0, (), jnp.float32),
        "w_up": normal_values(seeds[8], (D, FF), D ** -0.5, 0.21875, ((1, 4),)),
        "b_up": normal_values(seeds[9], (FF,), 0.5, 3.0, ((0, 4),), jnp.float32),
        "w_down": normal_values(seeds[10], (FF, D), FF ** -0.5, 0.109375, ((0, 4),)),
        "cotangent": normal_values(seeds[11], (TOKENS, D), 1.0, 6.0, ((0, 32),)),
    }


EPSILON = 1e-06

@jax.custom_vjp
def low(v):
    return lax.optimization_barrier(v.astype(jnp.bfloat16)).astype(jnp.float32)

@jax.custom_vjp
def low_back(v):
    return v

def low_keep(v):
    return (low(v), None)

def low_pass(kept, grad):
    return (grad,)

def back_keep(v):
    return (v, None)

def back_low(kept, grad):
    return (low(grad),)
low.defvjp(low_keep, low_pass)
low_back.defvjp(back_keep, back_low)

def layout(group_counts):
    positions = jnp.arange(TOK_DEV, dtype=jnp.int32)
    area_small = SIDE_S * SIDE_S
    area_middle = SIDE_M * SIDE_M
    area_large = SIDE_L * SIDE_L
    end_small = group_counts[0] * area_small
    end_middle = end_small + group_counts[1] * area_middle
    end_large = end_middle + group_counts[2] * area_large
    size_class = (positions >= end_small).astype(jnp.int32) + (positions >= end_middle).astype(jnp.int32)
    begins = jnp.where(size_class == 0, 0, jnp.where(size_class == 1, end_small, end_middle))
    area_len = jnp.where(size_class == 0, area_small, jnp.where(size_class == 1, area_middle, area_large))
    side_len = jnp.where(size_class == 0, SIDE_S, jnp.where(size_class == 1, SIDE_M, SIDE_L))
    within = positions - begins
    picture_index = within // area_len
    within_image = within % area_len
    is_valid = positions < end_large
    segment = jnp.where(is_valid, size_class * 16 + picture_index, 255)
    grid_row = (within_image // side_len).astype(jnp.float32)
    grid_col = (within_image % side_len).astype(jnp.float32)
    return (segment, grid_row, grid_col, is_valid.astype(jnp.float32))

def normalize(values, gain_row, shift_row):
    centred = values - lax.optimization_barrier(jnp.mean(values, axis=-1, keepdims=True))
    spread = lax.optimization_barrier(jnp.mean(centred * centred, axis=-1, keepdims=True))
    return centred * lax.rsqrt(spread + EPSILON) * gain_row + shift_row

def slopes_of(first_head, count_heads):
    head_number = (first_head + jnp.arange(count_heads)).astype(jnp.float32) + 1.0
    return jnp.exp2(-8.0 * head_number / HEADS)

def distances(row_query, col_query, row_key, col_key):
    delta_row = row_query[:, None] - row_key[None, :]
    delta_col = col_query[:, None] - col_key[None, :]
    return jnp.sqrt(delta_row * delta_row + delta_col * delta_col)

def group_layer(values, group_counts, norm_gain, norm_bias, w_qkv, b_qv, w_out, out_bias, w_up, b_up, w_down):
    highest = lax.Precision.HIGHEST
    segment, grid_row, grid_col, is_valid = layout(group_counts)
    keep_rows = is_valid[:, None]
    normed = low(normalize(values, norm_gain[0], norm_bias[0]))
    projected = jnp.einsum('td,dsc->tsc', normed, w_qkv, precision=highest)
    queries = low_back(low(projected[:, 0] + b_qv[0])).reshape(TOK_DEV, HEADS, HEAD_DIM)
    keys_all = low_back(low(projected[:, 1])).reshape(TOK_DEV, HEADS, HEAD_DIM)
    values_all = low_back(low(projected[:, 2] + b_qv[1])).reshape(TOK_DEV, HEADS, HEAD_DIM)
    slopes = slopes_of(0, HEADS)
    bias_all = slopes[:, None, None] * distances(grid_row, grid_col, grid_row, grid_col)[None]
    scores = jnp.einsum('qhe,khe->hqk', queries, keys_all, precision=highest) * HEAD_DIM ** (-0.5) - bias_all
    scores = low_back(scores)
    same_image = segment[:, None] == segment[None, :]
    scores = jnp.where(same_image[None], scores, -1e+30)
    weights = jax.nn.softmax(scores, axis=-1)
    mixed_rows = jnp.einsum('hqk,khe->qhe', low(weights), values_all, precision=highest).reshape(TOK_DEV, D)
    mixed_rows = low_back(low(mixed_rows))
    attended = low_back(jnp.dot(mixed_rows, w_out, precision=highest))
    after_attn = values + keep_rows * (attended + out_bias[0])
    normed_two = low(normalize(after_attn, norm_gain[1], norm_bias[1]))
    hidden_pre = low_back(jnp.dot(normed_two, w_up, precision=highest) + b_up)
    hidden = low(jax.nn.gelu(hidden_pre, approximate=False))
    branch = low_back(jnp.dot(hidden, w_down, precision=highest))
    return after_attn + keep_rows * (branch + out_bias[1])

def reference(patches, counts, norm_gain, norm_bias, w_qkv, b_qv, w_out, out_bias, w_up, b_up, w_down, cotangent):
    layer_step = jax.checkpoint(group_layer)

    def forward(inputs, gain_rows, shift_rows, qkv_weight, qv_bias, out_weight, outer_bias, up_weight, up_bias, down_weight):
        grouped = inputs.reshape(GROUPS, TOK_DEV, D)

        def one_group(group_pair):
            return layer_step(group_pair[0], group_pair[1], gain_rows, shift_rows, qkv_weight, qv_bias, out_weight, outer_bias, up_weight, up_bias, down_weight)
        return lax.map(one_group, (grouped, counts)).reshape(GROUPS * TOK_DEV, D)
    result, pullback = jax.vjp(forward, patches.astype(jnp.float32), norm_gain, norm_bias, w_qkv.astype(jnp.float32), b_qv, w_out.astype(jnp.float32), out_bias, w_up.astype(jnp.float32), b_up, w_down.astype(jnp.float32))
    gradients = pullback(cotangent.astype(jnp.float32))
    return (result.astype(jnp.bfloat16), gradients[0].astype(jnp.bfloat16), gradients[1], gradients[2], gradients[3], gradients[4], gradients[5], gradients[6], gradients[7], gradients[8], gradients[9])
```

```python
import functools

import jax
import jax.numpy as jnp
from jax import lax
from jax.sharding import PartitionSpec as P

D = 768
HEADS = 12
HEAD_DIM = 64
FF = 3072
SIDE_S = 12
SIDE_M = 15
SIDE_L = 20
BLOCK = 512
TOK_DEV = 2048


EPSILON = 1e-06


def layout(group_counts):
    positions = jnp.arange(TOK_DEV, dtype=jnp.int32)
    area_small = SIDE_S * SIDE_S
    area_middle = SIDE_M * SIDE_M
    area_large = SIDE_L * SIDE_L
    end_small = group_counts[0] * area_small
    end_middle = end_small + group_counts[1] * area_middle
    end_large = end_middle + group_counts[2] * area_large
    size_class = (positions >= end_small).astype(jnp.int32) + (positions >= end_middle).astype(
        jnp.int32
    )
    begins = jnp.where(size_class == 0, 0, jnp.where(size_class == 1, end_small, end_middle))
    area_len = jnp.where(
        size_class == 0, area_small, jnp.where(size_class == 1, area_middle, area_large)
    )
    side_len = jnp.where(size_class == 0, SIDE_S, jnp.where(size_class == 1, SIDE_M, SIDE_L))
    within = positions - begins
    picture_index = within // area_len
    within_image = within % area_len
    is_valid = positions < end_large
    segment = jnp.where(is_valid, size_class * 16 + picture_index, 255)
    grid_row = (within_image // side_len).astype(jnp.float32)
    grid_col = (within_image % side_len).astype(jnp.float32)
    return (segment, grid_row, grid_col, is_valid.astype(jnp.float32))


def normalize(values, gain_row, shift_row):
    centred = values - jnp.mean(values, axis=-1, keepdims=True)
    spread = jnp.mean(centred * centred, axis=-1, keepdims=True)
    return centred * lax.rsqrt(spread + EPSILON) * gain_row + shift_row


def slopes_of(first_head, count_heads):
    head_number = (first_head + jnp.arange(count_heads, dtype=jnp.int32)).astype(jnp.float32) + 1.0
    return jnp.exp2(-8.0 * head_number / HEADS)


def distances(row_query, col_query, row_key, col_key):
    delta_row = row_query[:, None] - row_key[None, :]
    delta_col = col_query[:, None] - col_key[None, :]
    return jnp.sqrt(delta_row * delta_row + delta_col * delta_col)


def scatter_rows(parts, dp_size):
    width = parts.shape[1]
    padded = -(-width // 1024) * 1024
    parts = jnp.pad(parts, ((0, 0), (0, padded - width))).reshape(dp_size * padded // 128, 128)
    summed = lax.psum_scatter(parts, "dp", scatter_dimension=0, tiled=True)
    return summed.reshape(-1)[:width]


def on_device(
    dp_size,
    patches,
    counts,
    norm_gain,
    norm_bias,
    w_qkv,
    b_qv,
    w_out,
    out_bias,
    w_up,
    b_up,
    w_down,
    cotangent,
):
    local_rows = patches.shape[0]
    width_here = w_qkv.shape[2]
    heads_here = width_here // HEAD_DIM
    ff_here = w_up.shape[1]
    tensor_pos = lax.axis_index("tensor")
    score_scale = HEAD_DIM ** (-0.5)
    block_count = TOK_DEV // BLOCK
    segment, grid_row, grid_col, is_valid = layout(counts[0])
    keep_rows = lax.dynamic_slice_in_dim(is_valid, tensor_pos * local_rows, local_rows)[:, None]
    slopes = slopes_of(tensor_pos * heads_here, heads_here)
    inputs = patches.astype(jnp.float32)
    normed_local = normalize(inputs, norm_gain[0], norm_bias[0]).astype(jnp.bfloat16)
    normed = lax.all_gather(normed_local, "tensor", axis=0, tiled=True)
    projected = jnp.einsum("td,dsc->tsc", normed, w_qkv, preferred_element_type=jnp.float32)
    queries = (projected[:, 0] + b_qv[0]).astype(jnp.bfloat16)
    key_heads = projected[:, 1].astype(jnp.bfloat16).reshape(TOK_DEV, heads_here, HEAD_DIM)
    value_heads = (
        (projected[:, 2] + b_qv[1]).astype(jnp.bfloat16).reshape(TOK_DEV, heads_here, HEAD_DIM)
    )

    def block_scores(offset):
        query_block = lax.dynamic_slice_in_dim(queries, offset, BLOCK).reshape(
            BLOCK, heads_here, HEAD_DIM
        )
        raw_scores = (
            jnp.einsum("qhe,khe->hqk", query_block, key_heads, preferred_element_type=jnp.float32)
            * score_scale
        )
        near_dist = distances(
            lax.dynamic_slice_in_dim(grid_row, offset, BLOCK),
            lax.dynamic_slice_in_dim(grid_col, offset, BLOCK),
            grid_row,
            grid_col,
        )
        same_image = lax.dynamic_slice_in_dim(segment, offset, BLOCK)[:, None] == segment[None, :]
        return (
            query_block,
            jnp.where(
                same_image[None], raw_scores - slopes[:, None, None] * near_dist[None], -1e30
            ),
        )

    def attend_block(block_index):
        _, scores = block_scores(block_index * BLOCK)
        highest_score = jnp.max(scores, axis=-1, keepdims=True)
        exp_terms = jnp.exp(scores - highest_score)
        totals = jnp.sum(exp_terms, axis=-1, keepdims=True)
        weights = (exp_terms / totals).astype(jnp.bfloat16)
        mixed_block = jnp.einsum(
            "hqk,khe->qhe", weights, value_heads, preferred_element_type=jnp.float32
        )
        return (
            mixed_block.reshape(BLOCK, width_here).astype(jnp.bfloat16),
            highest_score[..., 0] + jnp.log(totals[..., 0]),
        )

    mixed_blocks, log_totals = lax.map(attend_block, jnp.arange(block_count, dtype=jnp.int32))
    mixed_rows = mixed_blocks.reshape(TOK_DEV, width_here)
    attended = lax.psum_scatter(
        jnp.dot(mixed_rows, w_out, preferred_element_type=jnp.float32).astype(jnp.bfloat16),
        "tensor",
        scatter_dimension=0,
        tiled=True,
    ).astype(jnp.float32)
    after_attn = inputs + keep_rows * (attended + out_bias[0])
    normed_two_local = normalize(after_attn, norm_gain[1], norm_bias[1]).astype(jnp.bfloat16)
    normed_two = lax.all_gather(normed_two_local, "tensor", axis=0, tiled=True)
    hidden_pre = jnp.dot(normed_two, w_up, preferred_element_type=jnp.float32) + b_up
    hidden = jax.nn.gelu(hidden_pre, approximate=False).astype(jnp.bfloat16)
    branch = lax.psum_scatter(
        jnp.dot(hidden, w_down, preferred_element_type=jnp.float32).astype(jnp.bfloat16),
        "tensor",
        scatter_dimension=0,
        tiled=True,
    ).astype(jnp.float32)
    result = (after_attn + keep_rows * (branch + out_bias[1])).astype(jnp.bfloat16)
    upstream = cotangent.astype(jnp.float32)
    down_bias_grad = jnp.sum(keep_rows * upstream, axis=0)
    branch_grad = lax.all_gather(
        (keep_rows * upstream).astype(jnp.bfloat16), "tensor", axis=0, tiled=True
    )
    w_down_grad_t = jnp.einsum(
        "td,tf->df", branch_grad, hidden, preferred_element_type=jnp.float32
    )
    hidden_grad = jnp.einsum("td,fd->tf", branch_grad, w_down, preferred_element_type=jnp.float32)
    _, gelu_back = jax.vjp(lambda pre_act: jax.nn.gelu(pre_act, approximate=False), hidden_pre)
    pre_grad = gelu_back(hidden_grad)[0].astype(jnp.bfloat16)
    up_bias_grad = jnp.sum(pre_grad, axis=0, dtype=jnp.float32)
    w_up_grad = jnp.einsum("td,tf->df", normed_two, pre_grad, preferred_element_type=jnp.float32)
    normed_two_grad = lax.psum_scatter(
        jnp.einsum("tf,df->td", pre_grad, w_up, preferred_element_type=jnp.float32).astype(
            jnp.bfloat16
        ),
        "tensor",
        scatter_dimension=0,
        tiled=True,
    ).astype(jnp.float32)
    _, norm_two_back = jax.vjp(normalize, after_attn, norm_gain[1], norm_bias[1])
    through_two, gain_two_grad, shift_two_grad = norm_two_back(normed_two_grad)
    after_grad = upstream + through_two
    attn_bias_grad = jnp.sum(keep_rows * after_grad, axis=0)
    attn_local = (keep_rows * after_grad).astype(jnp.bfloat16)
    attn_grad = lax.all_gather(attn_local, "tensor", axis=0, tiled=True)
    w_out_grad_t = jnp.einsum(
        "td,tc->dc", attn_grad, mixed_rows, preferred_element_type=jnp.float32
    )
    mixed_grad = jnp.einsum(
        "td,cd->tc", attn_grad, w_out, preferred_element_type=jnp.float32
    ).astype(jnp.bfloat16)
    early_parts = jnp.concatenate(
        [
            w_down_grad_t.reshape(dp_size, -1),
            w_up_grad.reshape(dp_size, -1),
            w_out_grad_t.reshape(dp_size, -1),
        ],
        axis=1,
    )
    early_parts, mixed_grad = lax.optimization_barrier((early_parts, mixed_grad))
    early_sum = scatter_rows(early_parts, dp_size)
    mixed_heads = mixed_grad.reshape(TOK_DEV, heads_here, HEAD_DIM)

    def back_block(running, block_index):
        key_acc, value_acc = running
        offset = block_index * BLOCK
        query_block, scores = block_scores(offset)
        weights = jnp.exp(
            scores - lax.dynamic_index_in_dim(log_totals, block_index, keepdims=False)[..., None]
        )
        grad_block = lax.dynamic_slice_in_dim(mixed_heads, offset, BLOCK)
        value_acc = value_acc + jnp.einsum(
            "hqk,qhe->khe",
            weights.astype(jnp.bfloat16),
            grad_block,
            preferred_element_type=jnp.float32,
        )
        weight_grad = jnp.einsum(
            "qhe,khe->hqk", grad_block, value_heads, preferred_element_type=jnp.float32
        )
        score_grad = (
            weights * (weight_grad - jnp.sum(weights * weight_grad, axis=-1, keepdims=True))
        ).astype(jnp.bfloat16)
        query_grad_block = (
            jnp.einsum("hqk,khe->qhe", score_grad, key_heads, preferred_element_type=jnp.float32)
            * score_scale
        )
        key_acc = (
            key_acc
            + jnp.einsum(
                "hqk,qhe->khe", score_grad, query_block, preferred_element_type=jnp.float32
            )
            * score_scale
        )
        return (
            (key_acc, value_acc),
            query_grad_block.reshape(BLOCK, width_here).astype(jnp.bfloat16),
        )

    zero_heads = jnp.zeros((TOK_DEV, heads_here, HEAD_DIM), jnp.float32)
    half_count = block_count // 2
    running, query_first = lax.scan(
        back_block, (zero_heads, zero_heads), jnp.arange(half_count, dtype=jnp.int32)
    )
    running, early_sum = lax.optimization_barrier((running, early_sum))
    (key_acc, value_acc), query_second = lax.scan(
        back_block, running, jnp.arange(half_count, block_count, dtype=jnp.int32)
    )
    query_blocks = jnp.concatenate([query_first, query_second], axis=0)
    query_grad = query_blocks.reshape(TOK_DEV, width_here)
    key_grad = key_acc.reshape(TOK_DEV, width_here).astype(jnp.bfloat16)
    value_grad = value_acc.reshape(TOK_DEV, width_here).astype(jnp.bfloat16)
    projected_grad = jnp.stack([query_grad, key_grad, value_grad], axis=1)
    qv_bias_grad = jnp.stack(
        [
            jnp.sum(query_grad, axis=0, dtype=jnp.float32),
            jnp.sum(value_grad, axis=0, dtype=jnp.float32),
        ]
    )
    w_qkv_grad = jnp.einsum(
        "td,tsc->dsc", normed, projected_grad, preferred_element_type=jnp.float32
    )
    normed_grad = lax.psum_scatter(
        jnp.einsum("tsc,dsc->td", projected_grad, w_qkv, preferred_element_type=jnp.float32).astype(
            jnp.bfloat16
        ),
        "tensor",
        scatter_dimension=0,
        tiled=True,
    ).astype(jnp.float32)
    _, norm_one_back = jax.vjp(normalize, inputs, norm_gain[0], norm_bias[0])
    through_one, gain_one_grad, shift_one_grad = norm_one_back(normed_grad)
    input_grad = (after_grad + through_one).astype(jnp.bfloat16)
    small = jnp.concatenate(
        [
            jnp.stack([gain_one_grad, gain_two_grad]).reshape(-1),
            jnp.stack([shift_one_grad, shift_two_grad]).reshape(-1),
            jnp.stack([attn_bias_grad, down_bias_grad]).reshape(-1),
            qv_bias_grad.reshape(-1),
            up_bias_grad,
        ]
    )
    late_parts = jnp.concatenate(
        [w_qkv_grad.reshape(dp_size, -1), jnp.broadcast_to(small, (dp_size,) + small.shape)],
        axis=1,
    )
    late_sum = scatter_rows(late_parts, dp_size)
    qkv_size = w_qkv_grad.size // dp_size
    rows_dp = D // dp_size
    qkv_part = late_sum[:qkv_size].reshape(rows_dp, 3, width_here)
    small_all = lax.all_gather(late_sum[qkv_size:], "tensor", axis=0, tiled=False)
    tensor_size = small_all.shape[0]
    summed = jnp.sum(small_all[:, : 6 * D], axis=0)
    gains_grad = summed[: 2 * D].reshape(2, D)
    shifts_grad = summed[2 * D : 4 * D].reshape(2, D)
    outer_grad = summed[4 * D : 6 * D].reshape(2, D)
    qv_sum = (
        small_all[:, 6 * D : 6 * D + 2 * width_here]
        .reshape(tensor_size, 2, width_here)
        .transpose(1, 0, 2)
        .reshape(2, D)
    )
    up_sum = small_all[:, 6 * D + 2 * width_here :].reshape(FF)
    down_size = D * ff_here // dp_size
    up_size = D * ff_here // dp_size
    down_part = early_sum[:down_size].reshape(rows_dp, ff_here).T
    up_part = early_sum[down_size : down_size + up_size].reshape(rows_dp, ff_here)
    out_part = early_sum[down_size + up_size :].reshape(rows_dp, width_here).T
    return (
        result,
        input_grad,
        gains_grad,
        shifts_grad,
        qkv_part,
        qv_sum,
        out_part,
        outer_grad,
        up_part,
        up_sum,
        down_part,
    )


def solution(mesh):
    placed = (
        P(("dp", "tensor"), None),
        P("dp", None),
        P(),
        P(),
        P(None, None, "tensor"),
        P(None, "tensor"),
        P("tensor", None),
        P(),
        P(None, "tensor"),
        P("tensor"),
        P("tensor", None),
        P(("dp", "tensor"), None),
    )
    return jax.shard_map(
        functools.partial(on_device, mesh.shape["dp"]),
        mesh=mesh,
        in_specs=placed,
        out_specs=(
            P(("dp", "tensor"), None),
            P(("dp", "tensor"), None),
            P(),
            P(),
            P("dp", None, "tensor"),
            P(),
            P("tensor", "dp"),
            P(),
            P("dp", "tensor"),
            P(),
            P("tensor", "dp"),
        ),
        check_vma=False,
    )
```

```python
import functools

import jax
import jax.numpy as jnp
from jax import lax
from jax.sharding import PartitionSpec as P

D = 768
HEADS = 12
HEAD_DIM = 64
FF = 3072
SIDE_S = 12
SIDE_M = 15
SIDE_L = 20
BLOCK = 512
TOK_DEV = 2048


EPSILON = 1e-06


def layout(group_counts):
    positions = jnp.arange(TOK_DEV, dtype=jnp.int32)
    area_small = SIDE_S * SIDE_S
    area_middle = SIDE_M * SIDE_M
    area_large = SIDE_L * SIDE_L
    end_small = group_counts[0] * area_small
    end_middle = end_small + group_counts[1] * area_middle
    end_large = end_middle + group_counts[2] * area_large
    size_class = (positions >= end_small).astype(jnp.int32) + (positions >= end_middle).astype(
        jnp.int32
    )
    begins = jnp.where(size_class == 0, 0, jnp.where(size_class == 1, end_small, end_middle))
    area_len = jnp.where(
        size_class == 0, area_small, jnp.where(size_class == 1, area_middle, area_large)
    )
    side_len = jnp.where(size_class == 0, SIDE_S, jnp.where(size_class == 1, SIDE_M, SIDE_L))
    within = positions - begins
    picture_index = within // area_len
    within_image = within % area_len
    is_valid = positions < end_large
    segment = jnp.where(is_valid, size_class * 16 + picture_index, 255)
    grid_row = (within_image // side_len).astype(jnp.float32)
    grid_col = (within_image % side_len).astype(jnp.float32)
    return (segment, grid_row, grid_col, is_valid.astype(jnp.float32))


def normalize(values, gain_row, shift_row):
    centred = values - jnp.mean(values, axis=-1, keepdims=True)
    spread = jnp.mean(centred * centred, axis=-1, keepdims=True)
    return centred * lax.rsqrt(spread + EPSILON) * gain_row + shift_row


def slopes_of(first_head, count_heads):
    head_number = (first_head + jnp.arange(count_heads, dtype=jnp.int32)).astype(jnp.float32) + 1.0
    return jnp.exp2(-8.0 * head_number / HEADS)


def distances(row_query, col_query, row_key, col_key):
    delta_row = row_query[:, None] - row_key[None, :]
    delta_col = col_query[:, None] - col_key[None, :]
    return jnp.sqrt(delta_row * delta_row + delta_col * delta_col)


def scatter_rows(parts, dp_size):
    width = parts.shape[1]
    padded = -(-width // 1024) * 1024
    parts = jnp.pad(parts, ((0, 0), (0, padded - width))).reshape(dp_size * padded // 128, 128)
    summed = lax.psum_scatter(parts, "dp", scatter_dimension=0, tiled=True)
    return summed.reshape(-1)[:width]


def on_device(
    dp_size,
    patches,
    counts,
    norm_gain,
    norm_bias,
    w_qkv,
    b_qv,
    w_out,
    out_bias,
    w_up,
    b_up,
    w_down,
    cotangent,
):
    local_rows = patches.shape[0]
    width_here = w_qkv.shape[2]
    heads_here = width_here // HEAD_DIM
    ff_here = w_up.shape[1]
    tensor_pos = lax.axis_index("tensor")
    score_scale = HEAD_DIM ** (-0.5)
    block_count = TOK_DEV // BLOCK
    segment, grid_row, grid_col, is_valid = layout(counts[0])
    keep_rows = lax.dynamic_slice_in_dim(is_valid, tensor_pos * local_rows, local_rows)[:, None]
    slopes = slopes_of(tensor_pos * heads_here, heads_here)
    inputs = patches.astype(jnp.float32)
    normed_local = normalize(inputs, norm_gain[0], norm_bias[0]).astype(jnp.bfloat16)
    normed = lax.all_gather(normed_local, "tensor", axis=0, tiled=True)
    projected = jnp.einsum("td,dsc->tsc", normed, w_qkv, preferred_element_type=jnp.float32)
    queries = (projected[:, 0] + b_qv[0]).astype(jnp.bfloat16)
    key_heads = projected[:, 1].astype(jnp.bfloat16).reshape(TOK_DEV, heads_here, HEAD_DIM)
    value_heads = (
        (projected[:, 2] + b_qv[1]).astype(jnp.bfloat16).reshape(TOK_DEV, heads_here, HEAD_DIM)
    )

    def block_scores(offset):
        query_block = lax.dynamic_slice_in_dim(queries, offset, BLOCK).reshape(
            BLOCK, heads_here, HEAD_DIM
        )
        raw_scores = (
            jnp.einsum("qhe,khe->hqk", query_block, key_heads, preferred_element_type=jnp.float32)
            * score_scale
        )
        near_dist = distances(
            lax.dynamic_slice_in_dim(grid_row, offset, BLOCK),
            lax.dynamic_slice_in_dim(grid_col, offset, BLOCK),
            grid_row,
            grid_col,
        )
        same_image = lax.dynamic_slice_in_dim(segment, offset, BLOCK)[:, None] == segment[None, :]
        return (
            query_block,
            jnp.where(
                same_image[None], raw_scores - slopes[:, None, None] * near_dist[None], -1e30
            ),
        )

    def attend_block(block_index):
        _, scores = block_scores(block_index * BLOCK)
        highest_score = jnp.max(scores, axis=-1, keepdims=True)
        exp_terms = jnp.exp(scores - highest_score)
        totals = jnp.sum(exp_terms, axis=-1, keepdims=True)
        weights = (exp_terms / totals).astype(jnp.bfloat16)
        mixed_block = jnp.einsum(
            "hqk,khe->qhe", weights, value_heads, preferred_element_type=jnp.float32
        )
        return (
            mixed_block.reshape(BLOCK, width_here).astype(jnp.bfloat16),
            highest_score[..., 0] + jnp.log(totals[..., 0]),
        )

    mixed_blocks, log_totals = lax.map(attend_block, jnp.arange(block_count, dtype=jnp.int32))
    upstream = cotangent.astype(jnp.float32)
    branch_grad = lax.all_gather(
        (keep_rows * upstream).astype(jnp.bfloat16), "tensor", axis=0, tiled=True
    )
    mixed_blocks, log_totals, branch_grad = lax.optimization_barrier(
        (mixed_blocks, log_totals, branch_grad)
    )
    mixed_rows = mixed_blocks.reshape(TOK_DEV, width_here)
    attended = lax.psum_scatter(
        jnp.dot(mixed_rows, w_out, preferred_element_type=jnp.float32).astype(jnp.bfloat16),
        "tensor",
        scatter_dimension=0,
        tiled=True,
    ).astype(jnp.float32)
    after_attn = inputs + keep_rows * (attended + out_bias[0])
    normed_two_local = normalize(after_attn, norm_gain[1], norm_bias[1]).astype(jnp.bfloat16)
    normed_two = lax.all_gather(normed_two_local, "tensor", axis=0, tiled=True)
    hidden_pre = jnp.dot(normed_two, w_up, preferred_element_type=jnp.float32) + b_up
    hidden = jax.nn.gelu(hidden_pre, approximate=False).astype(jnp.bfloat16)
    branch_partial = jnp.dot(hidden, w_down, preferred_element_type=jnp.float32).astype(
        jnp.bfloat16
    )
    down_bias_grad = jnp.sum(keep_rows * upstream, axis=0)
    w_down_grad_t = jnp.einsum(
        "td,tf->df", branch_grad, hidden, preferred_element_type=jnp.float32
    )
    hidden_grad = jnp.einsum("td,fd->tf", branch_grad, w_down, preferred_element_type=jnp.float32)
    _, gelu_back = jax.vjp(lambda pre_act: jax.nn.gelu(pre_act, approximate=False), hidden_pre)
    pre_grad = gelu_back(hidden_grad)[0].astype(jnp.bfloat16)
    up_bias_grad = jnp.sum(pre_grad, axis=0, dtype=jnp.float32)
    w_up_grad = jnp.einsum("td,tf->df", normed_two, pre_grad, preferred_element_type=jnp.float32)
    normed_two_grad = lax.psum_scatter(
        jnp.einsum("tf,df->td", pre_grad, w_up, preferred_element_type=jnp.float32).astype(
            jnp.bfloat16
        ),
        "tensor",
        scatter_dimension=0,
        tiled=True,
    ).astype(jnp.float32)
    _, norm_two_back = jax.vjp(normalize, after_attn, norm_gain[1], norm_bias[1])
    through_two, gain_two_grad, shift_two_grad = norm_two_back(normed_two_grad)
    after_grad = upstream + through_two
    attn_bias_grad = jnp.sum(keep_rows * after_grad, axis=0)
    attn_local = (keep_rows * after_grad).astype(jnp.bfloat16)
    attn_grad = lax.all_gather(attn_local, "tensor", axis=0, tiled=True)
    w_out_grad_t = jnp.einsum(
        "td,tc->dc", attn_grad, mixed_rows, preferred_element_type=jnp.float32
    )
    mixed_grad = jnp.einsum(
        "td,cd->tc", attn_grad, w_out, preferred_element_type=jnp.float32
    ).astype(jnp.bfloat16)
    early_parts = jnp.concatenate(
        [
            w_down_grad_t.reshape(dp_size, -1),
            w_up_grad.reshape(dp_size, -1),
            w_out_grad_t.reshape(dp_size, -1),
        ],
        axis=1,
    )
    early_parts, mixed_grad, branch_partial = lax.optimization_barrier(
        (early_parts, mixed_grad, branch_partial)
    )
    branch = lax.psum_scatter(branch_partial, "tensor", scatter_dimension=0, tiled=True).astype(
        jnp.float32
    )
    result = (after_attn + keep_rows * (branch + out_bias[1])).astype(jnp.bfloat16)
    early_sum = scatter_rows(early_parts, dp_size)
    mixed_heads = mixed_grad.reshape(TOK_DEV, heads_here, HEAD_DIM)

    def back_block(running, block_index):
        key_acc, value_acc = running
        offset = block_index * BLOCK
        query_block, scores = block_scores(offset)
        weights = jnp.exp(
            scores - lax.dynamic_index_in_dim(log_totals, block_index, keepdims=False)[..., None]
        )
        grad_block = lax.dynamic_slice_in_dim(mixed_heads, offset, BLOCK)
        value_acc = value_acc + jnp.einsum(
            "hqk,qhe->khe",
            weights.astype(jnp.bfloat16),
            grad_block,
            preferred_element_type=jnp.float32,
        )
        weight_grad = jnp.einsum(
            "qhe,khe->hqk", grad_block, value_heads, preferred_element_type=jnp.float32
        )
        score_grad = (
            weights * (weight_grad - jnp.sum(weights * weight_grad, axis=-1, keepdims=True))
        ).astype(jnp.bfloat16)
        query_grad_block = (
            jnp.einsum("hqk,khe->qhe", score_grad, key_heads, preferred_element_type=jnp.float32)
            * score_scale
        )
        key_acc = (
            key_acc
            + jnp.einsum(
                "hqk,qhe->khe", score_grad, query_block, preferred_element_type=jnp.float32
            )
            * score_scale
        )
        return (
            (key_acc, value_acc),
            query_grad_block.reshape(BLOCK, width_here).astype(jnp.bfloat16),
        )

    zero_heads = jnp.zeros((TOK_DEV, heads_here, HEAD_DIM), jnp.float32)
    (key_acc, value_acc), query_blocks = lax.scan(
        back_block, (zero_heads, zero_heads), jnp.arange(block_count, dtype=jnp.int32)
    )
    key_acc, value_acc, query_blocks, early_sum, result = lax.optimization_barrier(
        (key_acc, value_acc, query_blocks, early_sum, result)
    )
    query_grad = query_blocks.reshape(TOK_DEV, width_here)
    key_grad = key_acc.reshape(TOK_DEV, width_here).astype(jnp.bfloat16)
    value_grad = value_acc.reshape(TOK_DEV, width_here).astype(jnp.bfloat16)
    projected_grad = jnp.stack([query_grad, key_grad, value_grad], axis=1)
    qv_bias_grad = jnp.stack(
        [
            jnp.sum(query_grad, axis=0, dtype=jnp.float32),
            jnp.sum(value_grad, axis=0, dtype=jnp.float32),
        ]
    )
    w_qkv_grad = jnp.einsum(
        "td,tsc->dsc", normed, projected_grad, preferred_element_type=jnp.float32
    )
    normed_grad = lax.psum_scatter(
        jnp.einsum("tsc,dsc->td", projected_grad, w_qkv, preferred_element_type=jnp.float32).astype(
            jnp.bfloat16
        ),
        "tensor",
        scatter_dimension=0,
        tiled=True,
    ).astype(jnp.float32)
    _, norm_one_back = jax.vjp(normalize, inputs, norm_gain[0], norm_bias[0])
    through_one, gain_one_grad, shift_one_grad = norm_one_back(normed_grad)
    input_grad = (after_grad + through_one).astype(jnp.bfloat16)
    small = jnp.concatenate(
        [
            jnp.stack([gain_one_grad, gain_two_grad]).reshape(-1),
            jnp.stack([shift_one_grad, shift_two_grad]).reshape(-1),
            jnp.stack([attn_bias_grad, down_bias_grad]).reshape(-1),
            qv_bias_grad.reshape(-1),
            up_bias_grad,
        ]
    )
    late_parts = jnp.concatenate(
        [w_qkv_grad.reshape(dp_size, -1), jnp.broadcast_to(small, (dp_size,) + small.shape)],
        axis=1,
    )
    late_sum = scatter_rows(late_parts, dp_size)
    qkv_size = w_qkv_grad.size // dp_size
    rows_dp = D // dp_size
    qkv_part = late_sum[:qkv_size].reshape(rows_dp, 3, width_here)
    small_all = lax.all_gather(late_sum[qkv_size:], "tensor", axis=0, tiled=False)
    tensor_size = small_all.shape[0]
    summed = jnp.sum(small_all[:, : 6 * D], axis=0)
    gains_grad = summed[: 2 * D].reshape(2, D)
    shifts_grad = summed[2 * D : 4 * D].reshape(2, D)
    outer_grad = summed[4 * D : 6 * D].reshape(2, D)
    qv_sum = (
        small_all[:, 6 * D : 6 * D + 2 * width_here]
        .reshape(tensor_size, 2, width_here)
        .transpose(1, 0, 2)
        .reshape(2, D)
    )
    up_sum = small_all[:, 6 * D + 2 * width_here :].reshape(FF)
    down_size = D * ff_here // dp_size
    up_size = D * ff_here // dp_size
    down_part = early_sum[:down_size].reshape(rows_dp, ff_here).T
    up_part = early_sum[down_size : down_size + up_size].reshape(rows_dp, ff_here)
    out_part = early_sum[down_size + up_size :].reshape(rows_dp, width_here).T
    return (
        result,
        input_grad,
        gains_grad,
        shifts_grad,
        qkv_part,
        qv_sum,
        out_part,
        outer_grad,
        up_part,
        up_sum,
        down_part,
    )


def solution(mesh):
    placed = (
        P(("dp", "tensor"), None),
        P("dp", None),
        P(),
        P(),
        P(None, None, "tensor"),
        P(None, "tensor"),
        P("tensor", None),
        P(),
        P(None, "tensor"),
        P("tensor"),
        P("tensor", None),
        P(("dp", "tensor"), None),
    )
    return jax.shard_map(
        functools.partial(on_device, mesh.shape["dp"]),
        mesh=mesh,
        in_specs=placed,
        out_specs=(
            P(("dp", "tensor"), None),
            P(("dp", "tensor"), None),
            P(),
            P(),
            P("dp", None, "tensor"),
            P(),
            P("tensor", "dp"),
            P(),
            P("dp", "tensor"),
            P(),
            P("tensor", "dp"),
        ),
        check_vma=False,
    )
```

```python
import functools

import jax
import jax.numpy as jnp
from jax import lax
from jax.experimental import pallas as pl
from jax.experimental.pallas import tpu as pltpu
from jax.sharding import PartitionSpec as P

D = 768
HEADS = 12
HEAD_DIM = 64
FF = 3072
SIDE_S = 12
SIDE_M = 15
SIDE_L = 20
TOK_DEV = 2048


EPSILON = 1e-06


def layout(group_counts):
    positions = jnp.arange(TOK_DEV, dtype=jnp.int32)
    area_small = SIDE_S * SIDE_S
    area_middle = SIDE_M * SIDE_M
    area_large = SIDE_L * SIDE_L
    end_small = group_counts[0] * area_small
    end_middle = end_small + group_counts[1] * area_middle
    end_large = end_middle + group_counts[2] * area_large
    size_class = (positions >= end_small).astype(jnp.int32) + (positions >= end_middle).astype(
        jnp.int32
    )
    begins = jnp.where(size_class == 0, 0, jnp.where(size_class == 1, end_small, end_middle))
    area_len = jnp.where(
        size_class == 0, area_small, jnp.where(size_class == 1, area_middle, area_large)
    )
    side_len = jnp.where(size_class == 0, SIDE_S, jnp.where(size_class == 1, SIDE_M, SIDE_L))
    within = positions - begins
    picture_index = within // area_len
    within_image = within % area_len
    is_valid = positions < end_large
    segment = jnp.where(is_valid, size_class * 16 + picture_index, 255)
    grid_row = (within_image // side_len).astype(jnp.float32)
    grid_col = (within_image % side_len).astype(jnp.float32)
    return (segment, grid_row, grid_col, is_valid.astype(jnp.float32))


def normalize(values, gain_row, shift_row):
    centred = values - jnp.mean(values, axis=-1, keepdims=True)
    spread = jnp.mean(centred * centred, axis=-1, keepdims=True)
    return centred * lax.rsqrt(spread + EPSILON) * gain_row + shift_row


def slopes_of(first_head, count_heads):
    head_number = (first_head + jnp.arange(count_heads, dtype=jnp.int32)).astype(jnp.float32) + 1.0
    return jnp.exp2(-8.0 * head_number / HEADS)


def distances(row_query, col_query, row_key, col_key):
    delta_row = row_query[:, None] - row_key[None, :]
    delta_col = col_query[:, None] - col_key[None, :]
    return jnp.sqrt(delta_row * delta_row + delta_col * delta_col)

Q_BLOCK = 256
K_BLOCK = 256
NEG = -1e30


def key_ranges(segment, tokens):
    starts = jnp.arange(0, tokens, Q_BLOCK)
    first = segment[starts]
    last = segment[starts + Q_BLOCK - 1]
    key_lo = jnp.sum(segment[None, :] < first[:, None], axis=1)
    key_hi = jnp.sum(segment[None, :] <= last[:, None], axis=1)
    return (key_lo // K_BLOCK).astype(jnp.int32), ((key_hi + K_BLOCK - 1) // K_BLOCK).astype(jnp.int32)


def block_geometry(qi_ref, ki_ref, start):
    rq = qi_ref[:, 0:1]
    cq = qi_ref[:, 1:2]
    sq = qi_ref[:, 2:3]
    rk = ki_ref[0:1, pl.ds(start, K_BLOCK)]
    ck = ki_ref[1:2, pl.ds(start, K_BLOCK)]
    sk = ki_ref[2:3, pl.ds(start, K_BLOCK)]
    dr = rq - rk
    dc = cq - ck
    return jnp.sqrt(dr * dr + dc * dc), sq == sk


def fwd_kernel(heads, scale, lo_ref, hi_ref, slope_ref, q_ref, k_ref, v_ref, qi_ref, ki_ref, o_ref, lse_ref):
    i = pl.program_id(0)
    queries = [q_ref[h] for h in range(heads)]
    width = q_ref.shape[2]

    def body(kb, carry):
        start = pl.multiple_of(kb * K_BLOCK, K_BLOCK)
        dist, allowed = block_geometry(qi_ref, ki_ref, start)
        out = []
        for h in range(heads):
            m_old, l_old, acc_old = carry[h]
            keys = k_ref[h, pl.ds(start, K_BLOCK), :]
            vals = v_ref[h, pl.ds(start, K_BLOCK), :]
            s = lax.dot_general(queries[h], keys, (((1,), (1,)), ((), ())),
                                preferred_element_type=jnp.float32) * scale - slope_ref[h] * dist
            s = jnp.where(allowed, s, NEG)
            m_new = jnp.maximum(m_old, jnp.max(s, axis=1, keepdims=True))
            alpha = jnp.exp(m_old - m_new)
            p = jnp.exp(s - m_new)
            l_new = alpha * l_old + jnp.sum(p, axis=1, keepdims=True)
            acc_new = alpha * acc_old + jnp.dot(p.astype(jnp.bfloat16), vals,
                                                preferred_element_type=jnp.float32)
            out.append((m_new, l_new, acc_new))
        return tuple(out)

    init = tuple(
        (jnp.full((Q_BLOCK, 1), NEG, jnp.float32), jnp.zeros((Q_BLOCK, 1), jnp.float32),
         jnp.zeros((Q_BLOCK, width), jnp.float32))
        for _ in range(heads)
    )
    final = lax.fori_loop(lo_ref[i], hi_ref[i], body, init)
    for h in range(heads):
        m, l, acc = final[h]
        o_ref[h] = acc / l
        lse_ref[h] = m + jnp.log(l)


def bwd_kernel(heads, scale, lo_ref, hi_ref, slope_ref, q_ref, k_ref, v_ref, qi_ref, ki_ref,
               o_ref, do_ref, lse_ref, dq_ref, dk_ref, dv_ref):
    i = pl.program_id(0)

    @pl.when(i == 0)
    def _():
        dk_ref[...] = jnp.zeros_like(dk_ref)
        dv_ref[...] = jnp.zeros_like(dv_ref)

    queries = [q_ref[h] for h in range(heads)]
    grads = [do_ref[h] for h in range(heads)]
    lses = [lse_ref[h] for h in range(heads)]
    deltas = [jnp.sum(grads[h].astype(jnp.float32) * o_ref[h], axis=1, keepdims=True)
              for h in range(heads)]
    width = q_ref.shape[2]

    def body(kb, carry):
        start = pl.multiple_of(kb * K_BLOCK, K_BLOCK)
        dist, allowed = block_geometry(qi_ref, ki_ref, start)
        out = []
        for h in range(heads):
            keys = k_ref[h, pl.ds(start, K_BLOCK), :]
            vals = v_ref[h, pl.ds(start, K_BLOCK), :]
            s = lax.dot_general(queries[h], keys, (((1,), (1,)), ((), ())),
                                preferred_element_type=jnp.float32) * scale - slope_ref[h] * dist
            p = jnp.where(allowed, jnp.exp(s - lses[h]), 0.0)
            dp = lax.dot_general(grads[h], vals, (((1,), (1,)), ((), ())),
                                 preferred_element_type=jnp.float32)
            ds = (p * (dp - deltas[h])).astype(jnp.bfloat16)
            out.append(carry[h] + jnp.dot(ds, keys, preferred_element_type=jnp.float32))
            dk_ref[h, pl.ds(start, K_BLOCK), :] += lax.dot_general(
                ds, queries[h], (((0,), (0,)), ((), ())), preferred_element_type=jnp.float32)
            dv_ref[h, pl.ds(start, K_BLOCK), :] += lax.dot_general(
                p.astype(jnp.bfloat16), grads[h], (((0,), (0,)), ((), ())),
                preferred_element_type=jnp.float32)
        return tuple(out)

    init = tuple(jnp.zeros((Q_BLOCK, width), jnp.float32) for _ in range(heads))
    final = lax.fori_loop(lo_ref[i], hi_ref[i], body, init)
    for h in range(heads):
        dq_ref[h] = final[h]


def attention_fwd(lo, hi, slopes, q, k, v, qinfo, kinfo, scale):
    heads, tokens, width = q.shape
    grid = (tokens // Q_BLOCK,)
    whole = lambda i, lo, hi: (0, 0, 0)
    rows = lambda i, lo, hi: (0, i, 0)
    return pl.pallas_call(
        functools.partial(fwd_kernel, heads, scale),
        grid_spec=pltpu.PrefetchScalarGridSpec(
            num_scalar_prefetch=2,
            grid=grid,
            in_specs=[
                pl.BlockSpec(memory_space=pltpu.SMEM),
                pl.BlockSpec((heads, Q_BLOCK, width), rows),
                pl.BlockSpec((heads, tokens, width), whole),
                pl.BlockSpec((heads, tokens, width), whole),
                pl.BlockSpec((Q_BLOCK, 3), lambda i, lo, hi: (i, 0)),
                pl.BlockSpec((3, tokens), lambda i, lo, hi: (0, 0)),
            ],
            out_specs=[
                pl.BlockSpec((heads, Q_BLOCK, width), rows),
                pl.BlockSpec((heads, Q_BLOCK, 1), rows),
            ],
        ),
        out_shape=[
            jax.ShapeDtypeStruct((heads, tokens, width), jnp.float32),
            jax.ShapeDtypeStruct((heads, tokens, 1), jnp.float32),
        ],
        compiler_params=pltpu.CompilerParams(dimension_semantics=("arbitrary",)),
    )(lo, hi, slopes, q, k, v, qinfo, kinfo)


def attention_bwd(lo, hi, slopes, q, k, v, qinfo, kinfo, o, do, lse, scale):
    heads, tokens, width = q.shape
    grid = (tokens // Q_BLOCK,)
    whole = lambda i, lo, hi: (0, 0, 0)
    rows = lambda i, lo, hi: (0, i, 0)
    return pl.pallas_call(
        functools.partial(bwd_kernel, heads, scale),
        grid_spec=pltpu.PrefetchScalarGridSpec(
            num_scalar_prefetch=2,
            grid=grid,
            in_specs=[
                pl.BlockSpec(memory_space=pltpu.SMEM),
                pl.BlockSpec((heads, Q_BLOCK, width), rows),
                pl.BlockSpec((heads, tokens, width), whole),
                pl.BlockSpec((heads, tokens, width), whole),
                pl.BlockSpec((Q_BLOCK, 3), lambda i, lo, hi: (i, 0)),
                pl.BlockSpec((3, tokens), lambda i, lo, hi: (0, 0)),
                pl.BlockSpec((heads, Q_BLOCK, width), rows),
                pl.BlockSpec((heads, Q_BLOCK, width), rows),
                pl.BlockSpec((heads, Q_BLOCK, 1), rows),
            ],
            out_specs=[
                pl.BlockSpec((heads, Q_BLOCK, width), rows),
                pl.BlockSpec((heads, tokens, width), whole),
                pl.BlockSpec((heads, tokens, width), whole),
            ],
        ),
        out_shape=[
            jax.ShapeDtypeStruct((heads, tokens, width), jnp.float32),
            jax.ShapeDtypeStruct((heads, tokens, width), jnp.float32),
            jax.ShapeDtypeStruct((heads, tokens, width), jnp.float32),
        ],
        compiler_params=pltpu.CompilerParams(dimension_semantics=("arbitrary",)),
    )(lo, hi, slopes, q, k, v, qinfo, kinfo, o, do, lse)


def scatter_rows(parts, dp_size):
    width = parts.shape[1]
    padded = -(-width // 1024) * 1024
    parts = jnp.pad(parts, ((0, 0), (0, padded - width))).reshape(dp_size * padded // 128, 128)
    summed = lax.psum_scatter(parts, "dp", scatter_dimension=0, tiled=True)
    return summed.reshape(-1)[:width]


def on_device(
    dp_size,
    patches,
    counts,
    norm_gain,
    norm_bias,
    w_qkv,
    b_qv,
    w_out,
    out_bias,
    w_up,
    b_up,
    w_down,
    cotangent,
):
    local_rows = patches.shape[0]
    width_here = w_qkv.shape[2]
    heads_here = width_here // HEAD_DIM
    ff_here = w_up.shape[1]
    tensor_pos = lax.axis_index("tensor")
    score_scale = HEAD_DIM ** (-0.5)
    segment, grid_row, grid_col, is_valid = layout(counts[0])
    keep_rows = lax.dynamic_slice_in_dim(is_valid, tensor_pos * local_rows, local_rows)[:, None]
    slopes = slopes_of(tensor_pos * heads_here, heads_here)
    inputs = patches.astype(jnp.float32)
    normed_local = normalize(inputs, norm_gain[0], norm_bias[0]).astype(jnp.bfloat16)
    normed = lax.all_gather(normed_local, "tensor", axis=0, tiled=True)
    projected = jnp.einsum("td,dsc->tsc", normed, w_qkv, preferred_element_type=jnp.float32)
    queries = (projected[:, 0] + b_qv[0]).astype(jnp.bfloat16)
    keys = projected[:, 1].astype(jnp.bfloat16)
    values = (projected[:, 2] + b_qv[1]).astype(jnp.bfloat16)

    def head_major(rows):
        return rows.reshape(TOK_DEV, heads_here, HEAD_DIM).transpose(1, 0, 2)

    def row_major(heads):
        return heads.transpose(1, 0, 2).reshape(TOK_DEV, width_here)

    key_lo, key_hi = key_ranges(segment, TOK_DEV)
    segment_f = segment.astype(jnp.float32)
    query_info = jnp.stack([grid_row, grid_col, segment_f], axis=1)
    key_info = jnp.stack([grid_row, grid_col, segment_f], axis=0)
    query_heads = head_major(queries)
    key_heads = head_major(keys)
    value_heads = head_major(values)
    mixed_f32, log_totals = attention_fwd(
        key_lo, key_hi, slopes, query_heads, key_heads, value_heads, query_info, key_info, score_scale
    )
    upstream = cotangent.astype(jnp.float32)
    branch_grad = lax.all_gather(
        (keep_rows * upstream).astype(jnp.bfloat16), "tensor", axis=0, tiled=True
    )
    mixed_f32, log_totals, branch_grad = lax.optimization_barrier(
        (mixed_f32, log_totals, branch_grad)
    )
    mixed_rows = row_major(mixed_f32).astype(jnp.bfloat16)
    attended = lax.psum_scatter(
        jnp.dot(mixed_rows, w_out, preferred_element_type=jnp.float32).astype(jnp.bfloat16),
        "tensor",
        scatter_dimension=0,
        tiled=True,
    ).astype(jnp.float32)
    after_attn = inputs + keep_rows * (attended + out_bias[0])
    normed_two_local = normalize(after_attn, norm_gain[1], norm_bias[1]).astype(jnp.bfloat16)
    normed_two = lax.all_gather(normed_two_local, "tensor", axis=0, tiled=True)
    hidden_pre = jnp.dot(normed_two, w_up, preferred_element_type=jnp.float32) + b_up
    hidden = jax.nn.gelu(hidden_pre, approximate=False).astype(jnp.bfloat16)
    branch_partial = jnp.dot(hidden, w_down, preferred_element_type=jnp.float32).astype(
        jnp.bfloat16
    )
    down_bias_grad = jnp.sum(keep_rows * upstream, axis=0)
    w_down_grad_t = jnp.einsum(
        "td,tf->df", branch_grad, hidden, preferred_element_type=jnp.float32
    )
    hidden_grad = jnp.einsum("td,fd->tf", branch_grad, w_down, preferred_element_type=jnp.float32)
    _, gelu_back = jax.vjp(lambda pre_act: jax.nn.gelu(pre_act, approximate=False), hidden_pre)
    pre_grad = gelu_back(hidden_grad)[0].astype(jnp.bfloat16)
    up_bias_grad = jnp.sum(pre_grad, axis=0, dtype=jnp.float32)
    w_up_grad = jnp.einsum("td,tf->df", normed_two, pre_grad, preferred_element_type=jnp.float32)
    normed_two_grad = lax.psum_scatter(
        jnp.einsum("tf,df->td", pre_grad, w_up, preferred_element_type=jnp.float32).astype(
            jnp.bfloat16
        ),
        "tensor",
        scatter_dimension=0,
        tiled=True,
    ).astype(jnp.float32)
    _, norm_two_back = jax.vjp(normalize, after_attn, norm_gain[1], norm_bias[1])
    through_two, gain_two_grad, shift_two_grad = norm_two_back(normed_two_grad)
    after_grad = upstream + through_two
    attn_bias_grad = jnp.sum(keep_rows * after_grad, axis=0)
    attn_local = (keep_rows * after_grad).astype(jnp.bfloat16)
    attn_grad = lax.all_gather(attn_local, "tensor", axis=0, tiled=True)
    w_out_grad_t = jnp.einsum(
        "td,tc->dc", attn_grad, mixed_rows, preferred_element_type=jnp.float32
    )
    mixed_grad = jnp.einsum(
        "td,cd->tc", attn_grad, w_out, preferred_element_type=jnp.float32
    ).astype(jnp.bfloat16)
    early_parts = jnp.concatenate(
        [
            w_down_grad_t.reshape(dp_size, -1),
            w_up_grad.reshape(dp_size, -1),
            w_out_grad_t.reshape(dp_size, -1),
        ],
        axis=1,
    )
    early_parts, mixed_grad, branch_partial = lax.optimization_barrier(
        (early_parts, mixed_grad, branch_partial)
    )
    branch = lax.psum_scatter(branch_partial, "tensor", scatter_dimension=0, tiled=True).astype(
        jnp.float32
    )
    result = (after_attn + keep_rows * (branch + out_bias[1])).astype(jnp.bfloat16)
    early_sum = scatter_rows(early_parts, dp_size)
    query_acc, key_acc, value_acc = attention_bwd(
        key_lo, key_hi, slopes, query_heads, key_heads, value_heads, query_info, key_info,
        mixed_f32, head_major(mixed_grad), log_totals, score_scale,
    )
    query_acc, key_acc, value_acc, early_sum, result = lax.optimization_barrier(
        (query_acc, key_acc, value_acc, early_sum, result)
    )
    query_grad = row_major(query_acc * score_scale).astype(jnp.bfloat16)
    key_grad = row_major(key_acc * score_scale).astype(jnp.bfloat16)
    value_grad = row_major(value_acc).astype(jnp.bfloat16)
    projected_grad = jnp.stack([query_grad, key_grad, value_grad], axis=1)
    qv_bias_grad = jnp.stack(
        [
            jnp.sum(query_grad, axis=0, dtype=jnp.float32),
            jnp.sum(value_grad, axis=0, dtype=jnp.float32),
        ]
    )
    w_qkv_grad = jnp.einsum(
        "td,tsc->dsc", normed, projected_grad, preferred_element_type=jnp.float32
    )
    normed_grad = lax.psum_scatter(
        jnp.einsum("tsc,dsc->td", projected_grad, w_qkv, preferred_element_type=jnp.float32).astype(
            jnp.bfloat16
        ),
        "tensor",
        scatter_dimension=0,
        tiled=True,
    ).astype(jnp.float32)
    _, norm_one_back = jax.vjp(normalize, inputs, norm_gain[0], norm_bias[0])
    through_one, gain_one_grad, shift_one_grad = norm_one_back(normed_grad)
    input_grad = (after_grad + through_one).astype(jnp.bfloat16)
    small = jnp.concatenate(
        [
            jnp.stack([gain_one_grad, gain_two_grad]).reshape(-1),
            jnp.stack([shift_one_grad, shift_two_grad]).reshape(-1),
            jnp.stack([attn_bias_grad, down_bias_grad]).reshape(-1),
            qv_bias_grad.reshape(-1),
            up_bias_grad,
        ]
    )
    late_parts = jnp.concatenate(
        [w_qkv_grad.reshape(dp_size, -1), jnp.broadcast_to(small, (dp_size,) + small.shape)],
        axis=1,
    )
    late_sum = scatter_rows(late_parts, dp_size)
    qkv_size = w_qkv_grad.size // dp_size
    rows_dp = D // dp_size
    qkv_part = late_sum[:qkv_size].reshape(rows_dp, 3, width_here)
    small_all = lax.all_gather(late_sum[qkv_size:], "tensor", axis=0, tiled=False)
    tensor_size = small_all.shape[0]
    summed = jnp.sum(small_all[:, : 6 * D], axis=0)
    gains_grad = summed[: 2 * D].reshape(2, D)
    shifts_grad = summed[2 * D : 4 * D].reshape(2, D)
    outer_grad = summed[4 * D : 6 * D].reshape(2, D)
    qv_sum = (
        small_all[:, 6 * D : 6 * D + 2 * width_here]
        .reshape(tensor_size, 2, width_here)
        .transpose(1, 0, 2)
        .reshape(2, D)
    )
    up_sum = small_all[:, 6 * D + 2 * width_here :].reshape(FF)
    down_size = D * ff_here // dp_size
    up_size = D * ff_here // dp_size
    down_part = early_sum[:down_size].reshape(rows_dp, ff_here).T
    up_part = early_sum[down_size : down_size + up_size].reshape(rows_dp, ff_here)
    out_part = early_sum[down_size + up_size :].reshape(rows_dp, width_here).T
    return (
        result,
        input_grad,
        gains_grad,
        shifts_grad,
        qkv_part,
        qv_sum,
        out_part,
        outer_grad,
        up_part,
        up_sum,
        down_part,
    )


def solution(mesh):
    placed = (
        P(("dp", "tensor"), None),
        P("dp", None),
        P(),
        P(),
        P(None, None, "tensor"),
        P(None, "tensor"),
        P("tensor", None),
        P(),
        P(None, "tensor"),
        P("tensor"),
        P("tensor", None),
        P(("dp", "tensor"), None),
    )
    return jax.shard_map(
        functools.partial(on_device, mesh.shape["dp"]),
        mesh=mesh,
        in_specs=placed,
        out_specs=(
            P(("dp", "tensor"), None),
            P(("dp", "tensor"), None),
            P(),
            P(),
            P("dp", None, "tensor"),
            P(),
            P("tensor", "dp"),
            P(),
            P("dp", "tensor"),
            P(),
            P("tensor", "dp"),
        ),
        check_vma=False,
    )
```

```python
import functools

import jax
import jax.numpy as jnp
from jax import lax
from jax.experimental import pallas as pl
from jax.experimental.pallas import tpu as pltpu
from jax.sharding import PartitionSpec as P

D = 768
HEADS = 12
HEAD_DIM = 64
FF = 3072
SIDE_S = 12
SIDE_M = 15
SIDE_L = 20
TOK_DEV = 2048


EPSILON = 1e-06


def layout(group_counts):
    positions = jnp.arange(TOK_DEV, dtype=jnp.int32)
    area_small = SIDE_S * SIDE_S
    area_middle = SIDE_M * SIDE_M
    area_large = SIDE_L * SIDE_L
    end_small = group_counts[0] * area_small
    end_middle = end_small + group_counts[1] * area_middle
    end_large = end_middle + group_counts[2] * area_large
    size_class = (positions >= end_small).astype(jnp.int32) + (positions >= end_middle).astype(
        jnp.int32
    )
    begins = jnp.where(size_class == 0, 0, jnp.where(size_class == 1, end_small, end_middle))
    area_len = jnp.where(
        size_class == 0, area_small, jnp.where(size_class == 1, area_middle, area_large)
    )
    side_len = jnp.where(size_class == 0, SIDE_S, jnp.where(size_class == 1, SIDE_M, SIDE_L))
    within = positions - begins
    picture_index = within // area_len
    within_image = within % area_len
    is_valid = positions < end_large
    segment = jnp.where(is_valid, size_class * 16 + picture_index, 255)
    grid_row = (within_image // side_len).astype(jnp.float32)
    grid_col = (within_image % side_len).astype(jnp.float32)
    return (segment, grid_row, grid_col, is_valid.astype(jnp.float32))


def normalize(values, gain_row, shift_row):
    centred = values - jnp.mean(values, axis=-1, keepdims=True)
    spread = jnp.mean(centred * centred, axis=-1, keepdims=True)
    return centred * lax.rsqrt(spread + EPSILON) * gain_row + shift_row


def slopes_of(first_head, count_heads):
    head_number = (first_head + jnp.arange(count_heads, dtype=jnp.int32)).astype(jnp.float32) + 1.0
    return jnp.exp2(-8.0 * head_number / HEADS)


def distances(row_query, col_query, row_key, col_key):
    delta_row = row_query[:, None] - row_key[None, :]
    delta_col = col_query[:, None] - col_key[None, :]
    return jnp.sqrt(delta_row * delta_row + delta_col * delta_col)

Q_BLOCK = 256
K_BLOCK = 256
NEG = -1e30


def key_ranges(segment, tokens):
    starts = jnp.arange(0, tokens, Q_BLOCK)
    first = segment[starts]
    last = segment[starts + Q_BLOCK - 1]
    key_lo = jnp.sum(segment[None, :] < first[:, None], axis=1)
    key_hi = jnp.sum(segment[None, :] <= last[:, None], axis=1)
    return (key_lo // K_BLOCK).astype(jnp.int32), ((key_hi + K_BLOCK - 1) // K_BLOCK).astype(jnp.int32)


def block_geometry(qi_ref, ki_ref, start):
    rq = qi_ref[:, 0:1]
    cq = qi_ref[:, 1:2]
    sq = qi_ref[:, 2:3]
    rk = ki_ref[0:1, pl.ds(start, K_BLOCK)]
    ck = ki_ref[1:2, pl.ds(start, K_BLOCK)]
    sk = ki_ref[2:3, pl.ds(start, K_BLOCK)]
    dr = rq - rk
    dc = cq - ck
    return jnp.sqrt(dr * dr + dc * dc), sq == sk


def fwd_kernel(heads, scale, lo_ref, hi_ref, slope_ref, q_ref, k_ref, v_ref, qi_ref, ki_ref, o_ref, lse_ref):
    i = pl.program_id(0)
    queries = [q_ref[h] for h in range(heads)]
    width = q_ref.shape[2]

    def body(kb, carry):
        start = pl.multiple_of(kb * K_BLOCK, K_BLOCK)
        dist, allowed = block_geometry(qi_ref, ki_ref, start)
        out = []
        for h in range(heads):
            m_old, l_old, acc_old = carry[h]
            keys = k_ref[h, pl.ds(start, K_BLOCK), :]
            vals = v_ref[h, pl.ds(start, K_BLOCK), :]
            s = lax.dot_general(queries[h], keys, (((1,), (1,)), ((), ())),
                                preferred_element_type=jnp.float32) * scale - slope_ref[h] * dist
            s = jnp.where(allowed, s, NEG)
            m_new = jnp.maximum(m_old, jnp.max(s, axis=1, keepdims=True))
            alpha = jnp.exp(m_old - m_new)
            p = jnp.exp(s - m_new)
            l_new = alpha * l_old + jnp.sum(p, axis=1, keepdims=True)
            acc_new = alpha * acc_old + jnp.dot(p.astype(jnp.bfloat16), vals,
                                                preferred_element_type=jnp.float32)
            out.append((m_new, l_new, acc_new))
        return tuple(out)

    init = tuple(
        (jnp.full((Q_BLOCK, 1), NEG, jnp.float32), jnp.zeros((Q_BLOCK, 1), jnp.float32),
         jnp.zeros((Q_BLOCK, width), jnp.float32))
        for _ in range(heads)
    )
    final = lax.fori_loop(lo_ref[i], hi_ref[i], body, init)
    for h in range(heads):
        m, l, acc = final[h]
        o_ref[h] = acc / l
        lse_ref[h] = m + jnp.log(l)


def bwd_kernel(heads, scale, lo_ref, hi_ref, slope_ref, q_ref, k_ref, v_ref, qi_ref, ki_ref,
               o_ref, do_ref, lse_ref, dq_ref, dk_ref, dv_ref):
    i = pl.program_id(0)

    @pl.when(i == 0)
    def _():
        dk_ref[...] = jnp.zeros_like(dk_ref)
        dv_ref[...] = jnp.zeros_like(dv_ref)

    queries = [q_ref[h] for h in range(heads)]
    grads = [do_ref[h] for h in range(heads)]
    lses = [lse_ref[h] for h in range(heads)]
    deltas = [jnp.sum(grads[h].astype(jnp.float32) * o_ref[h], axis=1, keepdims=True)
              for h in range(heads)]
    width = q_ref.shape[2]

    def body(kb, carry):
        start = pl.multiple_of(kb * K_BLOCK, K_BLOCK)
        dist, allowed = block_geometry(qi_ref, ki_ref, start)
        out = []
        for h in range(heads):
            keys = k_ref[h, pl.ds(start, K_BLOCK), :]
            vals = v_ref[h, pl.ds(start, K_BLOCK), :]
            s = lax.dot_general(queries[h], keys, (((1,), (1,)), ((), ())),
                                preferred_element_type=jnp.float32) * scale - slope_ref[h] * dist
            p = jnp.where(allowed, jnp.exp(s - lses[h]), 0.0)
            dp = lax.dot_general(grads[h], vals, (((1,), (1,)), ((), ())),
                                 preferred_element_type=jnp.float32)
            ds = (p * (dp - deltas[h])).astype(jnp.bfloat16)
            out.append(carry[h] + jnp.dot(ds, keys, preferred_element_type=jnp.float32))
            dk_ref[h, pl.ds(start, K_BLOCK), :] += lax.dot_general(
                ds, queries[h], (((0,), (0,)), ((), ())), preferred_element_type=jnp.float32)
            dv_ref[h, pl.ds(start, K_BLOCK), :] += lax.dot_general(
                p.astype(jnp.bfloat16), grads[h], (((0,), (0,)), ((), ())),
                preferred_element_type=jnp.float32)
        return tuple(out)

    init = tuple(jnp.zeros((Q_BLOCK, width), jnp.float32) for _ in range(heads))
    final = lax.fori_loop(lo_ref[i], hi_ref[i], body, init)
    for h in range(heads):
        dq_ref[h] = final[h]


def attention_fwd(lo, hi, slopes, q, k, v, qinfo, kinfo, scale):
    heads, tokens, width = q.shape
    grid = (tokens // Q_BLOCK,)
    whole = lambda i, lo, hi: (0, 0, 0)
    rows = lambda i, lo, hi: (0, i, 0)
    return pl.pallas_call(
        functools.partial(fwd_kernel, heads, scale),
        grid_spec=pltpu.PrefetchScalarGridSpec(
            num_scalar_prefetch=2,
            grid=grid,
            in_specs=[
                pl.BlockSpec(memory_space=pltpu.SMEM),
                pl.BlockSpec((heads, Q_BLOCK, width), rows),
                pl.BlockSpec((heads, tokens, width), whole),
                pl.BlockSpec((heads, tokens, width), whole),
                pl.BlockSpec((Q_BLOCK, 3), lambda i, lo, hi: (i, 0)),
                pl.BlockSpec((3, tokens), lambda i, lo, hi: (0, 0)),
            ],
            out_specs=[
                pl.BlockSpec((heads, Q_BLOCK, width), rows),
                pl.BlockSpec((heads, Q_BLOCK, 1), rows),
            ],
        ),
        out_shape=[
            jax.ShapeDtypeStruct((heads, tokens, width), jnp.float32),
            jax.ShapeDtypeStruct((heads, tokens, 1), jnp.float32),
        ],
        compiler_params=pltpu.CompilerParams(dimension_semantics=("arbitrary",)),
    )(lo, hi, slopes, q, k, v, qinfo, kinfo)


def attention_bwd(lo, hi, slopes, q, k, v, qinfo, kinfo, o, do, lse, scale):
    heads, tokens, width = q.shape
    grid = (tokens // Q_BLOCK,)
    whole = lambda i, lo, hi: (0, 0, 0)
    rows = lambda i, lo, hi: (0, i, 0)
    return pl.pallas_call(
        functools.partial(bwd_kernel, heads, scale),
        grid_spec=pltpu.PrefetchScalarGridSpec(
            num_scalar_prefetch=2,
            grid=grid,
            in_specs=[
                pl.BlockSpec(memory_space=pltpu.SMEM),
                pl.BlockSpec((heads, Q_BLOCK, width), rows),
                pl.BlockSpec((heads, tokens, width), whole),
                pl.BlockSpec((heads, tokens, width), whole),
                pl.BlockSpec((Q_BLOCK, 3), lambda i, lo, hi: (i, 0)),
                pl.BlockSpec((3, tokens), lambda i, lo, hi: (0, 0)),
                pl.BlockSpec((heads, Q_BLOCK, width), rows),
                pl.BlockSpec((heads, Q_BLOCK, width), rows),
                pl.BlockSpec((heads, Q_BLOCK, 1), rows),
            ],
            out_specs=[
                pl.BlockSpec((heads, Q_BLOCK, width), rows),
                pl.BlockSpec((heads, tokens, width), whole),
                pl.BlockSpec((heads, tokens, width), whole),
            ],
        ),
        out_shape=[
            jax.ShapeDtypeStruct((heads, tokens, width), jnp.float32),
            jax.ShapeDtypeStruct((heads, tokens, width), jnp.float32),
            jax.ShapeDtypeStruct((heads, tokens, width), jnp.float32),
        ],
        compiler_params=pltpu.CompilerParams(dimension_semantics=("arbitrary",)),
    )(lo, hi, slopes, q, k, v, qinfo, kinfo, o, do, lse)


def scatter_rows(parts, dp_size):
    width = parts.shape[1]
    padded = -(-width // 1024) * 1024
    parts = jnp.pad(parts, ((0, 0), (0, padded - width))).reshape(dp_size * padded // 128, 128)
    summed = lax.psum_scatter(parts, "dp", scatter_dimension=0, tiled=True)
    return summed.reshape(-1)[:width]


def on_device(
    dp_size,
    patches,
    counts,
    norm_gain,
    norm_bias,
    w_qkv,
    b_qv,
    w_out,
    out_bias,
    w_up,
    b_up,
    w_down,
    cotangent,
):
    local_rows = patches.shape[0]
    width_here = w_qkv.shape[2]
    heads_here = width_here // HEAD_DIM
    ff_here = w_up.shape[1]
    tensor_pos = lax.axis_index("tensor")
    score_scale = HEAD_DIM ** (-0.5)
    segment, grid_row, grid_col, is_valid = layout(counts[0])
    keep_rows = lax.dynamic_slice_in_dim(is_valid, tensor_pos * local_rows, local_rows)[:, None]
    slopes = slopes_of(tensor_pos * heads_here, heads_here)
    inputs = patches.astype(jnp.float32)
    inputs_all = lax.all_gather(patches, "tensor", axis=0, tiled=True).astype(jnp.float32)
    normed = normalize(inputs_all, norm_gain[0], norm_bias[0]).astype(jnp.bfloat16)
    projected = jnp.einsum("td,dsc->tsc", normed, w_qkv, preferred_element_type=jnp.float32)
    queries = (projected[:, 0] + b_qv[0]).astype(jnp.bfloat16)
    keys = projected[:, 1].astype(jnp.bfloat16)
    values = (projected[:, 2] + b_qv[1]).astype(jnp.bfloat16)

    def head_major(rows):
        return rows.reshape(TOK_DEV, heads_here, HEAD_DIM).transpose(1, 0, 2)

    def row_major(heads):
        return heads.transpose(1, 0, 2).reshape(TOK_DEV, width_here)

    key_lo, key_hi = key_ranges(segment, TOK_DEV)
    segment_f = segment.astype(jnp.float32)
    query_info = jnp.stack([grid_row, grid_col, segment_f], axis=1)
    key_info = jnp.stack([grid_row, grid_col, segment_f], axis=0)
    query_heads = head_major(queries)
    key_heads = head_major(keys)
    value_heads = head_major(values)
    mixed_f32, log_totals = attention_fwd(
        key_lo, key_hi, slopes, query_heads, key_heads, value_heads, query_info, key_info, score_scale
    )
    upstream = cotangent.astype(jnp.float32)
    branch_grad = lax.all_gather(
        (keep_rows * upstream).astype(jnp.bfloat16), "tensor", axis=0, tiled=True
    )
    mixed_f32, log_totals, branch_grad = lax.optimization_barrier(
        (mixed_f32, log_totals, branch_grad)
    )
    mixed_rows = row_major(mixed_f32).astype(jnp.bfloat16)
    mixed_all = lax.all_gather(mixed_rows, "tensor", axis=1, tiled=True)
    w_out_all = lax.all_gather(w_out, "tensor", axis=0, tiled=True)
    attended = jnp.dot(mixed_all, w_out_all, preferred_element_type=jnp.float32)
    after_attn_all = inputs_all + is_valid[:, None] * (attended + out_bias[0])
    after_attn = lax.dynamic_slice_in_dim(after_attn_all, tensor_pos * local_rows, local_rows)
    normed_two = normalize(after_attn_all, norm_gain[1], norm_bias[1]).astype(jnp.bfloat16)
    hidden_pre = jnp.dot(normed_two, w_up, preferred_element_type=jnp.float32) + b_up
    hidden = jax.nn.gelu(hidden_pre, approximate=False).astype(jnp.bfloat16)
    branch_partial = jnp.dot(hidden, w_down, preferred_element_type=jnp.float32).astype(
        jnp.bfloat16
    )
    down_bias_grad = jnp.sum(keep_rows * upstream, axis=0)
    w_down_grad_t = jnp.einsum(
        "td,tf->df", branch_grad, hidden, preferred_element_type=jnp.float32
    )
    hidden_grad = jnp.einsum("td,fd->tf", branch_grad, w_down, preferred_element_type=jnp.float32)
    _, gelu_back = jax.vjp(lambda pre_act: jax.nn.gelu(pre_act, approximate=False), hidden_pre)
    pre_grad = gelu_back(hidden_grad)[0].astype(jnp.bfloat16)
    up_bias_grad = jnp.sum(pre_grad, axis=0, dtype=jnp.float32)
    w_up_grad = jnp.einsum("td,tf->df", normed_two, pre_grad, preferred_element_type=jnp.float32)
    normed_two_grad = lax.psum_scatter(
        jnp.einsum("tf,df->td", pre_grad, w_up, preferred_element_type=jnp.float32).astype(
            jnp.bfloat16
        ),
        "tensor",
        scatter_dimension=0,
        tiled=True,
    ).astype(jnp.float32)
    _, norm_two_back = jax.vjp(normalize, after_attn, norm_gain[1], norm_bias[1])
    through_two, gain_two_grad, shift_two_grad = norm_two_back(normed_two_grad)
    after_grad = upstream + through_two
    attn_bias_grad = jnp.sum(keep_rows * after_grad, axis=0)
    attn_local = (keep_rows * after_grad).astype(jnp.bfloat16)
    attn_grad = lax.all_gather(attn_local, "tensor", axis=0, tiled=True)
    w_out_grad_t = jnp.einsum(
        "td,tc->dc", attn_grad, mixed_rows, preferred_element_type=jnp.float32
    )
    mixed_grad = jnp.einsum(
        "td,cd->tc", attn_grad, w_out, preferred_element_type=jnp.float32
    ).astype(jnp.bfloat16)
    early_parts = jnp.concatenate(
        [
            w_down_grad_t.reshape(dp_size, -1),
            w_up_grad.reshape(dp_size, -1),
            w_out_grad_t.reshape(dp_size, -1),
        ],
        axis=1,
    )
    early_parts, mixed_grad, branch_partial = lax.optimization_barrier(
        (early_parts, mixed_grad, branch_partial)
    )
    branch = lax.psum_scatter(branch_partial, "tensor", scatter_dimension=0, tiled=True).astype(
        jnp.float32
    )
    result = (after_attn + keep_rows * (branch + out_bias[1])).astype(jnp.bfloat16)
    early_sum = scatter_rows(early_parts, dp_size)
    query_acc, key_acc, value_acc = attention_bwd(
        key_lo, key_hi, slopes, query_heads, key_heads, value_heads, query_info, key_info,
        mixed_f32, head_major(mixed_grad), log_totals, score_scale,
    )
    query_acc, key_acc, value_acc, early_sum, result = lax.optimization_barrier(
        (query_acc, key_acc, value_acc, early_sum, result)
    )
    query_grad = row_major(query_acc * score_scale).astype(jnp.bfloat16)
    key_grad = row_major(key_acc * score_scale).astype(jnp.bfloat16)
    value_grad = row_major(value_acc).astype(jnp.bfloat16)
    projected_grad = jnp.stack([query_grad, key_grad, value_grad], axis=1)
    qv_bias_grad = jnp.stack(
        [
            jnp.sum(query_grad, axis=0, dtype=jnp.float32),
            jnp.sum(value_grad, axis=0, dtype=jnp.float32),
        ]
    )
    w_qkv_grad = jnp.einsum(
        "td,tsc->dsc", normed, projected_grad, preferred_element_type=jnp.float32
    )
    normed_grad = lax.psum_scatter(
        jnp.einsum("tsc,dsc->td", projected_grad, w_qkv, preferred_element_type=jnp.float32).astype(
            jnp.bfloat16
        ),
        "tensor",
        scatter_dimension=0,
        tiled=True,
    ).astype(jnp.float32)
    _, norm_one_back = jax.vjp(normalize, inputs, norm_gain[0], norm_bias[0])
    through_one, gain_one_grad, shift_one_grad = norm_one_back(normed_grad)
    input_grad = (after_grad + through_one).astype(jnp.bfloat16)
    small = jnp.concatenate(
        [
            jnp.stack([gain_one_grad, gain_two_grad]).reshape(-1),
            jnp.stack([shift_one_grad, shift_two_grad]).reshape(-1),
            jnp.stack([attn_bias_grad, down_bias_grad]).reshape(-1),
            qv_bias_grad.reshape(-1),
            up_bias_grad,
        ]
    )
    late_parts = jnp.concatenate(
        [w_qkv_grad.reshape(dp_size, -1), jnp.broadcast_to(small, (dp_size,) + small.shape)],
        axis=1,
    )
    late_sum = scatter_rows(late_parts, dp_size)
    qkv_size = w_qkv_grad.size // dp_size
    rows_dp = D // dp_size
    qkv_part = late_sum[:qkv_size].reshape(rows_dp, 3, width_here)
    small_all = lax.all_gather(late_sum[qkv_size:], "tensor", axis=0, tiled=False)
    tensor_size = small_all.shape[0]
    summed = jnp.sum(small_all[:, : 6 * D], axis=0)
    gains_grad = summed[: 2 * D].reshape(2, D)
    shifts_grad = summed[2 * D : 4 * D].reshape(2, D)
    outer_grad = summed[4 * D : 6 * D].reshape(2, D)
    qv_sum = (
        small_all[:, 6 * D : 6 * D + 2 * width_here]
        .reshape(tensor_size, 2, width_here)
        .transpose(1, 0, 2)
        .reshape(2, D)
    )
    up_sum = small_all[:, 6 * D + 2 * width_here :].reshape(FF)
    down_size = D * ff_here // dp_size
    up_size = D * ff_here // dp_size
    down_part = early_sum[:down_size].reshape(rows_dp, ff_here).T
    up_part = early_sum[down_size : down_size + up_size].reshape(rows_dp, ff_here)
    out_part = early_sum[down_size + up_size :].reshape(rows_dp, width_here).T
    return (
        result,
        input_grad,
        gains_grad,
        shifts_grad,
        qkv_part,
        qv_sum,
        out_part,
        outer_grad,
        up_part,
        up_sum,
        down_part,
    )


def solution(mesh):
    placed = (
        P(("dp", "tensor"), None),
        P("dp", None),
        P(),
        P(),
        P(None, None, "tensor"),
        P(None, "tensor"),
        P("tensor", None),
        P(),
        P(None, "tensor"),
        P("tensor"),
        P("tensor", None),
        P(("dp", "tensor"), None),
    )
    return jax.shard_map(
        functools.partial(on_device, mesh.shape["dp"]),
        mesh=mesh,
        in_specs=placed,
        out_specs=(
            P(("dp", "tensor"), None),
            P(("dp", "tensor"), None),
            P(),
            P(),
            P("dp", None, "tensor"),
            P(),
            P("tensor", "dp"),
            P(),
            P("dp", "tensor"),
            P(),
            P("tensor", "dp"),
        ),
        check_vma=False,
    )
```

```python
import functools

import jax
import jax.numpy as jnp
from jax import lax
from jax.experimental import pallas as pl
from jax.experimental.pallas import tpu as pltpu
from jax.sharding import PartitionSpec as P

D = 768
HEADS = 12
HEAD_DIM = 64
FF = 3072
SIDE_S = 12
SIDE_M = 15
SIDE_L = 20
TOK_DEV = 2048


EPSILON = 1e-06


def layout(group_counts):
    positions = jnp.arange(TOK_DEV, dtype=jnp.int32)
    area_small = SIDE_S * SIDE_S
    area_middle = SIDE_M * SIDE_M
    area_large = SIDE_L * SIDE_L
    end_small = group_counts[0] * area_small
    end_middle = end_small + group_counts[1] * area_middle
    end_large = end_middle + group_counts[2] * area_large
    size_class = (positions >= end_small).astype(jnp.int32) + (positions >= end_middle).astype(
        jnp.int32
    )
    begins = jnp.where(size_class == 0, 0, jnp.where(size_class == 1, end_small, end_middle))
    area_len = jnp.where(
        size_class == 0, area_small, jnp.where(size_class == 1, area_middle, area_large)
    )
    side_len = jnp.where(size_class == 0, SIDE_S, jnp.where(size_class == 1, SIDE_M, SIDE_L))
    within = positions - begins
    picture_index = within // area_len
    within_image = within % area_len
    is_valid = positions < end_large
    segment = jnp.where(is_valid, size_class * 16 + picture_index, 255)
    grid_row = (within_image // side_len).astype(jnp.float32)
    grid_col = (within_image % side_len).astype(jnp.float32)
    return (segment, grid_row, grid_col, is_valid.astype(jnp.float32))


def normalize(values, gain_row, shift_row):
    centred = values - jnp.mean(values, axis=-1, keepdims=True)
    spread = jnp.mean(centred * centred, axis=-1, keepdims=True)
    return centred * lax.rsqrt(spread + EPSILON) * gain_row + shift_row


def slopes_of(first_head, count_heads):
    head_number = (first_head + jnp.arange(count_heads, dtype=jnp.int32)).astype(jnp.float32) + 1.0
    return jnp.exp2(-8.0 * head_number / HEADS)


def distances(row_query, col_query, row_key, col_key):
    delta_row = row_query[:, None] - row_key[None, :]
    delta_col = col_query[:, None] - col_key[None, :]
    return jnp.sqrt(delta_row * delta_row + delta_col * delta_col)

Q_BLOCK = 256
K_BLOCK = 256
NEG = -1e30


def key_ranges(segment, tokens):
    starts = jnp.arange(0, tokens, Q_BLOCK)
    first = segment[starts]
    last = segment[starts + Q_BLOCK - 1]
    key_lo = jnp.sum(segment[None, :] < first[:, None], axis=1)
    key_hi = jnp.sum(segment[None, :] <= last[:, None], axis=1)
    return (key_lo // K_BLOCK).astype(jnp.int32), ((key_hi + K_BLOCK - 1) // K_BLOCK).astype(jnp.int32)


def block_geometry(qi_ref, ki_ref, start):
    rq = qi_ref[:, 0:1]
    cq = qi_ref[:, 1:2]
    sq = qi_ref[:, 2:3]
    rk = ki_ref[0:1, pl.ds(start, K_BLOCK)]
    ck = ki_ref[1:2, pl.ds(start, K_BLOCK)]
    sk = ki_ref[2:3, pl.ds(start, K_BLOCK)]
    dr = rq - rk
    dc = cq - ck
    return jnp.sqrt(dr * dr + dc * dc), sq == sk


def fwd_kernel(heads, scale, lo_ref, hi_ref, slope_ref, q_ref, k_ref, v_ref, qi_ref, ki_ref, o_ref, lse_ref):
    i = pl.program_id(0)
    queries = [q_ref[h] for h in range(heads)]
    width = q_ref.shape[2]

    def body(kb, carry):
        start = pl.multiple_of(kb * K_BLOCK, K_BLOCK)
        dist, allowed = block_geometry(qi_ref, ki_ref, start)
        out = []
        for h in range(heads):
            m_old, l_old, acc_old = carry[h]
            keys = k_ref[h, pl.ds(start, K_BLOCK), :]
            vals = v_ref[h, pl.ds(start, K_BLOCK), :]
            s = lax.dot_general(queries[h], keys, (((1,), (1,)), ((), ())),
                                preferred_element_type=jnp.float32) * scale - slope_ref[h] * dist
            s = jnp.where(allowed, s, NEG)
            m_new = jnp.maximum(m_old, jnp.max(s, axis=1, keepdims=True))
            alpha = jnp.exp(m_old - m_new)
            p = jnp.exp(s - m_new)
            l_new = alpha * l_old + jnp.sum(p, axis=1, keepdims=True)
            acc_new = alpha * acc_old + jnp.dot(p.astype(jnp.bfloat16), vals,
                                                preferred_element_type=jnp.float32)
            out.append((m_new, l_new, acc_new))
        return tuple(out)

    init = tuple(
        (jnp.full((Q_BLOCK, 1), NEG, jnp.float32), jnp.zeros((Q_BLOCK, 1), jnp.float32),
         jnp.zeros((Q_BLOCK, width), jnp.float32))
        for _ in range(heads)
    )
    final = lax.fori_loop(lo_ref[i], hi_ref[i], body, init)
    for h in range(heads):
        m, l, acc = final[h]
        o_ref[h] = acc / l
        lse_ref[h] = m + jnp.log(l)


def bwd_kernel(heads, scale, lo_ref, hi_ref, slope_ref, q_ref, k_ref, v_ref, qi_ref, ki_ref,
               o_ref, do_ref, lse_ref, dq_ref, dk_ref, dv_ref):
    i = pl.program_id(0)

    @pl.when(i == 0)
    def _():
        dk_ref[...] = jnp.zeros_like(dk_ref)
        dv_ref[...] = jnp.zeros_like(dv_ref)

    queries = [q_ref[h] for h in range(heads)]
    grads = [do_ref[h] for h in range(heads)]
    lses = [lse_ref[h] for h in range(heads)]
    deltas = [jnp.sum(grads[h].astype(jnp.float32) * o_ref[h], axis=1, keepdims=True)
              for h in range(heads)]
    width = q_ref.shape[2]

    def body(kb, carry):
        start = pl.multiple_of(kb * K_BLOCK, K_BLOCK)
        dist, allowed = block_geometry(qi_ref, ki_ref, start)
        out = []
        for h in range(heads):
            keys = k_ref[h, pl.ds(start, K_BLOCK), :]
            vals = v_ref[h, pl.ds(start, K_BLOCK), :]
            s = lax.dot_general(queries[h], keys, (((1,), (1,)), ((), ())),
                                preferred_element_type=jnp.float32) * scale - slope_ref[h] * dist
            p = jnp.where(allowed, jnp.exp(s - lses[h]), 0.0)
            dp = lax.dot_general(grads[h], vals, (((1,), (1,)), ((), ())),
                                 preferred_element_type=jnp.float32)
            ds = (p * (dp - deltas[h])).astype(jnp.bfloat16)
            out.append(carry[h] + jnp.dot(ds, keys, preferred_element_type=jnp.float32))
            dk_ref[h, pl.ds(start, K_BLOCK), :] += lax.dot_general(
                ds, queries[h], (((0,), (0,)), ((), ())), preferred_element_type=jnp.float32)
            dv_ref[h, pl.ds(start, K_BLOCK), :] += lax.dot_general(
                p.astype(jnp.bfloat16), grads[h], (((0,), (0,)), ((), ())),
                preferred_element_type=jnp.float32)
        return tuple(out)

    init = tuple(jnp.zeros((Q_BLOCK, width), jnp.float32) for _ in range(heads))
    final = lax.fori_loop(lo_ref[i], hi_ref[i], body, init)
    for h in range(heads):
        dq_ref[h] = final[h]


def attention_fwd(lo, hi, slopes, q, k, v, qinfo, kinfo, scale):
    heads, tokens, width = q.shape
    grid = (tokens // Q_BLOCK,)
    whole = lambda i, lo, hi: (0, 0, 0)
    rows = lambda i, lo, hi: (0, i, 0)
    return pl.pallas_call(
        functools.partial(fwd_kernel, heads, scale),
        grid_spec=pltpu.PrefetchScalarGridSpec(
            num_scalar_prefetch=2,
            grid=grid,
            in_specs=[
                pl.BlockSpec(memory_space=pltpu.SMEM),
                pl.BlockSpec((heads, Q_BLOCK, width), rows),
                pl.BlockSpec((heads, tokens, width), whole),
                pl.BlockSpec((heads, tokens, width), whole),
                pl.BlockSpec((Q_BLOCK, 3), lambda i, lo, hi: (i, 0)),
                pl.BlockSpec((3, tokens), lambda i, lo, hi: (0, 0)),
            ],
            out_specs=[
                pl.BlockSpec((heads, Q_BLOCK, width), rows),
                pl.BlockSpec((heads, Q_BLOCK, 1), rows),
            ],
        ),
        out_shape=[
            jax.ShapeDtypeStruct((heads, tokens, width), jnp.float32),
            jax.ShapeDtypeStruct((heads, tokens, 1), jnp.float32),
        ],
        compiler_params=pltpu.CompilerParams(dimension_semantics=("arbitrary",)),
    )(lo, hi, slopes, q, k, v, qinfo, kinfo)


def attention_bwd(lo, hi, slopes, q, k, v, qinfo, kinfo, o, do, lse, scale):
    heads, tokens, width = q.shape
    grid = (tokens // Q_BLOCK,)
    whole = lambda i, lo, hi: (0, 0, 0)
    rows = lambda i, lo, hi: (0, i, 0)
    return pl.pallas_call(
        functools.partial(bwd_kernel, heads, scale),
        grid_spec=pltpu.PrefetchScalarGridSpec(
            num_scalar_prefetch=2,
            grid=grid,
            in_specs=[
                pl.BlockSpec(memory_space=pltpu.SMEM),
                pl.BlockSpec((heads, Q_BLOCK, width), rows),
                pl.BlockSpec((heads, tokens, width), whole),
                pl.BlockSpec((heads, tokens, width), whole),
                pl.BlockSpec((Q_BLOCK, 3), lambda i, lo, hi: (i, 0)),
                pl.BlockSpec((3, tokens), lambda i, lo, hi: (0, 0)),
                pl.BlockSpec((heads, Q_BLOCK, width), rows),
                pl.BlockSpec((heads, Q_BLOCK, width), rows),
                pl.BlockSpec((heads, Q_BLOCK, 1), rows),
            ],
            out_specs=[
                pl.BlockSpec((heads, Q_BLOCK, width), rows),
                pl.BlockSpec((heads, tokens, width), whole),
                pl.BlockSpec((heads, tokens, width), whole),
            ],
        ),
        out_shape=[
            jax.ShapeDtypeStruct((heads, tokens, width), jnp.float32),
            jax.ShapeDtypeStruct((heads, tokens, width), jnp.float32),
            jax.ShapeDtypeStruct((heads, tokens, width), jnp.float32),
        ],
        compiler_params=pltpu.CompilerParams(dimension_semantics=("arbitrary",)),
    )(lo, hi, slopes, q, k, v, qinfo, kinfo, o, do, lse)


def scatter_tensor(partial, tensor_size):
    me = lax.axis_index("tensor")
    blocks = partial.reshape(tensor_size, -1, partial.shape[1])
    total = lax.dynamic_index_in_dim(blocks, me, keepdims=False).astype(jnp.float32)
    for shift in range(1, tensor_size):
        outgoing = lax.dynamic_index_in_dim(blocks, (me + shift) % tensor_size, keepdims=False)
        pairs = [(i, (i + shift) % tensor_size) for i in range(tensor_size)]
        total = total + lax.ppermute(outgoing.astype(jnp.bfloat16), "tensor", pairs).astype(
            jnp.float32
        )
    return total


def scatter_rows(parts, dp_size):
    width = parts.shape[1]
    padded = -(-width // 2048) * 2048
    parts = jnp.pad(parts, ((0, 0), (0, padded - width))).reshape(dp_size * padded // 128, 128)
    summed = lax.psum_scatter(parts, "dp", scatter_dimension=0, tiled=True)
    return summed.reshape(-1)[:width]


def on_device(
    dp_size,
    patches,
    counts,
    norm_gain,
    norm_bias,
    w_qkv,
    b_qv,
    w_out,
    out_bias,
    w_up,
    b_up,
    w_down,
    cotangent,
):
    local_rows = patches.shape[0]
    width_here = w_qkv.shape[2]
    heads_here = width_here // HEAD_DIM
    ff_here = w_up.shape[1]
    tensor_pos = lax.axis_index("tensor")
    tensor_size = D // width_here
    score_scale = HEAD_DIM ** (-0.5)
    segment, grid_row, grid_col, is_valid = layout(counts[0])
    keep_rows = lax.dynamic_slice_in_dim(is_valid, tensor_pos * local_rows, local_rows)[:, None]
    slopes = slopes_of(tensor_pos * heads_here, heads_here)
    inputs = patches.astype(jnp.float32)
    inputs_all = lax.all_gather(patches, "tensor", axis=0, tiled=True).astype(jnp.float32)
    normed = normalize(inputs_all, norm_gain[0], norm_bias[0]).astype(jnp.bfloat16)
    projected = jnp.einsum("td,dsc->tsc", normed, w_qkv, preferred_element_type=jnp.float32)
    queries = (projected[:, 0] + b_qv[0]).astype(jnp.bfloat16)
    keys = projected[:, 1].astype(jnp.bfloat16)
    values = (projected[:, 2] + b_qv[1]).astype(jnp.bfloat16)

    def head_major(rows):
        return rows.reshape(TOK_DEV, heads_here, HEAD_DIM).transpose(1, 0, 2)

    def row_major(heads):
        return heads.transpose(1, 0, 2).reshape(TOK_DEV, width_here)

    key_lo, key_hi = key_ranges(segment, TOK_DEV)
    segment_f = segment.astype(jnp.float32)
    query_info = jnp.stack([grid_row, grid_col, segment_f], axis=1)
    key_info = jnp.stack([grid_row, grid_col, segment_f], axis=0)
    query_heads = head_major(queries)
    key_heads = head_major(keys)
    value_heads = head_major(values)
    mixed_f32, log_totals = attention_fwd(
        key_lo, key_hi, slopes, query_heads, key_heads, value_heads, query_info, key_info, score_scale
    )
    upstream = cotangent.astype(jnp.float32)
    branch_grad = lax.all_gather(
        (keep_rows * upstream).astype(jnp.bfloat16), "tensor", axis=0, tiled=True
    )
    mixed_f32, log_totals, branch_grad = lax.optimization_barrier(
        (mixed_f32, log_totals, branch_grad)
    )
    mixed_rows = row_major(mixed_f32).astype(jnp.bfloat16)
    mixed_all = lax.all_gather(mixed_rows, "tensor", axis=1, tiled=True)
    w_out_all = lax.all_gather(w_out, "tensor", axis=0, tiled=True)
    attended = jnp.dot(mixed_all, w_out_all, preferred_element_type=jnp.float32)
    after_attn_all = inputs_all + is_valid[:, None] * (attended + out_bias[0])
    after_attn = lax.dynamic_slice_in_dim(after_attn_all, tensor_pos * local_rows, local_rows)
    normed_two = normalize(after_attn_all, norm_gain[1], norm_bias[1]).astype(jnp.bfloat16)
    hidden_pre = jnp.dot(normed_two, w_up, preferred_element_type=jnp.float32) + b_up
    hidden = jax.nn.gelu(hidden_pre, approximate=False).astype(jnp.bfloat16)
    branch_partial = jnp.dot(hidden, w_down, preferred_element_type=jnp.float32)
    down_bias_grad = jnp.sum(keep_rows * upstream, axis=0)
    w_down_grad_t = jnp.einsum(
        "td,tf->df", branch_grad, hidden, preferred_element_type=jnp.float32
    )
    hidden_grad = jnp.einsum("td,fd->tf", branch_grad, w_down, preferred_element_type=jnp.float32)
    _, gelu_back = jax.vjp(lambda pre_act: jax.nn.gelu(pre_act, approximate=False), hidden_pre)
    pre_grad = gelu_back(hidden_grad)[0].astype(jnp.bfloat16)
    up_bias_grad = jnp.sum(pre_grad, axis=0, dtype=jnp.float32)
    w_up_grad = jnp.einsum("td,tf->df", normed_two, pre_grad, preferred_element_type=jnp.float32)
    normed_two_grad = lax.psum_scatter(
        jnp.einsum("tf,df->td", pre_grad, w_up, preferred_element_type=jnp.float32).astype(
            jnp.bfloat16
        ),
        "tensor",
        scatter_dimension=0,
        tiled=True,
    ).astype(jnp.float32)
    _, norm_two_back = jax.vjp(normalize, after_attn, norm_gain[1], norm_bias[1])
    through_two, gain_two_grad, shift_two_grad = norm_two_back(normed_two_grad)
    after_grad = upstream + through_two
    attn_bias_grad = jnp.sum(keep_rows * after_grad, axis=0)
    attn_local = (keep_rows * after_grad).astype(jnp.bfloat16)
    attn_grad = lax.all_gather(attn_local, "tensor", axis=0, tiled=True)
    w_out_grad_t = jnp.einsum(
        "td,tc->dc", attn_grad, mixed_rows, preferred_element_type=jnp.float32
    )
    mixed_grad = jnp.einsum(
        "td,cd->tc", attn_grad, w_out, preferred_element_type=jnp.float32
    ).astype(jnp.bfloat16)
    early_parts = jnp.concatenate(
        [
            w_down_grad_t.reshape(dp_size, -1),
            w_up_grad.reshape(dp_size, -1),
            w_out_grad_t.reshape(dp_size, -1),
        ],
        axis=1,
    )
    early_parts, mixed_grad, branch_partial = lax.optimization_barrier(
        (early_parts, mixed_grad, branch_partial)
    )
    branch = scatter_tensor(branch_partial, tensor_size)
    result = (after_attn + keep_rows * (branch + out_bias[1])).astype(jnp.bfloat16)
    early_sum = scatter_rows(early_parts.astype(jnp.bfloat16), dp_size).astype(jnp.float32)
    query_acc, key_acc, value_acc = attention_bwd(
        key_lo, key_hi, slopes, query_heads, key_heads, value_heads, query_info, key_info,
        mixed_f32, head_major(mixed_grad), log_totals, score_scale,
    )
    query_acc, key_acc, value_acc, early_sum, result = lax.optimization_barrier(
        (query_acc, key_acc, value_acc, early_sum, result)
    )
    query_grad = row_major(query_acc * score_scale).astype(jnp.bfloat16)
    key_grad = row_major(key_acc * score_scale).astype(jnp.bfloat16)
    value_grad = row_major(value_acc).astype(jnp.bfloat16)
    projected_grad = jnp.stack([query_grad, key_grad, value_grad], axis=1)
    qv_bias_grad = jnp.stack(
        [
            jnp.sum(query_grad, axis=0, dtype=jnp.float32),
            jnp.sum(value_grad, axis=0, dtype=jnp.float32),
        ]
    )
    w_qkv_grad = jnp.einsum(
        "td,tsc->dsc", normed, projected_grad, preferred_element_type=jnp.float32
    )
    normed_grad = scatter_tensor(
        jnp.einsum("tsc,dsc->td", projected_grad, w_qkv, preferred_element_type=jnp.float32),
        tensor_size,
    )
    _, norm_one_back = jax.vjp(normalize, inputs, norm_gain[0], norm_bias[0])
    through_one, gain_one_grad, shift_one_grad = norm_one_back(normed_grad)
    input_grad = (after_grad + through_one).astype(jnp.bfloat16)
    small = jnp.concatenate(
        [
            jnp.stack([gain_one_grad, gain_two_grad]).reshape(-1),
            jnp.stack([shift_one_grad, shift_two_grad]).reshape(-1),
            jnp.stack([attn_bias_grad, down_bias_grad]).reshape(-1),
            qv_bias_grad.reshape(-1),
            up_bias_grad,
        ]
    )
    late_parts = jnp.concatenate(
        [w_qkv_grad.reshape(dp_size, -1), jnp.broadcast_to(small, (dp_size,) + small.shape)],
        axis=1,
    )
    late_sum = scatter_rows(late_parts, dp_size)
    qkv_size = w_qkv_grad.size // dp_size
    rows_dp = D // dp_size
    qkv_part = late_sum[:qkv_size].reshape(rows_dp, 3, width_here)
    small_all = lax.all_gather(late_sum[qkv_size:], "tensor", axis=0, tiled=False)
    summed = jnp.sum(small_all[:, : 6 * D], axis=0)
    gains_grad = summed[: 2 * D].reshape(2, D)
    shifts_grad = summed[2 * D : 4 * D].reshape(2, D)
    outer_grad = summed[4 * D : 6 * D].reshape(2, D)
    qv_sum = (
        small_all[:, 6 * D : 6 * D + 2 * width_here]
        .reshape(tensor_size, 2, width_here)
        .transpose(1, 0, 2)
        .reshape(2, D)
    )
    up_sum = small_all[:, 6 * D + 2 * width_here :].reshape(FF)
    down_size = D * ff_here // dp_size
    up_size = D * ff_here // dp_size
    down_part = early_sum[:down_size].reshape(rows_dp, ff_here).T
    up_part = early_sum[down_size : down_size + up_size].reshape(rows_dp, ff_here)
    out_part = early_sum[down_size + up_size :].reshape(rows_dp, width_here).T
    return (
        result,
        input_grad,
        gains_grad,
        shifts_grad,
        qkv_part,
        qv_sum,
        out_part,
        outer_grad,
        up_part,
        up_sum,
        down_part,
    )


def solution(mesh):
    placed = (
        P(("dp", "tensor"), None),
        P("dp", None),
        P(),
        P(),
        P(None, None, "tensor"),
        P(None, "tensor"),
        P("tensor", None),
        P(),
        P(None, "tensor"),
        P("tensor"),
        P("tensor", None),
        P(("dp", "tensor"), None),
    )
    return jax.shard_map(
        functools.partial(on_device, mesh.shape["dp"]),
        mesh=mesh,
        in_specs=placed,
        out_specs=(
            P(("dp", "tensor"), None),
            P(("dp", "tensor"), None),
            P(),
            P(),
            P("dp", None, "tensor"),
            P(),
            P("tensor", "dp"),
            P(),
            P("dp", "tensor"),
            P(),
            P("tensor", "dp"),
        ),
        check_vma=False,
    )
```

```python
import functools

import jax
import jax.numpy as jnp
from jax import lax
from jax.experimental import pallas as pl
from jax.experimental.pallas import tpu as pltpu
from jax.sharding import PartitionSpec as P

D = 768
HEADS = 12
HEAD_DIM = 64
FF = 3072
SIDE_S = 12
SIDE_M = 15
SIDE_L = 20
TOK_DEV = 2048


EPSILON = 1e-06


def layout(group_counts):
    positions = jnp.arange(TOK_DEV, dtype=jnp.int32)
    area_small = SIDE_S * SIDE_S
    area_middle = SIDE_M * SIDE_M
    area_large = SIDE_L * SIDE_L
    end_small = group_counts[0] * area_small
    end_middle = end_small + group_counts[1] * area_middle
    end_large = end_middle + group_counts[2] * area_large
    size_class = (positions >= end_small).astype(jnp.int32) + (positions >= end_middle).astype(
        jnp.int32
    )
    begins = jnp.where(size_class == 0, 0, jnp.where(size_class == 1, end_small, end_middle))
    area_len = jnp.where(
        size_class == 0, area_small, jnp.where(size_class == 1, area_middle, area_large)
    )
    side_len = jnp.where(size_class == 0, SIDE_S, jnp.where(size_class == 1, SIDE_M, SIDE_L))
    within = positions - begins
    picture_index = within // area_len
    within_image = within % area_len
    is_valid = positions < end_large
    segment = jnp.where(is_valid, size_class * 16 + picture_index, 255)
    grid_row = (within_image // side_len).astype(jnp.float32)
    grid_col = (within_image % side_len).astype(jnp.float32)
    return (segment, grid_row, grid_col, is_valid.astype(jnp.float32))


def normalize(values, gain_row, shift_row):
    centred = values - jnp.mean(values, axis=-1, keepdims=True)
    spread = jnp.mean(centred * centred, axis=-1, keepdims=True)
    return centred * lax.rsqrt(spread + EPSILON) * gain_row + shift_row


def slopes_of(first_head, count_heads):
    head_number = (first_head + jnp.arange(count_heads, dtype=jnp.int32)).astype(jnp.float32) + 1.0
    return jnp.exp2(-8.0 * head_number / HEADS)


def distances(row_query, col_query, row_key, col_key):
    delta_row = row_query[:, None] - row_key[None, :]
    delta_col = col_query[:, None] - col_key[None, :]
    return jnp.sqrt(delta_row * delta_row + delta_col * delta_col)

Q_BLOCK = 256
K_BLOCK = 256
NEG = -1e30


def key_ranges(segment, tokens):
    starts = jnp.arange(0, tokens, Q_BLOCK)
    first = segment[starts]
    last = segment[starts + Q_BLOCK - 1]
    key_lo = jnp.sum(segment[None, :] < first[:, None], axis=1)
    key_hi = jnp.sum(segment[None, :] <= last[:, None], axis=1)
    return (key_lo // K_BLOCK).astype(jnp.int32), ((key_hi + K_BLOCK - 1) // K_BLOCK).astype(jnp.int32)


def block_geometry(qi_ref, ki_ref, start):
    rq = qi_ref[:, 0:1]
    cq = qi_ref[:, 1:2]
    sq = qi_ref[:, 2:3]
    rk = ki_ref[0:1, pl.ds(start, K_BLOCK)]
    ck = ki_ref[1:2, pl.ds(start, K_BLOCK)]
    sk = ki_ref[2:3, pl.ds(start, K_BLOCK)]
    dr = rq - rk
    dc = cq - ck
    return jnp.sqrt(dr * dr + dc * dc), sq == sk


def fwd_kernel(heads, scale, lo_ref, hi_ref, slope_ref, q_ref, k_ref, v_ref, qi_ref, ki_ref, o_ref, lse_ref):
    i = pl.program_id(0)
    queries = [q_ref[h] for h in range(heads)]
    width = q_ref.shape[2]

    def body(kb, carry):
        start = pl.multiple_of(kb * K_BLOCK, K_BLOCK)
        dist, allowed = block_geometry(qi_ref, ki_ref, start)
        out = []
        for h in range(heads):
            m_old, l_old, acc_old = carry[h]
            keys = k_ref[h, pl.ds(start, K_BLOCK), :]
            vals = v_ref[h, pl.ds(start, K_BLOCK), :]
            s = lax.dot_general(queries[h], keys, (((1,), (1,)), ((), ())),
                                preferred_element_type=jnp.float32) * scale - slope_ref[h] * dist
            s = jnp.where(allowed, s, NEG)
            m_new = jnp.maximum(m_old, jnp.max(s, axis=1, keepdims=True))
            alpha = jnp.exp(m_old - m_new)
            p = jnp.exp(s - m_new)
            l_new = alpha * l_old + jnp.sum(p, axis=1, keepdims=True)
            acc_new = alpha * acc_old + jnp.dot(p.astype(jnp.bfloat16), vals,
                                                preferred_element_type=jnp.float32)
            out.append((m_new, l_new, acc_new))
        return tuple(out)

    init = tuple(
        (jnp.full((Q_BLOCK, 1), NEG, jnp.float32), jnp.zeros((Q_BLOCK, 1), jnp.float32),
         jnp.zeros((Q_BLOCK, width), jnp.float32))
        for _ in range(heads)
    )
    final = lax.fori_loop(lo_ref[i], hi_ref[i], body, init)
    for h in range(heads):
        m, l, acc = final[h]
        o_ref[h] = acc / l
        lse_ref[h] = m + jnp.log(l)


def bwd_kernel(heads, scale, lo_ref, hi_ref, slope_ref, q_ref, k_ref, v_ref, qi_ref, ki_ref,
               o_ref, do_ref, lse_ref, dq_ref, dk_ref, dv_ref):
    i = pl.program_id(0)

    @pl.when(i == 0)
    def _():
        dk_ref[...] = jnp.zeros_like(dk_ref)
        dv_ref[...] = jnp.zeros_like(dv_ref)

    queries = [q_ref[h] for h in range(heads)]
    grads = [do_ref[h] for h in range(heads)]
    lses = [lse_ref[h] for h in range(heads)]
    deltas = [jnp.sum(grads[h].astype(jnp.float32) * o_ref[h], axis=1, keepdims=True)
              for h in range(heads)]
    width = q_ref.shape[2]

    def body(kb, carry):
        start = pl.multiple_of(kb * K_BLOCK, K_BLOCK)
        dist, allowed = block_geometry(qi_ref, ki_ref, start)
        out = []
        for h in range(heads):
            keys = k_ref[h, pl.ds(start, K_BLOCK), :]
            vals = v_ref[h, pl.ds(start, K_BLOCK), :]
            s = lax.dot_general(queries[h], keys, (((1,), (1,)), ((), ())),
                                preferred_element_type=jnp.float32) * scale - slope_ref[h] * dist
            p = jnp.where(allowed, jnp.exp(s - lses[h]), 0.0)
            dp = lax.dot_general(grads[h], vals, (((1,), (1,)), ((), ())),
                                 preferred_element_type=jnp.float32)
            ds = (p * (dp - deltas[h])).astype(jnp.bfloat16)
            out.append(carry[h] + jnp.dot(ds, keys, preferred_element_type=jnp.float32))
            dk_ref[h, pl.ds(start, K_BLOCK), :] += lax.dot_general(
                ds, queries[h], (((0,), (0,)), ((), ())), preferred_element_type=jnp.float32)
            dv_ref[h, pl.ds(start, K_BLOCK), :] += lax.dot_general(
                p.astype(jnp.bfloat16), grads[h], (((0,), (0,)), ((), ())),
                preferred_element_type=jnp.float32)
        return tuple(out)

    init = tuple(jnp.zeros((Q_BLOCK, width), jnp.float32) for _ in range(heads))
    final = lax.fori_loop(lo_ref[i], hi_ref[i], body, init)
    for h in range(heads):
        dq_ref[h] = final[h]


def attention_fwd(lo, hi, slopes, q, k, v, qinfo, kinfo, scale):
    heads, tokens, width = q.shape
    grid = (tokens // Q_BLOCK,)
    whole = lambda i, lo, hi: (0, 0, 0)
    rows = lambda i, lo, hi: (0, i, 0)
    return pl.pallas_call(
        functools.partial(fwd_kernel, heads, scale),
        grid_spec=pltpu.PrefetchScalarGridSpec(
            num_scalar_prefetch=2,
            grid=grid,
            in_specs=[
                pl.BlockSpec(memory_space=pltpu.SMEM),
                pl.BlockSpec((heads, Q_BLOCK, width), rows),
                pl.BlockSpec((heads, tokens, width), whole),
                pl.BlockSpec((heads, tokens, width), whole),
                pl.BlockSpec((Q_BLOCK, 3), lambda i, lo, hi: (i, 0)),
                pl.BlockSpec((3, tokens), lambda i, lo, hi: (0, 0)),
            ],
            out_specs=[
                pl.BlockSpec((heads, Q_BLOCK, width), rows),
                pl.BlockSpec((heads, Q_BLOCK, 1), rows),
            ],
        ),
        out_shape=[
            jax.ShapeDtypeStruct((heads, tokens, width), jnp.float32),
            jax.ShapeDtypeStruct((heads, tokens, 1), jnp.float32),
        ],
        compiler_params=pltpu.CompilerParams(dimension_semantics=("arbitrary",)),
    )(lo, hi, slopes, q, k, v, qinfo, kinfo)


def attention_bwd(lo, hi, slopes, q, k, v, qinfo, kinfo, o, do, lse, scale):
    heads, tokens, width = q.shape
    grid = (tokens // Q_BLOCK,)
    whole = lambda i, lo, hi: (0, 0, 0)
    rows = lambda i, lo, hi: (0, i, 0)
    return pl.pallas_call(
        functools.partial(bwd_kernel, heads, scale),
        grid_spec=pltpu.PrefetchScalarGridSpec(
            num_scalar_prefetch=2,
            grid=grid,
            in_specs=[
                pl.BlockSpec(memory_space=pltpu.SMEM),
                pl.BlockSpec((heads, Q_BLOCK, width), rows),
                pl.BlockSpec((heads, tokens, width), whole),
                pl.BlockSpec((heads, tokens, width), whole),
                pl.BlockSpec((Q_BLOCK, 3), lambda i, lo, hi: (i, 0)),
                pl.BlockSpec((3, tokens), lambda i, lo, hi: (0, 0)),
                pl.BlockSpec((heads, Q_BLOCK, width), rows),
                pl.BlockSpec((heads, Q_BLOCK, width), rows),
                pl.BlockSpec((heads, Q_BLOCK, 1), rows),
            ],
            out_specs=[
                pl.BlockSpec((heads, Q_BLOCK, width), rows),
                pl.BlockSpec((heads, tokens, width), whole),
                pl.BlockSpec((heads, tokens, width), whole),
            ],
        ),
        out_shape=[
            jax.ShapeDtypeStruct((heads, tokens, width), jnp.float32),
            jax.ShapeDtypeStruct((heads, tokens, width), jnp.float32),
            jax.ShapeDtypeStruct((heads, tokens, width), jnp.float32),
        ],
        compiler_params=pltpu.CompilerParams(dimension_semantics=("arbitrary",)),
    )(lo, hi, slopes, q, k, v, qinfo, kinfo, o, do, lse)


def scatter_tensor(partial, tensor_size):
    me = lax.axis_index("tensor")
    blocks = partial.reshape(tensor_size, -1, partial.shape[1])
    total = lax.dynamic_index_in_dim(blocks, me, keepdims=False).astype(jnp.float32)
    for shift in range(1, tensor_size):
        outgoing = lax.dynamic_index_in_dim(blocks, (me + shift) % tensor_size, keepdims=False)
        pairs = [(i, (i + shift) % tensor_size) for i in range(tensor_size)]
        total = total + lax.ppermute(outgoing.astype(jnp.bfloat16), "tensor", pairs).astype(
            jnp.float32
        )
    return total


def scatter_rows(parts, dp_size):
    width = parts.shape[1]
    padded = -(-width // 2048) * 2048
    parts = jnp.pad(parts, ((0, 0), (0, padded - width))).reshape(dp_size * padded // 128, 128)
    summed = lax.psum_scatter(parts, "dp", scatter_dimension=0, tiled=True)
    return summed.reshape(-1)[:width]


def on_device(
    dp_size,
    patches,
    counts,
    norm_gain,
    norm_bias,
    w_qkv,
    b_qv,
    w_out,
    out_bias,
    w_up,
    b_up,
    w_down,
    cotangent,
):
    local_rows = patches.shape[0]
    width_here = w_qkv.shape[2]
    heads_here = width_here // HEAD_DIM
    ff_here = w_up.shape[1]
    tensor_pos = lax.axis_index("tensor")
    tensor_size = D // width_here
    score_scale = HEAD_DIM ** (-0.5)
    segment, grid_row, grid_col, is_valid = layout(counts[0])
    keep_rows = lax.dynamic_slice_in_dim(is_valid, tensor_pos * local_rows, local_rows)[:, None]
    slopes = slopes_of(tensor_pos * heads_here, heads_here)
    inputs = patches.astype(jnp.float32)
    inputs_all = lax.all_gather(patches, "tensor", axis=0, tiled=True).astype(jnp.float32)
    normed = normalize(inputs_all, norm_gain[0], norm_bias[0]).astype(jnp.bfloat16)
    projected = jnp.einsum("td,dsc->tsc", normed, w_qkv, preferred_element_type=jnp.float32)
    queries = (projected[:, 0] + b_qv[0]).astype(jnp.bfloat16)
    keys = projected[:, 1].astype(jnp.bfloat16)
    values = (projected[:, 2] + b_qv[1]).astype(jnp.bfloat16)

    def head_major(rows):
        return rows.reshape(TOK_DEV, heads_here, HEAD_DIM).transpose(1, 0, 2)

    def row_major(heads):
        return heads.transpose(1, 0, 2).reshape(TOK_DEV, width_here)

    key_lo, key_hi = key_ranges(segment, TOK_DEV)
    segment_f = segment.astype(jnp.float32)
    query_info = jnp.stack([grid_row, grid_col, segment_f], axis=1)
    key_info = jnp.stack([grid_row, grid_col, segment_f], axis=0)
    query_heads = head_major(queries)
    key_heads = head_major(keys)
    value_heads = head_major(values)
    mixed_f32, log_totals = attention_fwd(
        key_lo, key_hi, slopes, query_heads, key_heads, value_heads, query_info, key_info, score_scale
    )
    upstream = cotangent.astype(jnp.float32)
    branch_grad = lax.all_gather(
        (keep_rows * upstream).astype(jnp.bfloat16), "tensor", axis=0, tiled=True
    )
    mixed_f32, log_totals, branch_grad = lax.optimization_barrier(
        (mixed_f32, log_totals, branch_grad)
    )
    mixed_rows = row_major(mixed_f32).astype(jnp.bfloat16)
    mixed_all = lax.all_gather(mixed_rows, "tensor", axis=1, tiled=True)
    w_out_all = lax.all_gather(w_out, "tensor", axis=0, tiled=True)
    attended = jnp.dot(mixed_all, w_out_all, preferred_element_type=jnp.float32)
    after_attn_all = inputs_all + is_valid[:, None] * (attended + out_bias[0])
    after_attn = lax.dynamic_slice_in_dim(after_attn_all, tensor_pos * local_rows, local_rows)
    normed_two = normalize(after_attn_all, norm_gain[1], norm_bias[1]).astype(jnp.bfloat16)
    hidden_pre = jnp.dot(normed_two, w_up, preferred_element_type=jnp.float32) + b_up
    hidden = jax.nn.gelu(hidden_pre, approximate=False).astype(jnp.bfloat16)
    branch_partial = jnp.dot(hidden, w_down, preferred_element_type=jnp.float32)
    down_bias_grad = jnp.sum(keep_rows * upstream, axis=0)
    w_down_grad_t = jnp.einsum(
        "td,tf->df", branch_grad, hidden, preferred_element_type=jnp.float32
    )
    hidden_grad = jnp.einsum("td,fd->tf", branch_grad, w_down, preferred_element_type=jnp.float32)
    _, gelu_back = jax.vjp(lambda pre_act: jax.nn.gelu(pre_act, approximate=False), hidden_pre)
    pre_grad = gelu_back(hidden_grad)[0].astype(jnp.bfloat16)
    up_bias_grad = jnp.sum(pre_grad, axis=0, dtype=jnp.float32)
    w_up_grad = jnp.einsum("td,tf->df", normed_two, pre_grad, preferred_element_type=jnp.float32)
    normed_two_grad = lax.psum_scatter(
        jnp.einsum("tf,df->td", pre_grad, w_up, preferred_element_type=jnp.float32).astype(
            jnp.bfloat16
        ),
        "tensor",
        scatter_dimension=0,
        tiled=True,
    ).astype(jnp.float32)
    _, norm_two_back = jax.vjp(normalize, after_attn, norm_gain[1], norm_bias[1])
    through_two, gain_two_grad, shift_two_grad = norm_two_back(normed_two_grad)
    after_grad = upstream + through_two
    attn_bias_grad = jnp.sum(keep_rows * after_grad, axis=0)
    attn_local = (keep_rows * after_grad).astype(jnp.bfloat16)
    attn_grad = lax.all_gather(attn_local, "tensor", axis=0, tiled=True)
    w_out_grad_t = jnp.einsum(
        "td,tc->dc", attn_grad, mixed_rows, preferred_element_type=jnp.float32
    )
    mixed_grad = jnp.einsum(
        "td,cd->tc", attn_grad, w_out, preferred_element_type=jnp.float32
    ).astype(jnp.bfloat16)
    early_parts = jnp.concatenate([w_down_grad_t, w_up_grad, w_out_grad_t], axis=1).astype(
        jnp.bfloat16
    )
    early_parts, mixed_grad, branch_partial = lax.optimization_barrier(
        (early_parts, mixed_grad, branch_partial)
    )
    branch = scatter_tensor(branch_partial, tensor_size)
    result = (after_attn + keep_rows * (branch + out_bias[1])).astype(jnp.bfloat16)
    early_sum = lax.psum_scatter(early_parts, "dp", scatter_dimension=0, tiled=True).astype(
        jnp.float32
    )
    query_acc, key_acc, value_acc = attention_bwd(
        key_lo, key_hi, slopes, query_heads, key_heads, value_heads, query_info, key_info,
        mixed_f32, head_major(mixed_grad), log_totals, score_scale,
    )
    query_acc, key_acc, value_acc, early_sum, result = lax.optimization_barrier(
        (query_acc, key_acc, value_acc, early_sum, result)
    )
    query_grad = row_major(query_acc * score_scale).astype(jnp.bfloat16)
    key_grad = row_major(key_acc * score_scale).astype(jnp.bfloat16)
    value_grad = row_major(value_acc).astype(jnp.bfloat16)
    projected_grad = jnp.stack([query_grad, key_grad, value_grad], axis=1)
    qv_bias_grad = jnp.stack(
        [
            jnp.sum(query_grad, axis=0, dtype=jnp.float32),
            jnp.sum(value_grad, axis=0, dtype=jnp.float32),
        ]
    )
    w_qkv_grad = jnp.einsum(
        "td,tsc->dsc", normed, projected_grad, preferred_element_type=jnp.float32
    )
    normed_grad = scatter_tensor(
        jnp.einsum("tsc,dsc->td", projected_grad, w_qkv, preferred_element_type=jnp.float32),
        tensor_size,
    )
    _, norm_one_back = jax.vjp(normalize, inputs, norm_gain[0], norm_bias[0])
    through_one, gain_one_grad, shift_one_grad = norm_one_back(normed_grad)
    input_grad = (after_grad + through_one).astype(jnp.bfloat16)
    small = jnp.concatenate(
        [
            jnp.stack([gain_one_grad, gain_two_grad]).reshape(-1),
            jnp.stack([shift_one_grad, shift_two_grad]).reshape(-1),
            jnp.stack([attn_bias_grad, down_bias_grad]).reshape(-1),
            qv_bias_grad.reshape(-1),
            up_bias_grad,
        ]
    )
    qkv_part = (
        lax.psum_scatter(
            w_qkv_grad.reshape(D, 3 * width_here).astype(jnp.bfloat16),
            "dp",
            scatter_dimension=0,
            tiled=True,
        )
        .astype(jnp.float32)
        .reshape(-1, 3, width_here)
    )
    small_all = lax.all_gather(small, ("dp", "tensor"), axis=0, tiled=False)
    small_all = jnp.sum(small_all.reshape(dp_size, tensor_size, -1), axis=0)
    summed = jnp.sum(small_all[:, : 6 * D], axis=0)
    gains_grad = summed[: 2 * D].reshape(2, D)
    shifts_grad = summed[2 * D : 4 * D].reshape(2, D)
    outer_grad = summed[4 * D : 6 * D].reshape(2, D)
    qv_sum = (
        small_all[:, 6 * D : 6 * D + 2 * width_here]
        .reshape(tensor_size, 2, width_here)
        .transpose(1, 0, 2)
        .reshape(2, D)
    )
    up_sum = small_all[:, 6 * D + 2 * width_here :].reshape(FF)
    down_part = early_sum[:, :ff_here].T
    up_part = early_sum[:, ff_here : 2 * ff_here]
    out_part = early_sum[:, 2 * ff_here :].T
    return (
        result,
        input_grad,
        gains_grad,
        shifts_grad,
        qkv_part,
        qv_sum,
        out_part,
        outer_grad,
        up_part,
        up_sum,
        down_part,
    )


def solution(mesh):
    placed = (
        P(("dp", "tensor"), None),
        P("dp", None),
        P(),
        P(),
        P(None, None, "tensor"),
        P(None, "tensor"),
        P("tensor", None),
        P(),
        P(None, "tensor"),
        P("tensor"),
        P("tensor", None),
        P(("dp", "tensor"), None),
    )
    return jax.shard_map(
        functools.partial(on_device, mesh.shape["dp"]),
        mesh=mesh,
        in_specs=placed,
        out_specs=(
            P(("dp", "tensor"), None),
            P(("dp", "tensor"), None),
            P(),
            P(),
            P("dp", None, "tensor"),
            P(),
            P("tensor", "dp"),
            P(),
            P("dp", "tensor"),
            P(),
            P("tensor", "dp"),
        ),
        check_vma=False,
    )
```

```python
import functools

import jax
import jax.numpy as jnp
from jax import lax
from jax.experimental import pallas as pl
from jax.experimental.pallas import tpu as pltpu
from jax.sharding import PartitionSpec as P

D = 768
HEADS = 12
HEAD_DIM = 64
FF = 3072
SIDE_S = 12
SIDE_M = 15
SIDE_L = 20
TOK_DEV = 2048


EPSILON = 1e-06


def layout(group_counts):
    positions = jnp.arange(TOK_DEV, dtype=jnp.int32)
    area_small = SIDE_S * SIDE_S
    area_middle = SIDE_M * SIDE_M
    area_large = SIDE_L * SIDE_L
    end_small = group_counts[0] * area_small
    end_middle = end_small + group_counts[1] * area_middle
    end_large = end_middle + group_counts[2] * area_large
    size_class = (positions >= end_small).astype(jnp.int32) + (positions >= end_middle).astype(
        jnp.int32
    )
    begins = jnp.where(size_class == 0, 0, jnp.where(size_class == 1, end_small, end_middle))
    area_len = jnp.where(
        size_class == 0, area_small, jnp.where(size_class == 1, area_middle, area_large)
    )
    side_len = jnp.where(size_class == 0, SIDE_S, jnp.where(size_class == 1, SIDE_M, SIDE_L))
    within = positions - begins
    picture_index = within // area_len
    within_image = within % area_len
    is_valid = positions < end_large
    segment = jnp.where(is_valid, size_class * 16 + picture_index, 255)
    grid_row = (within_image // side_len).astype(jnp.float32)
    grid_col = (within_image % side_len).astype(jnp.float32)
    return (segment, grid_row, grid_col, is_valid.astype(jnp.float32))


def normalize(values, gain_row, shift_row):
    centred = values - jnp.mean(values, axis=-1, keepdims=True)
    spread = jnp.mean(centred * centred, axis=-1, keepdims=True)
    return centred * lax.rsqrt(spread + EPSILON) * gain_row + shift_row


def slopes_of(first_head, count_heads):
    head_number = (first_head + jnp.arange(count_heads, dtype=jnp.int32)).astype(jnp.float32) + 1.0
    return jnp.exp2(-8.0 * head_number / HEADS)


def distances(row_query, col_query, row_key, col_key):
    delta_row = row_query[:, None] - row_key[None, :]
    delta_col = col_query[:, None] - col_key[None, :]
    return jnp.sqrt(delta_row * delta_row + delta_col * delta_col)

Q_BLOCK = 256
K_BLOCK = 256
NEG = -1e30


def key_ranges(segment, tokens):
    starts = jnp.arange(0, tokens, Q_BLOCK)
    first = segment[starts]
    last = segment[starts + Q_BLOCK - 1]
    key_lo = jnp.sum(segment[None, :] < first[:, None], axis=1)
    key_hi = jnp.sum(segment[None, :] <= last[:, None], axis=1)
    return (key_lo // K_BLOCK).astype(jnp.int32), ((key_hi + K_BLOCK - 1) // K_BLOCK).astype(jnp.int32)


def block_geometry(qi_ref, ki_ref, start):
    rq = qi_ref[:, 0:1]
    cq = qi_ref[:, 1:2]
    sq = qi_ref[:, 2:3]
    rk = ki_ref[0:1, pl.ds(start, K_BLOCK)]
    ck = ki_ref[1:2, pl.ds(start, K_BLOCK)]
    sk = ki_ref[2:3, pl.ds(start, K_BLOCK)]
    dr = rq - rk
    dc = cq - ck
    return jnp.sqrt(dr * dr + dc * dc), sq == sk


def fwd_kernel(heads, scale, lo_ref, hi_ref, slope_ref, q_ref, k_ref, v_ref, qi_ref, ki_ref, o_ref, lse_ref):
    i = pl.program_id(0)
    queries = [q_ref[h] for h in range(heads)]
    width = q_ref.shape[2]

    def body(kb, carry):
        start = pl.multiple_of(kb * K_BLOCK, K_BLOCK)
        dist, allowed = block_geometry(qi_ref, ki_ref, start)
        out = []
        for h in range(heads):
            m_old, l_old, acc_old = carry[h]
            keys = k_ref[h, pl.ds(start, K_BLOCK), :]
            vals = v_ref[h, pl.ds(start, K_BLOCK), :]
            s = lax.dot_general(queries[h], keys, (((1,), (1,)), ((), ())),
                                preferred_element_type=jnp.float32) * scale - slope_ref[h] * dist
            s = jnp.where(allowed, s, NEG)
            m_new = jnp.maximum(m_old, jnp.max(s, axis=1, keepdims=True))
            alpha = jnp.exp(m_old - m_new)
            p = jnp.exp(s - m_new)
            l_new = alpha * l_old + jnp.sum(p, axis=1, keepdims=True)
            acc_new = alpha * acc_old + jnp.dot(p.astype(jnp.bfloat16), vals,
                                                preferred_element_type=jnp.float32)
            out.append((m_new, l_new, acc_new))
        return tuple(out)

    init = tuple(
        (jnp.full((Q_BLOCK, 1), NEG, jnp.float32), jnp.zeros((Q_BLOCK, 1), jnp.float32),
         jnp.zeros((Q_BLOCK, width), jnp.float32))
        for _ in range(heads)
    )
    final = lax.fori_loop(lo_ref[i], hi_ref[i], body, init)
    for h in range(heads):
        m, l, acc = final[h]
        o_ref[h] = acc / l
        lse_ref[h] = m + jnp.log(l)


def bwd_kernel(heads, scale, lo_ref, hi_ref, slope_ref, q_ref, k_ref, v_ref, qi_ref, ki_ref,
               o_ref, do_ref, lse_ref, dq_ref, dk_ref, dv_ref):
    i = pl.program_id(0)

    @pl.when(i == 0)
    def _():
        dk_ref[...] = jnp.zeros_like(dk_ref)
        dv_ref[...] = jnp.zeros_like(dv_ref)

    queries = [q_ref[h] for h in range(heads)]
    grads = [do_ref[h] for h in range(heads)]
    lses = [lse_ref[h] for h in range(heads)]
    deltas = [jnp.sum(grads[h].astype(jnp.float32) * o_ref[h], axis=1, keepdims=True)
              for h in range(heads)]
    width = q_ref.shape[2]

    def body(kb, carry):
        start = pl.multiple_of(kb * K_BLOCK, K_BLOCK)
        dist, allowed = block_geometry(qi_ref, ki_ref, start)
        out = []
        for h in range(heads):
            keys = k_ref[h, pl.ds(start, K_BLOCK), :]
            vals = v_ref[h, pl.ds(start, K_BLOCK), :]
            s = lax.dot_general(queries[h], keys, (((1,), (1,)), ((), ())),
                                preferred_element_type=jnp.float32) * scale - slope_ref[h] * dist
            p = jnp.where(allowed, jnp.exp(s - lses[h]), 0.0)
            dp = lax.dot_general(grads[h], vals, (((1,), (1,)), ((), ())),
                                 preferred_element_type=jnp.float32)
            ds = (p * (dp - deltas[h])).astype(jnp.bfloat16)
            out.append(carry[h] + jnp.dot(ds, keys, preferred_element_type=jnp.float32))
            dk_ref[h, pl.ds(start, K_BLOCK), :] += lax.dot_general(
                ds, queries[h], (((0,), (0,)), ((), ())), preferred_element_type=jnp.float32)
            dv_ref[h, pl.ds(start, K_BLOCK), :] += lax.dot_general(
                p.astype(jnp.bfloat16), grads[h], (((0,), (0,)), ((), ())),
                preferred_element_type=jnp.float32)
        return tuple(out)

    init = tuple(jnp.zeros((Q_BLOCK, width), jnp.float32) for _ in range(heads))
    final = lax.fori_loop(lo_ref[i], hi_ref[i], body, init)
    for h in range(heads):
        dq_ref[h] = final[h]


def attention_fwd(lo, hi, slopes, q, k, v, qinfo, kinfo, scale):
    heads, tokens, width = q.shape
    grid = (tokens // Q_BLOCK,)
    whole = lambda i, lo, hi: (0, 0, 0)
    rows = lambda i, lo, hi: (0, i, 0)
    return pl.pallas_call(
        functools.partial(fwd_kernel, heads, scale),
        grid_spec=pltpu.PrefetchScalarGridSpec(
            num_scalar_prefetch=2,
            grid=grid,
            in_specs=[
                pl.BlockSpec(memory_space=pltpu.SMEM),
                pl.BlockSpec((heads, Q_BLOCK, width), rows),
                pl.BlockSpec((heads, tokens, width), whole),
                pl.BlockSpec((heads, tokens, width), whole),
                pl.BlockSpec((Q_BLOCK, 3), lambda i, lo, hi: (i, 0)),
                pl.BlockSpec((3, tokens), lambda i, lo, hi: (0, 0)),
            ],
            out_specs=[
                pl.BlockSpec((heads, Q_BLOCK, width), rows),
                pl.BlockSpec((heads, Q_BLOCK, 1), rows),
            ],
        ),
        out_shape=[
            jax.ShapeDtypeStruct((heads, tokens, width), jnp.float32),
            jax.ShapeDtypeStruct((heads, tokens, 1), jnp.float32),
        ],
        compiler_params=pltpu.CompilerParams(dimension_semantics=("arbitrary",)),
    )(lo, hi, slopes, q, k, v, qinfo, kinfo)


def attention_bwd(lo, hi, slopes, q, k, v, qinfo, kinfo, o, do, lse, scale):
    heads, tokens, width = q.shape
    grid = (tokens // Q_BLOCK,)
    whole = lambda i, lo, hi: (0, 0, 0)
    rows = lambda i, lo, hi: (0, i, 0)
    return pl.pallas_call(
        functools.partial(bwd_kernel, heads, scale),
        grid_spec=pltpu.PrefetchScalarGridSpec(
            num_scalar_prefetch=2,
            grid=grid,
            in_specs=[
                pl.BlockSpec(memory_space=pltpu.SMEM),
                pl.BlockSpec((heads, Q_BLOCK, width), rows),
                pl.BlockSpec((heads, tokens, width), whole),
                pl.BlockSpec((heads, tokens, width), whole),
                pl.BlockSpec((Q_BLOCK, 3), lambda i, lo, hi: (i, 0)),
                pl.BlockSpec((3, tokens), lambda i, lo, hi: (0, 0)),
                pl.BlockSpec((heads, Q_BLOCK, width), rows),
                pl.BlockSpec((heads, Q_BLOCK, width), rows),
                pl.BlockSpec((heads, Q_BLOCK, 1), rows),
            ],
            out_specs=[
                pl.BlockSpec((heads, Q_BLOCK, width), rows),
                pl.BlockSpec((heads, tokens, width), whole),
                pl.BlockSpec((heads, tokens, width), whole),
            ],
        ),
        out_shape=[
            jax.ShapeDtypeStruct((heads, tokens, width), jnp.float32),
            jax.ShapeDtypeStruct((heads, tokens, width), jnp.float32),
            jax.ShapeDtypeStruct((heads, tokens, width), jnp.float32),
        ],
        compiler_params=pltpu.CompilerParams(dimension_semantics=("arbitrary",)),
    )(lo, hi, slopes, q, k, v, qinfo, kinfo, o, do, lse)


def scatter_tensor(partial, tensor_size):
    me = lax.axis_index("tensor")
    blocks = partial.reshape(tensor_size, -1, partial.shape[1])
    total = lax.dynamic_index_in_dim(blocks, me, keepdims=False).astype(jnp.float32)
    for shift in range(1, tensor_size):
        outgoing = lax.dynamic_index_in_dim(blocks, (me + shift) % tensor_size, keepdims=False)
        pairs = [(i, (i + shift) % tensor_size) for i in range(tensor_size)]
        total = total + lax.ppermute(outgoing.astype(jnp.bfloat16), "tensor", pairs).astype(
            jnp.float32
        )
    return total


def halving_scatter(blocks, axis_name):
    me = lax.axis_index(axis_name)
    bit = 0
    while blocks.shape[0] > 1:
        pairs = [(i, i ^ (1 << bit)) for i in range(blocks.shape[0] << bit)]
        halves = blocks.reshape((blocks.shape[0] // 2, 2) + blocks.shape[1:])
        mine = (me >> bit) & 1
        keep = lax.dynamic_index_in_dim(halves, mine, axis=1, keepdims=False)
        send = lax.dynamic_index_in_dim(halves, 1 - mine, axis=1, keepdims=False)
        blocks = keep + lax.ppermute(send, axis_name, pairs)
        bit += 1
    return blocks[0]


def doubling_sum(values, axis_name, size):
    bit = 0
    while (1 << bit) < size:
        pairs = [(i, i ^ (1 << bit)) for i in range(size)]
        values = values + lax.ppermute(values, axis_name, pairs)
        bit += 1
    return values


def scatter_rows(parts, dp_size):
    width = parts.shape[1]
    padded = -(-width // 2048) * 2048
    parts = jnp.pad(parts, ((0, 0), (0, padded - width))).reshape(dp_size * padded // 128, 128)
    summed = lax.psum_scatter(parts, "dp", scatter_dimension=0, tiled=True)
    return summed.reshape(-1)[:width]


def on_device(
    dp_size,
    patches,
    counts,
    norm_gain,
    norm_bias,
    w_qkv,
    b_qv,
    w_out,
    out_bias,
    w_up,
    b_up,
    w_down,
    cotangent,
):
    local_rows = patches.shape[0]
    width_here = w_qkv.shape[2]
    heads_here = width_here // HEAD_DIM
    ff_here = w_up.shape[1]
    tensor_pos = lax.axis_index("tensor")
    tensor_size = D // width_here
    score_scale = HEAD_DIM ** (-0.5)
    segment, grid_row, grid_col, is_valid = layout(counts[0])
    keep_rows = lax.dynamic_slice_in_dim(is_valid, tensor_pos * local_rows, local_rows)[:, None]
    slopes = slopes_of(tensor_pos * heads_here, heads_here)
    inputs = patches.astype(jnp.float32)
    inputs_all = lax.all_gather(patches, "tensor", axis=0, tiled=True).astype(jnp.float32)
    normed = normalize(inputs_all, norm_gain[0], norm_bias[0]).astype(jnp.bfloat16)
    projected = jnp.einsum("td,dsc->tsc", normed, w_qkv, preferred_element_type=jnp.float32)
    queries = (projected[:, 0] + b_qv[0]).astype(jnp.bfloat16)
    keys = projected[:, 1].astype(jnp.bfloat16)
    values = (projected[:, 2] + b_qv[1]).astype(jnp.bfloat16)

    def head_major(rows):
        return rows.reshape(TOK_DEV, heads_here, HEAD_DIM).transpose(1, 0, 2)

    def row_major(heads):
        return heads.transpose(1, 0, 2).reshape(TOK_DEV, width_here)

    key_lo, key_hi = key_ranges(segment, TOK_DEV)
    segment_f = segment.astype(jnp.float32)
    query_info = jnp.stack([grid_row, grid_col, segment_f], axis=1)
    key_info = jnp.stack([grid_row, grid_col, segment_f], axis=0)
    query_heads = head_major(queries)
    key_heads = head_major(keys)
    value_heads = head_major(values)
    mixed_f32, log_totals = attention_fwd(
        key_lo, key_hi, slopes, query_heads, key_heads, value_heads, query_info, key_info, score_scale
    )
    upstream = cotangent.astype(jnp.float32)
    branch_grad = lax.all_gather(
        (keep_rows * upstream).astype(jnp.bfloat16), "tensor", axis=0, tiled=True
    )
    mixed_f32, log_totals, branch_grad = lax.optimization_barrier(
        (mixed_f32, log_totals, branch_grad)
    )
    mixed_rows = row_major(mixed_f32).astype(jnp.bfloat16)
    mixed_all = lax.all_gather(mixed_rows, "tensor", axis=1, tiled=True)
    w_out_all = lax.all_gather(w_out, "tensor", axis=0, tiled=True)
    attended = jnp.dot(mixed_all, w_out_all, preferred_element_type=jnp.float32)
    after_attn_all = inputs_all + is_valid[:, None] * (attended + out_bias[0])
    after_attn = lax.dynamic_slice_in_dim(after_attn_all, tensor_pos * local_rows, local_rows)
    normed_two = normalize(after_attn_all, norm_gain[1], norm_bias[1]).astype(jnp.bfloat16)
    hidden_pre = jnp.dot(normed_two, w_up, preferred_element_type=jnp.float32) + b_up
    hidden = jax.nn.gelu(hidden_pre, approximate=False).astype(jnp.bfloat16)
    branch_partial = jnp.dot(hidden, w_down, preferred_element_type=jnp.float32)
    down_bias_grad = jnp.sum(keep_rows * upstream, axis=0)
    w_down_grad_t = jnp.einsum(
        "td,tf->df", branch_grad, hidden, preferred_element_type=jnp.float32
    )
    hidden_grad = jnp.einsum("td,fd->tf", branch_grad, w_down, preferred_element_type=jnp.float32)
    _, gelu_back = jax.vjp(lambda pre_act: jax.nn.gelu(pre_act, approximate=False), hidden_pre)
    pre_grad = gelu_back(hidden_grad)[0].astype(jnp.bfloat16)
    up_bias_grad = jnp.sum(pre_grad, axis=0, dtype=jnp.float32)
    w_up_grad = jnp.einsum("td,tf->df", normed_two, pre_grad, preferred_element_type=jnp.float32)
    normed_two_grad = lax.psum_scatter(
        jnp.einsum("tf,df->td", pre_grad, w_up, preferred_element_type=jnp.float32).astype(
            jnp.bfloat16
        ),
        "tensor",
        scatter_dimension=0,
        tiled=True,
    ).astype(jnp.float32)
    _, norm_two_back = jax.vjp(normalize, after_attn, norm_gain[1], norm_bias[1])
    through_two, gain_two_grad, shift_two_grad = norm_two_back(normed_two_grad)
    after_grad = upstream + through_two
    attn_bias_grad = jnp.sum(keep_rows * after_grad, axis=0)
    attn_local = (keep_rows * after_grad).astype(jnp.bfloat16)
    attn_grad = lax.all_gather(attn_local, "tensor", axis=0, tiled=True)
    w_out_grad_t = jnp.einsum(
        "td,tc->dc", attn_grad, mixed_rows, preferred_element_type=jnp.float32
    )
    mixed_grad = jnp.einsum(
        "td,cd->tc", attn_grad, w_out, preferred_element_type=jnp.float32
    ).astype(jnp.bfloat16)
    early_parts = jnp.concatenate([w_down_grad_t, w_up_grad, w_out_grad_t], axis=1).astype(
        jnp.bfloat16
    )
    early_parts, mixed_grad, branch_partial = lax.optimization_barrier(
        (early_parts, mixed_grad, branch_partial)
    )
    branch = scatter_tensor(branch_partial, tensor_size)
    result = (after_attn + keep_rows * (branch + out_bias[1])).astype(jnp.bfloat16)
    early_sum = lax.psum_scatter(early_parts, "dp", scatter_dimension=0, tiled=True).astype(
        jnp.float32
    )
    query_acc, key_acc, value_acc = attention_bwd(
        key_lo, key_hi, slopes, query_heads, key_heads, value_heads, query_info, key_info,
        mixed_f32, head_major(mixed_grad), log_totals, score_scale,
    )
    query_acc, key_acc, value_acc, early_sum, result = lax.optimization_barrier(
        (query_acc, key_acc, value_acc, early_sum, result)
    )
    query_grad = row_major(query_acc * score_scale).astype(jnp.bfloat16)
    key_grad = row_major(key_acc * score_scale).astype(jnp.bfloat16)
    value_grad = row_major(value_acc).astype(jnp.bfloat16)
    projected_grad = jnp.stack([query_grad, key_grad, value_grad], axis=1)
    qv_bias_grad = jnp.stack(
        [
            jnp.sum(query_grad, axis=0, dtype=jnp.float32),
            jnp.sum(value_grad, axis=0, dtype=jnp.float32),
        ]
    )
    w_qkv_grad = jnp.einsum(
        "td,tsc->dsc", normed, projected_grad, preferred_element_type=jnp.float32
    )
    normed_grad_partial = jnp.einsum(
        "tsc,dsc->td", projected_grad, w_qkv, preferred_element_type=jnp.float32
    )
    centred_all = inputs_all - jnp.mean(inputs_all, axis=-1, keepdims=True)
    unit_all = centred_all * lax.rsqrt(
        jnp.mean(centred_all * centred_all, axis=-1, keepdims=True) + EPSILON
    )
    gain_one_grad = jnp.sum(normed_grad_partial * unit_all, axis=0)
    shift_one_grad = jnp.sum(normed_grad_partial, axis=0)
    normed_grad = scatter_tensor(normed_grad_partial, tensor_size)
    _, norm_one_back = jax.vjp(normalize, inputs, norm_gain[0], norm_bias[0])
    through_one = norm_one_back(normed_grad)[0]
    input_grad = (after_grad + through_one).astype(jnp.bfloat16)
    qv_full = lax.dynamic_update_slice_in_dim(
        jnp.zeros((2, D), jnp.float32), qv_bias_grad, tensor_pos * width_here, 1
    )
    up_full = lax.dynamic_update_slice_in_dim(
        jnp.zeros((FF,), jnp.float32), up_bias_grad, tensor_pos * ff_here, 0
    )
    small = jnp.concatenate(
        [
            jnp.stack([gain_one_grad, gain_two_grad]).reshape(-1),
            jnp.stack([shift_one_grad, shift_two_grad]).reshape(-1),
            jnp.stack([attn_bias_grad, down_bias_grad]).reshape(-1),
            qv_full.reshape(-1),
            up_full,
        ]
    )
    late_blocks = jnp.concatenate(
        [
            w_qkv_grad.reshape(dp_size, -1),
            jnp.broadcast_to(small, (dp_size,) + small.shape),
        ],
        axis=1,
    )
    late_sum = halving_scatter(late_blocks, "dp")
    qkv_size = w_qkv_grad.size // dp_size
    qkv_part = late_sum[:qkv_size].reshape(-1, 3, width_here)
    summed = doubling_sum(late_sum[qkv_size:], "tensor", tensor_size)
    gains_grad = summed[: 2 * D].reshape(2, D)
    shifts_grad = summed[2 * D : 4 * D].reshape(2, D)
    outer_grad = summed[4 * D : 6 * D].reshape(2, D)
    qv_sum = summed[6 * D : 8 * D].reshape(2, D)
    up_sum = summed[8 * D :]
    down_part = early_sum[:, :ff_here].T
    up_part = early_sum[:, ff_here : 2 * ff_here]
    out_part = early_sum[:, 2 * ff_here :].T
    return (
        result,
        input_grad,
        gains_grad,
        shifts_grad,
        qkv_part,
        qv_sum,
        out_part,
        outer_grad,
        up_part,
        up_sum,
        down_part,
    )


def solution(mesh):
    placed = (
        P(("dp", "tensor"), None),
        P("dp", None),
        P(),
        P(),
        P(None, None, "tensor"),
        P(None, "tensor"),
        P("tensor", None),
        P(),
        P(None, "tensor"),
        P("tensor"),
        P("tensor", None),
        P(("dp", "tensor"), None),
    )
    return jax.shard_map(
        functools.partial(on_device, mesh.shape["dp"]),
        mesh=mesh,
        in_specs=placed,
        out_specs=(
            P(("dp", "tensor"), None),
            P(("dp", "tensor"), None),
            P(),
            P(),
            P("dp", None, "tensor"),
            P(),
            P("tensor", "dp"),
            P(),
            P("dp", "tensor"),
            P(),
            P("tensor", "dp"),
        ),
        check_vma=False,
    )
```

```python
import functools

import jax
import jax.numpy as jnp
from jax import lax
from jax.experimental import pallas as pl
from jax.experimental.pallas import tpu as pltpu
from jax.sharding import PartitionSpec as P

D = 768
HEADS = 12
HEAD_DIM = 64
FF = 3072
SIDE_S = 12
SIDE_M = 15
SIDE_L = 20
TOK_DEV = 2048


EPSILON = 1e-06


def layout(group_counts):
    positions = jnp.arange(TOK_DEV, dtype=jnp.int32)
    area_small = SIDE_S * SIDE_S
    area_middle = SIDE_M * SIDE_M
    area_large = SIDE_L * SIDE_L
    end_small = group_counts[0] * area_small
    end_middle = end_small + group_counts[1] * area_middle
    end_large = end_middle + group_counts[2] * area_large
    size_class = (positions >= end_small).astype(jnp.int32) + (positions >= end_middle).astype(
        jnp.int32
    )
    begins = jnp.where(size_class == 0, 0, jnp.where(size_class == 1, end_small, end_middle))
    area_len = jnp.where(
        size_class == 0, area_small, jnp.where(size_class == 1, area_middle, area_large)
    )
    side_len = jnp.where(size_class == 0, SIDE_S, jnp.where(size_class == 1, SIDE_M, SIDE_L))
    within = positions - begins
    picture_index = within // area_len
    within_image = within % area_len
    is_valid = positions < end_large
    segment = jnp.where(is_valid, size_class * 16 + picture_index, 255)
    grid_row = (within_image // side_len).astype(jnp.float32)
    grid_col = (within_image % side_len).astype(jnp.float32)
    return (segment, grid_row, grid_col, is_valid.astype(jnp.float32))


def normalize(values, gain_row, shift_row):
    centred = values - jnp.mean(values, axis=-1, keepdims=True)
    spread = jnp.mean(centred * centred, axis=-1, keepdims=True)
    return centred * lax.rsqrt(spread + EPSILON) * gain_row + shift_row


def slopes_of(first_head, count_heads):
    head_number = (first_head + jnp.arange(count_heads, dtype=jnp.int32)).astype(jnp.float32) + 1.0
    return jnp.exp2(-8.0 * head_number / HEADS)


def distances(row_query, col_query, row_key, col_key):
    delta_row = row_query[:, None] - row_key[None, :]
    delta_col = col_query[:, None] - col_key[None, :]
    return jnp.sqrt(delta_row * delta_row + delta_col * delta_col)

Q_BLOCK = 256
K_BLOCK = 256
NEG = -1e30


def key_ranges(segment, tokens):
    starts = jnp.arange(0, tokens, Q_BLOCK)
    first = segment[starts]
    last = segment[starts + Q_BLOCK - 1]
    key_lo = jnp.sum(segment[None, :] < first[:, None], axis=1)
    key_hi = jnp.sum(segment[None, :] <= last[:, None], axis=1)
    return (key_lo // K_BLOCK).astype(jnp.int32), ((key_hi + K_BLOCK - 1) // K_BLOCK).astype(jnp.int32)


def block_geometry(qi_ref, ki_ref, start):
    rq = qi_ref[:, 0:1]
    cq = qi_ref[:, 1:2]
    sq = qi_ref[:, 2:3]
    rk = ki_ref[0:1, pl.ds(start, K_BLOCK)]
    ck = ki_ref[1:2, pl.ds(start, K_BLOCK)]
    sk = ki_ref[2:3, pl.ds(start, K_BLOCK)]
    dr = rq - rk
    dc = cq - ck
    return jnp.sqrt(dr * dr + dc * dc), sq == sk


def fwd_kernel(heads, scale, lo_ref, hi_ref, slope_ref, q_ref, k_ref, v_ref, qi_ref, ki_ref, o_ref, lse_ref):
    i = pl.program_id(0)
    queries = [q_ref[h] for h in range(heads)]
    width = q_ref.shape[2]

    def body(kb, carry):
        start = pl.multiple_of(kb * K_BLOCK, K_BLOCK)
        dist, allowed = block_geometry(qi_ref, ki_ref, start)
        out = []
        for h in range(heads):
            m_old, l_old, acc_old = carry[h]
            keys = k_ref[h, pl.ds(start, K_BLOCK), :]
            vals = v_ref[h, pl.ds(start, K_BLOCK), :]
            s = lax.dot_general(queries[h], keys, (((1,), (1,)), ((), ())),
                                preferred_element_type=jnp.float32) * scale - slope_ref[h] * dist
            s = jnp.where(allowed, s, NEG)
            m_new = jnp.maximum(m_old, jnp.max(s, axis=1, keepdims=True))
            alpha = jnp.exp(m_old - m_new)
            p = jnp.exp(s - m_new)
            l_new = alpha * l_old + jnp.sum(p, axis=1, keepdims=True)
            acc_new = alpha * acc_old + jnp.dot(p.astype(jnp.bfloat16), vals,
                                                preferred_element_type=jnp.float32)
            out.append((m_new, l_new, acc_new))
        return tuple(out)

    init = tuple(
        (jnp.full((Q_BLOCK, 1), NEG, jnp.float32), jnp.zeros((Q_BLOCK, 1), jnp.float32),
         jnp.zeros((Q_BLOCK, width), jnp.float32))
        for _ in range(heads)
    )
    final = lax.fori_loop(lo_ref[i], hi_ref[i], body, init)
    for h in range(heads):
        m, l, acc = final[h]
        o_ref[h] = acc / l
        lse_ref[h] = m + jnp.log(l)


def bwd_kernel(heads, scale, lo_ref, hi_ref, slope_ref, q_ref, k_ref, v_ref, qi_ref, ki_ref,
               o_ref, do_ref, lse_ref, dq_ref, dk_ref, dv_ref):
    i = pl.program_id(0)

    @pl.when(i == 0)
    def _():
        dk_ref[...] = jnp.zeros_like(dk_ref)
        dv_ref[...] = jnp.zeros_like(dv_ref)

    queries = [q_ref[h] for h in range(heads)]
    grads = [do_ref[h] for h in range(heads)]
    lses = [lse_ref[h] for h in range(heads)]
    deltas = [jnp.sum(grads[h].astype(jnp.float32) * o_ref[h], axis=1, keepdims=True)
              for h in range(heads)]
    width = q_ref.shape[2]

    def body(kb, carry):
        start = pl.multiple_of(kb * K_BLOCK, K_BLOCK)
        dist, allowed = block_geometry(qi_ref, ki_ref, start)
        out = []
        for h in range(heads):
            keys = k_ref[h, pl.ds(start, K_BLOCK), :]
            vals = v_ref[h, pl.ds(start, K_BLOCK), :]
            s = lax.dot_general(queries[h], keys, (((1,), (1,)), ((), ())),
                                preferred_element_type=jnp.float32) * scale - slope_ref[h] * dist
            p = jnp.where(allowed, jnp.exp(s - lses[h]), 0.0)
            dp = lax.dot_general(grads[h], vals, (((1,), (1,)), ((), ())),
                                 preferred_element_type=jnp.float32)
            ds = (p * (dp - deltas[h])).astype(jnp.bfloat16)
            out.append(carry[h] + jnp.dot(ds, keys, preferred_element_type=jnp.float32))
            dk_ref[h, pl.ds(start, K_BLOCK), :] += lax.dot_general(
                ds, queries[h], (((0,), (0,)), ((), ())), preferred_element_type=jnp.float32)
            dv_ref[h, pl.ds(start, K_BLOCK), :] += lax.dot_general(
                p.astype(jnp.bfloat16), grads[h], (((0,), (0,)), ((), ())),
                preferred_element_type=jnp.float32)
        return tuple(out)

    init = tuple(jnp.zeros((Q_BLOCK, width), jnp.float32) for _ in range(heads))
    final = lax.fori_loop(lo_ref[i], hi_ref[i], body, init)
    for h in range(heads):
        dq_ref[h] = final[h]


def attention_fwd(lo, hi, slopes, q, k, v, qinfo, kinfo, scale):
    heads, tokens, width = q.shape
    grid = (tokens // Q_BLOCK,)
    whole = lambda i, lo, hi: (0, 0, 0)
    rows = lambda i, lo, hi: (0, i, 0)
    return pl.pallas_call(
        functools.partial(fwd_kernel, heads, scale),
        grid_spec=pltpu.PrefetchScalarGridSpec(
            num_scalar_prefetch=2,
            grid=grid,
            in_specs=[
                pl.BlockSpec(memory_space=pltpu.SMEM),
                pl.BlockSpec((heads, Q_BLOCK, width), rows),
                pl.BlockSpec((heads, tokens, width), whole),
                pl.BlockSpec((heads, tokens, width), whole),
                pl.BlockSpec((Q_BLOCK, 3), lambda i, lo, hi: (i, 0)),
                pl.BlockSpec((3, tokens), lambda i, lo, hi: (0, 0)),
            ],
            out_specs=[
                pl.BlockSpec((heads, Q_BLOCK, width), rows),
                pl.BlockSpec((heads, Q_BLOCK, 1), rows),
            ],
        ),
        out_shape=[
            jax.ShapeDtypeStruct((heads, tokens, width), jnp.float32),
            jax.ShapeDtypeStruct((heads, tokens, 1), jnp.float32),
        ],
        compiler_params=pltpu.CompilerParams(dimension_semantics=("arbitrary",)),
    )(lo, hi, slopes, q, k, v, qinfo, kinfo)


def attention_bwd(lo, hi, slopes, q, k, v, qinfo, kinfo, o, do, lse, scale):
    heads, tokens, width = q.shape
    grid = (tokens // Q_BLOCK,)
    whole = lambda i, lo, hi: (0, 0, 0)
    rows = lambda i, lo, hi: (0, i, 0)
    return pl.pallas_call(
        functools.partial(bwd_kernel, heads, scale),
        grid_spec=pltpu.PrefetchScalarGridSpec(
            num_scalar_prefetch=2,
            grid=grid,
            in_specs=[
                pl.BlockSpec(memory_space=pltpu.SMEM),
                pl.BlockSpec((heads, Q_BLOCK, width), rows),
                pl.BlockSpec((heads, tokens, width), whole),
                pl.BlockSpec((heads, tokens, width), whole),
                pl.BlockSpec((Q_BLOCK, 3), lambda i, lo, hi: (i, 0)),
                pl.BlockSpec((3, tokens), lambda i, lo, hi: (0, 0)),
                pl.BlockSpec((heads, Q_BLOCK, width), rows),
                pl.BlockSpec((heads, Q_BLOCK, width), rows),
                pl.BlockSpec((heads, Q_BLOCK, 1), rows),
            ],
            out_specs=[
                pl.BlockSpec((heads, Q_BLOCK, width), rows),
                pl.BlockSpec((heads, tokens, width), whole),
                pl.BlockSpec((heads, tokens, width), whole),
            ],
        ),
        out_shape=[
            jax.ShapeDtypeStruct((heads, tokens, width), jnp.float32),
            jax.ShapeDtypeStruct((heads, tokens, width), jnp.float32),
            jax.ShapeDtypeStruct((heads, tokens, width), jnp.float32),
        ],
        compiler_params=pltpu.CompilerParams(dimension_semantics=("arbitrary",)),
    )(lo, hi, slopes, q, k, v, qinfo, kinfo, o, do, lse)


def scatter_tensor(partial, tensor_size):
    me = lax.axis_index("tensor")
    blocks = partial.reshape(tensor_size, -1, partial.shape[1])
    total = lax.dynamic_index_in_dim(blocks, me, keepdims=False).astype(jnp.float32)
    for shift in range(1, tensor_size):
        outgoing = lax.dynamic_index_in_dim(blocks, (me + shift) % tensor_size, keepdims=False)
        pairs = [(i, (i + shift) % tensor_size) for i in range(tensor_size)]
        total = total + lax.ppermute(outgoing.astype(jnp.bfloat16), "tensor", pairs).astype(
            jnp.float32
        )
    return total


def halving_scatter(blocks, axis_name):
    me = lax.axis_index(axis_name)
    bit = 0
    while blocks.shape[0] > 1:
        pairs = [(i, i ^ (1 << bit)) for i in range(blocks.shape[0] << bit)]
        halves = blocks.reshape((blocks.shape[0] // 2, 2) + blocks.shape[1:])
        mine = (me >> bit) & 1
        keep = lax.dynamic_index_in_dim(halves, mine, axis=1, keepdims=False)
        send = lax.dynamic_index_in_dim(halves, 1 - mine, axis=1, keepdims=False)
        blocks = keep + lax.ppermute(send, axis_name, pairs)
        bit += 1
    return blocks[0]


def doubling_sum(values, axis_name, size):
    bit = 0
    while (1 << bit) < size:
        pairs = [(i, i ^ (1 << bit)) for i in range(size)]
        values = values + lax.ppermute(values, axis_name, pairs)
        bit += 1
    return values


def scatter_rows(parts, dp_size):
    width = parts.shape[1]
    padded = -(-width // 2048) * 2048
    parts = jnp.pad(parts, ((0, 0), (0, padded - width))).reshape(dp_size * padded // 128, 128)
    summed = lax.psum_scatter(parts, "dp", scatter_dimension=0, tiled=True)
    return summed.reshape(-1)[:width]


def on_device(
    dp_size,
    patches,
    counts,
    norm_gain,
    norm_bias,
    w_qkv,
    b_qv,
    w_out,
    out_bias,
    w_up,
    b_up,
    w_down,
    cotangent,
):
    local_rows = patches.shape[0]
    width_here = w_qkv.shape[2]
    heads_here = width_here // HEAD_DIM
    ff_here = w_up.shape[1]
    tensor_pos = lax.axis_index("tensor")
    tensor_size = D // width_here
    score_scale = HEAD_DIM ** (-0.5)
    segment, grid_row, grid_col, is_valid = layout(counts[0])
    keep_rows = lax.dynamic_slice_in_dim(is_valid, tensor_pos * local_rows, local_rows)[:, None]
    slopes = slopes_of(tensor_pos * heads_here, heads_here)
    inputs = patches.astype(jnp.float32)
    inputs_all = lax.all_gather(patches, "tensor", axis=0, tiled=True).astype(jnp.float32)
    normed = normalize(inputs_all, norm_gain[0], norm_bias[0]).astype(jnp.bfloat16)
    projected = jnp.einsum("td,dsc->tsc", normed, w_qkv, preferred_element_type=jnp.float32)
    queries = (projected[:, 0] + b_qv[0]).astype(jnp.bfloat16)
    keys = projected[:, 1].astype(jnp.bfloat16)
    values = (projected[:, 2] + b_qv[1]).astype(jnp.bfloat16)

    def head_major(rows):
        return rows.reshape(TOK_DEV, heads_here, HEAD_DIM).transpose(1, 0, 2)

    def row_major(heads):
        return heads.transpose(1, 0, 2).reshape(TOK_DEV, width_here)

    key_lo, key_hi = key_ranges(segment, TOK_DEV)
    segment_f = segment.astype(jnp.float32)
    query_info = jnp.stack([grid_row, grid_col, segment_f], axis=1)
    key_info = jnp.stack([grid_row, grid_col, segment_f], axis=0)
    query_heads = head_major(queries)
    key_heads = head_major(keys)
    value_heads = head_major(values)
    mixed_f32, log_totals = attention_fwd(
        key_lo, key_hi, slopes, query_heads, key_heads, value_heads, query_info, key_info, score_scale
    )
    upstream = cotangent.astype(jnp.float32)
    branch_grad = lax.all_gather(
        (keep_rows * upstream).astype(jnp.bfloat16), "tensor", axis=0, tiled=True
    )
    mixed_f32, log_totals, branch_grad = lax.optimization_barrier(
        (mixed_f32, log_totals, branch_grad)
    )
    mixed_rows = row_major(mixed_f32).astype(jnp.bfloat16)
    mixed_all = lax.all_gather(mixed_rows, "tensor", axis=1, tiled=True)
    w_out_all = lax.all_gather(w_out, "tensor", axis=0, tiled=True)
    attended = jnp.dot(mixed_all, w_out_all, preferred_element_type=jnp.float32)
    after_attn_all = inputs_all + is_valid[:, None] * (attended + out_bias[0])
    after_attn = lax.dynamic_slice_in_dim(after_attn_all, tensor_pos * local_rows, local_rows)
    normed_two = normalize(after_attn_all, norm_gain[1], norm_bias[1]).astype(jnp.bfloat16)
    hidden_pre = jnp.dot(normed_two, w_up, preferred_element_type=jnp.float32) + b_up
    hidden = jax.nn.gelu(hidden_pre, approximate=False).astype(jnp.bfloat16)
    branch_partial = jnp.dot(hidden, w_down, preferred_element_type=jnp.float32)
    down_bias_grad = jnp.sum(keep_rows * upstream, axis=0)
    w_down_grad_t = jnp.einsum(
        "td,tf->df", branch_grad, hidden, preferred_element_type=jnp.float32
    )
    hidden_grad = jnp.einsum("td,fd->tf", branch_grad, w_down, preferred_element_type=jnp.float32)
    _, gelu_back = jax.vjp(lambda pre_act: jax.nn.gelu(pre_act, approximate=False), hidden_pre)
    pre_grad = gelu_back(hidden_grad)[0].astype(jnp.bfloat16)
    up_bias_grad = jnp.sum(pre_grad, axis=0, dtype=jnp.float32)
    w_up_grad = jnp.einsum("td,tf->df", normed_two, pre_grad, preferred_element_type=jnp.float32)
    normed_two_grad = lax.psum_scatter(
        jnp.einsum("tf,df->td", pre_grad, w_up, preferred_element_type=jnp.float32).astype(
            jnp.bfloat16
        ),
        "tensor",
        scatter_dimension=0,
        tiled=True,
    ).astype(jnp.float32)
    _, norm_two_back = jax.vjp(normalize, after_attn, norm_gain[1], norm_bias[1])
    through_two, gain_two_grad, shift_two_grad = norm_two_back(normed_two_grad)
    after_grad = upstream + through_two
    attn_bias_grad = jnp.sum(keep_rows * after_grad, axis=0)
    attn_local = (keep_rows * after_grad).astype(jnp.bfloat16)
    attn_grad = lax.all_gather(attn_local, "tensor", axis=0, tiled=True)
    w_out_grad_t = jnp.einsum(
        "td,tc->dc", attn_grad, mixed_rows, preferred_element_type=jnp.float32
    )
    mixed_grad = jnp.einsum(
        "td,cd->tc", attn_grad, w_out, preferred_element_type=jnp.float32
    ).astype(jnp.bfloat16)
    early_parts = jnp.concatenate([w_down_grad_t, w_up_grad, w_out_grad_t], axis=1).astype(
        jnp.bfloat16
    )
    early_parts, mixed_grad, branch_partial = lax.optimization_barrier(
        (early_parts, mixed_grad, branch_partial)
    )
    branch = scatter_tensor(branch_partial, tensor_size)
    result = (after_attn + keep_rows * (branch + out_bias[1])).astype(jnp.bfloat16)
    early_sum = lax.psum_scatter(early_parts, "dp", scatter_dimension=0, tiled=True).astype(
        jnp.float32
    )
    query_acc, key_acc, value_acc = attention_bwd(
        key_lo, key_hi, slopes, query_heads, key_heads, value_heads, query_info, key_info,
        mixed_f32, head_major(mixed_grad), log_totals, score_scale,
    )
    query_acc, key_acc, value_acc, early_sum, result = lax.optimization_barrier(
        (query_acc, key_acc, value_acc, early_sum, result)
    )
    query_grad = row_major(query_acc * score_scale).astype(jnp.bfloat16)
    key_grad = row_major(key_acc * score_scale).astype(jnp.bfloat16)
    value_grad = row_major(value_acc).astype(jnp.bfloat16)
    projected_grad = jnp.concatenate([query_grad, key_grad, value_grad], axis=1)
    qv_bias_grad = jnp.stack(
        [
            jnp.sum(query_grad, axis=0, dtype=jnp.float32),
            jnp.sum(value_grad, axis=0, dtype=jnp.float32),
        ]
    )
    w_qkv_grad = jnp.einsum(
        "td,tc->dc", normed, projected_grad, preferred_element_type=jnp.float32
    )
    normed_grad_partial = jnp.einsum(
        "tc,dc->td",
        projected_grad,
        w_qkv.reshape(D, 3 * width_here),
        preferred_element_type=jnp.float32,
    )
    centred_all = inputs_all - jnp.mean(inputs_all, axis=-1, keepdims=True)
    unit_all = centred_all * lax.rsqrt(
        jnp.mean(centred_all * centred_all, axis=-1, keepdims=True) + EPSILON
    )
    gain_one_grad = jnp.sum(normed_grad_partial * unit_all, axis=0)
    shift_one_grad = jnp.sum(normed_grad_partial, axis=0)
    normed_grad = scatter_tensor(normed_grad_partial, tensor_size)
    _, norm_one_back = jax.vjp(normalize, inputs, norm_gain[0], norm_bias[0])
    through_one = norm_one_back(normed_grad)[0]
    input_grad = (after_grad + through_one).astype(jnp.bfloat16)
    qv_full = lax.dynamic_update_slice_in_dim(
        jnp.zeros((2, D), jnp.float32), qv_bias_grad, tensor_pos * width_here, 1
    )
    up_full = lax.dynamic_update_slice_in_dim(
        jnp.zeros((FF,), jnp.float32), up_bias_grad, tensor_pos * ff_here, 0
    )
    small = jnp.concatenate(
        [
            jnp.stack([gain_one_grad, gain_two_grad]).reshape(-1),
            jnp.stack([shift_one_grad, shift_two_grad]).reshape(-1),
            jnp.stack([attn_bias_grad, down_bias_grad]).reshape(-1),
            qv_full.reshape(-1),
            up_full,
        ]
    )
    late_blocks = jnp.concatenate(
        [
            w_qkv_grad.reshape(dp_size, -1),
            jnp.broadcast_to(small, (dp_size,) + small.shape),
        ],
        axis=1,
    )
    late_sum = halving_scatter(late_blocks, "dp")
    qkv_size = w_qkv_grad.size // dp_size
    qkv_part = late_sum[:qkv_size].reshape(-1, 3, width_here)
    summed = doubling_sum(late_sum[qkv_size:], "tensor", tensor_size)
    gains_grad = summed[: 2 * D].reshape(2, D)
    shifts_grad = summed[2 * D : 4 * D].reshape(2, D)
    outer_grad = summed[4 * D : 6 * D].reshape(2, D)
    qv_sum = summed[6 * D : 8 * D].reshape(2, D)
    up_sum = summed[8 * D :]
    down_part = early_sum[:, :ff_here].T
    up_part = early_sum[:, ff_here : 2 * ff_here]
    out_part = early_sum[:, 2 * ff_here :].T
    return (
        result,
        input_grad,
        gains_grad,
        shifts_grad,
        qkv_part,
        qv_sum,
        out_part,
        outer_grad,
        up_part,
        up_sum,
        down_part,
    )


def solution(mesh):
    placed = (
        P(("dp", "tensor"), None),
        P("dp", None),
        P(),
        P(),
        P(None, None, "tensor"),
        P(None, "tensor"),
        P("tensor", None),
        P(),
        P(None, "tensor"),
        P("tensor"),
        P("tensor", None),
        P(("dp", "tensor"), None),
    )
    return jax.shard_map(
        functools.partial(on_device, mesh.shape["dp"]),
        mesh=mesh,
        in_specs=placed,
        out_specs=(
            P(("dp", "tensor"), None),
            P(("dp", "tensor"), None),
            P(),
            P(),
            P("dp", None, "tensor"),
            P(),
            P("tensor", "dp"),
            P(),
            P("dp", "tensor"),
            P(),
            P("tensor", "dp"),
        ),
        check_vma=False,
    )
```

```python
import functools

import jax
import jax.numpy as jnp
from jax import lax
from jax.experimental import pallas as pl
from jax.experimental.pallas import tpu as pltpu
from jax.sharding import PartitionSpec as P


D = 768
HEADS = 12
HEAD_DIM = 64
FF = 3072
SIDE_S = 12
SIDE_M = 15
SIDE_L = 20
TOK_DEV = 2048


EPSILON = 1e-06


def layout(group_counts):
    positions = jnp.arange(TOK_DEV, dtype=jnp.int32)
    area_small = SIDE_S * SIDE_S
    area_middle = SIDE_M * SIDE_M
    area_large = SIDE_L * SIDE_L
    end_small = group_counts[0] * area_small
    end_middle = end_small + group_counts[1] * area_middle
    end_large = end_middle + group_counts[2] * area_large
    size_class = (positions >= end_small).astype(jnp.int32) + (positions >= end_middle).astype(
        jnp.int32
    )
    begins = jnp.where(size_class == 0, 0, jnp.where(size_class == 1, end_small, end_middle))
    area_len = jnp.where(
        size_class == 0, area_small, jnp.where(size_class == 1, area_middle, area_large)
    )
    side_len = jnp.where(size_class == 0, SIDE_S, jnp.where(size_class == 1, SIDE_M, SIDE_L))
    within = positions - begins
    picture_index = within // area_len
    within_image = within % area_len
    is_valid = positions < end_large
    segment = jnp.where(is_valid, size_class * 16 + picture_index, 255)
    grid_row = (within_image // side_len).astype(jnp.float32)
    grid_col = (within_image % side_len).astype(jnp.float32)
    return (segment, grid_row, grid_col, is_valid.astype(jnp.float32))


def normalize(values, gain_row, shift_row):
    centred = values - jnp.mean(values, axis=-1, keepdims=True)
    spread = jnp.mean(centred * centred, axis=-1, keepdims=True)
    return centred * lax.rsqrt(spread + EPSILON) * gain_row + shift_row


def slopes_of(first_head, count_heads):
    head_number = (first_head + jnp.arange(count_heads, dtype=jnp.int32)).astype(jnp.float32) + 1.0
    return jnp.exp2(-8.0 * head_number / HEADS)


Q_BLOCK = 256
K_BLOCK = 256
NEG = -1e30


def key_ranges(segment, tokens):
    starts = jnp.arange(0, tokens, Q_BLOCK)
    first = segment[starts]
    last = segment[starts + Q_BLOCK - 1]
    key_lo = jnp.sum(segment[None, :] < first[:, None], axis=1)
    key_hi = jnp.sum(segment[None, :] <= last[:, None], axis=1)
    return (key_lo // K_BLOCK).astype(jnp.int32), ((key_hi + K_BLOCK - 1) // K_BLOCK).astype(jnp.int32)


def block_geometry(qi_ref, ki_ref, start):
    rq = qi_ref[:, 0:1]
    cq = qi_ref[:, 1:2]
    sq = qi_ref[:, 2:3]
    rk = ki_ref[0:1, pl.ds(start, K_BLOCK)]
    ck = ki_ref[1:2, pl.ds(start, K_BLOCK)]
    sk = ki_ref[2:3, pl.ds(start, K_BLOCK)]
    dr = rq - rk
    dc = cq - ck
    return jnp.sqrt(dr * dr + dc * dc), sq == sk


def fwd_kernel(heads, scale, lo_ref, hi_ref, slope_ref, q_ref, k_ref, v_ref, qi_ref, ki_ref, o_ref, lse_ref):
    i = pl.program_id(0)
    queries = [q_ref[h] for h in range(heads)]
    width = q_ref.shape[2]

    def body(kb, carry):
        start = pl.multiple_of(kb * K_BLOCK, K_BLOCK)
        dist, allowed = block_geometry(qi_ref, ki_ref, start)
        out = []
        for h in range(heads):
            m_old, l_old, acc_old = carry[h]
            keys = k_ref[h, pl.ds(start, K_BLOCK), :]
            vals = v_ref[h, pl.ds(start, K_BLOCK), :]
            s = lax.dot_general(queries[h], keys, (((1,), (1,)), ((), ())),
                                preferred_element_type=jnp.float32) * scale - slope_ref[h] * dist
            s = jnp.where(allowed, s, NEG)
            m_new = jnp.maximum(m_old, jnp.max(s, axis=1, keepdims=True))
            alpha = jnp.exp(m_old - m_new)
            p = jnp.exp(s - m_new)
            l_new = alpha * l_old + jnp.sum(p, axis=1, keepdims=True)
            acc_new = alpha * acc_old + jnp.dot(p.astype(jnp.bfloat16), vals,
                                                preferred_element_type=jnp.float32)
            out.append((m_new, l_new, acc_new))
        return tuple(out)

    init = tuple(
        (jnp.full((Q_BLOCK, 1), NEG, jnp.float32), jnp.zeros((Q_BLOCK, 1), jnp.float32),
         jnp.zeros((Q_BLOCK, width), jnp.float32))
        for _ in range(heads)
    )
    final = lax.fori_loop(lo_ref[i], hi_ref[i], body, init)
    for h in range(heads):
        m, l, acc = final[h]
        o_ref[h] = acc / l
        lse_ref[h] = m + jnp.log(l)


def bwd_kernel(heads, scale, lo_ref, hi_ref, slope_ref, q_ref, k_ref, v_ref, qi_ref, ki_ref,
               o_ref, do_ref, lse_ref, dq_ref, dk_ref, dv_ref):
    i = pl.program_id(0)

    @pl.when(i == 0)
    def _():
        dk_ref[...] = jnp.zeros_like(dk_ref)
        dv_ref[...] = jnp.zeros_like(dv_ref)

    queries = [q_ref[h] for h in range(heads)]
    grads = [do_ref[h] for h in range(heads)]
    lses = [lse_ref[h] for h in range(heads)]
    deltas = [jnp.sum(grads[h].astype(jnp.float32) * o_ref[h], axis=1, keepdims=True)
              for h in range(heads)]
    width = q_ref.shape[2]

    def body(kb, carry):
        start = pl.multiple_of(kb * K_BLOCK, K_BLOCK)
        dist, allowed = block_geometry(qi_ref, ki_ref, start)
        out = []
        for h in range(heads):
            keys = k_ref[h, pl.ds(start, K_BLOCK), :]
            vals = v_ref[h, pl.ds(start, K_BLOCK), :]
            s = lax.dot_general(queries[h], keys, (((1,), (1,)), ((), ())),
                                preferred_element_type=jnp.float32) * scale - slope_ref[h] * dist
            p = jnp.where(allowed, jnp.exp(s - lses[h]), 0.0)
            dp = lax.dot_general(grads[h], vals, (((1,), (1,)), ((), ())),
                                 preferred_element_type=jnp.float32)
            ds = (p * (dp - deltas[h])).astype(jnp.bfloat16)
            out.append(carry[h] + jnp.dot(ds, keys, preferred_element_type=jnp.float32))
            dk_ref[h, pl.ds(start, K_BLOCK), :] += lax.dot_general(
                ds, queries[h], (((0,), (0,)), ((), ())), preferred_element_type=jnp.float32)
            dv_ref[h, pl.ds(start, K_BLOCK), :] += lax.dot_general(
                p.astype(jnp.bfloat16), grads[h], (((0,), (0,)), ((), ())),
                preferred_element_type=jnp.float32)
        return tuple(out)

    init = tuple(jnp.zeros((Q_BLOCK, width), jnp.float32) for _ in range(heads))
    final = lax.fori_loop(lo_ref[i], hi_ref[i], body, init)
    for h in range(heads):
        dq_ref[h] = final[h]


def attention_fwd(lo, hi, slopes, q, k, v, qinfo, kinfo, scale):
    heads, tokens, width = q.shape
    grid = (tokens // Q_BLOCK,)
    whole = lambda i, lo, hi: (0, 0, 0)
    rows = lambda i, lo, hi: (0, i, 0)
    return pl.pallas_call(
        functools.partial(fwd_kernel, heads, scale),
        grid_spec=pltpu.PrefetchScalarGridSpec(
            num_scalar_prefetch=2,
            grid=grid,
            in_specs=[
                pl.BlockSpec(memory_space=pltpu.SMEM),
                pl.BlockSpec((heads, Q_BLOCK, width), rows),
                pl.BlockSpec((heads, tokens, width), whole),
                pl.BlockSpec((heads, tokens, width), whole),
                pl.BlockSpec((Q_BLOCK, 3), lambda i, lo, hi: (i, 0)),
                pl.BlockSpec((3, tokens), lambda i, lo, hi: (0, 0)),
            ],
            out_specs=[
                pl.BlockSpec((heads, Q_BLOCK, width), rows),
                pl.BlockSpec((heads, Q_BLOCK, 1), rows),
            ],
        ),
        out_shape=[
            jax.ShapeDtypeStruct((heads, tokens, width), jnp.float32),
            jax.ShapeDtypeStruct((heads, tokens, 1), jnp.float32),
        ],
        compiler_params=pltpu.CompilerParams(dimension_semantics=("arbitrary",)),
    )(lo, hi, slopes, q, k, v, qinfo, kinfo)


def attention_bwd(lo, hi, slopes, q, k, v, qinfo, kinfo, o, do, lse, scale):
    heads, tokens, width = q.shape
    grid = (tokens // Q_BLOCK,)
    whole = lambda i, lo, hi: (0, 0, 0)
    rows = lambda i, lo, hi: (0, i, 0)
    return pl.pallas_call(
        functools.partial(bwd_kernel, heads, scale),
        grid_spec=pltpu.PrefetchScalarGridSpec(
            num_scalar_prefetch=2,
            grid=grid,
            in_specs=[
                pl.BlockSpec(memory_space=pltpu.SMEM),
                pl.BlockSpec((heads, Q_BLOCK, width), rows),
                pl.BlockSpec((heads, tokens, width), whole),
                pl.BlockSpec((heads, tokens, width), whole),
                pl.BlockSpec((Q_BLOCK, 3), lambda i, lo, hi: (i, 0)),
                pl.BlockSpec((3, tokens), lambda i, lo, hi: (0, 0)),
                pl.BlockSpec((heads, Q_BLOCK, width), rows),
                pl.BlockSpec((heads, Q_BLOCK, width), rows),
                pl.BlockSpec((heads, Q_BLOCK, 1), rows),
            ],
            out_specs=[
                pl.BlockSpec((heads, Q_BLOCK, width), rows),
                pl.BlockSpec((heads, tokens, width), whole),
                pl.BlockSpec((heads, tokens, width), whole),
            ],
        ),
        out_shape=[
            jax.ShapeDtypeStruct((heads, tokens, width), jnp.float32),
            jax.ShapeDtypeStruct((heads, tokens, width), jnp.float32),
            jax.ShapeDtypeStruct((heads, tokens, width), jnp.float32),
        ],
        compiler_params=pltpu.CompilerParams(dimension_semantics=("arbitrary",)),
    )(lo, hi, slopes, q, k, v, qinfo, kinfo, o, do, lse)


def scatter_tensor(partial, tensor_size):
    me = lax.axis_index("tensor")
    blocks = partial.reshape(tensor_size, -1, partial.shape[1])
    total = lax.dynamic_index_in_dim(blocks, me, keepdims=False).astype(jnp.float32)
    for shift in range(1, tensor_size):
        outgoing = lax.dynamic_index_in_dim(blocks, (me + shift) % tensor_size, keepdims=False)
        pairs = [(i, (i + shift) % tensor_size) for i in range(tensor_size)]
        total = total + lax.ppermute(outgoing.astype(jnp.bfloat16), "tensor", pairs).astype(
            jnp.float32
        )
    return total


def halving_scatter(blocks, axis_name):
    me = lax.axis_index(axis_name)
    bit = 0
    while blocks.shape[0] > 1:
        pairs = [(i, i ^ (1 << bit)) for i in range(blocks.shape[0] << bit)]
        halves = blocks.reshape((blocks.shape[0] // 2, 2) + blocks.shape[1:])
        mine = (me >> bit) & 1
        keep = lax.dynamic_index_in_dim(halves, mine, axis=1, keepdims=False)
        send = lax.dynamic_index_in_dim(halves, 1 - mine, axis=1, keepdims=False)
        blocks = keep + lax.ppermute(send, axis_name, pairs)
        bit += 1
    return blocks[0]


def doubling_sum(values, axis_name, size):
    bit = 0
    while (1 << bit) < size:
        pairs = [(i, i ^ (1 << bit)) for i in range(size)]
        values = values + lax.ppermute(values, axis_name, pairs)
        bit += 1
    return values


def on_device_body(
    dp_size,
    patches,
    counts,
    norm_gain,
    norm_bias,
    w_qkv,
    b_qv,
    w_out,
    out_bias,
    w_up,
    b_up,
    w_down,
    cotangent,
):
    local_rows = patches.shape[0]
    width_here = w_qkv.shape[2]
    heads_here = width_here // HEAD_DIM
    ff_here = w_up.shape[1]
    tensor_pos = lax.axis_index("tensor")
    tensor_size = D // width_here
    score_scale = HEAD_DIM ** (-0.5)
    segment, grid_row, grid_col, is_valid = layout(counts[0])
    keep_rows = lax.dynamic_slice_in_dim(is_valid, tensor_pos * local_rows, local_rows)[:, None]
    slopes = slopes_of(tensor_pos * heads_here, heads_here)
    inputs = patches.astype(jnp.float32)
    inputs_all = lax.all_gather(patches, "tensor", axis=0, tiled=True).astype(jnp.float32)
    normed = normalize(inputs_all, norm_gain[0], norm_bias[0]).astype(jnp.bfloat16)
    projected = jnp.einsum("td,dsc->tsc", normed, w_qkv, preferred_element_type=jnp.float32)
    queries = (projected[:, 0] + b_qv[0]).astype(jnp.bfloat16)
    keys = projected[:, 1].astype(jnp.bfloat16)
    values = (projected[:, 2] + b_qv[1]).astype(jnp.bfloat16)

    def head_major(rows):
        return rows.reshape(TOK_DEV, heads_here, HEAD_DIM).transpose(1, 0, 2)

    def row_major(heads):
        return heads.transpose(1, 0, 2).reshape(TOK_DEV, width_here)

    key_lo, key_hi = key_ranges(segment, TOK_DEV)
    segment_f = segment.astype(jnp.float32)
    query_info = jnp.stack([grid_row, grid_col, segment_f], axis=1)
    key_info = jnp.stack([grid_row, grid_col, segment_f], axis=0)
    query_heads = head_major(queries)
    key_heads = head_major(keys)
    value_heads = head_major(values)
    mixed_f32, log_totals = attention_fwd(
        key_lo, key_hi, slopes, query_heads, key_heads, value_heads, query_info, key_info, score_scale
    )
    upstream = cotangent.astype(jnp.float32)
    branch_grad = lax.all_gather(
        (keep_rows * upstream).astype(jnp.bfloat16), "tensor", axis=0, tiled=True
    )
    mixed_f32, log_totals, branch_grad = lax.optimization_barrier(
        (mixed_f32, log_totals, branch_grad)
    )
    mixed_rows = row_major(mixed_f32).astype(jnp.bfloat16)
    mixed_all = lax.all_gather(mixed_rows, "tensor", axis=1, tiled=True)
    w_out_all = lax.all_gather(w_out, "tensor", axis=0, tiled=True)
    attended = jnp.dot(mixed_all, w_out_all, preferred_element_type=jnp.float32)
    after_attn_all = inputs_all + is_valid[:, None] * (attended + out_bias[0])
    after_attn = lax.dynamic_slice_in_dim(after_attn_all, tensor_pos * local_rows, local_rows)
    normed_two = normalize(after_attn_all, norm_gain[1], norm_bias[1]).astype(jnp.bfloat16)
    hidden_pre = jnp.dot(normed_two, w_up, preferred_element_type=jnp.float32) + b_up
    hidden = jax.nn.gelu(hidden_pre, approximate=False).astype(jnp.bfloat16)
    branch_partial = jnp.dot(hidden, w_down, preferred_element_type=jnp.float32)
    down_bias_grad = jnp.sum(keep_rows * upstream, axis=0)
    w_down_grad_t = jnp.einsum(
        "td,tf->df", branch_grad, hidden, preferred_element_type=jnp.float32
    )
    hidden_grad = jnp.einsum("td,fd->tf", branch_grad, w_down, preferred_element_type=jnp.float32)
    _, gelu_back = jax.vjp(lambda pre_act: jax.nn.gelu(pre_act, approximate=False), hidden_pre)
    pre_grad = gelu_back(hidden_grad)[0].astype(jnp.bfloat16)
    up_bias_grad = jnp.sum(pre_grad, axis=0, dtype=jnp.float32)
    w_up_grad = jnp.einsum("td,tf->df", normed_two, pre_grad, preferred_element_type=jnp.float32)
    normed_two_grad = lax.psum_scatter(
        jnp.einsum("tf,df->td", pre_grad, w_up, preferred_element_type=jnp.float32).astype(
            jnp.bfloat16
        ),
        "tensor",
        scatter_dimension=0,
        tiled=True,
    ).astype(jnp.float32)
    _, norm_two_back = jax.vjp(normalize, after_attn, norm_gain[1], norm_bias[1])
    through_two, gain_two_grad, shift_two_grad = norm_two_back(normed_two_grad)
    after_grad = upstream + through_two
    attn_bias_grad = jnp.sum(keep_rows * after_grad, axis=0)
    attn_local = (keep_rows * after_grad).astype(jnp.bfloat16)
    attn_grad = lax.all_gather(attn_local, "tensor", axis=0, tiled=True)
    w_out_grad_t = jnp.einsum(
        "td,tc->dc", attn_grad, mixed_rows, preferred_element_type=jnp.float32
    )
    mixed_grad = jnp.einsum(
        "td,cd->tc", attn_grad, w_out, preferred_element_type=jnp.float32
    ).astype(jnp.bfloat16)
    early_parts = jnp.concatenate([w_down_grad_t, w_up_grad, w_out_grad_t], axis=1).astype(
        jnp.bfloat16
    )
    early_parts, mixed_grad, branch_partial = lax.optimization_barrier(
        (early_parts, mixed_grad, branch_partial)
    )
    branch = scatter_tensor(branch_partial, tensor_size)
    result = (after_attn + keep_rows * (branch + out_bias[1])).astype(jnp.bfloat16)
    early_sum = lax.psum_scatter(early_parts, "dp", scatter_dimension=0, tiled=True).astype(
        jnp.float32
    )
    query_acc, key_acc, value_acc = attention_bwd(
        key_lo, key_hi, slopes, query_heads, key_heads, value_heads, query_info, key_info,
        mixed_f32, head_major(mixed_grad), log_totals, score_scale,
    )
    query_acc, key_acc, value_acc, early_sum, result = lax.optimization_barrier(
        (query_acc, key_acc, value_acc, early_sum, result)
    )
    query_grad = row_major(query_acc * score_scale).astype(jnp.bfloat16)
    key_grad = row_major(key_acc * score_scale).astype(jnp.bfloat16)
    value_grad = row_major(value_acc).astype(jnp.bfloat16)
    projected_grad = jnp.concatenate([query_grad, key_grad, value_grad], axis=1)
    qv_bias_grad = jnp.stack(
        [
            jnp.sum(query_grad, axis=0, dtype=jnp.float32),
            jnp.sum(value_grad, axis=0, dtype=jnp.float32),
        ]
    )
    w_qkv_grad = jnp.einsum("td,tc->dc", normed, projected_grad, preferred_element_type=jnp.float32)
    normed_grad_partial = jnp.einsum(
        "tc,dc->td",
        projected_grad,
        w_qkv.reshape(D, 3 * width_here),
        preferred_element_type=jnp.float32,
    )
    centred_all = inputs_all - jnp.mean(inputs_all, axis=-1, keepdims=True)
    unit_all = centred_all * lax.rsqrt(
        jnp.mean(centred_all * centred_all, axis=-1, keepdims=True) + EPSILON
    )
    gain_one_grad = jnp.sum(normed_grad_partial * unit_all, axis=0)
    shift_one_grad = jnp.sum(normed_grad_partial, axis=0)
    normed_grad = scatter_tensor(normed_grad_partial, tensor_size)
    _, norm_one_back = jax.vjp(normalize, inputs, norm_gain[0], norm_bias[0])
    through_one = norm_one_back(normed_grad)[0]
    input_grad = (after_grad + through_one).astype(jnp.bfloat16)
    qv_full = lax.dynamic_update_slice_in_dim(
        jnp.zeros((2, D), jnp.float32), qv_bias_grad, tensor_pos * width_here, 1
    )
    up_full = lax.dynamic_update_slice_in_dim(
        jnp.zeros((FF,), jnp.float32), up_bias_grad, tensor_pos * ff_here, 0
    )
    small = jnp.concatenate(
        [
            jnp.stack([gain_one_grad, gain_two_grad]).reshape(-1),
            jnp.stack([shift_one_grad, shift_two_grad]).reshape(-1),
            jnp.stack([attn_bias_grad, down_bias_grad]).reshape(-1),
            qv_full.reshape(-1),
            up_full,
        ]
    )
    late_blocks = jnp.concatenate(
        [
            w_qkv_grad.reshape(dp_size, -1),
            jnp.broadcast_to(small, (dp_size,) + small.shape),
        ],
        axis=1,
    )
    late_sum = halving_scatter(late_blocks, "dp")
    qkv_size = w_qkv_grad.size // dp_size
    qkv_part = late_sum[:qkv_size].reshape(-1, 3, width_here)
    summed = doubling_sum(late_sum[qkv_size:], "tensor", tensor_size)
    gains_grad = summed[: 2 * D].reshape(2, D)
    shifts_grad = summed[2 * D : 4 * D].reshape(2, D)
    outer_grad = summed[4 * D : 6 * D].reshape(2, D)
    qv_sum = summed[6 * D : 8 * D].reshape(2, D)
    up_sum = summed[8 * D :]
    down_part = early_sum[:, :ff_here].T
    up_part = early_sum[:, ff_here : 2 * ff_here]
    out_part = early_sum[:, 2 * ff_here :].T
    return (
        result,
        input_grad,
        gains_grad,
        shifts_grad,
        qkv_part,
        qv_sum,
        out_part,
        outer_grad,
        up_part,
        up_sum,
        down_part,
    )


def solution(mesh):
    placed = (
        P(("dp", "tensor"), None),
        P("dp", None),
        P(),
        P(),
        P(None, None, "tensor"),
        P(None, "tensor"),
        P("tensor", None),
        P(),
        P(None, "tensor"),
        P("tensor"),
        P("tensor", None),
        P(("dp", "tensor"), None),
    )
    return jax.shard_map(
        functools.partial(on_device_body, mesh.shape["dp"]),
        mesh=mesh,
        in_specs=placed,
        out_specs=(
            P(("dp", "tensor"), None),
            P(("dp", "tensor"), None),
            P(),
            P(),
            P("dp", None, "tensor"),
            P(),
            P("tensor", "dp"),
            P(),
            P("dp", "tensor"),
            P(),
            P("tensor", "dp"),
        ),
        check_vma=False,
    )
```

```python
import functools

import jax
import jax.numpy as jnp
from jax import lax
from jax.experimental import pallas as pl
from jax.experimental.pallas import tpu as pltpu
from jax.sharding import PartitionSpec as P


D = 768
HEADS = 12
HEAD_DIM = 64
FF = 3072
SIDE_S = 12
SIDE_M = 15
SIDE_L = 20
TOK_DEV = 2048


EPSILON = 1e-06


def layout(group_counts):
    positions = jnp.arange(TOK_DEV, dtype=jnp.int32)
    area_small = SIDE_S * SIDE_S
    area_middle = SIDE_M * SIDE_M
    area_large = SIDE_L * SIDE_L
    end_small = group_counts[0] * area_small
    end_middle = end_small + group_counts[1] * area_middle
    end_large = end_middle + group_counts[2] * area_large
    size_class = (positions >= end_small).astype(jnp.int32) + (positions >= end_middle).astype(
        jnp.int32
    )
    begins = jnp.where(size_class == 0, 0, jnp.where(size_class == 1, end_small, end_middle))
    area_len = jnp.where(
        size_class == 0, area_small, jnp.where(size_class == 1, area_middle, area_large)
    )
    side_len = jnp.where(size_class == 0, SIDE_S, jnp.where(size_class == 1, SIDE_M, SIDE_L))
    within = positions - begins
    picture_index = within // area_len
    within_image = within % area_len
    is_valid = positions < end_large
    segment = jnp.where(is_valid, size_class * 16 + picture_index, 255)
    grid_row = (within_image // side_len).astype(jnp.float32)
    grid_col = (within_image % side_len).astype(jnp.float32)
    return (segment, grid_row, grid_col, is_valid.astype(jnp.float32))


def normalize(values, gain_row, shift_row):
    centred = values - jnp.mean(values, axis=-1, keepdims=True)
    spread = jnp.mean(centred * centred, axis=-1, keepdims=True)
    return centred * lax.rsqrt(spread + EPSILON) * gain_row + shift_row


def slopes_of(first_head, count_heads):
    head_number = (first_head + jnp.arange(count_heads, dtype=jnp.int32)).astype(jnp.float32) + 1.0
    return jnp.exp2(-8.0 * head_number / HEADS)


Q_BLOCK = 256
K_BLOCK = 256
NEG = -1e30


def key_ranges(segment, tokens):
    starts = jnp.arange(0, tokens, Q_BLOCK)
    first = segment[starts]
    last = segment[starts + Q_BLOCK - 1]
    key_lo = jnp.sum(segment[None, :] < first[:, None], axis=1)
    key_hi = jnp.sum(segment[None, :] <= last[:, None], axis=1)
    return (key_lo // K_BLOCK).astype(jnp.int32), ((key_hi + K_BLOCK - 1) // K_BLOCK).astype(jnp.int32)


def block_geometry(qi_ref, ki_ref, start):
    rq = qi_ref[:, 0:1]
    cq = qi_ref[:, 1:2]
    sq = qi_ref[:, 2:3]
    rk = ki_ref[0:1, pl.ds(start, K_BLOCK)]
    ck = ki_ref[1:2, pl.ds(start, K_BLOCK)]
    sk = ki_ref[2:3, pl.ds(start, K_BLOCK)]
    dr = rq - rk
    dc = cq - ck
    return jnp.sqrt(dr * dr + dc * dc), sq == sk


def fwd_kernel(heads, scale, lo_ref, hi_ref, slope_ref, q_ref, k_ref, v_ref, qi_ref, ki_ref, o_ref, lse_ref):
    i = pl.program_id(0)
    queries = [q_ref[h] for h in range(heads)]
    width = q_ref.shape[2]

    def body(kb, carry):
        start = pl.multiple_of(kb * K_BLOCK, K_BLOCK)
        dist, allowed = block_geometry(qi_ref, ki_ref, start)
        out = []
        for h in range(heads):
            m_old, l_old, acc_old = carry[h]
            keys = k_ref[h, pl.ds(start, K_BLOCK), :]
            vals = v_ref[h, pl.ds(start, K_BLOCK), :]
            s = lax.dot_general(queries[h], keys, (((1,), (1,)), ((), ())),
                                preferred_element_type=jnp.float32) * scale - slope_ref[h] * dist
            s = jnp.where(allowed, s, NEG)
            m_new = jnp.maximum(m_old, jnp.max(s, axis=1, keepdims=True))
            alpha = jnp.exp(m_old - m_new)
            p = jnp.exp(s - m_new)
            l_new = alpha * l_old + jnp.sum(p, axis=1, keepdims=True)
            acc_new = alpha * acc_old + jnp.dot(p.astype(jnp.bfloat16), vals,
                                                preferred_element_type=jnp.float32)
            out.append((m_new, l_new, acc_new))
        return tuple(out)

    init = tuple(
        (jnp.full((Q_BLOCK, 1), NEG, jnp.float32), jnp.zeros((Q_BLOCK, 1), jnp.float32),
         jnp.zeros((Q_BLOCK, width), jnp.float32))
        for _ in range(heads)
    )
    final = lax.fori_loop(lo_ref[i], hi_ref[i], body, init)
    for h in range(heads):
        m, l, acc = final[h]
        o_ref[h] = acc / l
        lse_ref[h] = m + jnp.log(l)


def bwd_kernel(heads, scale, lo_ref, hi_ref, slope_ref, q_ref, k_ref, v_ref, qi_ref, ki_ref,
               o_ref, do_ref, lse_ref, dq_ref, dk_ref, dv_ref):
    i = pl.program_id(0)

    @pl.when(i == 0)
    def _():
        dk_ref[...] = jnp.zeros_like(dk_ref)
        dv_ref[...] = jnp.zeros_like(dv_ref)

    queries = [q_ref[h] for h in range(heads)]
    grads = [do_ref[h] for h in range(heads)]
    lses = [lse_ref[h] for h in range(heads)]
    deltas = [jnp.sum(grads[h].astype(jnp.float32) * o_ref[h], axis=1, keepdims=True)
              for h in range(heads)]
    width = q_ref.shape[2]

    def body(kb, carry):
        start = pl.multiple_of(kb * K_BLOCK, K_BLOCK)
        dist, allowed = block_geometry(qi_ref, ki_ref, start)
        out = []
        for h in range(heads):
            keys = k_ref[h, pl.ds(start, K_BLOCK), :]
            vals = v_ref[h, pl.ds(start, K_BLOCK), :]
            s = lax.dot_general(queries[h], keys, (((1,), (1,)), ((), ())),
                                preferred_element_type=jnp.float32) * scale - slope_ref[h] * dist
            p = jnp.where(allowed, jnp.exp(s - lses[h]), 0.0)
            dp = lax.dot_general(grads[h], vals, (((1,), (1,)), ((), ())),
                                 preferred_element_type=jnp.float32)
            ds = (p * (dp - deltas[h])).astype(jnp.bfloat16)
            out.append(carry[h] + jnp.dot(ds, keys, preferred_element_type=jnp.float32))
            dk_ref[h, pl.ds(start, K_BLOCK), :] += lax.dot_general(
                ds, queries[h], (((0,), (0,)), ((), ())), preferred_element_type=jnp.float32)
            dv_ref[h, pl.ds(start, K_BLOCK), :] += lax.dot_general(
                p.astype(jnp.bfloat16), grads[h], (((0,), (0,)), ((), ())),
                preferred_element_type=jnp.float32)
        return tuple(out)

    init = tuple(jnp.zeros((Q_BLOCK, width), jnp.float32) for _ in range(heads))
    final = lax.fori_loop(lo_ref[i], hi_ref[i], body, init)
    for h in range(heads):
        dq_ref[h] = final[h]


def attention_fwd(lo, hi, slopes, q, k, v, qinfo, kinfo, scale):
    heads, tokens, width = q.shape
    key_tokens = k.shape[1]
    grid = (tokens // Q_BLOCK,)
    whole = lambda i, lo, hi: (0, 0, 0)
    rows = lambda i, lo, hi: (0, i, 0)
    return pl.pallas_call(
        functools.partial(fwd_kernel, heads, scale),
        grid_spec=pltpu.PrefetchScalarGridSpec(
            num_scalar_prefetch=2,
            grid=grid,
            in_specs=[
                pl.BlockSpec(memory_space=pltpu.SMEM),
                pl.BlockSpec((heads, Q_BLOCK, width), rows),
                pl.BlockSpec((heads, key_tokens, width), whole),
                pl.BlockSpec((heads, key_tokens, width), whole),
                pl.BlockSpec((Q_BLOCK, 3), lambda i, lo, hi: (i, 0)),
                pl.BlockSpec((3, key_tokens), lambda i, lo, hi: (0, 0)),
            ],
            out_specs=[
                pl.BlockSpec((heads, Q_BLOCK, width), rows),
                pl.BlockSpec((heads, Q_BLOCK, 1), rows),
            ],
        ),
        out_shape=[
            jax.ShapeDtypeStruct((heads, tokens, width), jnp.float32),
            jax.ShapeDtypeStruct((heads, tokens, 1), jnp.float32),
        ],
        compiler_params=pltpu.CompilerParams(dimension_semantics=("arbitrary",)),
    )(lo, hi, slopes, q, k, v, qinfo, kinfo)


def attention_bwd(lo, hi, slopes, q, k, v, qinfo, kinfo, o, do, lse, scale):
    heads, tokens, width = q.shape
    grid = (tokens // Q_BLOCK,)
    whole = lambda i, lo, hi: (0, 0, 0)
    rows = lambda i, lo, hi: (0, i, 0)
    return pl.pallas_call(
        functools.partial(bwd_kernel, heads, scale),
        grid_spec=pltpu.PrefetchScalarGridSpec(
            num_scalar_prefetch=2,
            grid=grid,
            in_specs=[
                pl.BlockSpec(memory_space=pltpu.SMEM),
                pl.BlockSpec((heads, Q_BLOCK, width), rows),
                pl.BlockSpec((heads, tokens, width), whole),
                pl.BlockSpec((heads, tokens, width), whole),
                pl.BlockSpec((Q_BLOCK, 3), lambda i, lo, hi: (i, 0)),
                pl.BlockSpec((3, tokens), lambda i, lo, hi: (0, 0)),
                pl.BlockSpec((heads, Q_BLOCK, width), rows),
                pl.BlockSpec((heads, Q_BLOCK, width), rows),
                pl.BlockSpec((heads, Q_BLOCK, 1), rows),
            ],
            out_specs=[
                pl.BlockSpec((heads, Q_BLOCK, width), rows),
                pl.BlockSpec((heads, tokens, width), whole),
                pl.BlockSpec((heads, tokens, width), whole),
            ],
        ),
        out_shape=[
            jax.ShapeDtypeStruct((heads, tokens, width), jnp.float32),
            jax.ShapeDtypeStruct((heads, tokens, width), jnp.float32),
            jax.ShapeDtypeStruct((heads, tokens, width), jnp.float32),
        ],
        compiler_params=pltpu.CompilerParams(dimension_semantics=("arbitrary",)),
    )(lo, hi, slopes, q, k, v, qinfo, kinfo, o, do, lse)


def scatter_tensor(partial, tensor_size):
    me = lax.axis_index("tensor")
    blocks = partial.reshape(tensor_size, -1, partial.shape[1])
    total = lax.dynamic_index_in_dim(blocks, me, keepdims=False).astype(jnp.float32)
    for shift in range(1, tensor_size):
        outgoing = lax.dynamic_index_in_dim(blocks, (me + shift) % tensor_size, keepdims=False)
        pairs = [(i, (i + shift) % tensor_size) for i in range(tensor_size)]
        total = total + lax.ppermute(outgoing.astype(jnp.bfloat16), "tensor", pairs).astype(
            jnp.float32
        )
    return total


def halving_scatter(blocks, axis_name, wire):
    me = lax.axis_index(axis_name)
    bit = 0
    while blocks.shape[0] > 1:
        pairs = [(i, i ^ (1 << bit)) for i in range(blocks.shape[0] << bit)]
        halves = blocks.reshape((blocks.shape[0] // 2, 2) + blocks.shape[1:])
        mine = (me >> bit) & 1
        keep = lax.dynamic_index_in_dim(halves, mine, axis=1, keepdims=False)
        send = lax.dynamic_index_in_dim(halves, 1 - mine, axis=1, keepdims=False)
        arrived = lax.ppermute(send.astype(wire), axis_name, pairs)
        blocks = keep + arrived.astype(blocks.dtype)
        bit += 1
    return blocks[0]


def doubling_sum(values, axis_name, size):
    bit = 0
    while (1 << bit) < size:
        pairs = [(i, i ^ (1 << bit)) for i in range(size)]
        values = values + lax.ppermute(values, axis_name, pairs)
        bit += 1
    return values


def on_device_body(
    dp_size,
    patches,
    counts,
    norm_gain,
    norm_bias,
    w_qkv,
    b_qv,
    w_out,
    out_bias,
    w_up,
    b_up,
    w_down,
    cotangent,
):
    local_rows = patches.shape[0]
    width_here = w_qkv.shape[2]
    heads_here = width_here // HEAD_DIM
    ff_here = w_up.shape[1]
    tensor_pos = lax.axis_index("tensor")
    tensor_size = D // width_here
    score_scale = HEAD_DIM ** (-0.5)
    segment, grid_row, grid_col, is_valid = layout(counts[0])
    keep_rows = lax.dynamic_slice_in_dim(is_valid, tensor_pos * local_rows, local_rows)[:, None]
    slopes = slopes_of(tensor_pos * heads_here, heads_here)
    inputs = patches.astype(jnp.float32)
    inputs_all = lax.all_gather(patches, "tensor", axis=0, tiled=True).astype(jnp.float32)
    normed = normalize(inputs_all, norm_gain[0], norm_bias[0]).astype(jnp.bfloat16)
    projected = jnp.einsum("td,dsc->tsc", normed, w_qkv, preferred_element_type=jnp.float32)
    queries = (projected[:, 0] + b_qv[0]).astype(jnp.bfloat16)
    keys = projected[:, 1].astype(jnp.bfloat16)
    values = (projected[:, 2] + b_qv[1]).astype(jnp.bfloat16)

    def head_major(rows):
        return rows.reshape(TOK_DEV, heads_here, HEAD_DIM).transpose(1, 0, 2)

    def row_major(heads):
        return heads.transpose(1, 0, 2).reshape(heads.shape[1], width_here)

    key_lo, key_hi = key_ranges(segment, TOK_DEV)
    segment_f = segment.astype(jnp.float32)
    query_info = jnp.stack([grid_row, grid_col, segment_f], axis=1)
    key_info = jnp.stack([grid_row, grid_col, segment_f], axis=0)
    query_heads = head_major(queries)
    key_heads = head_major(keys)
    value_heads = head_major(values)
    half_rows = TOK_DEV // 2
    half_blocks = half_rows // Q_BLOCK

    def attend_half(part):
        rows = slice(part * half_rows, (part + 1) * half_rows)
        blocks = slice(part * half_blocks, (part + 1) * half_blocks)
        return attention_fwd(
            key_lo[blocks], key_hi[blocks], slopes, query_heads[:, rows], key_heads, value_heads,
            query_info[rows], key_info, score_scale,
        )

    upstream = cotangent.astype(jnp.float32)
    branch_grad = lax.all_gather(
        (keep_rows * upstream).astype(jnp.bfloat16), "tensor", axis=0, tiled=True
    )
    mixed_first, log_first = attend_half(0)
    mixed_first, log_first, branch_grad = lax.optimization_barrier(
        (mixed_first, log_first, branch_grad)
    )
    gathered_first = lax.all_gather(
        row_major(mixed_first).astype(jnp.bfloat16), "tensor", axis=1, tiled=True
    )
    mixed_second, log_second = attend_half(1)
    gathered_second = lax.all_gather(
        row_major(mixed_second).astype(jnp.bfloat16), "tensor", axis=1, tiled=True
    )
    mixed_f32 = jnp.concatenate([mixed_first, mixed_second], axis=1)
    log_totals = jnp.concatenate([log_first, log_second], axis=1)
    mixed_rows = row_major(mixed_f32).astype(jnp.bfloat16)
    mixed_all = jnp.concatenate([gathered_first, gathered_second], axis=0)
    w_out_all = lax.all_gather(w_out, "tensor", axis=0, tiled=True)
    attended = jnp.dot(mixed_all, w_out_all, preferred_element_type=jnp.float32)
    after_attn_all = inputs_all + is_valid[:, None] * (attended + out_bias[0])
    after_attn = lax.dynamic_slice_in_dim(after_attn_all, tensor_pos * local_rows, local_rows)
    normed_two = normalize(after_attn_all, norm_gain[1], norm_bias[1]).astype(jnp.bfloat16)
    hidden_pre = jnp.dot(normed_two, w_up, preferred_element_type=jnp.float32) + b_up
    hidden = jax.nn.gelu(hidden_pre, approximate=False).astype(jnp.bfloat16)
    branch_partial = jnp.dot(hidden, w_down, preferred_element_type=jnp.float32)
    down_bias_grad = jnp.sum(keep_rows * upstream, axis=0)
    w_down_grad_t = jnp.einsum(
        "td,tf->df", branch_grad, hidden, preferred_element_type=jnp.float32
    )
    hidden_grad = jnp.einsum("td,fd->tf", branch_grad, w_down, preferred_element_type=jnp.float32)
    _, gelu_back = jax.vjp(lambda pre_act: jax.nn.gelu(pre_act, approximate=False), hidden_pre)
    pre_grad = gelu_back(hidden_grad)[0].astype(jnp.bfloat16)
    up_bias_grad = jnp.sum(pre_grad, axis=0, dtype=jnp.float32)
    w_up_grad = jnp.einsum("td,tf->df", normed_two, pre_grad, preferred_element_type=jnp.float32)
    normed_two_grad = lax.psum_scatter(
        jnp.einsum("tf,df->td", pre_grad, w_up, preferred_element_type=jnp.float32).astype(
            jnp.bfloat16
        ),
        "tensor",
        scatter_dimension=0,
        tiled=True,
    ).astype(jnp.float32)
    _, norm_two_back = jax.vjp(normalize, after_attn, norm_gain[1], norm_bias[1])
    through_two, gain_two_grad, shift_two_grad = norm_two_back(normed_two_grad)
    after_grad = upstream + through_two
    attn_bias_grad = jnp.sum(keep_rows * after_grad, axis=0)
    attn_local = (keep_rows * after_grad).astype(jnp.bfloat16)
    attn_grad = lax.all_gather(attn_local, "tensor", axis=0, tiled=True)
    w_out_grad_t = jnp.einsum(
        "td,tc->dc", attn_grad, mixed_rows, preferred_element_type=jnp.float32
    )
    mixed_grad = jnp.einsum(
        "td,cd->tc", attn_grad, w_out, preferred_element_type=jnp.float32
    ).astype(jnp.bfloat16)
    early_parts = jnp.concatenate([w_down_grad_t, w_up_grad, w_out_grad_t], axis=1).astype(
        jnp.bfloat16
    )
    early_parts, mixed_grad, branch_partial = lax.optimization_barrier(
        (early_parts, mixed_grad, branch_partial)
    )
    branch = scatter_tensor(branch_partial, tensor_size)
    result = (after_attn + keep_rows * (branch + out_bias[1])).astype(jnp.bfloat16)
    early_sum = lax.psum_scatter(early_parts, "dp", scatter_dimension=0, tiled=True).astype(
        jnp.float32
    )
    query_acc, key_acc, value_acc = attention_bwd(
        key_lo, key_hi, slopes, query_heads, key_heads, value_heads, query_info, key_info,
        mixed_f32, head_major(mixed_grad), log_totals, score_scale,
    )
    query_acc, key_acc, value_acc, early_sum, result = lax.optimization_barrier(
        (query_acc, key_acc, value_acc, early_sum, result)
    )
    query_grad = row_major(query_acc * score_scale).astype(jnp.bfloat16)
    key_grad = row_major(key_acc * score_scale).astype(jnp.bfloat16)
    value_grad = row_major(value_acc).astype(jnp.bfloat16)
    projected_grad = jnp.concatenate([query_grad, key_grad, value_grad], axis=1)
    qv_bias_grad = jnp.stack(
        [
            jnp.sum(query_grad, axis=0, dtype=jnp.float32),
            jnp.sum(value_grad, axis=0, dtype=jnp.float32),
        ]
    )
    w_qkv_grad = jnp.einsum("td,tc->dc", normed, projected_grad, preferred_element_type=jnp.float32)
    normed_grad_partial = jnp.einsum(
        "tc,dc->td",
        projected_grad,
        w_qkv.reshape(D, 3 * width_here),
        preferred_element_type=jnp.float32,
    )
    centred_all = inputs_all - jnp.mean(inputs_all, axis=-1, keepdims=True)
    unit_all = centred_all * lax.rsqrt(
        jnp.mean(centred_all * centred_all, axis=-1, keepdims=True) + EPSILON
    )
    gain_one_grad = jnp.sum(normed_grad_partial * unit_all, axis=0)
    shift_one_grad = jnp.sum(normed_grad_partial, axis=0)
    normed_grad = scatter_tensor(normed_grad_partial, tensor_size)
    _, norm_one_back = jax.vjp(normalize, inputs, norm_gain[0], norm_bias[0])
    through_one = norm_one_back(normed_grad)[0]
    input_grad = (after_grad + through_one).astype(jnp.bfloat16)
    qv_full = lax.dynamic_update_slice_in_dim(
        jnp.zeros((2, D), jnp.float32), qv_bias_grad, tensor_pos * width_here, 1
    )
    up_full = lax.dynamic_update_slice_in_dim(
        jnp.zeros((FF,), jnp.float32), up_bias_grad, tensor_pos * ff_here, 0
    )
    small = jnp.concatenate(
        [
            jnp.stack([gain_one_grad, gain_two_grad]).reshape(-1),
            jnp.stack([shift_one_grad, shift_two_grad]).reshape(-1),
            jnp.stack([attn_bias_grad, down_bias_grad]).reshape(-1),
            qv_full.reshape(-1),
            up_full,
        ]
    )
    qkv_sum = halving_scatter(w_qkv_grad.reshape(dp_size, -1), "dp", jnp.bfloat16)
    qkv_part = qkv_sum.reshape(-1, 3, width_here)
    summed = doubling_sum(doubling_sum(small, "dp", dp_size), "tensor", tensor_size)
    gains_grad = summed[: 2 * D].reshape(2, D)
    shifts_grad = summed[2 * D : 4 * D].reshape(2, D)
    outer_grad = summed[4 * D : 6 * D].reshape(2, D)
    qv_sum = summed[6 * D : 8 * D].reshape(2, D)
    up_sum = summed[8 * D :]
    down_part = early_sum[:, :ff_here].T
    up_part = early_sum[:, ff_here : 2 * ff_here]
    out_part = early_sum[:, 2 * ff_here :].T
    return (
        result,
        input_grad,
        gains_grad,
        shifts_grad,
        qkv_part,
        qv_sum,
        out_part,
        outer_grad,
        up_part,
        up_sum,
        down_part,
    )


def solution(mesh):
    placed = (
        P(("dp", "tensor"), None),
        P("dp", None),
        P(),
        P(),
        P(None, None, "tensor"),
        P(None, "tensor"),
        P("tensor", None),
        P(),
        P(None, "tensor"),
        P("tensor"),
        P("tensor", None),
        P(("dp", "tensor"), None),
    )
    return jax.shard_map(
        functools.partial(on_device_body, mesh.shape["dp"]),
        mesh=mesh,
        in_specs=placed,
        out_specs=(
            P(("dp", "tensor"), None),
            P(("dp", "tensor"), None),
            P(),
            P(),
            P("dp", None, "tensor"),
            P(),
            P("tensor", "dp"),
            P(),
            P("dp", "tensor"),
            P(),
            P("tensor", "dp"),
        ),
        check_vma=False,
    )
```

```python
import functools

import jax
import jax.numpy as jnp
from jax import lax
from jax.experimental import pallas as pl
from jax.experimental.pallas import tpu as pltpu
from jax.sharding import PartitionSpec as P


D = 768
HEADS = 12
HEAD_DIM = 64
FF = 3072
SIDE_S = 12
SIDE_M = 15
SIDE_L = 20
TOK_DEV = 2048


EPSILON = 1e-06


def layout(group_counts):
    positions = jnp.arange(TOK_DEV, dtype=jnp.int32)
    area_small = SIDE_S * SIDE_S
    area_middle = SIDE_M * SIDE_M
    area_large = SIDE_L * SIDE_L
    end_small = group_counts[0] * area_small
    end_middle = end_small + group_counts[1] * area_middle
    end_large = end_middle + group_counts[2] * area_large
    size_class = (positions >= end_small).astype(jnp.int32) + (positions >= end_middle).astype(
        jnp.int32
    )
    begins = jnp.where(size_class == 0, 0, jnp.where(size_class == 1, end_small, end_middle))
    area_len = jnp.where(
        size_class == 0, area_small, jnp.where(size_class == 1, area_middle, area_large)
    )
    side_len = jnp.where(size_class == 0, SIDE_S, jnp.where(size_class == 1, SIDE_M, SIDE_L))
    within = positions - begins
    picture_index = within // area_len
    within_image = within % area_len
    is_valid = positions < end_large
    segment = jnp.where(is_valid, size_class * 16 + picture_index, 255)
    grid_row = (within_image // side_len).astype(jnp.float32)
    grid_col = (within_image % side_len).astype(jnp.float32)
    return (segment, grid_row, grid_col, is_valid.astype(jnp.float32))


def normalize(values, gain_row, shift_row):
    centred = values - jnp.mean(values, axis=-1, keepdims=True)
    spread = jnp.mean(centred * centred, axis=-1, keepdims=True)
    return centred * lax.rsqrt(spread + EPSILON) * gain_row + shift_row


def slopes_of(first_head, count_heads):
    head_number = (first_head + jnp.arange(count_heads, dtype=jnp.int32)).astype(jnp.float32) + 1.0
    return jnp.exp2(-8.0 * head_number / HEADS)


Q_BLOCK = 256
K_BLOCK = 256
NEG = -1e30


def key_ranges(segment, tokens):
    starts = jnp.arange(0, tokens, Q_BLOCK)
    first = segment[starts]
    last = segment[starts + Q_BLOCK - 1]
    key_lo = jnp.sum(segment[None, :] < first[:, None], axis=1)
    key_hi = jnp.sum(segment[None, :] <= last[:, None], axis=1)
    return (key_lo // K_BLOCK).astype(jnp.int32), ((key_hi + K_BLOCK - 1) // K_BLOCK).astype(jnp.int32)


def block_geometry(qi_ref, ki_ref, start):
    rq = qi_ref[:, 0:1]
    cq = qi_ref[:, 1:2]
    sq = qi_ref[:, 2:3]
    rk = ki_ref[0:1, pl.ds(start, K_BLOCK)]
    ck = ki_ref[1:2, pl.ds(start, K_BLOCK)]
    sk = ki_ref[2:3, pl.ds(start, K_BLOCK)]
    dr = rq - rk
    dc = cq - ck
    return jnp.sqrt(dr * dr + dc * dc), sq == sk


def fwd_kernel(heads, scale, lo_ref, hi_ref, slope_ref, q_ref, k_ref, v_ref, qi_ref, ki_ref, o_ref, lse_ref):
    i = pl.program_id(0)
    queries = [q_ref[h] for h in range(heads)]
    width = q_ref.shape[2]

    def body(kb, carry):
        start = pl.multiple_of(kb * K_BLOCK, K_BLOCK)
        dist, allowed = block_geometry(qi_ref, ki_ref, start)
        out = []
        for h in range(heads):
            m_old, l_old, acc_old = carry[h]
            keys = k_ref[h, pl.ds(start, K_BLOCK), :]
            vals = v_ref[h, pl.ds(start, K_BLOCK), :]
            s = lax.dot_general(queries[h], keys, (((1,), (1,)), ((), ())),
                                preferred_element_type=jnp.float32) * scale - slope_ref[h] * dist
            s = jnp.where(allowed, s, NEG)
            m_new = jnp.maximum(m_old, jnp.max(s, axis=1, keepdims=True))
            alpha = jnp.exp(m_old - m_new)
            p = jnp.exp(s - m_new)
            l_new = alpha * l_old + jnp.sum(p, axis=1, keepdims=True)
            acc_new = alpha * acc_old + jnp.dot(p.astype(jnp.bfloat16), vals,
                                                preferred_element_type=jnp.float32)
            out.append((m_new, l_new, acc_new))
        return tuple(out)

    init = tuple(
        (jnp.full((Q_BLOCK, 1), NEG, jnp.float32), jnp.zeros((Q_BLOCK, 1), jnp.float32),
         jnp.zeros((Q_BLOCK, width), jnp.float32))
        for _ in range(heads)
    )
    final = lax.fori_loop(lo_ref[i], hi_ref[i], body, init)
    for h in range(heads):
        m, l, acc = final[h]
        o_ref[h] = acc / l
        lse_ref[h] = m + jnp.log(l)


def bwd_kernel(heads, scale, lo_ref, hi_ref, slope_ref, q_ref, k_ref, v_ref, qi_ref, ki_ref,
               o_ref, do_ref, lse_ref, dq_ref, dk_ref, dv_ref):
    i = pl.program_id(0)

    @pl.when(i == 0)
    def _():
        dk_ref[...] = jnp.zeros_like(dk_ref)
        dv_ref[...] = jnp.zeros_like(dv_ref)

    queries = [q_ref[h] for h in range(heads)]
    grads = [do_ref[h] for h in range(heads)]
    lses = [lse_ref[h] for h in range(heads)]
    deltas = [jnp.sum(grads[h].astype(jnp.float32) * o_ref[h], axis=1, keepdims=True)
              for h in range(heads)]
    width = q_ref.shape[2]

    def body(kb, carry):
        start = pl.multiple_of(kb * K_BLOCK, K_BLOCK)
        dist, allowed = block_geometry(qi_ref, ki_ref, start)
        out = []
        for h in range(heads):
            keys = k_ref[h, pl.ds(start, K_BLOCK), :]
            vals = v_ref[h, pl.ds(start, K_BLOCK), :]
            s = lax.dot_general(queries[h], keys, (((1,), (1,)), ((), ())),
                                preferred_element_type=jnp.float32) * scale - slope_ref[h] * dist
            p = jnp.where(allowed, jnp.exp(s - lses[h]), 0.0)
            dp = lax.dot_general(grads[h], vals, (((1,), (1,)), ((), ())),
                                 preferred_element_type=jnp.float32)
            ds = (p * (dp - deltas[h])).astype(jnp.bfloat16)
            out.append(carry[h] + jnp.dot(ds, keys, preferred_element_type=jnp.float32))
            dk_ref[h, pl.ds(start, K_BLOCK), :] += lax.dot_general(
                ds, queries[h], (((0,), (0,)), ((), ())), preferred_element_type=jnp.float32)
            dv_ref[h, pl.ds(start, K_BLOCK), :] += lax.dot_general(
                p.astype(jnp.bfloat16), grads[h], (((0,), (0,)), ((), ())),
                preferred_element_type=jnp.float32)
        return tuple(out)

    init = tuple(jnp.zeros((Q_BLOCK, width), jnp.float32) for _ in range(heads))
    final = lax.fori_loop(lo_ref[i], hi_ref[i], body, init)
    for h in range(heads):
        dq_ref[h] = final[h]


def attention_fwd(lo, hi, slopes, q, k, v, qinfo, kinfo, scale):
    heads, tokens, width = q.shape
    grid = (tokens // Q_BLOCK,)
    whole = lambda i, lo, hi: (0, 0, 0)
    rows = lambda i, lo, hi: (0, i, 0)
    return pl.pallas_call(
        functools.partial(fwd_kernel, heads, scale),
        grid_spec=pltpu.PrefetchScalarGridSpec(
            num_scalar_prefetch=2,
            grid=grid,
            in_specs=[
                pl.BlockSpec(memory_space=pltpu.SMEM),
                pl.BlockSpec((heads, Q_BLOCK, width), rows),
                pl.BlockSpec((heads, tokens, width), whole),
                pl.BlockSpec((heads, tokens, width), whole),
                pl.BlockSpec((Q_BLOCK, 3), lambda i, lo, hi: (i, 0)),
                pl.BlockSpec((3, tokens), lambda i, lo, hi: (0, 0)),
            ],
            out_specs=[
                pl.BlockSpec((heads, Q_BLOCK, width), rows),
                pl.BlockSpec((heads, Q_BLOCK, 1), rows),
            ],
        ),
        out_shape=[
            jax.ShapeDtypeStruct((heads, tokens, width), jnp.float32),
            jax.ShapeDtypeStruct((heads, tokens, 1), jnp.float32),
        ],
        compiler_params=pltpu.CompilerParams(dimension_semantics=("arbitrary",)),
    )(lo, hi, slopes, q, k, v, qinfo, kinfo)


def attention_bwd(lo, hi, slopes, q, k, v, qinfo, kinfo, o, do, lse, scale):
    heads, tokens, width = q.shape
    grid = (tokens // Q_BLOCK,)
    whole = lambda i, lo, hi: (0, 0, 0)
    rows = lambda i, lo, hi: (0, i, 0)
    return pl.pallas_call(
        functools.partial(bwd_kernel, heads, scale),
        grid_spec=pltpu.PrefetchScalarGridSpec(
            num_scalar_prefetch=2,
            grid=grid,
            in_specs=[
                pl.BlockSpec(memory_space=pltpu.SMEM),
                pl.BlockSpec((heads, Q_BLOCK, width), rows),
                pl.BlockSpec((heads, tokens, width), whole),
                pl.BlockSpec((heads, tokens, width), whole),
                pl.BlockSpec((Q_BLOCK, 3), lambda i, lo, hi: (i, 0)),
                pl.BlockSpec((3, tokens), lambda i, lo, hi: (0, 0)),
                pl.BlockSpec((heads, Q_BLOCK, width), rows),
                pl.BlockSpec((heads, Q_BLOCK, width), rows),
                pl.BlockSpec((heads, Q_BLOCK, 1), rows),
            ],
            out_specs=[
                pl.BlockSpec((heads, Q_BLOCK, width), rows),
                pl.BlockSpec((heads, tokens, width), whole),
                pl.BlockSpec((heads, tokens, width), whole),
            ],
        ),
        out_shape=[
            jax.ShapeDtypeStruct((heads, tokens, width), jnp.float32),
            jax.ShapeDtypeStruct((heads, tokens, width), jnp.float32),
            jax.ShapeDtypeStruct((heads, tokens, width), jnp.float32),
        ],
        compiler_params=pltpu.CompilerParams(dimension_semantics=("arbitrary",)),
    )(lo, hi, slopes, q, k, v, qinfo, kinfo, o, do, lse)


def scatter_tensor(partial, tensor_size, axis_name="tensor"):
    me = lax.axis_index(axis_name)
    blocks = partial.reshape((tensor_size, -1) + partial.shape[1:])
    total = lax.dynamic_index_in_dim(blocks, me, keepdims=False).astype(jnp.float32)
    for shift in range(1, tensor_size):
        outgoing = lax.dynamic_index_in_dim(blocks, (me + shift) % tensor_size, keepdims=False)
        pairs = [(i, (i + shift) % tensor_size) for i in range(tensor_size)]
        total = total + lax.ppermute(outgoing.astype(jnp.bfloat16), axis_name, pairs).astype(
            jnp.float32
        )
    return total


def direct_sum(values, axis_name, size):
    total = values
    for shift in range(1, size):
        pairs = [(i, (i + shift) % size) for i in range(size)]
        total = total + lax.ppermute(values, axis_name, pairs)
    return total


def on_device_body(
    dp_size,
    patches,
    counts,
    norm_gain,
    norm_bias,
    w_qkv,
    b_qv,
    w_out,
    out_bias,
    w_up,
    b_up,
    w_down,
    cotangent,
):
    local_rows = patches.shape[0]
    width_here = w_qkv.shape[2]
    heads_here = width_here // HEAD_DIM
    ff_here = w_up.shape[1]
    tensor_pos = lax.axis_index("tensor")
    tensor_size = D // width_here
    score_scale = HEAD_DIM ** (-0.5)
    segment, grid_row, grid_col, is_valid = layout(counts[0])
    keep_rows = lax.dynamic_slice_in_dim(is_valid, tensor_pos * local_rows, local_rows)[:, None]
    slopes = slopes_of(tensor_pos * heads_here, heads_here)
    inputs = patches.astype(jnp.float32)
    inputs_all = lax.all_gather(patches, "tensor", axis=0, tiled=True).astype(jnp.float32)
    normed = normalize(inputs_all, norm_gain[0], norm_bias[0]).astype(jnp.bfloat16)
    projected = jnp.einsum("td,dsc->tsc", normed, w_qkv, preferred_element_type=jnp.float32)
    queries = (projected[:, 0] + b_qv[0]).astype(jnp.bfloat16)
    keys = projected[:, 1].astype(jnp.bfloat16)
    values = (projected[:, 2] + b_qv[1]).astype(jnp.bfloat16)

    def head_major(rows):
        return rows.reshape(TOK_DEV, heads_here, HEAD_DIM).transpose(1, 0, 2)

    def row_major(heads):
        return heads.transpose(1, 0, 2).reshape(TOK_DEV, width_here)

    key_lo, key_hi = key_ranges(segment, TOK_DEV)
    segment_f = segment.astype(jnp.float32)
    query_info = jnp.stack([grid_row, grid_col, segment_f], axis=1)
    key_info = jnp.stack([grid_row, grid_col, segment_f], axis=0)
    query_heads = head_major(queries)
    key_heads = head_major(keys)
    value_heads = head_major(values)
    mixed_f32, log_totals = attention_fwd(
        key_lo, key_hi, slopes, query_heads, key_heads, value_heads, query_info, key_info, score_scale
    )
    upstream = cotangent.astype(jnp.float32)
    branch_grad = lax.all_gather(
        (keep_rows * upstream).astype(jnp.bfloat16), "tensor", axis=0, tiled=True
    )
    mixed_f32, log_totals, branch_grad = lax.optimization_barrier(
        (mixed_f32, log_totals, branch_grad)
    )
    mixed_rows = row_major(mixed_f32).astype(jnp.bfloat16)
    mixed_all = lax.all_gather(mixed_rows, "tensor", axis=1, tiled=True)
    w_out_all = lax.all_gather(w_out, "tensor", axis=0, tiled=True)
    attended = jnp.dot(mixed_all, w_out_all, preferred_element_type=jnp.float32)
    after_attn_all = inputs_all + is_valid[:, None] * (attended + out_bias[0])
    after_attn = lax.dynamic_slice_in_dim(after_attn_all, tensor_pos * local_rows, local_rows)
    normed_two = normalize(after_attn_all, norm_gain[1], norm_bias[1]).astype(jnp.bfloat16)
    hidden_pre = jnp.dot(normed_two, w_up, preferred_element_type=jnp.float32) + b_up
    hidden = jax.nn.gelu(hidden_pre, approximate=False).astype(jnp.bfloat16)
    branch_partial = jnp.dot(hidden, w_down, preferred_element_type=jnp.float32)
    down_bias_grad = jnp.sum(keep_rows * upstream, axis=0)
    w_down_grad_t = jnp.einsum(
        "td,tf->df", branch_grad, hidden, preferred_element_type=jnp.float32
    )
    hidden_grad = jnp.einsum("td,fd->tf", branch_grad, w_down, preferred_element_type=jnp.float32)
    _, gelu_back = jax.vjp(lambda pre_act: jax.nn.gelu(pre_act, approximate=False), hidden_pre)
    pre_grad = gelu_back(hidden_grad)[0].astype(jnp.bfloat16)
    up_bias_grad = jnp.sum(pre_grad, axis=0, dtype=jnp.float32)
    w_up_grad = jnp.einsum("td,tf->df", normed_two, pre_grad, preferred_element_type=jnp.float32)
    normed_two_grad = lax.psum_scatter(
        jnp.einsum("tf,df->td", pre_grad, w_up, preferred_element_type=jnp.float32).astype(
            jnp.bfloat16
        ),
        "tensor",
        scatter_dimension=0,
        tiled=True,
    ).astype(jnp.float32)
    _, norm_two_back = jax.vjp(normalize, after_attn, norm_gain[1], norm_bias[1])
    through_two, gain_two_grad, shift_two_grad = norm_two_back(normed_two_grad)
    after_grad = upstream + through_two
    attn_bias_grad = jnp.sum(keep_rows * after_grad, axis=0)
    attn_local = (keep_rows * after_grad).astype(jnp.bfloat16)
    attn_grad = lax.all_gather(attn_local, "tensor", axis=0, tiled=True)
    w_out_grad_t = jnp.einsum(
        "td,tc->dc", attn_grad, mixed_rows, preferred_element_type=jnp.float32
    )
    mixed_grad = jnp.einsum(
        "td,cd->tc", attn_grad, w_out, preferred_element_type=jnp.float32
    ).astype(jnp.bfloat16)
    early_parts = jnp.concatenate([w_down_grad_t, w_up_grad, w_out_grad_t], axis=1).astype(
        jnp.bfloat16
    )
    early_parts, mixed_grad, branch_partial = lax.optimization_barrier(
        (early_parts, mixed_grad, branch_partial)
    )
    branch = scatter_tensor(branch_partial, tensor_size)
    result = (after_attn + keep_rows * (branch + out_bias[1])).astype(jnp.bfloat16)
    early_sum = lax.psum_scatter(early_parts, "dp", scatter_dimension=0, tiled=True).astype(
        jnp.float32
    )
    query_acc, key_acc, value_acc = attention_bwd(
        key_lo, key_hi, slopes, query_heads, key_heads, value_heads, query_info, key_info,
        mixed_f32, head_major(mixed_grad), log_totals, score_scale,
    )
    query_acc, key_acc, value_acc, early_sum, result = lax.optimization_barrier(
        (query_acc, key_acc, value_acc, early_sum, result)
    )
    query_grad = row_major(query_acc * score_scale).astype(jnp.bfloat16)
    key_grad = row_major(key_acc * score_scale).astype(jnp.bfloat16)
    value_grad = row_major(value_acc).astype(jnp.bfloat16)
    projected_grad = jnp.concatenate([query_grad, key_grad, value_grad], axis=1)
    qv_bias_grad = jnp.stack(
        [
            jnp.sum(query_grad, axis=0, dtype=jnp.float32),
            jnp.sum(value_grad, axis=0, dtype=jnp.float32),
        ]
    )
    w_qkv_grad = jnp.einsum("td,tc->dc", normed, projected_grad, preferred_element_type=jnp.float32)
    normed_grad_partial = jnp.einsum(
        "tc,dc->td",
        projected_grad,
        w_qkv.reshape(D, 3 * width_here),
        preferred_element_type=jnp.float32,
    )
    centred_all = inputs_all - jnp.mean(inputs_all, axis=-1, keepdims=True)
    unit_all = centred_all * lax.rsqrt(
        jnp.mean(centred_all * centred_all, axis=-1, keepdims=True) + EPSILON
    )
    gain_one_grad = jnp.sum(normed_grad_partial * unit_all, axis=0)
    shift_one_grad = jnp.sum(normed_grad_partial, axis=0)
    normed_grad = scatter_tensor(normed_grad_partial, tensor_size)
    _, norm_one_back = jax.vjp(normalize, inputs, norm_gain[0], norm_bias[0])
    through_one = norm_one_back(normed_grad)[0]
    input_grad = (after_grad + through_one).astype(jnp.bfloat16)
    qv_full = lax.dynamic_update_slice_in_dim(
        jnp.zeros((2, D), jnp.float32), qv_bias_grad, tensor_pos * width_here, 1
    )
    up_full = lax.dynamic_update_slice_in_dim(
        jnp.zeros((FF,), jnp.float32), up_bias_grad, tensor_pos * ff_here, 0
    )
    small = jnp.concatenate(
        [
            jnp.stack([gain_one_grad, gain_two_grad]).reshape(-1),
            jnp.stack([shift_one_grad, shift_two_grad]).reshape(-1),
            jnp.stack([attn_bias_grad, down_bias_grad]).reshape(-1),
            qv_full.reshape(-1),
            up_full,
        ]
    )
    qkv_sum = scatter_tensor(w_qkv_grad.reshape(dp_size, -1), dp_size, "dp")
    qkv_part = qkv_sum.reshape(-1, 3, width_here)
    summed = direct_sum(direct_sum(small, "tensor", tensor_size), "dp", dp_size)
    gains_grad = summed[: 2 * D].reshape(2, D)
    shifts_grad = summed[2 * D : 4 * D].reshape(2, D)
    outer_grad = summed[4 * D : 6 * D].reshape(2, D)
    qv_sum = summed[6 * D : 8 * D].reshape(2, D)
    up_sum = summed[8 * D :]
    down_part = early_sum[:, :ff_here].T
    up_part = early_sum[:, ff_here : 2 * ff_here]
    out_part = early_sum[:, 2 * ff_here :].T
    return (
        result,
        input_grad,
        gains_grad,
        shifts_grad,
        qkv_part,
        qv_sum,
        out_part,
        outer_grad,
        up_part,
        up_sum,
        down_part,
    )


def solution(mesh):
    placed = (
        P(("dp", "tensor"), None),
        P("dp", None),
        P(),
        P(),
        P(None, None, "tensor"),
        P(None, "tensor"),
        P("tensor", None),
        P(),
        P(None, "tensor"),
        P("tensor"),
        P("tensor", None),
        P(("dp", "tensor"), None),
    )
    return jax.shard_map(
        functools.partial(on_device_body, mesh.shape["dp"]),
        mesh=mesh,
        in_specs=placed,
        out_specs=(
            P(("dp", "tensor"), None),
            P(("dp", "tensor"), None),
            P(),
            P(),
            P("dp", None, "tensor"),
            P(),
            P("tensor", "dp"),
            P(),
            P("dp", "tensor"),
            P(),
            P("tensor", "dp"),
        ),
        check_vma=False,
    )
```

```python
import functools

import jax
import jax.numpy as jnp
from jax import lax
from jax.experimental import pallas as pl
from jax.experimental.pallas import tpu as pltpu
from jax.sharding import PartitionSpec as P


D = 768
HEADS = 12
HEAD_DIM = 64
FF = 3072
SIDE_S = 12
SIDE_M = 15
SIDE_L = 20
TOK_DEV = 2048


EPSILON = 1e-06


def layout(group_counts):
    positions = jnp.arange(TOK_DEV, dtype=jnp.int32)
    area_small = SIDE_S * SIDE_S
    area_middle = SIDE_M * SIDE_M
    area_large = SIDE_L * SIDE_L
    end_small = group_counts[0] * area_small
    end_middle = end_small + group_counts[1] * area_middle
    end_large = end_middle + group_counts[2] * area_large
    size_class = (positions >= end_small).astype(jnp.int32) + (positions >= end_middle).astype(
        jnp.int32
    )
    begins = jnp.where(size_class == 0, 0, jnp.where(size_class == 1, end_small, end_middle))
    area_len = jnp.where(
        size_class == 0, area_small, jnp.where(size_class == 1, area_middle, area_large)
    )
    side_len = jnp.where(size_class == 0, SIDE_S, jnp.where(size_class == 1, SIDE_M, SIDE_L))
    within = positions - begins
    picture_index = within // area_len
    within_image = within % area_len
    is_valid = positions < end_large
    segment = jnp.where(is_valid, size_class * 16 + picture_index, 255)
    grid_row = (within_image // side_len).astype(jnp.float32)
    grid_col = (within_image % side_len).astype(jnp.float32)
    return (segment, grid_row, grid_col, is_valid.astype(jnp.float32))


def normalize(values, gain_row, shift_row):
    centred = values - jnp.mean(values, axis=-1, keepdims=True)
    spread = jnp.mean(centred * centred, axis=-1, keepdims=True)
    return centred * lax.rsqrt(spread + EPSILON) * gain_row + shift_row


def slopes_of(first_head, count_heads):
    head_number = (first_head + jnp.arange(count_heads, dtype=jnp.int32)).astype(jnp.float32) + 1.0
    return jnp.exp2(-8.0 * head_number / HEADS)


Q_BLOCK = 256
K_BLOCK = 256
NEG = -1e30


def key_ranges(segment, tokens):
    starts = jnp.arange(0, tokens, Q_BLOCK)
    first = segment[starts]
    last = segment[starts + Q_BLOCK - 1]
    key_lo = jnp.sum(segment[None, :] < first[:, None], axis=1)
    key_hi = jnp.sum(segment[None, :] <= last[:, None], axis=1)
    return (key_lo // K_BLOCK).astype(jnp.int32), ((key_hi + K_BLOCK - 1) // K_BLOCK).astype(jnp.int32)


def block_geometry(qi_ref, ki_ref, start):
    rq = qi_ref[:, 0:1]
    cq = qi_ref[:, 1:2]
    sq = qi_ref[:, 2:3]
    rk = ki_ref[0:1, pl.ds(start, K_BLOCK)]
    ck = ki_ref[1:2, pl.ds(start, K_BLOCK)]
    sk = ki_ref[2:3, pl.ds(start, K_BLOCK)]
    dr = rq - rk
    dc = cq - ck
    return jnp.sqrt(dr * dr + dc * dc), sq == sk


def fwd_kernel(heads, scale, lo_ref, hi_ref, slope_ref, q_ref, k_ref, v_ref, qi_ref, ki_ref, o_ref, lse_ref):
    i = pl.program_id(0)
    queries = [q_ref[h] for h in range(heads)]
    width = q_ref.shape[2]

    def body(kb, carry):
        start = pl.multiple_of(kb * K_BLOCK, K_BLOCK)
        dist, allowed = block_geometry(qi_ref, ki_ref, start)
        out = []
        for h in range(heads):
            m_old, l_old, acc_old = carry[h]
            keys = k_ref[h, pl.ds(start, K_BLOCK), :]
            vals = v_ref[h, pl.ds(start, K_BLOCK), :]
            s = lax.dot_general(queries[h], keys, (((1,), (1,)), ((), ())),
                                preferred_element_type=jnp.float32) * scale - slope_ref[h] * dist
            s = jnp.where(allowed, s, NEG)
            m_new = jnp.maximum(m_old, jnp.max(s, axis=1, keepdims=True))
            alpha = jnp.exp(m_old - m_new)
            p = jnp.exp(s - m_new)
            l_new = alpha * l_old + jnp.sum(p, axis=1, keepdims=True)
            acc_new = alpha * acc_old + jnp.dot(p.astype(jnp.bfloat16), vals,
                                                preferred_element_type=jnp.float32)
            out.append((m_new, l_new, acc_new))
        return tuple(out)

    init = tuple(
        (jnp.full((Q_BLOCK, 1), NEG, jnp.float32), jnp.zeros((Q_BLOCK, 1), jnp.float32),
         jnp.zeros((Q_BLOCK, width), jnp.float32))
        for _ in range(heads)
    )
    final = lax.fori_loop(lo_ref[i], hi_ref[i], body, init)
    for h in range(heads):
        m, l, acc = final[h]
        o_ref[h] = acc / l
        lse_ref[h] = m + jnp.log(l)


def bwd_kernel(heads, scale, lo_ref, hi_ref, slope_ref, q_ref, k_ref, v_ref, qi_ref, ki_ref,
               o_ref, do_ref, lse_ref, dq_ref, dk_ref, dv_ref):
    i = pl.program_id(0)

    @pl.when(i == 0)
    def _():
        dk_ref[...] = jnp.zeros_like(dk_ref)
        dv_ref[...] = jnp.zeros_like(dv_ref)

    queries = [q_ref[h] for h in range(heads)]
    grads = [do_ref[h] for h in range(heads)]
    lses = [lse_ref[h] for h in range(heads)]
    deltas = [jnp.sum(grads[h].astype(jnp.float32) * o_ref[h], axis=1, keepdims=True)
              for h in range(heads)]
    width = q_ref.shape[2]

    def body(kb, carry):
        start = pl.multiple_of(kb * K_BLOCK, K_BLOCK)
        dist, allowed = block_geometry(qi_ref, ki_ref, start)
        out = []
        for h in range(heads):
            keys = k_ref[h, pl.ds(start, K_BLOCK), :]
            vals = v_ref[h, pl.ds(start, K_BLOCK), :]
            s = lax.dot_general(queries[h], keys, (((1,), (1,)), ((), ())),
                                preferred_element_type=jnp.float32) * scale - slope_ref[h] * dist
            p = jnp.where(allowed, jnp.exp(s - lses[h]), 0.0)
            dp = lax.dot_general(grads[h], vals, (((1,), (1,)), ((), ())),
                                 preferred_element_type=jnp.float32)
            ds = (p * (dp - deltas[h])).astype(jnp.bfloat16)
            out.append(carry[h] + jnp.dot(ds, keys, preferred_element_type=jnp.float32))
            dk_ref[h, pl.ds(start, K_BLOCK), :] += lax.dot_general(
                ds, queries[h], (((0,), (0,)), ((), ())), preferred_element_type=jnp.float32)
            dv_ref[h, pl.ds(start, K_BLOCK), :] += lax.dot_general(
                p.astype(jnp.bfloat16), grads[h], (((0,), (0,)), ((), ())),
                preferred_element_type=jnp.float32)
        return tuple(out)

    init = tuple(jnp.zeros((Q_BLOCK, width), jnp.float32) for _ in range(heads))
    final = lax.fori_loop(lo_ref[i], hi_ref[i], body, init)
    for h in range(heads):
        dq_ref[h] = final[h]


def attention_fwd(lo, hi, slopes, q, k, v, qinfo, kinfo, scale):
    heads, tokens, width = q.shape
    grid = (tokens // Q_BLOCK,)
    whole = lambda i, lo, hi: (0, 0, 0)
    rows = lambda i, lo, hi: (0, i, 0)
    return pl.pallas_call(
        functools.partial(fwd_kernel, heads, scale),
        grid_spec=pltpu.PrefetchScalarGridSpec(
            num_scalar_prefetch=2,
            grid=grid,
            in_specs=[
                pl.BlockSpec(memory_space=pltpu.SMEM),
                pl.BlockSpec((heads, Q_BLOCK, width), rows),
                pl.BlockSpec((heads, tokens, width), whole),
                pl.BlockSpec((heads, tokens, width), whole),
                pl.BlockSpec((Q_BLOCK, 3), lambda i, lo, hi: (i, 0)),
                pl.BlockSpec((3, tokens), lambda i, lo, hi: (0, 0)),
            ],
            out_specs=[
                pl.BlockSpec((heads, Q_BLOCK, width), rows),
                pl.BlockSpec((heads, Q_BLOCK, 1), rows),
            ],
        ),
        out_shape=[
            jax.ShapeDtypeStruct((heads, tokens, width), jnp.float32),
            jax.ShapeDtypeStruct((heads, tokens, 1), jnp.float32),
        ],
        compiler_params=pltpu.CompilerParams(dimension_semantics=("arbitrary",)),
    )(lo, hi, slopes, q, k, v, qinfo, kinfo)


def attention_bwd(lo, hi, slopes, q, k, v, qinfo, kinfo, o, do, lse, scale):
    heads, tokens, width = q.shape
    grid = (tokens // Q_BLOCK,)
    whole = lambda i, lo, hi: (0, 0, 0)
    rows = lambda i, lo, hi: (0, i, 0)
    return pl.pallas_call(
        functools.partial(bwd_kernel, heads, scale),
        grid_spec=pltpu.PrefetchScalarGridSpec(
            num_scalar_prefetch=2,
            grid=grid,
            in_specs=[
                pl.BlockSpec(memory_space=pltpu.SMEM),
                pl.BlockSpec((heads, Q_BLOCK, width), rows),
                pl.BlockSpec((heads, tokens, width), whole),
                pl.BlockSpec((heads, tokens, width), whole),
                pl.BlockSpec((Q_BLOCK, 3), lambda i, lo, hi: (i, 0)),
                pl.BlockSpec((3, tokens), lambda i, lo, hi: (0, 0)),
                pl.BlockSpec((heads, Q_BLOCK, width), rows),
                pl.BlockSpec((heads, Q_BLOCK, width), rows),
                pl.BlockSpec((heads, Q_BLOCK, 1), rows),
            ],
            out_specs=[
                pl.BlockSpec((heads, Q_BLOCK, width), rows),
                pl.BlockSpec((heads, tokens, width), whole),
                pl.BlockSpec((heads, tokens, width), whole),
            ],
        ),
        out_shape=[
            jax.ShapeDtypeStruct((heads, tokens, width), jnp.float32),
            jax.ShapeDtypeStruct((heads, tokens, width), jnp.float32),
            jax.ShapeDtypeStruct((heads, tokens, width), jnp.float32),
        ],
        compiler_params=pltpu.CompilerParams(dimension_semantics=("arbitrary",)),
    )(lo, hi, slopes, q, k, v, qinfo, kinfo, o, do, lse)


def scatter_tensor(partial, tensor_size):
    me = lax.axis_index("tensor")
    blocks = partial.reshape(tensor_size, -1, partial.shape[1])
    total = lax.dynamic_index_in_dim(blocks, me, keepdims=False).astype(jnp.float32)
    for shift in range(1, tensor_size):
        outgoing = lax.dynamic_index_in_dim(blocks, (me + shift) % tensor_size, keepdims=False)
        pairs = [(i, (i + shift) % tensor_size) for i in range(tensor_size)]
        total = total + lax.ppermute(outgoing.astype(jnp.bfloat16), "tensor", pairs).astype(
            jnp.float32
        )
    return total


def halving_scatter(blocks, axis_name, wire):
    me = lax.axis_index(axis_name)
    bit = 0
    while blocks.shape[0] > 1:
        pairs = [(i, i ^ (1 << bit)) for i in range(blocks.shape[0] << bit)]
        halves = blocks.reshape((blocks.shape[0] // 2, 2) + blocks.shape[1:])
        mine = (me >> bit) & 1
        keep = lax.dynamic_index_in_dim(halves, mine, axis=1, keepdims=False)
        send = lax.dynamic_index_in_dim(halves, 1 - mine, axis=1, keepdims=False)
        arrived = lax.ppermute(send.astype(wire), axis_name, pairs)
        blocks = keep + arrived.astype(blocks.dtype)
        bit += 1
    return blocks[0]


def doubling_sum(values, axis_name, size):
    bit = 0
    while (1 << bit) < size:
        pairs = [(i, i ^ (1 << bit)) for i in range(size)]
        values = values + lax.ppermute(values, axis_name, pairs)
        bit += 1
    return values


def on_device_body(
    dp_size,
    patches,
    counts,
    norm_gain,
    norm_bias,
    w_qkv,
    b_qv,
    w_out,
    out_bias,
    w_up,
    b_up,
    w_down,
    cotangent,
):
    local_rows = patches.shape[0]
    width_here = w_qkv.shape[2]
    heads_here = width_here // HEAD_DIM
    ff_here = w_up.shape[1]
    tensor_pos = lax.axis_index("tensor")
    tensor_size = D // width_here
    score_scale = HEAD_DIM ** (-0.5)
    segment, grid_row, grid_col, is_valid = layout(counts[0])
    keep_rows = lax.dynamic_slice_in_dim(is_valid, tensor_pos * local_rows, local_rows)[:, None]
    slopes = slopes_of(tensor_pos * heads_here, heads_here)
    inputs = patches.astype(jnp.float32)
    inputs_all = lax.all_gather(patches, "tensor", axis=0, tiled=True).astype(jnp.float32)
    normed = normalize(inputs_all, norm_gain[0], norm_bias[0]).astype(jnp.bfloat16)
    projected = jnp.einsum("td,dsc->tsc", normed, w_qkv, preferred_element_type=jnp.float32)
    queries = (projected[:, 0] + b_qv[0]).astype(jnp.bfloat16)
    keys = projected[:, 1].astype(jnp.bfloat16)
    values = (projected[:, 2] + b_qv[1]).astype(jnp.bfloat16)

    def head_major(rows):
        return rows.reshape(TOK_DEV, heads_here, HEAD_DIM).transpose(1, 0, 2)

    def row_major(heads):
        return heads.transpose(1, 0, 2).reshape(TOK_DEV, width_here)

    key_lo, key_hi = key_ranges(segment, TOK_DEV)
    segment_f = segment.astype(jnp.float32)
    query_info = jnp.stack([grid_row, grid_col, segment_f], axis=1)
    key_info = jnp.stack([grid_row, grid_col, segment_f], axis=0)
    query_heads = head_major(queries)
    key_heads = head_major(keys)
    value_heads = head_major(values)
    mixed_f32, log_totals = attention_fwd(
        key_lo, key_hi, slopes, query_heads, key_heads, value_heads, query_info, key_info, score_scale
    )
    upstream = cotangent.astype(jnp.float32)
    branch_grad = lax.all_gather(
        (keep_rows * upstream).astype(jnp.bfloat16), "tensor", axis=0, tiled=True
    )
    mixed_f32, log_totals, branch_grad = lax.optimization_barrier(
        (mixed_f32, log_totals, branch_grad)
    )
    mixed_rows = row_major(mixed_f32).astype(jnp.bfloat16)
    mixed_all = lax.all_gather(mixed_rows, "tensor", axis=1, tiled=True)
    w_out_all = lax.all_gather(w_out, "tensor", axis=0, tiled=True)
    attended = jnp.dot(mixed_all, w_out_all, preferred_element_type=jnp.float32)
    after_attn_all = inputs_all + is_valid[:, None] * (attended + out_bias[0])
    after_attn = lax.dynamic_slice_in_dim(after_attn_all, tensor_pos * local_rows, local_rows)
    normed_two = normalize(after_attn_all, norm_gain[1], norm_bias[1]).astype(jnp.bfloat16)
    hidden_pre = jnp.dot(normed_two, w_up, preferred_element_type=jnp.float32) + b_up
    hidden = jax.nn.gelu(hidden_pre, approximate=False).astype(jnp.bfloat16)
    branch_partial = jnp.dot(hidden, w_down, preferred_element_type=jnp.float32)
    down_bias_grad = jnp.sum(keep_rows * upstream, axis=0)
    w_down_grad_t = jnp.einsum("td,tf->df", branch_grad, hidden, preferred_element_type=jnp.float32)
    hidden_grad = jnp.einsum("td,fd->tf", branch_grad, w_down, preferred_element_type=jnp.float32)
    _, gelu_back = jax.vjp(lambda pre_act: jax.nn.gelu(pre_act, approximate=False), hidden_pre)
    pre_grad = gelu_back(hidden_grad)[0].astype(jnp.bfloat16)
    up_bias_grad = jnp.sum(pre_grad, axis=0, dtype=jnp.float32)
    w_up_grad = jnp.einsum("td,tf->df", normed_two, pre_grad, preferred_element_type=jnp.float32)
    two_partial = jnp.einsum("tf,df->td", pre_grad, w_up, preferred_element_type=jnp.float32)
    normed_two_grad = lax.psum_scatter(
        two_partial.astype(jnp.bfloat16), "tensor", scatter_dimension=0, tiled=True
    ).astype(jnp.float32)
    _, norm_two_back = jax.vjp(normalize, after_attn, norm_gain[1], norm_bias[1])
    through_two, gain_two_grad, shift_two_grad = norm_two_back(normed_two_grad)
    after_grad = upstream + through_two
    attn_bias_grad = jnp.sum(keep_rows * after_grad, axis=0)
    attn_local = (keep_rows * after_grad).astype(jnp.bfloat16)
    attn_grad = lax.all_gather(attn_local, "tensor", axis=0, tiled=True)
    w_out_grad_t = jnp.einsum(
        "td,tc->dc", attn_grad, mixed_rows, preferred_element_type=jnp.float32
    )
    mixed_grad = jnp.einsum(
        "td,cd->tc", attn_grad, w_out, preferred_element_type=jnp.float32
    ).astype(jnp.bfloat16)
    early_parts = jnp.concatenate([w_down_grad_t, w_up_grad, w_out_grad_t], axis=1).astype(
        jnp.bfloat16
    )
    early_parts, mixed_grad, branch_partial = lax.optimization_barrier(
        (early_parts, mixed_grad, branch_partial)
    )
    branch = scatter_tensor(branch_partial, tensor_size)
    result = (after_attn + keep_rows * (branch + out_bias[1])).astype(jnp.bfloat16)
    early_sum = lax.psum_scatter(early_parts, "dp", scatter_dimension=0, tiled=True).astype(
        jnp.float32
    )
    query_acc, key_acc, value_acc = attention_bwd(
        key_lo, key_hi, slopes, query_heads, key_heads, value_heads, query_info, key_info,
        mixed_f32, head_major(mixed_grad), log_totals, score_scale,
    )
    query_acc, key_acc, value_acc, early_sum, result = lax.optimization_barrier(
        (query_acc, key_acc, value_acc, early_sum, result)
    )
    query_grad = row_major(query_acc * score_scale).astype(jnp.bfloat16)
    key_grad = row_major(key_acc * score_scale).astype(jnp.bfloat16)
    value_grad = row_major(value_acc).astype(jnp.bfloat16)
    projected_grad = jnp.concatenate([query_grad, key_grad, value_grad], axis=1)
    qv_bias_grad = jnp.stack(
        [
            jnp.sum(query_grad, axis=0, dtype=jnp.float32),
            jnp.sum(value_grad, axis=0, dtype=jnp.float32),
        ]
    )
    w_qkv_grad = jnp.einsum("td,tc->dc", normed, projected_grad, preferred_element_type=jnp.float32)
    normed_grad_partial = jnp.einsum(
        "tc,dc->td",
        projected_grad,
        w_qkv.reshape(D, 3 * width_here),
        preferred_element_type=jnp.float32,
    )
    centred_all = inputs_all - jnp.mean(inputs_all, axis=-1, keepdims=True)
    unit_all = centred_all * lax.rsqrt(
        jnp.mean(centred_all * centred_all, axis=-1, keepdims=True) + EPSILON
    )
    gain_one_grad = jnp.sum(normed_grad_partial * unit_all, axis=0)
    shift_one_grad = jnp.sum(normed_grad_partial, axis=0)
    normed_grad = scatter_tensor(normed_grad_partial, tensor_size)
    _, norm_one_back = jax.vjp(normalize, inputs, norm_gain[0], norm_bias[0])
    through_one = norm_one_back(normed_grad)[0]
    input_grad = (after_grad + through_one).astype(jnp.bfloat16)
    qv_full = lax.dynamic_update_slice_in_dim(
        jnp.zeros((2, D), jnp.float32), qv_bias_grad, tensor_pos * width_here, 1
    )
    up_full = lax.dynamic_update_slice_in_dim(
        jnp.zeros((FF,), jnp.float32), up_bias_grad, tensor_pos * ff_here, 0
    )
    small = jnp.concatenate(
        [
            jnp.stack([gain_one_grad, gain_two_grad]).reshape(-1),
            jnp.stack([shift_one_grad, shift_two_grad]).reshape(-1),
            jnp.stack([attn_bias_grad, down_bias_grad]).reshape(-1),
            qv_full.reshape(-1),
            up_full,
        ]
    )
    qkv_sum = halving_scatter(w_qkv_grad.reshape(dp_size, -1), "dp", jnp.bfloat16)
    qkv_part = qkv_sum.reshape(-1, 3, width_here)
    summed = doubling_sum(doubling_sum(small, "dp", dp_size), "tensor", tensor_size)
    gains_grad = summed[: 2 * D].reshape(2, D)
    shifts_grad = summed[2 * D : 4 * D].reshape(2, D)
    outer_grad = summed[4 * D : 6 * D].reshape(2, D)
    qv_sum = summed[6 * D : 8 * D].reshape(2, D)
    up_sum = summed[8 * D :]
    down_part = early_sum[:, :ff_here].T
    up_part = early_sum[:, ff_here : 2 * ff_here]
    out_part = early_sum[:, 2 * ff_here :].T
    return (
        result,
        input_grad,
        gains_grad,
        shifts_grad,
        qkv_part,
        qv_sum,
        out_part,
        outer_grad,
        up_part,
        up_sum,
        down_part,
    )


def solution(mesh):
    placed = (
        P(("dp", "tensor"), None),
        P("dp", None),
        P(),
        P(),
        P(None, None, "tensor"),
        P(None, "tensor"),
        P("tensor", None),
        P(),
        P(None, "tensor"),
        P("tensor"),
        P("tensor", None),
        P(("dp", "tensor"), None),
    )
    return jax.shard_map(
        functools.partial(on_device_body, mesh.shape["dp"]),
        mesh=mesh,
        in_specs=placed,
        out_specs=(
            P(("dp", "tensor"), None),
            P(("dp", "tensor"), None),
            P(),
            P(),
            P("dp", None, "tensor"),
            P(),
            P("tensor", "dp"),
            P(),
            P("dp", "tensor"),
            P(),
            P("tensor", "dp"),
        ),
        check_vma=False,
    )
```

```python
import functools

import jax
import jax.numpy as jnp
from jax import lax
from jax.experimental import pallas as pl
from jax.experimental.pallas import tpu as pltpu
from jax.sharding import PartitionSpec as P


D = 768
HEADS = 12
HEAD_DIM = 64
FF = 3072
SIDE_S = 12
SIDE_M = 15
SIDE_L = 20
TOK_DEV = 2048


EPSILON = 1e-06


def layout(group_counts):
    positions = jnp.arange(TOK_DEV, dtype=jnp.int32)
    area_small = SIDE_S * SIDE_S
    area_middle = SIDE_M * SIDE_M
    area_large = SIDE_L * SIDE_L
    end_small = group_counts[0] * area_small
    end_middle = end_small + group_counts[1] * area_middle
    end_large = end_middle + group_counts[2] * area_large
    size_class = (positions >= end_small).astype(jnp.int32) + (positions >= end_middle).astype(
        jnp.int32
    )
    begins = jnp.where(size_class == 0, 0, jnp.where(size_class == 1, end_small, end_middle))
    area_len = jnp.where(
        size_class == 0, area_small, jnp.where(size_class == 1, area_middle, area_large)
    )
    side_len = jnp.where(size_class == 0, SIDE_S, jnp.where(size_class == 1, SIDE_M, SIDE_L))
    within = positions - begins
    picture_index = within // area_len
    within_image = within % area_len
    is_valid = positions < end_large
    segment = jnp.where(is_valid, size_class * 16 + picture_index, 255)
    grid_row = (within_image // side_len).astype(jnp.float32)
    grid_col = (within_image % side_len).astype(jnp.float32)
    return (segment, grid_row, grid_col, is_valid.astype(jnp.float32))


def normalize(values, gain_row, shift_row):
    centred = values - jnp.mean(values, axis=-1, keepdims=True)
    spread = jnp.mean(centred * centred, axis=-1, keepdims=True)
    return centred * lax.rsqrt(spread + EPSILON) * gain_row + shift_row


def slopes_of(first_head, count_heads):
    head_number = (first_head + jnp.arange(count_heads, dtype=jnp.int32)).astype(jnp.float32) + 1.0
    return jnp.exp2(-8.0 * head_number / HEADS)


Q_BLOCK = 256
K_BLOCK = 256
NEG = -1e30


def key_ranges(segment, tokens):
    starts = jnp.arange(0, tokens, Q_BLOCK)
    first = segment[starts]
    last = segment[starts + Q_BLOCK - 1]
    key_lo = jnp.sum(segment[None, :] < first[:, None], axis=1)
    key_hi = jnp.sum(segment[None, :] <= last[:, None], axis=1)
    return (key_lo // K_BLOCK).astype(jnp.int32), ((key_hi + K_BLOCK - 1) // K_BLOCK).astype(jnp.int32)


def block_geometry(qi_ref, ki_ref, start):
    rq = qi_ref[:, 0:1]
    cq = qi_ref[:, 1:2]
    sq = qi_ref[:, 2:3]
    rk = ki_ref[0:1, pl.ds(start, K_BLOCK)]
    ck = ki_ref[1:2, pl.ds(start, K_BLOCK)]
    sk = ki_ref[2:3, pl.ds(start, K_BLOCK)]
    dr = rq - rk
    dc = cq - ck
    return jnp.sqrt(dr * dr + dc * dc), sq == sk


def fwd_kernel(heads, scale, lo_ref, hi_ref, slope_ref, q_ref, k_ref, v_ref, qi_ref, ki_ref, o_ref, lse_ref):
    i = pl.program_id(0)
    queries = [q_ref[h] for h in range(heads)]
    width = q_ref.shape[2]

    def body(kb, carry):
        start = pl.multiple_of(kb * K_BLOCK, K_BLOCK)
        dist, allowed = block_geometry(qi_ref, ki_ref, start)
        out = []
        for h in range(heads):
            m_old, l_old, acc_old = carry[h]
            keys = k_ref[h, pl.ds(start, K_BLOCK), :]
            vals = v_ref[h, pl.ds(start, K_BLOCK), :]
            s = lax.dot_general(queries[h], keys, (((1,), (1,)), ((), ())),
                                preferred_element_type=jnp.float32) * scale - slope_ref[h] * dist
            s = jnp.where(allowed, s, NEG)
            m_new = jnp.maximum(m_old, jnp.max(s, axis=1, keepdims=True))
            alpha = jnp.exp(m_old - m_new)
            p = jnp.exp(s - m_new)
            l_new = alpha * l_old + jnp.sum(p, axis=1, keepdims=True)
            acc_new = alpha * acc_old + jnp.dot(p.astype(jnp.bfloat16), vals,
                                                preferred_element_type=jnp.float32)
            out.append((m_new, l_new, acc_new))
        return tuple(out)

    init = tuple(
        (jnp.full((Q_BLOCK, 1), NEG, jnp.float32), jnp.zeros((Q_BLOCK, 1), jnp.float32),
         jnp.zeros((Q_BLOCK, width), jnp.float32))
        for _ in range(heads)
    )
    final = lax.fori_loop(lo_ref[i], hi_ref[i], body, init)
    for h in range(heads):
        m, l, acc = final[h]
        o_ref[h] = acc / l
        lse_ref[h] = m + jnp.log(l)


def bwd_kernel(heads, scale, lo_ref, hi_ref, slope_ref, q_ref, k_ref, v_ref, qi_ref, ki_ref,
               o_ref, do_ref, lse_ref, dq_ref, dk_ref, dv_ref):
    i = pl.program_id(0)

    @pl.when(i == 0)
    def _():
        dk_ref[...] = jnp.zeros_like(dk_ref)
        dv_ref[...] = jnp.zeros_like(dv_ref)

    queries = [q_ref[h] for h in range(heads)]
    grads = [do_ref[h] for h in range(heads)]
    lses = [lse_ref[h] for h in range(heads)]
    deltas = [jnp.sum(grads[h].astype(jnp.float32) * o_ref[h], axis=1, keepdims=True)
              for h in range(heads)]
    width = q_ref.shape[2]

    def body(kb, carry):
        start = pl.multiple_of(kb * K_BLOCK, K_BLOCK)
        dist, allowed = block_geometry(qi_ref, ki_ref, start)
        out = []
        for h in range(heads):
            keys = k_ref[h, pl.ds(start, K_BLOCK), :]
            vals = v_ref[h, pl.ds(start, K_BLOCK), :]
            s = lax.dot_general(queries[h], keys, (((1,), (1,)), ((), ())),
                                preferred_element_type=jnp.float32) * scale - slope_ref[h] * dist
            p = jnp.where(allowed, jnp.exp(s - lses[h]), 0.0)
            dp = lax.dot_general(grads[h], vals, (((1,), (1,)), ((), ())),
                                 preferred_element_type=jnp.float32)
            ds = (p * (dp - deltas[h])).astype(jnp.bfloat16)
            out.append(carry[h] + jnp.dot(ds, keys, preferred_element_type=jnp.float32))
            dk_ref[h, pl.ds(start, K_BLOCK), :] += lax.dot_general(
                ds, queries[h], (((0,), (0,)), ((), ())), preferred_element_type=jnp.float32)
            dv_ref[h, pl.ds(start, K_BLOCK), :] += lax.dot_general(
                p.astype(jnp.bfloat16), grads[h], (((0,), (0,)), ((), ())),
                preferred_element_type=jnp.float32)
        return tuple(out)

    init = tuple(jnp.zeros((Q_BLOCK, width), jnp.float32) for _ in range(heads))
    final = lax.fori_loop(lo_ref[i], hi_ref[i], body, init)
    for h in range(heads):
        dq_ref[h] = final[h]


def attention_fwd(lo, hi, slopes, q, k, v, qinfo, kinfo, scale):
    heads, tokens, width = q.shape
    grid = (tokens // Q_BLOCK,)
    whole = lambda i, lo, hi: (0, 0, 0)
    rows = lambda i, lo, hi: (0, i, 0)
    return pl.pallas_call(
        functools.partial(fwd_kernel, heads, scale),
        grid_spec=pltpu.PrefetchScalarGridSpec(
            num_scalar_prefetch=2,
            grid=grid,
            in_specs=[
                pl.BlockSpec(memory_space=pltpu.SMEM),
                pl.BlockSpec((heads, Q_BLOCK, width), rows),
                pl.BlockSpec((heads, tokens, width), whole),
                pl.BlockSpec((heads, tokens, width), whole),
                pl.BlockSpec((Q_BLOCK, 3), lambda i, lo, hi: (i, 0)),
                pl.BlockSpec((3, tokens), lambda i, lo, hi: (0, 0)),
            ],
            out_specs=[
                pl.BlockSpec((heads, Q_BLOCK, width), rows),
                pl.BlockSpec((heads, Q_BLOCK, 1), rows),
            ],
        ),
        out_shape=[
            jax.ShapeDtypeStruct((heads, tokens, width), jnp.float32),
            jax.ShapeDtypeStruct((heads, tokens, 1), jnp.float32),
        ],
        compiler_params=pltpu.CompilerParams(dimension_semantics=("arbitrary",)),
    )(lo, hi, slopes, q, k, v, qinfo, kinfo)


def attention_bwd(lo, hi, slopes, q, k, v, qinfo, kinfo, o, do, lse, scale):
    heads, tokens, width = q.shape
    grid = (tokens // Q_BLOCK,)
    whole = lambda i, lo, hi: (0, 0, 0)
    rows = lambda i, lo, hi: (0, i, 0)
    return pl.pallas_call(
        functools.partial(bwd_kernel, heads, scale),
        grid_spec=pltpu.PrefetchScalarGridSpec(
            num_scalar_prefetch=2,
            grid=grid,
            in_specs=[
                pl.BlockSpec(memory_space=pltpu.SMEM),
                pl.BlockSpec((heads, Q_BLOCK, width), rows),
                pl.BlockSpec((heads, tokens, width), whole),
                pl.BlockSpec((heads, tokens, width), whole),
                pl.BlockSpec((Q_BLOCK, 3), lambda i, lo, hi: (i, 0)),
                pl.BlockSpec((3, tokens), lambda i, lo, hi: (0, 0)),
                pl.BlockSpec((heads, Q_BLOCK, width), rows),
                pl.BlockSpec((heads, Q_BLOCK, width), rows),
                pl.BlockSpec((heads, Q_BLOCK, 1), rows),
            ],
            out_specs=[
                pl.BlockSpec((heads, Q_BLOCK, width), rows),
                pl.BlockSpec((heads, tokens, width), whole),
                pl.BlockSpec((heads, tokens, width), whole),
            ],
        ),
        out_shape=[
            jax.ShapeDtypeStruct((heads, tokens, width), jnp.float32),
            jax.ShapeDtypeStruct((heads, tokens, width), jnp.float32),
            jax.ShapeDtypeStruct((heads, tokens, width), jnp.float32),
        ],
        compiler_params=pltpu.CompilerParams(dimension_semantics=("arbitrary",)),
    )(lo, hi, slopes, q, k, v, qinfo, kinfo, o, do, lse)


def scatter_tensor(partial, tensor_size):
    me = lax.axis_index("tensor")
    blocks = partial.reshape(tensor_size, -1, partial.shape[1])
    total = lax.dynamic_index_in_dim(blocks, me, keepdims=False).astype(jnp.float32)
    for shift in range(1, tensor_size):
        outgoing = lax.dynamic_index_in_dim(blocks, (me + shift) % tensor_size, keepdims=False)
        pairs = [(i, (i + shift) % tensor_size) for i in range(tensor_size)]
        total = total + lax.ppermute(outgoing.astype(jnp.bfloat16), "tensor", pairs).astype(
            jnp.float32
        )
    return total


def halving_scatter(blocks, axis_name, wire):
    me = lax.axis_index(axis_name)
    bit = 0
    while blocks.shape[0] > 1:
        pairs = [(i, i ^ (1 << bit)) for i in range(blocks.shape[0] << bit)]
        halves = blocks.reshape((blocks.shape[0] // 2, 2) + blocks.shape[1:])
        mine = (me >> bit) & 1
        keep = lax.dynamic_index_in_dim(halves, mine, axis=1, keepdims=False)
        send = lax.dynamic_index_in_dim(halves, 1 - mine, axis=1, keepdims=False)
        arrived = lax.ppermute(send.astype(wire), axis_name, pairs)
        blocks = keep + arrived.astype(blocks.dtype)
        bit += 1
    return blocks[0]


def doubling_sum(values, axis_name, size):
    bit = 0
    while (1 << bit) < size:
        pairs = [(i, i ^ (1 << bit)) for i in range(size)]
        values = values + lax.ppermute(values, axis_name, pairs)
        bit += 1
    return values


def on_device_body(
    dp_size,
    patches,
    counts,
    norm_gain,
    norm_bias,
    w_qkv,
    b_qv,
    w_out,
    out_bias,
    w_up,
    b_up,
    w_down,
    cotangent,
):
    local_rows = patches.shape[0]
    width_here = w_qkv.shape[2]
    heads_here = width_here // HEAD_DIM
    ff_here = w_up.shape[1]
    tensor_pos = lax.axis_index("tensor")
    tensor_size = D // width_here
    score_scale = HEAD_DIM ** (-0.5)
    segment, grid_row, grid_col, is_valid = layout(counts[0])
    keep_rows = lax.dynamic_slice_in_dim(is_valid, tensor_pos * local_rows, local_rows)[:, None]
    slopes = slopes_of(tensor_pos * heads_here, heads_here)
    inputs = patches.astype(jnp.float32)
    inputs_all = lax.all_gather(patches, "tensor", axis=0, tiled=True).astype(jnp.float32)
    normed = normalize(inputs_all, norm_gain[0], norm_bias[0]).astype(jnp.bfloat16)
    projected = jnp.einsum("td,dsc->tsc", normed, w_qkv, preferred_element_type=jnp.float32)
    queries = (projected[:, 0] + b_qv[0]).astype(jnp.bfloat16)
    keys = projected[:, 1].astype(jnp.bfloat16)
    values = (projected[:, 2] + b_qv[1]).astype(jnp.bfloat16)

    def head_major(rows):
        return rows.reshape(TOK_DEV, heads_here, HEAD_DIM).transpose(1, 0, 2)

    def row_major(heads):
        return heads.transpose(1, 0, 2).reshape(TOK_DEV, width_here)

    key_lo, key_hi = key_ranges(segment, TOK_DEV)
    segment_f = segment.astype(jnp.float32)
    query_info = jnp.stack([grid_row, grid_col, segment_f], axis=1)
    key_info = jnp.stack([grid_row, grid_col, segment_f], axis=0)
    query_heads = head_major(queries)
    key_heads = head_major(keys)
    value_heads = head_major(values)
    mixed_f32, log_totals = attention_fwd(
        key_lo, key_hi, slopes, query_heads, key_heads, value_heads, query_info, key_info, score_scale
    )
    upstream = cotangent.astype(jnp.float32)
    branch_grad = lax.all_gather(
        (keep_rows * upstream).astype(jnp.bfloat16), "tensor", axis=0, tiled=True
    )
    mixed_f32, log_totals, branch_grad = lax.optimization_barrier(
        (mixed_f32, log_totals, branch_grad)
    )
    mixed_rows = row_major(mixed_f32).astype(jnp.bfloat16)
    mixed_all = lax.all_gather(mixed_rows, "tensor", axis=1, tiled=True)
    w_out_all = lax.all_gather(w_out, "tensor", axis=0, tiled=True)
    attended = jnp.dot(mixed_all, w_out_all, preferred_element_type=jnp.float32)
    after_attn_all = inputs_all + is_valid[:, None] * (attended + out_bias[0])
    after_attn = lax.dynamic_slice_in_dim(after_attn_all, tensor_pos * local_rows, local_rows)
    normed_two = normalize(after_attn_all, norm_gain[1], norm_bias[1]).astype(jnp.bfloat16)
    hidden_pre = jnp.dot(normed_two, w_up, preferred_element_type=jnp.float32) + b_up
    hidden = jax.nn.gelu(hidden_pre, approximate=False).astype(jnp.bfloat16)
    branch_partial = jnp.dot(hidden, w_down, preferred_element_type=jnp.float32)
    down_bias_grad = jnp.sum(keep_rows * upstream, axis=0)
    w_down_grad_t = jnp.einsum(
        "td,tf->df", branch_grad, hidden, preferred_element_type=jnp.float32
    )
    hidden_grad = jnp.einsum("td,fd->tf", branch_grad, w_down, preferred_element_type=jnp.float32)
    _, gelu_back = jax.vjp(lambda pre_act: jax.nn.gelu(pre_act, approximate=False), hidden_pre)
    pre_grad = gelu_back(hidden_grad)[0].astype(jnp.bfloat16)
    up_bias_grad = jnp.sum(pre_grad, axis=0, dtype=jnp.float32)
    w_up_grad = jnp.einsum("td,tf->df", normed_two, pre_grad, preferred_element_type=jnp.float32)
    normed_two_grad = lax.psum_scatter(
        jnp.einsum("tf,df->td", pre_grad, w_up, preferred_element_type=jnp.float32).astype(
            jnp.bfloat16
        ),
        "tensor",
        scatter_dimension=0,
        tiled=True,
    ).astype(jnp.float32)
    _, norm_two_back = jax.vjp(normalize, after_attn, norm_gain[1], norm_bias[1])
    through_two, gain_two_grad, shift_two_grad = norm_two_back(normed_two_grad)
    after_grad = upstream + through_two
    attn_bias_grad = jnp.sum(keep_rows * after_grad, axis=0)
    attn_local = (keep_rows * after_grad).astype(jnp.bfloat16)
    attn_grad = lax.all_gather(attn_local, "tensor", axis=0, tiled=True)
    w_out_grad_t = jnp.einsum(
        "td,tc->dc", attn_grad, mixed_rows, preferred_element_type=jnp.float32
    )
    mixed_grad = jnp.einsum(
        "td,cd->tc", attn_grad, w_out, preferred_element_type=jnp.float32
    ).astype(jnp.bfloat16)
    early_parts = jnp.concatenate([w_down_grad_t, w_up_grad, w_out_grad_t], axis=1).astype(
        jnp.bfloat16
    )
    early_parts, mixed_grad, branch_partial = lax.optimization_barrier(
        (early_parts, mixed_grad, branch_partial)
    )
    branch = scatter_tensor(branch_partial, tensor_size)
    result = (after_attn + keep_rows * (branch + out_bias[1])).astype(jnp.bfloat16)
    early_sum = lax.psum_scatter(early_parts, "dp", scatter_dimension=0, tiled=True).astype(
        jnp.float32
    )
    query_acc, key_acc, value_acc = attention_bwd(
        key_lo, key_hi, slopes, query_heads, key_heads, value_heads, query_info, key_info,
        mixed_f32, head_major(mixed_grad), log_totals, score_scale,
    )
    query_acc, key_acc, value_acc, early_sum, result = lax.optimization_barrier(
        (query_acc, key_acc, value_acc, early_sum, result)
    )
    query_grad = row_major(query_acc * score_scale).astype(jnp.bfloat16)
    key_grad = row_major(key_acc * score_scale).astype(jnp.bfloat16)
    value_grad = row_major(value_acc).astype(jnp.bfloat16)
    projected_grad = jnp.concatenate([query_grad, key_grad, value_grad], axis=1)
    qv_bias_grad = jnp.stack(
        [
            jnp.sum(query_grad, axis=0, dtype=jnp.float32),
            jnp.sum(value_grad, axis=0, dtype=jnp.float32),
        ]
    )
    w_qkv_grad = jnp.einsum("td,tc->dc", normed, projected_grad, preferred_element_type=jnp.float32)
    normed_grad_partial = jnp.einsum(
        "tc,dc->td",
        projected_grad,
        w_qkv.reshape(D, 3 * width_here),
        preferred_element_type=jnp.float32,
    )
    centred_all = inputs_all - jnp.mean(inputs_all, axis=-1, keepdims=True)
    unit_all = centred_all * lax.rsqrt(
        jnp.mean(centred_all * centred_all, axis=-1, keepdims=True) + EPSILON
    )
    gain_one_grad = jnp.sum(normed_grad_partial * unit_all, axis=0)
    shift_one_grad = jnp.sum(normed_grad_partial, axis=0)
    normed_grad = scatter_tensor(normed_grad_partial, tensor_size)
    _, norm_one_back = jax.vjp(normalize, inputs, norm_gain[0], norm_bias[0])
    through_one = norm_one_back(normed_grad)[0]
    input_grad = (after_grad + through_one).astype(jnp.bfloat16)
    qv_full = lax.dynamic_update_slice_in_dim(
        jnp.zeros((2, D), jnp.float32), qv_bias_grad, tensor_pos * width_here, 1
    )
    up_full = lax.dynamic_update_slice_in_dim(
        jnp.zeros((FF,), jnp.float32), up_bias_grad, tensor_pos * ff_here, 0
    )
    small = jnp.concatenate(
        [
            jnp.stack([gain_one_grad, gain_two_grad]).reshape(-1),
            jnp.stack([shift_one_grad, shift_two_grad]).reshape(-1),
            jnp.stack([attn_bias_grad, down_bias_grad]).reshape(-1),
            qv_full.reshape(-1),
            up_full,
        ]
    )
    qkv_sum = halving_scatter(
        w_qkv_grad.reshape(dp_size, D // dp_size, -1), "dp", jnp.bfloat16
    )
    qkv_part = qkv_sum.reshape(-1, 3, width_here)
    summed = doubling_sum(doubling_sum(small, "dp", dp_size), "tensor", tensor_size)
    gains_grad = summed[: 2 * D].reshape(2, D)
    shifts_grad = summed[2 * D : 4 * D].reshape(2, D)
    outer_grad = summed[4 * D : 6 * D].reshape(2, D)
    qv_sum = summed[6 * D : 8 * D].reshape(2, D)
    up_sum = summed[8 * D :]
    down_part = early_sum[:, :ff_here].T
    up_part = early_sum[:, ff_here : 2 * ff_here]
    out_part = early_sum[:, 2 * ff_here :].T
    return (
        result,
        input_grad,
        gains_grad,
        shifts_grad,
        qkv_part,
        qv_sum,
        out_part,
        outer_grad,
        up_part,
        up_sum,
        down_part,
    )


def solution(mesh):
    placed = (
        P(("dp", "tensor"), None),
        P("dp", None),
        P(),
        P(),
        P(None, None, "tensor"),
        P(None, "tensor"),
        P("tensor", None),
        P(),
        P(None, "tensor"),
        P("tensor"),
        P("tensor", None),
        P(("dp", "tensor"), None),
    )
    return jax.shard_map(
        functools.partial(on_device_body, mesh.shape["dp"]),
        mesh=mesh,
        in_specs=placed,
        out_specs=(
            P(("dp", "tensor"), None),
            P(("dp", "tensor"), None),
            P(),
            P(),
            P("dp", None, "tensor"),
            P(),
            P("tensor", "dp"),
            P(),
            P("dp", "tensor"),
            P(),
            P("tensor", "dp"),
        ),
        check_vma=False,
    )
```

```python
import functools

import jax
import jax.numpy as jnp
from jax import lax
from jax.experimental import pallas as pl
from jax.experimental.pallas import tpu as pltpu
from jax.sharding import PartitionSpec as P


D = 768
HEADS = 12
HEAD_DIM = 64
FF = 3072
SIDE_S = 12
SIDE_M = 15
SIDE_L = 20
TOK_DEV = 2048


EPSILON = 1e-06


def layout(group_counts):
    positions = jnp.arange(TOK_DEV, dtype=jnp.int32)
    area_small = SIDE_S * SIDE_S
    area_middle = SIDE_M * SIDE_M
    area_large = SIDE_L * SIDE_L
    end_small = group_counts[0] * area_small
    end_middle = end_small + group_counts[1] * area_middle
    end_large = end_middle + group_counts[2] * area_large
    size_class = (positions >= end_small).astype(jnp.int32) + (positions >= end_middle).astype(
        jnp.int32
    )
    begins = jnp.where(size_class == 0, 0, jnp.where(size_class == 1, end_small, end_middle))
    area_len = jnp.where(
        size_class == 0, area_small, jnp.where(size_class == 1, area_middle, area_large)
    )
    side_len = jnp.where(size_class == 0, SIDE_S, jnp.where(size_class == 1, SIDE_M, SIDE_L))
    within = positions - begins
    picture_index = within // area_len
    within_image = within % area_len
    is_valid = positions < end_large
    segment = jnp.where(is_valid, size_class * 16 + picture_index, 255)
    grid_row = (within_image // side_len).astype(jnp.float32)
    grid_col = (within_image % side_len).astype(jnp.float32)
    return (segment, grid_row, grid_col, is_valid.astype(jnp.float32))


def normalize(values, gain_row, shift_row):
    centred = values - jnp.mean(values, axis=-1, keepdims=True)
    spread = jnp.mean(centred * centred, axis=-1, keepdims=True)
    return centred * lax.rsqrt(spread + EPSILON) * gain_row + shift_row


def slopes_of(first_head, count_heads):
    head_number = (first_head + jnp.arange(count_heads, dtype=jnp.int32)).astype(jnp.float32) + 1.0
    return jnp.exp2(-8.0 * head_number / HEADS)


Q_BLOCK = 256
K_BLOCK = 256
NEG = -1e30


def key_ranges(segment, tokens):
    starts = jnp.arange(0, tokens, Q_BLOCK)
    first = segment[starts]
    last = segment[starts + Q_BLOCK - 1]
    key_lo = jnp.sum(segment[None, :] < first[:, None], axis=1)
    key_hi = jnp.sum(segment[None, :] <= last[:, None], axis=1)
    return (key_lo // K_BLOCK).astype(jnp.int32), ((key_hi + K_BLOCK - 1) // K_BLOCK).astype(jnp.int32)


def block_geometry(qi_ref, ki_ref, start):
    rq = qi_ref[:, 0:1]
    cq = qi_ref[:, 1:2]
    sq = qi_ref[:, 2:3]
    rk = ki_ref[0:1, pl.ds(start, K_BLOCK)]
    ck = ki_ref[1:2, pl.ds(start, K_BLOCK)]
    sk = ki_ref[2:3, pl.ds(start, K_BLOCK)]
    dr = rq - rk
    dc = cq - ck
    return jnp.where(sq == sk, jnp.sqrt(dr * dr + dc * dc), jnp.inf)


def fwd_kernel(heads, lo_ref, hi_ref, slope_ref, q_ref, k_ref, v_ref, qi_ref, ki_ref, o_ref, lse_ref):
    i = pl.program_id(0)
    queries = [q_ref[h] for h in range(heads)]
    width = q_ref.shape[2]

    def body(kb, carry):
        start = pl.multiple_of(kb * K_BLOCK, K_BLOCK)
        dist = block_geometry(qi_ref, ki_ref, start)
        out = []
        for h in range(heads):
            m_old, l_old, acc_old = carry[h]
            keys = k_ref[h, pl.ds(start, K_BLOCK), :]
            vals = v_ref[h, pl.ds(start, K_BLOCK), :]
            s = lax.dot_general(queries[h], keys, (((1,), (1,)), ((), ())),
                                preferred_element_type=jnp.float32) - slope_ref[h] * dist
            m_new = jnp.maximum(m_old, jnp.max(s, axis=1, keepdims=True))
            alpha = jnp.exp(m_old - m_new)
            p = jnp.exp(s - m_new)
            l_new = alpha * l_old + jnp.sum(p, axis=1, keepdims=True)
            acc_new = alpha * acc_old + jnp.dot(p.astype(jnp.bfloat16), vals,
                                                preferred_element_type=jnp.float32)
            out.append((m_new, l_new, acc_new))
        return tuple(out)

    init = tuple(
        (jnp.full((Q_BLOCK, 1), NEG, jnp.float32), jnp.zeros((Q_BLOCK, 1), jnp.float32),
         jnp.zeros((Q_BLOCK, width), jnp.float32))
        for _ in range(heads)
    )
    final = lax.fori_loop(lo_ref[i], hi_ref[i], body, init)
    for h in range(heads):
        m, l, acc = final[h]
        o_ref[h] = acc / l
        lse_ref[h] = m + jnp.log(l)


def bwd_kernel(heads, lo_ref, hi_ref, slope_ref, q_ref, k_ref, v_ref, qi_ref, ki_ref,
               o_ref, do_ref, lse_ref, dq_ref, dk_ref, dv_ref):
    i = pl.program_id(0)

    @pl.when(i == 0)
    def _():
        dk_ref[...] = jnp.zeros_like(dk_ref)
        dv_ref[...] = jnp.zeros_like(dv_ref)

    queries = [q_ref[h] for h in range(heads)]
    grads = [do_ref[h] for h in range(heads)]
    lses = [lse_ref[h] for h in range(heads)]
    deltas = [jnp.sum(grads[h].astype(jnp.float32) * o_ref[h], axis=1, keepdims=True)
              for h in range(heads)]
    width = q_ref.shape[2]

    def body(kb, carry):
        start = pl.multiple_of(kb * K_BLOCK, K_BLOCK)
        dist = block_geometry(qi_ref, ki_ref, start)
        out = []
        for h in range(heads):
            keys = k_ref[h, pl.ds(start, K_BLOCK), :]
            vals = v_ref[h, pl.ds(start, K_BLOCK), :]
            s = lax.dot_general(queries[h], keys, (((1,), (1,)), ((), ())),
                                preferred_element_type=jnp.float32) - slope_ref[h] * dist
            p = jnp.exp(s - lses[h])
            dp = lax.dot_general(grads[h], vals, (((1,), (1,)), ((), ())),
                                 preferred_element_type=jnp.float32)
            ds = (p * (dp - deltas[h])).astype(jnp.bfloat16)
            out.append(carry[h] + jnp.dot(ds, keys, preferred_element_type=jnp.float32))
            dk_ref[h, pl.ds(start, K_BLOCK), :] += lax.dot_general(
                ds, queries[h], (((0,), (0,)), ((), ())), preferred_element_type=jnp.float32)
            dv_ref[h, pl.ds(start, K_BLOCK), :] += lax.dot_general(
                p.astype(jnp.bfloat16), grads[h], (((0,), (0,)), ((), ())),
                preferred_element_type=jnp.float32)
        return tuple(out)

    init = tuple(jnp.zeros((Q_BLOCK, width), jnp.float32) for _ in range(heads))
    final = lax.fori_loop(lo_ref[i], hi_ref[i], body, init)
    for h in range(heads):
        dq_ref[h] = final[h]


def attention_fwd(lo, hi, slopes, q, k, v, qinfo, kinfo):
    heads, tokens, width = q.shape
    grid = (tokens // Q_BLOCK,)
    whole = lambda i, lo, hi: (0, 0, 0)
    rows = lambda i, lo, hi: (0, i, 0)
    return pl.pallas_call(
        functools.partial(fwd_kernel, heads),
        grid_spec=pltpu.PrefetchScalarGridSpec(
            num_scalar_prefetch=2,
            grid=grid,
            in_specs=[
                pl.BlockSpec(memory_space=pltpu.SMEM),
                pl.BlockSpec((heads, Q_BLOCK, width), rows),
                pl.BlockSpec((heads, tokens, width), whole),
                pl.BlockSpec((heads, tokens, width), whole),
                pl.BlockSpec((Q_BLOCK, 3), lambda i, lo, hi: (i, 0)),
                pl.BlockSpec((3, tokens), lambda i, lo, hi: (0, 0)),
            ],
            out_specs=[
                pl.BlockSpec((heads, Q_BLOCK, width), rows),
                pl.BlockSpec((heads, Q_BLOCK, 1), rows),
            ],
        ),
        out_shape=[
            jax.ShapeDtypeStruct((heads, tokens, width), jnp.float32),
            jax.ShapeDtypeStruct((heads, tokens, 1), jnp.float32),
        ],
        compiler_params=pltpu.CompilerParams(dimension_semantics=("arbitrary",)),
    )(lo, hi, slopes, q, k, v, qinfo, kinfo)


def attention_bwd(lo, hi, slopes, q, k, v, qinfo, kinfo, o, do, lse):
    heads, tokens, width = q.shape
    grid = (tokens // Q_BLOCK,)
    whole = lambda i, lo, hi: (0, 0, 0)
    rows = lambda i, lo, hi: (0, i, 0)
    return pl.pallas_call(
        functools.partial(bwd_kernel, heads),
        grid_spec=pltpu.PrefetchScalarGridSpec(
            num_scalar_prefetch=2,
            grid=grid,
            in_specs=[
                pl.BlockSpec(memory_space=pltpu.SMEM),
                pl.BlockSpec((heads, Q_BLOCK, width), rows),
                pl.BlockSpec((heads, tokens, width), whole),
                pl.BlockSpec((heads, tokens, width), whole),
                pl.BlockSpec((Q_BLOCK, 3), lambda i, lo, hi: (i, 0)),
                pl.BlockSpec((3, tokens), lambda i, lo, hi: (0, 0)),
                pl.BlockSpec((heads, Q_BLOCK, width), rows),
                pl.BlockSpec((heads, Q_BLOCK, width), rows),
                pl.BlockSpec((heads, Q_BLOCK, 1), rows),
            ],
            out_specs=[
                pl.BlockSpec((heads, Q_BLOCK, width), rows),
                pl.BlockSpec((heads, tokens, width), whole),
                pl.BlockSpec((heads, tokens, width), whole),
            ],
        ),
        out_shape=[
            jax.ShapeDtypeStruct((heads, tokens, width), jnp.float32),
            jax.ShapeDtypeStruct((heads, tokens, width), jnp.float32),
            jax.ShapeDtypeStruct((heads, tokens, width), jnp.float32),
        ],
        compiler_params=pltpu.CompilerParams(dimension_semantics=("arbitrary",)),
    )(lo, hi, slopes, q, k, v, qinfo, kinfo, o, do, lse)


def scatter_tensor(partial, tensor_size):
    me = lax.axis_index("tensor")
    blocks = partial.reshape(tensor_size, -1, partial.shape[1])
    total = lax.dynamic_index_in_dim(blocks, me, keepdims=False).astype(jnp.float32)
    for shift in range(1, tensor_size):
        outgoing = lax.dynamic_index_in_dim(blocks, (me + shift) % tensor_size, keepdims=False)
        pairs = [(i, (i + shift) % tensor_size) for i in range(tensor_size)]
        total = total + lax.ppermute(outgoing.astype(jnp.bfloat16), "tensor", pairs).astype(
            jnp.float32
        )
    return total


def halving_scatter(blocks, axis_name, wire):
    me = lax.axis_index(axis_name)
    bit = 0
    while blocks.shape[0] > 1:
        pairs = [(i, i ^ (1 << bit)) for i in range(blocks.shape[0] << bit)]
        halves = blocks.reshape((blocks.shape[0] // 2, 2) + blocks.shape[1:])
        mine = (me >> bit) & 1
        keep = lax.dynamic_index_in_dim(halves, mine, axis=1, keepdims=False)
        send = lax.dynamic_index_in_dim(halves, 1 - mine, axis=1, keepdims=False)
        arrived = lax.ppermute(send.astype(wire), axis_name, pairs)
        blocks = keep + arrived.astype(blocks.dtype)
        bit += 1
    return blocks[0]


def doubling_sum(values, axis_name, size):
    bit = 0
    while (1 << bit) < size:
        pairs = [(i, i ^ (1 << bit)) for i in range(size)]
        values = values + lax.ppermute(values, axis_name, pairs)
        bit += 1
    return values


def on_device_body(
    dp_size,
    patches,
    counts,
    norm_gain,
    norm_bias,
    w_qkv,
    b_qv,
    w_out,
    out_bias,
    w_up,
    b_up,
    w_down,
    cotangent,
):
    local_rows = patches.shape[0]
    width_here = w_qkv.shape[2]
    heads_here = width_here // HEAD_DIM
    ff_here = w_up.shape[1]
    tensor_pos = lax.axis_index("tensor")
    tensor_size = D // width_here
    score_scale = HEAD_DIM ** (-0.5)
    segment, grid_row, grid_col, is_valid = layout(counts[0])
    keep_rows = lax.dynamic_slice_in_dim(is_valid, tensor_pos * local_rows, local_rows)[:, None]
    slopes = slopes_of(tensor_pos * heads_here, heads_here)
    inputs = patches.astype(jnp.float32)
    inputs_all = lax.all_gather(patches, "tensor", axis=0, tiled=True).astype(jnp.float32)
    normed = normalize(inputs_all, norm_gain[0], norm_bias[0]).astype(jnp.bfloat16)
    projected = jnp.einsum("td,dsc->tsc", normed, w_qkv, preferred_element_type=jnp.float32)
    queries = (projected[:, 0] + b_qv[0]).astype(jnp.bfloat16)
    keys = projected[:, 1].astype(jnp.bfloat16)
    values = (projected[:, 2] + b_qv[1]).astype(jnp.bfloat16)

    def head_major(rows):
        return rows.reshape(TOK_DEV, heads_here, HEAD_DIM).transpose(1, 0, 2)

    def row_major(heads):
        return heads.transpose(1, 0, 2).reshape(TOK_DEV, width_here)

    key_lo, key_hi = key_ranges(segment, TOK_DEV)
    segment_f = segment.astype(jnp.float32)
    query_info = jnp.stack([grid_row, grid_col, segment_f], axis=1)
    key_info = jnp.stack([grid_row, grid_col, segment_f], axis=0)
    query_heads = head_major(queries) * jnp.asarray(score_scale, jnp.bfloat16)
    key_heads = head_major(keys)
    value_heads = head_major(values)
    mixed_f32, log_totals = attention_fwd(
        key_lo, key_hi, slopes, query_heads, key_heads, value_heads, query_info, key_info
    )
    upstream = cotangent.astype(jnp.float32)
    branch_grad = lax.all_gather(
        (keep_rows * upstream).astype(jnp.bfloat16), "tensor", axis=0, tiled=True
    )
    mixed_f32, log_totals, branch_grad = lax.optimization_barrier(
        (mixed_f32, log_totals, branch_grad)
    )
    mixed_rows = row_major(mixed_f32).astype(jnp.bfloat16)
    mixed_all = lax.all_gather(mixed_rows, "tensor", axis=1, tiled=True)
    w_out_all = lax.all_gather(w_out, "tensor", axis=0, tiled=True)
    attended = jnp.dot(mixed_all, w_out_all, preferred_element_type=jnp.float32)
    after_attn_all = inputs_all + is_valid[:, None] * (attended + out_bias[0])
    after_attn = lax.dynamic_slice_in_dim(after_attn_all, tensor_pos * local_rows, local_rows)
    normed_two = normalize(after_attn_all, norm_gain[1], norm_bias[1]).astype(jnp.bfloat16)
    hidden_pre = jnp.dot(normed_two, w_up, preferred_element_type=jnp.float32) + b_up
    hidden = jax.nn.gelu(hidden_pre, approximate=False).astype(jnp.bfloat16)
    branch_partial = jnp.dot(hidden, w_down, preferred_element_type=jnp.float32)
    down_bias_grad = jnp.sum(keep_rows * upstream, axis=0)
    w_down_grad_t = jnp.einsum(
        "td,tf->df", branch_grad, hidden, preferred_element_type=jnp.float32
    )
    hidden_grad = jnp.einsum("td,fd->tf", branch_grad, w_down, preferred_element_type=jnp.float32)
    _, gelu_back = jax.vjp(lambda pre_act: jax.nn.gelu(pre_act, approximate=False), hidden_pre)
    pre_grad = gelu_back(hidden_grad)[0].astype(jnp.bfloat16)
    up_bias_grad = jnp.sum(pre_grad, axis=0, dtype=jnp.float32)
    w_up_grad = jnp.einsum("td,tf->df", normed_two, pre_grad, preferred_element_type=jnp.float32)
    normed_two_grad = lax.psum_scatter(
        jnp.einsum("tf,df->td", pre_grad, w_up, preferred_element_type=jnp.float32).astype(
            jnp.bfloat16
        ),
        "tensor",
        scatter_dimension=0,
        tiled=True,
    ).astype(jnp.float32)
    _, norm_two_back = jax.vjp(normalize, after_attn, norm_gain[1], norm_bias[1])
    through_two, gain_two_grad, shift_two_grad = norm_two_back(normed_two_grad)
    after_grad = upstream + through_two
    attn_bias_grad = jnp.sum(keep_rows * after_grad, axis=0)
    attn_local = (keep_rows * after_grad).astype(jnp.bfloat16)
    attn_grad = lax.all_gather(attn_local, "tensor", axis=0, tiled=True)
    w_out_grad_t = jnp.einsum(
        "td,tc->dc", attn_grad, mixed_rows, preferred_element_type=jnp.float32
    )
    mixed_grad = jnp.einsum(
        "td,cd->tc", attn_grad, w_out, preferred_element_type=jnp.float32
    ).astype(jnp.bfloat16)
    early_parts = jnp.concatenate([w_down_grad_t, w_up_grad, w_out_grad_t], axis=1).astype(
        jnp.bfloat16
    )
    early_parts, mixed_grad, branch_partial = lax.optimization_barrier(
        (early_parts, mixed_grad, branch_partial)
    )
    branch = scatter_tensor(branch_partial, tensor_size)
    result = (after_attn + keep_rows * (branch + out_bias[1])).astype(jnp.bfloat16)
    early_sum = lax.psum_scatter(early_parts, "dp", scatter_dimension=0, tiled=True).astype(
        jnp.float32
    )
    query_acc, key_acc, value_acc = attention_bwd(
        key_lo, key_hi, slopes, query_heads, key_heads, value_heads, query_info, key_info,
        mixed_f32, head_major(mixed_grad), log_totals,
    )
    query_acc, key_acc, value_acc, early_sum, result = lax.optimization_barrier(
        (query_acc, key_acc, value_acc, early_sum, result)
    )
    query_grad = row_major(query_acc * score_scale).astype(jnp.bfloat16)
    key_grad = row_major(key_acc).astype(jnp.bfloat16)
    value_grad = row_major(value_acc).astype(jnp.bfloat16)
    projected_grad = jnp.concatenate([query_grad, key_grad, value_grad], axis=1)
    qv_bias_grad = jnp.stack(
        [
            jnp.sum(query_grad, axis=0, dtype=jnp.float32),
            jnp.sum(value_grad, axis=0, dtype=jnp.float32),
        ]
    )
    w_qkv_grad = jnp.einsum("td,tc->dc", normed, projected_grad, preferred_element_type=jnp.float32)
    normed_grad_partial = jnp.einsum(
        "tc,dc->td",
        projected_grad,
        w_qkv.reshape(D, 3 * width_here),
        preferred_element_type=jnp.float32,
    )
    centred_all = inputs_all - jnp.mean(inputs_all, axis=-1, keepdims=True)
    unit_all = centred_all * lax.rsqrt(
        jnp.mean(centred_all * centred_all, axis=-1, keepdims=True) + EPSILON
    )
    gain_one_grad = jnp.sum(normed_grad_partial * unit_all, axis=0)
    shift_one_grad = jnp.sum(normed_grad_partial, axis=0)
    normed_grad = scatter_tensor(normed_grad_partial, tensor_size)
    _, norm_one_back = jax.vjp(normalize, inputs, norm_gain[0], norm_bias[0])
    through_one = norm_one_back(normed_grad)[0]
    input_grad = (after_grad + through_one).astype(jnp.bfloat16)
    qv_full = lax.dynamic_update_slice_in_dim(
        jnp.zeros((2, D), jnp.float32), qv_bias_grad, tensor_pos * width_here, 1
    )
    up_full = lax.dynamic_update_slice_in_dim(
        jnp.zeros((FF,), jnp.float32), up_bias_grad, tensor_pos * ff_here, 0
    )
    small = jnp.concatenate(
        [
            jnp.stack([gain_one_grad, gain_two_grad]).reshape(-1),
            jnp.stack([shift_one_grad, shift_two_grad]).reshape(-1),
            jnp.stack([attn_bias_grad, down_bias_grad]).reshape(-1),
            qv_full.reshape(-1),
            up_full,
        ]
    )
    qkv_sum = halving_scatter(
        w_qkv_grad.reshape(dp_size, D // dp_size, -1), "dp", jnp.bfloat16
    )
    qkv_part = qkv_sum.reshape(-1, 3, width_here)
    summed = doubling_sum(doubling_sum(small, "dp", dp_size), "tensor", tensor_size)
    gains_grad = summed[: 2 * D].reshape(2, D)
    shifts_grad = summed[2 * D : 4 * D].reshape(2, D)
    outer_grad = summed[4 * D : 6 * D].reshape(2, D)
    qv_sum = summed[6 * D : 8 * D].reshape(2, D)
    up_sum = summed[8 * D :]
    down_part = early_sum[:, :ff_here].T
    up_part = early_sum[:, ff_here : 2 * ff_here]
    out_part = early_sum[:, 2 * ff_here :].T
    return (
        result,
        input_grad,
        gains_grad,
        shifts_grad,
        qkv_part,
        qv_sum,
        out_part,
        outer_grad,
        up_part,
        up_sum,
        down_part,
    )


def solution(mesh):
    placed = (
        P(("dp", "tensor"), None),
        P("dp", None),
        P(),
        P(),
        P(None, None, "tensor"),
        P(None, "tensor"),
        P("tensor", None),
        P(),
        P(None, "tensor"),
        P("tensor"),
        P("tensor", None),
        P(("dp", "tensor"), None),
    )
    return jax.shard_map(
        functools.partial(on_device_body, mesh.shape["dp"]),
        mesh=mesh,
        in_specs=placed,
        out_specs=(
            P(("dp", "tensor"), None),
            P(("dp", "tensor"), None),
            P(),
            P(),
            P("dp", None, "tensor"),
            P(),
            P("tensor", "dp"),
            P(),
            P("dp", "tensor"),
            P(),
            P("tensor", "dp"),
        ),
        check_vma=False,
    )
```

```python
import functools

import jax
import jax.numpy as jnp
from jax import lax
from jax.experimental import pallas as pl
from jax.experimental.pallas import tpu as pltpu
from jax.sharding import PartitionSpec as P


D = 768
HEADS = 12
HEAD_DIM = 64
FF = 3072
SIDE_S = 12
SIDE_M = 15
SIDE_L = 20
TOK_DEV = 2048


EPSILON = 1e-06


def layout(group_counts):
    positions = jnp.arange(TOK_DEV, dtype=jnp.int32)
    area_small = SIDE_S * SIDE_S
    area_middle = SIDE_M * SIDE_M
    area_large = SIDE_L * SIDE_L
    end_small = group_counts[0] * area_small
    end_middle = end_small + group_counts[1] * area_middle
    end_large = end_middle + group_counts[2] * area_large
    size_class = (positions >= end_small).astype(jnp.int32) + (positions >= end_middle).astype(
        jnp.int32
    )
    begins = jnp.where(size_class == 0, 0, jnp.where(size_class == 1, end_small, end_middle))
    area_len = jnp.where(
        size_class == 0, area_small, jnp.where(size_class == 1, area_middle, area_large)
    )
    side_len = jnp.where(size_class == 0, SIDE_S, jnp.where(size_class == 1, SIDE_M, SIDE_L))
    within = positions - begins
    picture_index = within // area_len
    within_image = within % area_len
    is_valid = positions < end_large
    segment = jnp.where(is_valid, size_class * 16 + picture_index, 255)
    grid_row = (within_image // side_len).astype(jnp.float32)
    grid_col = (within_image % side_len).astype(jnp.float32)
    return (segment, grid_row, grid_col, is_valid.astype(jnp.float32))


def normalize(values, gain_row, shift_row):
    centred = values - jnp.mean(values, axis=-1, keepdims=True)
    spread = jnp.mean(centred * centred, axis=-1, keepdims=True)
    return centred * lax.rsqrt(spread + EPSILON) * gain_row + shift_row


def slopes_of(first_head, count_heads):
    head_number = (first_head + jnp.arange(count_heads, dtype=jnp.int32)).astype(jnp.float32) + 1.0
    return jnp.exp2(-8.0 * head_number / HEADS)


Q_BLOCK = 256
K_BLOCK = 256
NEG = -1e30


def key_ranges(segment, tokens):
    starts = jnp.arange(0, tokens, Q_BLOCK)
    first = segment[starts]
    last = segment[starts + Q_BLOCK - 1]
    key_lo = jnp.sum(segment[None, :] < first[:, None], axis=1)
    key_hi = jnp.sum(segment[None, :] <= last[:, None], axis=1)
    return (key_lo // K_BLOCK).astype(jnp.int32), ((key_hi + K_BLOCK - 1) // K_BLOCK).astype(jnp.int32)


def block_geometry(qi_ref, ki_ref, start):
    rq = qi_ref[:, 0:1]
    cq = qi_ref[:, 1:2]
    sq = qi_ref[:, 2:3]
    rk = ki_ref[0:1, pl.ds(start, K_BLOCK)]
    ck = ki_ref[1:2, pl.ds(start, K_BLOCK)]
    sk = ki_ref[2:3, pl.ds(start, K_BLOCK)]
    dr = rq - rk
    dc = cq - ck
    return jnp.where(sq == sk, jnp.sqrt(dr * dr + dc * dc), jnp.inf)


def fwd_kernel(heads, lo_ref, hi_ref, slope_ref, q_ref, k_ref, v_ref, qi_ref, ki_ref, o_ref, lse_ref):
    i = pl.program_id(0)
    queries = [q_ref[h] for h in range(heads)]
    width = q_ref.shape[2]

    def body(kb, carry):
        start = pl.multiple_of(kb * K_BLOCK, K_BLOCK)
        dist = block_geometry(qi_ref, ki_ref, start)
        out = []
        for h in range(heads):
            m_old, l_old, acc_old = carry[h]
            keys = k_ref[h, pl.ds(start, K_BLOCK), :]
            vals = v_ref[h, pl.ds(start, K_BLOCK), :]
            s = lax.dot_general(queries[h], keys, (((1,), (1,)), ((), ())),
                                preferred_element_type=jnp.float32) - slope_ref[h] * dist
            m_new = jnp.maximum(m_old, jnp.max(s, axis=1, keepdims=True))
            alpha = jnp.exp(m_old - m_new)
            p = jnp.exp(s - m_new)
            l_new = alpha * l_old + jnp.sum(p, axis=1, keepdims=True)
            acc_new = alpha * acc_old + jnp.dot(p.astype(jnp.bfloat16), vals,
                                                preferred_element_type=jnp.float32)
            out.append((m_new, l_new, acc_new))
        return tuple(out)

    init = tuple(
        (jnp.full((Q_BLOCK, 1), NEG, jnp.float32), jnp.zeros((Q_BLOCK, 1), jnp.float32),
         jnp.zeros((Q_BLOCK, width), jnp.float32))
        for _ in range(heads)
    )
    final = lax.fori_loop(lo_ref[i], hi_ref[i], body, init)
    for h in range(heads):
        m, l, acc = final[h]
        o_ref[h] = acc / l
        lse_ref[h] = m + jnp.log(l)


def bwd_kernel(heads, lo_ref, hi_ref, slope_ref, q_ref, k_ref, v_ref, qi_ref, ki_ref,
               o_ref, do_ref, lse_ref, dq_ref, dk_ref, dv_ref):
    i = pl.program_id(0)

    @pl.when(i == 0)
    def _():
        dk_ref[...] = jnp.zeros_like(dk_ref)
        dv_ref[...] = jnp.zeros_like(dv_ref)

    queries = [q_ref[h] for h in range(heads)]
    grads = [do_ref[h] for h in range(heads)]
    lses = [lse_ref[h] for h in range(heads)]
    deltas = [jnp.sum(grads[h].astype(jnp.float32) * o_ref[h], axis=1, keepdims=True)
              for h in range(heads)]
    width = q_ref.shape[2]

    def body(kb, carry):
        start = pl.multiple_of(kb * K_BLOCK, K_BLOCK)
        dist = block_geometry(qi_ref, ki_ref, start)
        out = []
        for h in range(heads):
            keys = k_ref[h, pl.ds(start, K_BLOCK), :]
            vals = v_ref[h, pl.ds(start, K_BLOCK), :]
            s = lax.dot_general(queries[h], keys, (((1,), (1,)), ((), ())),
                                preferred_element_type=jnp.float32) - slope_ref[h] * dist
            p = jnp.exp(s - lses[h])
            dp = lax.dot_general(grads[h], vals, (((1,), (1,)), ((), ())),
                                 preferred_element_type=jnp.float32)
            ds = (p * (dp - deltas[h])).astype(jnp.bfloat16)
            out.append(carry[h] + jnp.dot(ds, keys, preferred_element_type=jnp.float32))
            dk_ref[h, pl.ds(start, K_BLOCK), :] += lax.dot_general(
                ds, queries[h], (((0,), (0,)), ((), ())), preferred_element_type=jnp.float32)
            dv_ref[h, pl.ds(start, K_BLOCK), :] += lax.dot_general(
                p.astype(jnp.bfloat16), grads[h], (((0,), (0,)), ((), ())),
                preferred_element_type=jnp.float32)
        return tuple(out)

    init = tuple(jnp.zeros((Q_BLOCK, width), jnp.float32) for _ in range(heads))
    final = lax.fori_loop(lo_ref[i], hi_ref[i], body, init)
    for h in range(heads):
        dq_ref[h] = final[h]


def attention_fwd(lo, hi, slopes, q, k, v, qinfo, kinfo):
    heads, tokens, width = q.shape
    grid = (tokens // Q_BLOCK,)
    whole = lambda i, lo, hi: (0, 0, 0)
    rows = lambda i, lo, hi: (0, i, 0)
    return pl.pallas_call(
        functools.partial(fwd_kernel, heads),
        grid_spec=pltpu.PrefetchScalarGridSpec(
            num_scalar_prefetch=2,
            grid=grid,
            in_specs=[
                pl.BlockSpec(memory_space=pltpu.SMEM),
                pl.BlockSpec((heads, Q_BLOCK, width), rows),
                pl.BlockSpec((heads, tokens, width), whole),
                pl.BlockSpec((heads, tokens, width), whole),
                pl.BlockSpec((Q_BLOCK, 3), lambda i, lo, hi: (i, 0)),
                pl.BlockSpec((3, tokens), lambda i, lo, hi: (0, 0)),
            ],
            out_specs=[
                pl.BlockSpec((heads, Q_BLOCK, width), rows),
                pl.BlockSpec((heads, Q_BLOCK, 1), rows),
            ],
        ),
        out_shape=[
            jax.ShapeDtypeStruct((heads, tokens, width), jnp.float32),
            jax.ShapeDtypeStruct((heads, tokens, 1), jnp.float32),
        ],
        compiler_params=pltpu.CompilerParams(dimension_semantics=("arbitrary",)),
    )(lo, hi, slopes, q, k, v, qinfo, kinfo)


def attention_bwd(lo, hi, slopes, q, k, v, qinfo, kinfo, o, do, lse):
    heads, tokens, width = q.shape
    grid = (tokens // Q_BLOCK,)
    whole = lambda i, lo, hi: (0, 0, 0)
    rows = lambda i, lo, hi: (0, i, 0)
    return pl.pallas_call(
        functools.partial(bwd_kernel, heads),
        grid_spec=pltpu.PrefetchScalarGridSpec(
            num_scalar_prefetch=2,
            grid=grid,
            in_specs=[
                pl.BlockSpec(memory_space=pltpu.SMEM),
                pl.BlockSpec((heads, Q_BLOCK, width), rows),
                pl.BlockSpec((heads, tokens, width), whole),
                pl.BlockSpec((heads, tokens, width), whole),
                pl.BlockSpec((Q_BLOCK, 3), lambda i, lo, hi: (i, 0)),
                pl.BlockSpec((3, tokens), lambda i, lo, hi: (0, 0)),
                pl.BlockSpec((heads, Q_BLOCK, width), rows),
                pl.BlockSpec((heads, Q_BLOCK, width), rows),
                pl.BlockSpec((heads, Q_BLOCK, 1), rows),
            ],
            out_specs=[
                pl.BlockSpec((heads, Q_BLOCK, width), rows),
                pl.BlockSpec((heads, tokens, width), whole),
                pl.BlockSpec((heads, tokens, width), whole),
            ],
        ),
        out_shape=[
            jax.ShapeDtypeStruct((heads, tokens, width), jnp.float32),
            jax.ShapeDtypeStruct((heads, tokens, width), jnp.float32),
            jax.ShapeDtypeStruct((heads, tokens, width), jnp.float32),
        ],
        compiler_params=pltpu.CompilerParams(dimension_semantics=("arbitrary",)),
    )(lo, hi, slopes, q, k, v, qinfo, kinfo, o, do, lse)


def scatter_blocks(partial, tensor_size):
    me = lax.axis_index("tensor")
    blocks = partial.reshape(tensor_size, -1, partial.shape[1])
    own = lax.dynamic_index_in_dim(blocks, me, keepdims=False).astype(jnp.float32)
    outgoing = [
        lax.dynamic_index_in_dim(blocks, (me + shift) % tensor_size, keepdims=False).astype(
            jnp.bfloat16
        )
        for shift in range(1, tensor_size)
    ]
    return own, outgoing


def exchange_blocks(own, outgoing, tensor_size):
    total = own
    for shift in range(1, tensor_size):
        pairs = [(i, (i + shift) % tensor_size) for i in range(tensor_size)]
        total = total + lax.ppermute(outgoing[shift - 1], "tensor", pairs).astype(jnp.float32)
    return total


def scatter_tensor(partial, tensor_size):
    return exchange_blocks(*scatter_blocks(partial, tensor_size), tensor_size)


def halving_scatter(blocks, axis_name, wire):
    me = lax.axis_index(axis_name)
    bit = 0
    while blocks.shape[0] > 1:
        pairs = [(i, i ^ (1 << bit)) for i in range(blocks.shape[0] << bit)]
        halves = blocks.reshape((blocks.shape[0] // 2, 2) + blocks.shape[1:])
        mine = (me >> bit) & 1
        keep = lax.dynamic_index_in_dim(halves, mine, axis=1, keepdims=False)
        send = lax.dynamic_index_in_dim(halves, 1 - mine, axis=1, keepdims=False)
        arrived = lax.ppermute(send.astype(wire), axis_name, pairs)
        blocks = keep + arrived.astype(blocks.dtype)
        bit += 1
    return blocks[0]


def doubling_sum(values, axis_name, size):
    bit = 0
    while (1 << bit) < size:
        pairs = [(i, i ^ (1 << bit)) for i in range(size)]
        values = values + lax.ppermute(values, axis_name, pairs)
        bit += 1
    return values


def on_device_body(
    dp_size,
    patches,
    counts,
    norm_gain,
    norm_bias,
    w_qkv,
    b_qv,
    w_out,
    out_bias,
    w_up,
    b_up,
    w_down,
    cotangent,
):
    local_rows = patches.shape[0]
    width_here = w_qkv.shape[2]
    heads_here = width_here // HEAD_DIM
    ff_here = w_up.shape[1]
    tensor_pos = lax.axis_index("tensor")
    tensor_size = D // width_here
    score_scale = HEAD_DIM ** (-0.5)
    segment, grid_row, grid_col, is_valid = layout(counts[0])
    keep_rows = lax.dynamic_slice_in_dim(is_valid, tensor_pos * local_rows, local_rows)[:, None]
    slopes = slopes_of(tensor_pos * heads_here, heads_here)
    inputs = patches.astype(jnp.float32)
    inputs_all = lax.all_gather(patches, "tensor", axis=0, tiled=True).astype(jnp.float32)
    normed = normalize(inputs_all, norm_gain[0], norm_bias[0]).astype(jnp.bfloat16)
    projected = jnp.einsum("td,dsc->tsc", normed, w_qkv, preferred_element_type=jnp.float32)
    queries = (projected[:, 0] + b_qv[0]).astype(jnp.bfloat16)
    keys = projected[:, 1].astype(jnp.bfloat16)
    values = (projected[:, 2] + b_qv[1]).astype(jnp.bfloat16)

    def head_major(rows):
        return rows.reshape(TOK_DEV, heads_here, HEAD_DIM).transpose(1, 0, 2)

    def row_major(heads):
        return heads.transpose(1, 0, 2).reshape(TOK_DEV, width_here)

    key_lo, key_hi = key_ranges(segment, TOK_DEV)
    segment_f = segment.astype(jnp.float32)
    query_info = jnp.stack([grid_row, grid_col, segment_f], axis=1)
    key_info = jnp.stack([grid_row, grid_col, segment_f], axis=0)
    query_heads = head_major(queries) * jnp.asarray(score_scale, jnp.bfloat16)
    key_heads = head_major(keys)
    value_heads = head_major(values)
    mixed_f32, log_totals = attention_fwd(
        key_lo, key_hi, slopes, query_heads, key_heads, value_heads, query_info, key_info
    )
    upstream = cotangent.astype(jnp.float32)
    branch_grad = lax.all_gather(
        (keep_rows * upstream).astype(jnp.bfloat16), "tensor", axis=0, tiled=True
    )
    mixed_f32, log_totals, branch_grad = lax.optimization_barrier(
        (mixed_f32, log_totals, branch_grad)
    )
    mixed_rows = row_major(mixed_f32).astype(jnp.bfloat16)
    mixed_all = lax.all_gather(mixed_rows, "tensor", axis=1, tiled=True)
    w_out_all = lax.all_gather(w_out, "tensor", axis=0, tiled=True)
    attended = jnp.dot(mixed_all, w_out_all, preferred_element_type=jnp.float32)
    after_attn_all = inputs_all + is_valid[:, None] * (attended + out_bias[0])
    after_attn = lax.dynamic_slice_in_dim(after_attn_all, tensor_pos * local_rows, local_rows)
    normed_two = normalize(after_attn_all, norm_gain[1], norm_bias[1]).astype(jnp.bfloat16)
    hidden_pre = jnp.dot(normed_two, w_up, preferred_element_type=jnp.float32) + b_up
    hidden = jax.nn.gelu(hidden_pre, approximate=False).astype(jnp.bfloat16)
    branch_partial = jnp.dot(hidden, w_down, preferred_element_type=jnp.float32)
    down_bias_grad = jnp.sum(keep_rows * upstream, axis=0)
    w_down_grad_t = jnp.einsum(
        "td,tf->df", branch_grad, hidden, preferred_element_type=jnp.float32
    )
    hidden_grad = jnp.einsum("td,fd->tf", branch_grad, w_down, preferred_element_type=jnp.float32)
    _, gelu_back = jax.vjp(lambda pre_act: jax.nn.gelu(pre_act, approximate=False), hidden_pre)
    pre_grad = gelu_back(hidden_grad)[0].astype(jnp.bfloat16)
    up_bias_grad = jnp.sum(pre_grad, axis=0, dtype=jnp.float32)
    w_up_grad = jnp.einsum("td,tf->df", normed_two, pre_grad, preferred_element_type=jnp.float32)
    normed_two_grad = lax.psum_scatter(
        jnp.einsum("tf,df->td", pre_grad, w_up, preferred_element_type=jnp.float32).astype(
            jnp.bfloat16
        ),
        "tensor",
        scatter_dimension=0,
        tiled=True,
    ).astype(jnp.float32)
    branch_own, branch_out = scatter_blocks(branch_partial, tensor_size)
    normed_two_grad, branch_own, branch_out = lax.optimization_barrier(
        (normed_two_grad, branch_own, branch_out)
    )
    _, norm_two_back = jax.vjp(normalize, after_attn, norm_gain[1], norm_bias[1])
    through_two, gain_two_grad, shift_two_grad = norm_two_back(normed_two_grad)
    after_grad = upstream + through_two
    attn_bias_grad = jnp.sum(keep_rows * after_grad, axis=0)
    attn_local = (keep_rows * after_grad).astype(jnp.bfloat16)
    attn_grad = lax.all_gather(attn_local, "tensor", axis=0, tiled=True)
    w_out_grad_t = jnp.einsum(
        "td,tc->dc", attn_grad, mixed_rows, preferred_element_type=jnp.float32
    )
    mixed_grad = jnp.einsum(
        "td,cd->tc", attn_grad, w_out, preferred_element_type=jnp.float32
    ).astype(jnp.bfloat16)
    early_parts = jnp.concatenate([w_down_grad_t, w_up_grad, w_out_grad_t], axis=1).astype(
        jnp.bfloat16
    )
    early_parts, mixed_grad, branch_own, branch_out = lax.optimization_barrier(
        (early_parts, mixed_grad, branch_own, branch_out)
    )
    branch = exchange_blocks(branch_own, branch_out, tensor_size)
    result = (after_attn + keep_rows * (branch + out_bias[1])).astype(jnp.bfloat16)
    early_sum = lax.psum_scatter(early_parts, "dp", scatter_dimension=0, tiled=True).astype(
        jnp.float32
    )
    query_acc, key_acc, value_acc = attention_bwd(
        key_lo, key_hi, slopes, query_heads, key_heads, value_heads, query_info, key_info,
        mixed_f32, head_major(mixed_grad), log_totals,
    )
    query_acc, key_acc, value_acc, early_sum, result = lax.optimization_barrier(
        (query_acc, key_acc, value_acc, early_sum, result)
    )
    query_grad = row_major(query_acc * score_scale).astype(jnp.bfloat16)
    key_grad = row_major(key_acc).astype(jnp.bfloat16)
    value_grad = row_major(value_acc).astype(jnp.bfloat16)
    projected_grad = jnp.concatenate([query_grad, key_grad, value_grad], axis=1)
    qv_bias_grad = jnp.stack(
        [
            jnp.sum(query_grad, axis=0, dtype=jnp.float32),
            jnp.sum(value_grad, axis=0, dtype=jnp.float32),
        ]
    )
    w_qkv_grad = jnp.einsum("td,tc->dc", normed, projected_grad, preferred_element_type=jnp.float32)
    normed_grad_partial = jnp.einsum(
        "tc,dc->td",
        projected_grad,
        w_qkv.reshape(D, 3 * width_here),
        preferred_element_type=jnp.float32,
    )
    centred_all = inputs_all - jnp.mean(inputs_all, axis=-1, keepdims=True)
    unit_all = centred_all * lax.rsqrt(
        jnp.mean(centred_all * centred_all, axis=-1, keepdims=True) + EPSILON
    )
    gain_one_grad = jnp.sum(normed_grad_partial * unit_all, axis=0)
    shift_one_grad = jnp.sum(normed_grad_partial, axis=0)
    normed_grad = scatter_tensor(normed_grad_partial, tensor_size)
    _, norm_one_back = jax.vjp(normalize, inputs, norm_gain[0], norm_bias[0])
    through_one = norm_one_back(normed_grad)[0]
    input_grad = (after_grad + through_one).astype(jnp.bfloat16)
    qv_full = lax.dynamic_update_slice_in_dim(
        jnp.zeros((2, D), jnp.float32), qv_bias_grad, tensor_pos * width_here, 1
    )
    up_full = lax.dynamic_update_slice_in_dim(
        jnp.zeros((FF,), jnp.float32), up_bias_grad, tensor_pos * ff_here, 0
    )
    small = jnp.concatenate(
        [
            jnp.stack([gain_one_grad, gain_two_grad]).reshape(-1),
            jnp.stack([shift_one_grad, shift_two_grad]).reshape(-1),
            jnp.stack([attn_bias_grad, down_bias_grad]).reshape(-1),
            qv_full.reshape(-1),
            up_full,
        ]
    )
    qkv_sum = halving_scatter(
        w_qkv_grad.reshape(dp_size, D // dp_size, -1), "dp", jnp.bfloat16
    )
    qkv_part = qkv_sum.reshape(-1, 3, width_here)
    summed = doubling_sum(doubling_sum(small, "dp", dp_size), "tensor", tensor_size)
    gains_grad = summed[: 2 * D].reshape(2, D)
    shifts_grad = summed[2 * D : 4 * D].reshape(2, D)
    outer_grad = summed[4 * D : 6 * D].reshape(2, D)
    qv_sum = summed[6 * D : 8 * D].reshape(2, D)
    up_sum = summed[8 * D :]
    down_part = early_sum[:, :ff_here].T
    up_part = early_sum[:, ff_here : 2 * ff_here]
    out_part = early_sum[:, 2 * ff_here :].T
    return (
        result,
        input_grad,
        gains_grad,
        shifts_grad,
        qkv_part,
        qv_sum,
        out_part,
        outer_grad,
        up_part,
        up_sum,
        down_part,
    )


def solution(mesh):
    placed = (
        P(("dp", "tensor"), None),
        P("dp", None),
        P(),
        P(),
        P(None, None, "tensor"),
        P(None, "tensor"),
        P("tensor", None),
        P(),
        P(None, "tensor"),
        P("tensor"),
        P("tensor", None),
        P(("dp", "tensor"), None),
    )
    return jax.shard_map(
        functools.partial(on_device_body, mesh.shape["dp"]),
        mesh=mesh,
        in_specs=placed,
        out_specs=(
            P(("dp", "tensor"), None),
            P(("dp", "tensor"), None),
            P(),
            P(),
            P("dp", None, "tensor"),
            P(),
            P("tensor", "dp"),
            P(),
            P("dp", "tensor"),
            P(),
            P("tensor", "dp"),
        ),
        check_vma=False,
    )
```

```python
import functools

import jax
import jax.numpy as jnp
from jax import lax
from jax.experimental import pallas as pl
from jax.experimental.pallas import tpu as pltpu
from jax.sharding import PartitionSpec as P


D = 768
HEADS = 12
HEAD_DIM = 64
FF = 3072
SIDE_S = 12
SIDE_M = 15
SIDE_L = 20
TOK_DEV = 2048


EPSILON = 1e-06


def layout(group_counts):
    positions = jnp.arange(TOK_DEV, dtype=jnp.int32)
    area_small = SIDE_S * SIDE_S
    area_middle = SIDE_M * SIDE_M
    area_large = SIDE_L * SIDE_L
    end_small = group_counts[0] * area_small
    end_middle = end_small + group_counts[1] * area_middle
    end_large = end_middle + group_counts[2] * area_large
    size_class = (positions >= end_small).astype(jnp.int32) + (positions >= end_middle).astype(
        jnp.int32
    )
    begins = jnp.where(size_class == 0, 0, jnp.where(size_class == 1, end_small, end_middle))
    area_len = jnp.where(
        size_class == 0, area_small, jnp.where(size_class == 1, area_middle, area_large)
    )
    side_len = jnp.where(size_class == 0, SIDE_S, jnp.where(size_class == 1, SIDE_M, SIDE_L))
    within = positions - begins
    picture_index = within // area_len
    within_image = within % area_len
    is_valid = positions < end_large
    segment = jnp.where(is_valid, size_class * 16 + picture_index, 255)
    grid_row = (within_image // side_len).astype(jnp.float32)
    grid_col = (within_image % side_len).astype(jnp.float32)
    return (segment, grid_row, grid_col, is_valid.astype(jnp.float32))


def normalize(values, gain_row, shift_row):
    centred = values - jnp.mean(values, axis=-1, keepdims=True)
    spread = jnp.mean(centred * centred, axis=-1, keepdims=True)
    return centred * lax.rsqrt(spread + EPSILON) * gain_row + shift_row


def slopes_of(first_head, count_heads):
    head_number = (first_head + jnp.arange(count_heads, dtype=jnp.int32)).astype(jnp.float32) + 1.0
    return jnp.exp2(-8.0 * head_number / HEADS)


Q_BLOCK = 256
K_BLOCK = 256
NEG = -1e30


def key_ranges(segment, tokens):
    starts = jnp.arange(0, tokens, Q_BLOCK)
    first = segment[starts]
    last = segment[starts + Q_BLOCK - 1]
    key_lo = jnp.sum(segment[None, :] < first[:, None], axis=1)
    key_hi = jnp.sum(segment[None, :] <= last[:, None], axis=1)
    return (key_lo // K_BLOCK).astype(jnp.int32), ((key_hi + K_BLOCK - 1) // K_BLOCK).astype(jnp.int32)


def block_geometry(qi_ref, ki_ref, start):
    rq = qi_ref[:, 0:1]
    cq = qi_ref[:, 1:2]
    sq = qi_ref[:, 2:3]
    rk = ki_ref[0:1, pl.ds(start, K_BLOCK)]
    ck = ki_ref[1:2, pl.ds(start, K_BLOCK)]
    sk = ki_ref[2:3, pl.ds(start, K_BLOCK)]
    dr = rq - rk
    dc = cq - ck
    return jnp.where(sq == sk, jnp.sqrt(dr * dr + dc * dc), jnp.inf)


def fwd_kernel(heads, lo_ref, hi_ref, slope_ref, q_ref, k_ref, v_ref, qi_ref, ki_ref, o_ref, lse_ref):
    i = pl.program_id(0)
    queries = [q_ref[h] for h in range(heads)]
    width = q_ref.shape[2]

    def body(kb, carry):
        start = pl.multiple_of(kb * K_BLOCK, K_BLOCK)
        dist = block_geometry(qi_ref, ki_ref, start)
        out = []
        for h in range(heads):
            m_old, l_old, acc_old = carry[h]
            keys = k_ref[h, pl.ds(start, K_BLOCK), :]
            vals = v_ref[h, pl.ds(start, K_BLOCK), :]
            s = lax.dot_general(queries[h], keys, (((1,), (1,)), ((), ())),
                                preferred_element_type=jnp.float32) - slope_ref[h] * dist
            m_new = jnp.maximum(m_old, jnp.max(s, axis=1, keepdims=True))
            alpha = jnp.exp(m_old - m_new)
            p = jnp.exp(s - m_new)
            l_new = alpha * l_old + jnp.sum(p, axis=1, keepdims=True)
            acc_new = alpha * acc_old + jnp.dot(p.astype(jnp.bfloat16), vals,
                                                preferred_element_type=jnp.float32)
            out.append((m_new, l_new, acc_new))
        return tuple(out)

    init = tuple(
        (jnp.full((Q_BLOCK, 1), NEG, jnp.float32), jnp.zeros((Q_BLOCK, 1), jnp.float32),
         jnp.zeros((Q_BLOCK, width), jnp.float32))
        for _ in range(heads)
    )
    final = lax.fori_loop(lo_ref[i], hi_ref[i], body, init)
    for h in range(heads):
        m, l, acc = final[h]
        o_ref[h] = acc / l
        lse_ref[h] = m + jnp.log(l)


def bwd_kernel(heads, lo_ref, hi_ref, slope_ref, q_ref, k_ref, v_ref, qi_ref, ki_ref,
               o_ref, do_ref, lse_ref, dq_ref, dk_ref, dv_ref):
    i = pl.program_id(0)

    @pl.when(i == 0)
    def _():
        dk_ref[...] = jnp.zeros_like(dk_ref)
        dv_ref[...] = jnp.zeros_like(dv_ref)

    queries = [q_ref[h] for h in range(heads)]
    grads = [do_ref[h] for h in range(heads)]
    lses = [lse_ref[h] for h in range(heads)]
    deltas = [jnp.sum(grads[h].astype(jnp.float32) * o_ref[h], axis=1, keepdims=True)
              for h in range(heads)]
    width = q_ref.shape[2]

    def body(kb, carry):
        start = pl.multiple_of(kb * K_BLOCK, K_BLOCK)
        dist = block_geometry(qi_ref, ki_ref, start)
        out = []
        for h in range(heads):
            keys = k_ref[h, pl.ds(start, K_BLOCK), :]
            vals = v_ref[h, pl.ds(start, K_BLOCK), :]
            s = lax.dot_general(queries[h], keys, (((1,), (1,)), ((), ())),
                                preferred_element_type=jnp.float32) - slope_ref[h] * dist
            p = jnp.exp(s - lses[h])
            dp = lax.dot_general(grads[h], vals, (((1,), (1,)), ((), ())),
                                 preferred_element_type=jnp.float32)
            ds = (p * (dp - deltas[h])).astype(jnp.bfloat16)
            out.append(carry[h] + jnp.dot(ds, keys, preferred_element_type=jnp.float32))
            dk_ref[h, pl.ds(start, K_BLOCK), :] += lax.dot_general(
                ds, queries[h], (((0,), (0,)), ((), ())), preferred_element_type=jnp.float32)
            dv_ref[h, pl.ds(start, K_BLOCK), :] += lax.dot_general(
                p.astype(jnp.bfloat16), grads[h], (((0,), (0,)), ((), ())),
                preferred_element_type=jnp.float32)
        return tuple(out)

    init = tuple(jnp.zeros((Q_BLOCK, width), jnp.float32) for _ in range(heads))
    final = lax.fori_loop(lo_ref[i], hi_ref[i], body, init)
    for h in range(heads):
        dq_ref[h] = final[h]


def attention_fwd(lo, hi, slopes, q, k, v, qinfo, kinfo):
    heads, tokens, width = q.shape
    grid = (tokens // Q_BLOCK,)
    whole = lambda i, lo, hi: (0, 0, 0)
    rows = lambda i, lo, hi: (0, i, 0)
    return pl.pallas_call(
        functools.partial(fwd_kernel, heads),
        grid_spec=pltpu.PrefetchScalarGridSpec(
            num_scalar_prefetch=2,
            grid=grid,
            in_specs=[
                pl.BlockSpec(memory_space=pltpu.SMEM),
                pl.BlockSpec((heads, Q_BLOCK, width), rows),
                pl.BlockSpec((heads, tokens, width), whole),
                pl.BlockSpec((heads, tokens, width), whole),
                pl.BlockSpec((Q_BLOCK, 3), lambda i, lo, hi: (i, 0)),
                pl.BlockSpec((3, tokens), lambda i, lo, hi: (0, 0)),
            ],
            out_specs=[
                pl.BlockSpec((heads, Q_BLOCK, width), rows),
                pl.BlockSpec((heads, Q_BLOCK, 1), rows),
            ],
        ),
        out_shape=[
            jax.ShapeDtypeStruct((heads, tokens, width), jnp.float32),
            jax.ShapeDtypeStruct((heads, tokens, 1), jnp.float32),
        ],
        compiler_params=pltpu.CompilerParams(dimension_semantics=("arbitrary",)),
    )(lo, hi, slopes, q, k, v, qinfo, kinfo)


def attention_bwd(lo, hi, slopes, q, k, v, qinfo, kinfo, o, do, lse):
    heads, tokens, width = q.shape
    grid = (tokens // Q_BLOCK,)
    whole = lambda i, lo, hi: (0, 0, 0)
    rows = lambda i, lo, hi: (0, i, 0)
    return pl.pallas_call(
        functools.partial(bwd_kernel, heads),
        grid_spec=pltpu.PrefetchScalarGridSpec(
            num_scalar_prefetch=2,
            grid=grid,
            in_specs=[
                pl.BlockSpec(memory_space=pltpu.SMEM),
                pl.BlockSpec((heads, Q_BLOCK, width), rows),
                pl.BlockSpec((heads, tokens, width), whole),
                pl.BlockSpec((heads, tokens, width), whole),
                pl.BlockSpec((Q_BLOCK, 3), lambda i, lo, hi: (i, 0)),
                pl.BlockSpec((3, tokens), lambda i, lo, hi: (0, 0)),
                pl.BlockSpec((heads, Q_BLOCK, width), rows),
                pl.BlockSpec((heads, Q_BLOCK, width), rows),
                pl.BlockSpec((heads, Q_BLOCK, 1), rows),
            ],
            out_specs=[
                pl.BlockSpec((heads, Q_BLOCK, width), rows),
                pl.BlockSpec((heads, tokens, width), whole),
                pl.BlockSpec((heads, tokens, width), whole),
            ],
        ),
        out_shape=[
            jax.ShapeDtypeStruct((heads, tokens, width), jnp.float32),
            jax.ShapeDtypeStruct((heads, tokens, width), jnp.float32),
            jax.ShapeDtypeStruct((heads, tokens, width), jnp.float32),
        ],
        compiler_params=pltpu.CompilerParams(dimension_semantics=("arbitrary",)),
    )(lo, hi, slopes, q, k, v, qinfo, kinfo, o, do, lse)


def scatter_blocks(partial, tensor_size):
    me = lax.axis_index("tensor")
    blocks = partial.reshape(tensor_size, -1, partial.shape[1])
    own = lax.dynamic_index_in_dim(blocks, me, keepdims=False).astype(jnp.float32)
    outgoing = [
        lax.dynamic_index_in_dim(blocks, (me + shift) % tensor_size, keepdims=False).astype(
            jnp.bfloat16
        )
        for shift in range(1, tensor_size)
    ]
    return own, outgoing


def exchange_blocks(own, outgoing, tensor_size):
    total = own
    for shift in range(1, tensor_size):
        pairs = [(i, (i + shift) % tensor_size) for i in range(tensor_size)]
        total = total + lax.ppermute(outgoing[shift - 1], "tensor", pairs).astype(jnp.float32)
    return total


def scatter_tensor(partial, tensor_size):
    return exchange_blocks(*scatter_blocks(partial, tensor_size), tensor_size)


def halving_scatter(blocks, axis_name, wire):
    me = lax.axis_index(axis_name)
    bit = 0
    while blocks.shape[0] > 1:
        pairs = [(i, i ^ (1 << bit)) for i in range(blocks.shape[0] << bit)]
        halves = blocks.reshape((blocks.shape[0] // 2, 2) + blocks.shape[1:])
        mine = (me >> bit) & 1
        keep = lax.dynamic_index_in_dim(halves, mine, axis=1, keepdims=False)
        send = lax.dynamic_index_in_dim(halves, 1 - mine, axis=1, keepdims=False)
        arrived = lax.ppermute(send.astype(wire), axis_name, pairs)
        blocks = keep + arrived.astype(blocks.dtype)
        bit += 1
    return blocks[0]


def doubling_sum(values, axis_name, size):
    bit = 0
    while (1 << bit) < size:
        pairs = [(i, i ^ (1 << bit)) for i in range(size)]
        values = values + lax.ppermute(values, axis_name, pairs)
        bit += 1
    return values


def on_device_body(
    dp_size,
    patches,
    counts,
    norm_gain,
    norm_bias,
    w_qkv,
    b_qv,
    w_out,
    out_bias,
    w_up,
    b_up,
    w_down,
    cotangent,
):
    local_rows = patches.shape[0]
    width_here = w_qkv.shape[2]
    heads_here = width_here // HEAD_DIM
    ff_here = w_up.shape[1]
    tensor_pos = lax.axis_index("tensor")
    tensor_size = D // width_here
    score_scale = HEAD_DIM ** (-0.5)
    segment, grid_row, grid_col, is_valid = layout(counts[0])
    keep_rows = lax.dynamic_slice_in_dim(is_valid, tensor_pos * local_rows, local_rows)[:, None]
    slopes = slopes_of(tensor_pos * heads_here, heads_here)
    inputs = patches.astype(jnp.float32)
    inputs_all = lax.all_gather(patches, "tensor", axis=0, tiled=True).astype(jnp.float32)
    normed = normalize(inputs_all, norm_gain[0], norm_bias[0]).astype(jnp.bfloat16)
    projected = jnp.einsum("td,dsc->tsc", normed, w_qkv, preferred_element_type=jnp.float32)
    queries = (projected[:, 0] + b_qv[0]).astype(jnp.bfloat16)
    keys = projected[:, 1].astype(jnp.bfloat16)
    values = (projected[:, 2] + b_qv[1]).astype(jnp.bfloat16)

    def head_major(rows):
        return rows.reshape(TOK_DEV, heads_here, HEAD_DIM).transpose(1, 0, 2)

    def row_major(heads):
        return heads.transpose(1, 0, 2).reshape(TOK_DEV, width_here)

    key_lo, key_hi = key_ranges(segment, TOK_DEV)
    segment_f = segment.astype(jnp.float32)
    query_info = jnp.stack([grid_row, grid_col, segment_f], axis=1)
    key_info = jnp.stack([grid_row, grid_col, segment_f], axis=0)
    query_heads = head_major(queries) * jnp.asarray(score_scale, jnp.bfloat16)
    key_heads = head_major(keys)
    value_heads = head_major(values)
    mixed_f32, log_totals = attention_fwd(
        key_lo, key_hi, slopes, query_heads, key_heads, value_heads, query_info, key_info
    )
    upstream = cotangent.astype(jnp.float32)
    branch_grad = lax.all_gather(
        (keep_rows * upstream).astype(jnp.bfloat16), "tensor", axis=0, tiled=True
    )
    mixed_f32, log_totals, branch_grad = lax.optimization_barrier(
        (mixed_f32, log_totals, branch_grad)
    )
    mixed_rows = row_major(mixed_f32).astype(jnp.bfloat16)
    mixed_all = lax.all_gather(mixed_rows, "tensor", axis=1, tiled=True)
    w_out_all = lax.all_gather(w_out, "tensor", axis=0, tiled=True)
    attended = jnp.dot(mixed_all, w_out_all, preferred_element_type=jnp.float32)
    after_attn_all = inputs_all + is_valid[:, None] * (attended + out_bias[0])
    after_attn = lax.dynamic_slice_in_dim(after_attn_all, tensor_pos * local_rows, local_rows)
    normed_two = normalize(after_attn_all, norm_gain[1], norm_bias[1]).astype(jnp.bfloat16)
    hidden_pre = jnp.dot(normed_two, w_up, preferred_element_type=jnp.float32) + b_up
    hidden = jax.nn.gelu(hidden_pre, approximate=False).astype(jnp.bfloat16)
    branch_partial = jnp.dot(hidden, w_down, preferred_element_type=jnp.float32)
    down_bias_grad = jnp.sum(keep_rows * upstream, axis=0)
    w_down_grad_t = jnp.einsum(
        "td,tf->df", branch_grad, hidden, preferred_element_type=jnp.float32
    )
    hidden_grad = jnp.einsum("td,fd->tf", branch_grad, w_down, preferred_element_type=jnp.float32)
    _, gelu_back = jax.vjp(lambda pre_act: jax.nn.gelu(pre_act, approximate=False), hidden_pre)
    pre_grad = gelu_back(hidden_grad)[0].astype(jnp.bfloat16)
    up_bias_grad = jnp.sum(pre_grad, axis=0, dtype=jnp.float32)
    w_up_grad = jnp.einsum("td,tf->df", normed_two, pre_grad, preferred_element_type=jnp.float32)
    normed_two_grad = lax.psum_scatter(
        jnp.einsum("tf,df->td", pre_grad, w_up, preferred_element_type=jnp.float32).astype(
            jnp.bfloat16
        ),
        "tensor",
        scatter_dimension=0,
        tiled=True,
    ).astype(jnp.float32)
    branch_own, branch_out = scatter_blocks(branch_partial, tensor_size)
    normed_two_grad, branch_own, branch_out = lax.optimization_barrier(
        (normed_two_grad, branch_own, branch_out)
    )
    _, norm_two_back = jax.vjp(normalize, after_attn, norm_gain[1], norm_bias[1])
    through_two, gain_two_grad, shift_two_grad = norm_two_back(normed_two_grad)
    after_grad = upstream + through_two
    attn_bias_grad = jnp.sum(keep_rows * after_grad, axis=0)
    attn_local = (keep_rows * after_grad).astype(jnp.bfloat16)
    attn_grad = lax.all_gather(attn_local, "tensor", axis=0, tiled=True)
    w_out_grad_t = jnp.einsum(
        "td,tc->dc", attn_grad, mixed_rows, preferred_element_type=jnp.float32
    )
    mixed_grad = jnp.einsum(
        "td,cd->tc", attn_grad, w_out, preferred_element_type=jnp.float32
    ).astype(jnp.bfloat16)
    early_parts = jnp.concatenate([w_down_grad_t, w_up_grad, w_out_grad_t], axis=1).astype(
        jnp.bfloat16
    )
    early_parts, mixed_grad, branch_own, branch_out = lax.optimization_barrier(
        (early_parts, mixed_grad, branch_own, branch_out)
    )
    branch = exchange_blocks(branch_own, branch_out, tensor_size)
    result = (after_attn + keep_rows * (branch + out_bias[1])).astype(jnp.bfloat16)
    early_sum = lax.psum_scatter(early_parts, "dp", scatter_dimension=0, tiled=True).astype(
        jnp.float32
    )
    query_acc, key_acc, value_acc = attention_bwd(
        key_lo, key_hi, slopes, query_heads, key_heads, value_heads, query_info, key_info,
        mixed_f32, head_major(mixed_grad), log_totals,
    )
    query_acc, key_acc, value_acc, result = lax.optimization_barrier(
        (query_acc, key_acc, value_acc, result)
    )
    query_grad = row_major(query_acc * score_scale).astype(jnp.bfloat16)
    key_grad = row_major(key_acc).astype(jnp.bfloat16)
    value_grad = row_major(value_acc).astype(jnp.bfloat16)
    projected_grad = jnp.concatenate([query_grad, key_grad, value_grad], axis=1)
    projected_grad, early_sum = lax.optimization_barrier((projected_grad, early_sum))
    qv_bias_grad = jnp.stack(
        [
            jnp.sum(query_grad, axis=0, dtype=jnp.float32),
            jnp.sum(value_grad, axis=0, dtype=jnp.float32),
        ]
    )
    w_qkv_grad = jnp.einsum("td,tc->dc", normed, projected_grad, preferred_element_type=jnp.float32)
    normed_grad_partial = jnp.einsum(
        "tc,dc->td",
        projected_grad,
        w_qkv.reshape(D, 3 * width_here),
        preferred_element_type=jnp.float32,
    )
    centred_all = inputs_all - jnp.mean(inputs_all, axis=-1, keepdims=True)
    unit_all = centred_all * lax.rsqrt(
        jnp.mean(centred_all * centred_all, axis=-1, keepdims=True) + EPSILON
    )
    gain_one_grad = jnp.sum(normed_grad_partial * unit_all, axis=0)
    shift_one_grad = jnp.sum(normed_grad_partial, axis=0)
    normed_grad = scatter_tensor(normed_grad_partial, tensor_size)
    _, norm_one_back = jax.vjp(normalize, inputs, norm_gain[0], norm_bias[0])
    through_one = norm_one_back(normed_grad)[0]
    input_grad = (after_grad + through_one).astype(jnp.bfloat16)
    qv_full = lax.dynamic_update_slice_in_dim(
        jnp.zeros((2, D), jnp.float32), qv_bias_grad, tensor_pos * width_here, 1
    )
    up_full = lax.dynamic_update_slice_in_dim(
        jnp.zeros((FF,), jnp.float32), up_bias_grad, tensor_pos * ff_here, 0
    )
    small = jnp.concatenate(
        [
            jnp.stack([gain_one_grad, gain_two_grad]).reshape(-1),
            jnp.stack([shift_one_grad, shift_two_grad]).reshape(-1),
            jnp.stack([attn_bias_grad, down_bias_grad]).reshape(-1),
            qv_full.reshape(-1),
            up_full,
        ]
    )
    qkv_sum = halving_scatter(
        w_qkv_grad.reshape(dp_size, D // dp_size, -1), "dp", jnp.bfloat16
    )
    qkv_part = qkv_sum.reshape(-1, 3, width_here)
    summed = doubling_sum(doubling_sum(small, "dp", dp_size), "tensor", tensor_size)
    gains_grad = summed[: 2 * D].reshape(2, D)
    shifts_grad = summed[2 * D : 4 * D].reshape(2, D)
    outer_grad = summed[4 * D : 6 * D].reshape(2, D)
    qv_sum = summed[6 * D : 8 * D].reshape(2, D)
    up_sum = summed[8 * D :]
    down_part = early_sum[:, :ff_here].T
    up_part = early_sum[:, ff_here : 2 * ff_here]
    out_part = early_sum[:, 2 * ff_here :].T
    return (
        result,
        input_grad,
        gains_grad,
        shifts_grad,
        qkv_part,
        qv_sum,
        out_part,
        outer_grad,
        up_part,
        up_sum,
        down_part,
    )


def solution(mesh):
    placed = (
        P(("dp", "tensor"), None),
        P("dp", None),
        P(),
        P(),
        P(None, None, "tensor"),
        P(None, "tensor"),
        P("tensor", None),
        P(),
        P(None, "tensor"),
        P("tensor"),
        P("tensor", None),
        P(("dp", "tensor"), None),
    )
    return jax.shard_map(
        functools.partial(on_device_body, mesh.shape["dp"]),
        mesh=mesh,
        in_specs=placed,
        out_specs=(
            P(("dp", "tensor"), None),
            P(("dp", "tensor"), None),
            P(),
            P(),
            P("dp", None, "tensor"),
            P(),
            P("tensor", "dp"),
            P(),
            P("dp", "tensor"),
            P(),
            P("tensor", "dp"),
        ),
        check_vma=False,
    )
```

```python
import functools

import jax
import jax.numpy as jnp
from jax import lax
from jax.experimental import pallas as pl
from jax.experimental.pallas import tpu as pltpu
from jax.sharding import PartitionSpec as P


D = 768
HEADS = 12
HEAD_DIM = 64
FF = 3072
SIDE_S = 12
SIDE_M = 15
SIDE_L = 20
TOK_DEV = 2048


EPSILON = 1e-06


def layout(group_counts):
    positions = jnp.arange(TOK_DEV, dtype=jnp.int32)
    area_small = SIDE_S * SIDE_S
    area_middle = SIDE_M * SIDE_M
    area_large = SIDE_L * SIDE_L
    end_small = group_counts[0] * area_small
    end_middle = end_small + group_counts[1] * area_middle
    end_large = end_middle + group_counts[2] * area_large
    size_class = (positions >= end_small).astype(jnp.int32) + (positions >= end_middle).astype(
        jnp.int32
    )
    begins = jnp.where(size_class == 0, 0, jnp.where(size_class == 1, end_small, end_middle))
    area_len = jnp.where(
        size_class == 0, area_small, jnp.where(size_class == 1, area_middle, area_large)
    )
    side_len = jnp.where(size_class == 0, SIDE_S, jnp.where(size_class == 1, SIDE_M, SIDE_L))
    within = positions - begins
    picture_index = within // area_len
    within_image = within % area_len
    is_valid = positions < end_large
    segment = jnp.where(is_valid, size_class * 16 + picture_index, 255)
    grid_row = (within_image // side_len).astype(jnp.float32)
    grid_col = (within_image % side_len).astype(jnp.float32)
    return (segment, grid_row, grid_col, is_valid.astype(jnp.float32))


def normalize(values, gain_row, shift_row):
    centred = values - jnp.mean(values, axis=-1, keepdims=True)
    spread = jnp.mean(centred * centred, axis=-1, keepdims=True)
    return centred * lax.rsqrt(spread + EPSILON) * gain_row + shift_row


def slopes_of(first_head, count_heads):
    head_number = (first_head + jnp.arange(count_heads, dtype=jnp.int32)).astype(jnp.float32) + 1.0
    return jnp.exp2(-8.0 * head_number / HEADS)


Q_BLOCK = 256
K_BLOCK = 256
NEG = -1e30


def key_ranges(segment, tokens):
    starts = jnp.arange(0, tokens, Q_BLOCK)
    first = segment[starts]
    last = segment[starts + Q_BLOCK - 1]
    key_lo = jnp.sum(segment[None, :] < first[:, None], axis=1)
    key_hi = jnp.sum(segment[None, :] <= last[:, None], axis=1)
    return (key_lo // K_BLOCK).astype(jnp.int32), ((key_hi + K_BLOCK - 1) // K_BLOCK).astype(jnp.int32)


def block_geometry(qi_ref, ki_ref, start):
    rq = qi_ref[:, 0:1]
    cq = qi_ref[:, 1:2]
    sq = qi_ref[:, 2:3]
    rk = ki_ref[0:1, pl.ds(start, K_BLOCK)]
    ck = ki_ref[1:2, pl.ds(start, K_BLOCK)]
    sk = ki_ref[2:3, pl.ds(start, K_BLOCK)]
    dr = rq - rk
    dc = cq - ck
    return jnp.where(sq == sk, jnp.sqrt(dr * dr + dc * dc), jnp.inf)


def fwd_kernel(heads, lo_ref, hi_ref, slope_ref, q_ref, k_ref, v_ref, qi_ref, ki_ref, o_ref, lse_ref):
    i = pl.program_id(0)
    queries = [q_ref[h] for h in range(heads)]
    width = q_ref.shape[2]

    def body(kb, carry):
        start = pl.multiple_of(kb * K_BLOCK, K_BLOCK)
        dist = block_geometry(qi_ref, ki_ref, start)
        out = []
        for h in range(heads):
            m_old, l_old, acc_old = carry[h]
            keys = k_ref[h, pl.ds(start, K_BLOCK), :]
            vals = v_ref[h, pl.ds(start, K_BLOCK), :]
            s = lax.dot_general(queries[h], keys, (((1,), (1,)), ((), ())),
                                preferred_element_type=jnp.float32) - slope_ref[h] * dist
            m_new = jnp.maximum(m_old, jnp.max(s, axis=1, keepdims=True))
            alpha = jnp.exp(m_old - m_new)
            p = jnp.exp(s - m_new)
            l_new = alpha * l_old + jnp.sum(p, axis=1, keepdims=True)
            acc_new = alpha * acc_old + jnp.dot(p.astype(jnp.bfloat16), vals,
                                                preferred_element_type=jnp.float32)
            out.append((m_new, l_new, acc_new))
        return tuple(out)

    init = tuple(
        (jnp.full((Q_BLOCK, 1), NEG, jnp.float32), jnp.zeros((Q_BLOCK, 1), jnp.float32),
         jnp.zeros((Q_BLOCK, width), jnp.float32))
        for _ in range(heads)
    )
    final = lax.fori_loop(lo_ref[i], hi_ref[i], body, init)
    for h in range(heads):
        m, l, acc = final[h]
        o_ref[h] = acc / l
        lse_ref[h] = m + jnp.log(l)


def bwd_kernel(heads, lo_ref, hi_ref, slope_ref, q_ref, k_ref, v_ref, qi_ref, ki_ref,
               o_ref, do_ref, lse_ref, dq_ref, dk_ref, dv_ref):
    i = pl.program_id(0)

    @pl.when(i == 0)
    def _():
        dk_ref[...] = jnp.zeros_like(dk_ref)
        dv_ref[...] = jnp.zeros_like(dv_ref)

    queries = [q_ref[h] for h in range(heads)]
    grads = [do_ref[h] for h in range(heads)]
    lses = [lse_ref[h] for h in range(heads)]
    deltas = [jnp.sum(grads[h].astype(jnp.float32) * o_ref[h], axis=1, keepdims=True)
              for h in range(heads)]
    width = q_ref.shape[2]

    def body(kb, carry):
        start = pl.multiple_of(kb * K_BLOCK, K_BLOCK)
        dist = block_geometry(qi_ref, ki_ref, start)
        out = []
        for h in range(heads):
            keys = k_ref[h, pl.ds(start, K_BLOCK), :]
            vals = v_ref[h, pl.ds(start, K_BLOCK), :]
            s = lax.dot_general(queries[h], keys, (((1,), (1,)), ((), ())),
                                preferred_element_type=jnp.float32) - slope_ref[h] * dist
            p = jnp.exp(s - lses[h])
            dp = lax.dot_general(grads[h], vals, (((1,), (1,)), ((), ())),
                                 preferred_element_type=jnp.float32)
            ds = (p * (dp - deltas[h])).astype(jnp.bfloat16)
            out.append(carry[h] + jnp.dot(ds, keys, preferred_element_type=jnp.float32))
            dk_ref[h, pl.ds(start, K_BLOCK), :] += lax.dot_general(
                ds, queries[h], (((0,), (0,)), ((), ())), preferred_element_type=jnp.float32)
            dv_ref[h, pl.ds(start, K_BLOCK), :] += lax.dot_general(
                p.astype(jnp.bfloat16), grads[h], (((0,), (0,)), ((), ())),
                preferred_element_type=jnp.float32)
        return tuple(out)

    init = tuple(jnp.zeros((Q_BLOCK, width), jnp.float32) for _ in range(heads))
    final = lax.fori_loop(lo_ref[i], hi_ref[i], body, init)
    for h in range(heads):
        dq_ref[h] = final[h]


def attention_fwd(lo, hi, slopes, q, k, v, qinfo, kinfo):
    heads, tokens, width = q.shape
    grid = (tokens // Q_BLOCK,)
    whole = lambda i, lo, hi: (0, 0, 0)
    rows = lambda i, lo, hi: (0, i, 0)
    return pl.pallas_call(
        functools.partial(fwd_kernel, heads),
        grid_spec=pltpu.PrefetchScalarGridSpec(
            num_scalar_prefetch=2,
            grid=grid,
            in_specs=[
                pl.BlockSpec(memory_space=pltpu.SMEM),
                pl.BlockSpec((heads, Q_BLOCK, width), rows),
                pl.BlockSpec((heads, tokens, width), whole),
                pl.BlockSpec((heads, tokens, width), whole),
                pl.BlockSpec((Q_BLOCK, 3), lambda i, lo, hi: (i, 0)),
                pl.BlockSpec((3, tokens), lambda i, lo, hi: (0, 0)),
            ],
            out_specs=[
                pl.BlockSpec((heads, Q_BLOCK, width), rows),
                pl.BlockSpec((heads, Q_BLOCK, 1), rows),
            ],
        ),
        out_shape=[
            jax.ShapeDtypeStruct((heads, tokens, width), jnp.float32),
            jax.ShapeDtypeStruct((heads, tokens, 1), jnp.float32),
        ],
        compiler_params=pltpu.CompilerParams(dimension_semantics=("arbitrary",)),
    )(lo, hi, slopes, q, k, v, qinfo, kinfo)


def attention_bwd(lo, hi, slopes, q, k, v, qinfo, kinfo, o, do, lse):
    heads, tokens, width = q.shape
    grid = (tokens // Q_BLOCK,)
    whole = lambda i, lo, hi: (0, 0, 0)
    rows = lambda i, lo, hi: (0, i, 0)
    return pl.pallas_call(
        functools.partial(bwd_kernel, heads),
        grid_spec=pltpu.PrefetchScalarGridSpec(
            num_scalar_prefetch=2,
            grid=grid,
            in_specs=[
                pl.BlockSpec(memory_space=pltpu.SMEM),
                pl.BlockSpec((heads, Q_BLOCK, width), rows),
                pl.BlockSpec((heads, tokens, width), whole),
                pl.BlockSpec((heads, tokens, width), whole),
                pl.BlockSpec((Q_BLOCK, 3), lambda i, lo, hi: (i, 0)),
                pl.BlockSpec((3, tokens), lambda i, lo, hi: (0, 0)),
                pl.BlockSpec((heads, Q_BLOCK, width), rows),
                pl.BlockSpec((heads, Q_BLOCK, width), rows),
                pl.BlockSpec((heads, Q_BLOCK, 1), rows),
            ],
            out_specs=[
                pl.BlockSpec((heads, Q_BLOCK, width), rows),
                pl.BlockSpec((heads, tokens, width), whole),
                pl.BlockSpec((heads, tokens, width), whole),
            ],
        ),
        out_shape=[
            jax.ShapeDtypeStruct((heads, tokens, width), jnp.float32),
            jax.ShapeDtypeStruct((heads, tokens, width), jnp.float32),
            jax.ShapeDtypeStruct((heads, tokens, width), jnp.float32),
        ],
        compiler_params=pltpu.CompilerParams(dimension_semantics=("arbitrary",)),
    )(lo, hi, slopes, q, k, v, qinfo, kinfo, o, do, lse)


def scatter_blocks(partial, tensor_size):
    me = lax.axis_index("tensor")
    blocks = partial.reshape(tensor_size, -1, partial.shape[1])
    own = lax.dynamic_index_in_dim(blocks, me, keepdims=False).astype(jnp.float32)
    outgoing = [
        lax.dynamic_index_in_dim(blocks, (me + shift) % tensor_size, keepdims=False).astype(
            jnp.bfloat16
        )
        for shift in range(1, tensor_size)
    ]
    return own, outgoing


def exchange_blocks(own, outgoing, tensor_size):
    total = own
    for shift in range(1, tensor_size):
        pairs = [(i, (i + shift) % tensor_size) for i in range(tensor_size)]
        total = total + lax.ppermute(outgoing[shift - 1], "tensor", pairs).astype(jnp.float32)
    return total


def scatter_tensor(partial, tensor_size):
    return exchange_blocks(*scatter_blocks(partial, tensor_size), tensor_size)


def halving_scatter(blocks, axis_name, wire):
    me = lax.axis_index(axis_name)
    bit = 0
    while blocks.shape[0] > 1:
        pairs = [(i, i ^ (1 << bit)) for i in range(blocks.shape[0] << bit)]
        halves = blocks.reshape((blocks.shape[0] // 2, 2) + blocks.shape[1:])
        mine = (me >> bit) & 1
        keep = lax.dynamic_index_in_dim(halves, mine, axis=1, keepdims=False)
        send = lax.dynamic_index_in_dim(halves, 1 - mine, axis=1, keepdims=False)
        arrived = lax.ppermute(send.astype(wire), axis_name, pairs)
        blocks = keep + arrived.astype(blocks.dtype)
        bit += 1
    return blocks[0]


def doubling_sum(values, axis_name, size):
    bit = 0
    while (1 << bit) < size:
        pairs = [(i, i ^ (1 << bit)) for i in range(size)]
        values = values + lax.ppermute(values, axis_name, pairs)
        bit += 1
    return values


def on_device_body(
    dp_size,
    patches,
    counts,
    norm_gain,
    norm_bias,
    w_qkv,
    b_qv,
    w_out,
    out_bias,
    w_up,
    b_up,
    w_down,
    cotangent,
):
    local_rows = patches.shape[0]
    width_here = w_qkv.shape[2]
    heads_here = width_here // HEAD_DIM
    ff_here = w_up.shape[1]
    tensor_pos = lax.axis_index("tensor")
    tensor_size = D // width_here
    score_scale = HEAD_DIM ** (-0.5)
    segment, grid_row, grid_col, is_valid = layout(counts[0])
    keep_rows = lax.dynamic_slice_in_dim(is_valid, tensor_pos * local_rows, local_rows)[:, None]
    slopes = slopes_of(tensor_pos * heads_here, heads_here)
    inputs = patches.astype(jnp.float32)
    inputs_all = lax.all_gather(patches, "tensor", axis=0, tiled=True).astype(jnp.float32)
    normed = normalize(inputs_all, norm_gain[0], norm_bias[0]).astype(jnp.bfloat16)
    projected = jnp.einsum(
        "td,dshe->shte",
        normed,
        w_qkv.reshape(D, 3, heads_here, HEAD_DIM),
        preferred_element_type=jnp.float32,
    )
    bias_heads = b_qv.reshape(2, heads_here, 1, HEAD_DIM)
    query_heads = (projected[0] + bias_heads[0]).astype(jnp.bfloat16) * jnp.asarray(
        score_scale, jnp.bfloat16
    )
    key_heads = projected[1].astype(jnp.bfloat16)
    value_heads = (projected[2] + bias_heads[1]).astype(jnp.bfloat16)

    def head_major(rows):
        return rows.reshape(TOK_DEV, heads_here, HEAD_DIM).transpose(1, 0, 2)

    def row_major(heads):
        return heads.transpose(1, 0, 2).reshape(TOK_DEV, width_here)

    key_lo, key_hi = key_ranges(segment, TOK_DEV)
    segment_f = segment.astype(jnp.float32)
    query_info = jnp.stack([grid_row, grid_col, segment_f], axis=1)
    key_info = jnp.stack([grid_row, grid_col, segment_f], axis=0)
    mixed_f32, log_totals = attention_fwd(
        key_lo, key_hi, slopes, query_heads, key_heads, value_heads, query_info, key_info
    )
    upstream = cotangent.astype(jnp.float32)
    branch_grad = lax.all_gather(
        (keep_rows * upstream).astype(jnp.bfloat16), "tensor", axis=0, tiled=True
    )
    mixed_f32, log_totals, branch_grad = lax.optimization_barrier(
        (mixed_f32, log_totals, branch_grad)
    )
    mixed_rows = row_major(mixed_f32).astype(jnp.bfloat16)
    mixed_all = lax.all_gather(mixed_rows, "tensor", axis=1, tiled=True)
    w_out_all = lax.all_gather(w_out, "tensor", axis=0, tiled=True)
    attended = jnp.dot(mixed_all, w_out_all, preferred_element_type=jnp.float32)
    after_attn_all = inputs_all + is_valid[:, None] * (attended + out_bias[0])
    after_attn = lax.dynamic_slice_in_dim(after_attn_all, tensor_pos * local_rows, local_rows)
    normed_two = normalize(after_attn_all, norm_gain[1], norm_bias[1]).astype(jnp.bfloat16)
    hidden_pre = jnp.dot(normed_two, w_up, preferred_element_type=jnp.float32) + b_up
    hidden = jax.nn.gelu(hidden_pre, approximate=False).astype(jnp.bfloat16)
    branch_partial = jnp.dot(hidden, w_down, preferred_element_type=jnp.float32)
    down_bias_grad = jnp.sum(keep_rows * upstream, axis=0)
    w_down_grad_t = jnp.einsum(
        "td,tf->df", branch_grad, hidden, preferred_element_type=jnp.float32
    )
    hidden_grad = jnp.einsum("td,fd->tf", branch_grad, w_down, preferred_element_type=jnp.float32)
    _, gelu_back = jax.vjp(lambda pre_act: jax.nn.gelu(pre_act, approximate=False), hidden_pre)
    pre_grad = gelu_back(hidden_grad)[0].astype(jnp.bfloat16)
    up_bias_grad = jnp.sum(pre_grad, axis=0, dtype=jnp.float32)
    w_up_grad = jnp.einsum("td,tf->df", normed_two, pre_grad, preferred_element_type=jnp.float32)
    normed_two_grad = lax.psum_scatter(
        jnp.einsum("tf,df->td", pre_grad, w_up, preferred_element_type=jnp.float32).astype(
            jnp.bfloat16
        ),
        "tensor",
        scatter_dimension=0,
        tiled=True,
    ).astype(jnp.float32)
    branch_own, branch_out = scatter_blocks(branch_partial, tensor_size)
    normed_two_grad, branch_own, branch_out = lax.optimization_barrier(
        (normed_two_grad, branch_own, branch_out)
    )
    _, norm_two_back = jax.vjp(normalize, after_attn, norm_gain[1], norm_bias[1])
    through_two, gain_two_grad, shift_two_grad = norm_two_back(normed_two_grad)
    after_grad = upstream + through_two
    attn_bias_grad = jnp.sum(keep_rows * after_grad, axis=0)
    attn_local = (keep_rows * after_grad).astype(jnp.bfloat16)
    attn_grad = lax.all_gather(attn_local, "tensor", axis=0, tiled=True)
    w_out_grad_t = jnp.einsum(
        "td,tc->dc", attn_grad, mixed_rows, preferred_element_type=jnp.float32
    )
    mixed_grad = jnp.einsum(
        "td,cd->tc", attn_grad, w_out, preferred_element_type=jnp.float32
    ).astype(jnp.bfloat16)
    early_parts = jnp.concatenate([w_down_grad_t, w_up_grad, w_out_grad_t], axis=1).astype(
        jnp.bfloat16
    )
    early_parts, mixed_grad, branch_own, branch_out = lax.optimization_barrier(
        (early_parts, mixed_grad, branch_own, branch_out)
    )
    branch = exchange_blocks(branch_own, branch_out, tensor_size)
    result = (after_attn + keep_rows * (branch + out_bias[1])).astype(jnp.bfloat16)
    early_sum = lax.psum_scatter(early_parts, "dp", scatter_dimension=0, tiled=True).astype(
        jnp.float32
    )
    query_acc, key_acc, value_acc = attention_bwd(
        key_lo, key_hi, slopes, query_heads, key_heads, value_heads, query_info, key_info,
        mixed_f32, head_major(mixed_grad), log_totals,
    )
    query_acc, key_acc, value_acc, result = lax.optimization_barrier(
        (query_acc, key_acc, value_acc, result)
    )
    query_grad = row_major(query_acc * score_scale).astype(jnp.bfloat16)
    key_grad = row_major(key_acc).astype(jnp.bfloat16)
    value_grad = row_major(value_acc).astype(jnp.bfloat16)
    projected_grad = jnp.concatenate([query_grad, key_grad, value_grad], axis=1)
    projected_grad, early_sum = lax.optimization_barrier((projected_grad, early_sum))
    qv_bias_grad = jnp.stack(
        [
            jnp.sum(query_grad, axis=0, dtype=jnp.float32),
            jnp.sum(value_grad, axis=0, dtype=jnp.float32),
        ]
    )
    w_qkv_grad = jnp.einsum("td,tc->dc", normed, projected_grad, preferred_element_type=jnp.float32)
    normed_grad_partial = jnp.einsum(
        "tc,dc->td",
        projected_grad,
        w_qkv.reshape(D, 3 * width_here),
        preferred_element_type=jnp.float32,
    )
    centred_all = inputs_all - jnp.mean(inputs_all, axis=-1, keepdims=True)
    unit_all = centred_all * lax.rsqrt(
        jnp.mean(centred_all * centred_all, axis=-1, keepdims=True) + EPSILON
    )
    gain_one_grad = jnp.sum(normed_grad_partial * unit_all, axis=0)
    shift_one_grad = jnp.sum(normed_grad_partial, axis=0)
    normed_grad = scatter_tensor(normed_grad_partial, tensor_size)
    _, norm_one_back = jax.vjp(normalize, inputs, norm_gain[0], norm_bias[0])
    through_one = norm_one_back(normed_grad)[0]
    input_grad = (after_grad + through_one).astype(jnp.bfloat16)
    qv_full = lax.dynamic_update_slice_in_dim(
        jnp.zeros((2, D), jnp.float32), qv_bias_grad, tensor_pos * width_here, 1
    )
    up_full = lax.dynamic_update_slice_in_dim(
        jnp.zeros((FF,), jnp.float32), up_bias_grad, tensor_pos * ff_here, 0
    )
    small = jnp.concatenate(
        [
            jnp.stack([gain_one_grad, gain_two_grad]).reshape(-1),
            jnp.stack([shift_one_grad, shift_two_grad]).reshape(-1),
            jnp.stack([attn_bias_grad, down_bias_grad]).reshape(-1),
            qv_full.reshape(-1),
            up_full,
        ]
    )
    qkv_sum = halving_scatter(
        w_qkv_grad.reshape(dp_size, D // dp_size, -1), "dp", jnp.bfloat16
    )
    qkv_part = qkv_sum.reshape(-1, 3, width_here)
    summed = doubling_sum(doubling_sum(small, "dp", dp_size), "tensor", tensor_size)
    gains_grad = summed[: 2 * D].reshape(2, D)
    shifts_grad = summed[2 * D : 4 * D].reshape(2, D)
    outer_grad = summed[4 * D : 6 * D].reshape(2, D)
    qv_sum = summed[6 * D : 8 * D].reshape(2, D)
    up_sum = summed[8 * D :]
    down_part = early_sum[:, :ff_here].T
    up_part = early_sum[:, ff_here : 2 * ff_here]
    out_part = early_sum[:, 2 * ff_here :].T
    return (
        result,
        input_grad,
        gains_grad,
        shifts_grad,
        qkv_part,
        qv_sum,
        out_part,
        outer_grad,
        up_part,
        up_sum,
        down_part,
    )


def solution(mesh):
    placed = (
        P(("dp", "tensor"), None),
        P("dp", None),
        P(),
        P(),
        P(None, None, "tensor"),
        P(None, "tensor"),
        P("tensor", None),
        P(),
        P(None, "tensor"),
        P("tensor"),
        P("tensor", None),
        P(("dp", "tensor"), None),
    )
    return jax.shard_map(
        functools.partial(on_device_body, mesh.shape["dp"]),
        mesh=mesh,
        in_specs=placed,
        out_specs=(
            P(("dp", "tensor"), None),
            P(("dp", "tensor"), None),
            P(),
            P(),
            P("dp", None, "tensor"),
            P(),
            P("tensor", "dp"),
            P(),
            P("dp", "tensor"),
            P(),
            P("tensor", "dp"),
        ),
        check_vma=False,
    )
```

```python
import functools

import jax
import jax.numpy as jnp
from jax import lax
from jax.experimental import pallas as pl
from jax.experimental.pallas import tpu as pltpu
from jax.sharding import PartitionSpec as P


D = 768
HEADS = 12
HEAD_DIM = 64
FF = 3072
SIDE_S = 12
SIDE_M = 15
SIDE_L = 20
TOK_DEV = 2048


EPSILON = 1e-06


def layout(group_counts):
    positions = jnp.arange(TOK_DEV, dtype=jnp.int32)
    area_small = SIDE_S * SIDE_S
    area_middle = SIDE_M * SIDE_M
    area_large = SIDE_L * SIDE_L
    end_small = group_counts[0] * area_small
    end_middle = end_small + group_counts[1] * area_middle
    end_large = end_middle + group_counts[2] * area_large
    size_class = (positions >= end_small).astype(jnp.int32) + (positions >= end_middle).astype(
        jnp.int32
    )
    begins = jnp.where(size_class == 0, 0, jnp.where(size_class == 1, end_small, end_middle))
    area_len = jnp.where(
        size_class == 0, area_small, jnp.where(size_class == 1, area_middle, area_large)
    )
    side_len = jnp.where(size_class == 0, SIDE_S, jnp.where(size_class == 1, SIDE_M, SIDE_L))
    within = positions - begins
    picture_index = within // area_len
    within_image = within % area_len
    is_valid = positions < end_large
    segment = jnp.where(is_valid, size_class * 16 + picture_index, 255)
    grid_row = (within_image // side_len).astype(jnp.float32)
    grid_col = (within_image % side_len).astype(jnp.float32)
    return (segment, grid_row, grid_col, is_valid.astype(jnp.float32))


def normalize(values, gain_row, shift_row):
    centred = values - jnp.mean(values, axis=-1, keepdims=True)
    spread = jnp.mean(centred * centred, axis=-1, keepdims=True)
    return centred * lax.rsqrt(spread + EPSILON) * gain_row + shift_row


def slopes_of(first_head, count_heads):
    head_number = (first_head + jnp.arange(count_heads, dtype=jnp.int32)).astype(jnp.float32) + 1.0
    return jnp.exp2(-8.0 * head_number / HEADS)


Q_BLOCK = 256
K_BLOCK = 256
NEG = -1e30


def key_ranges(segment, tokens):
    starts = jnp.arange(0, tokens, Q_BLOCK)
    first = segment[starts]
    last = segment[starts + Q_BLOCK - 1]
    key_lo = jnp.sum(segment[None, :] < first[:, None], axis=1)
    key_hi = jnp.sum(segment[None, :] <= last[:, None], axis=1)
    return (key_lo // K_BLOCK).astype(jnp.int32), ((key_hi + K_BLOCK - 1) // K_BLOCK).astype(jnp.int32)


def block_geometry(qi_ref, ki_ref, start):
    rq = qi_ref[:, 0:1]
    cq = qi_ref[:, 1:2]
    sq = qi_ref[:, 2:3]
    rk = ki_ref[0:1, pl.ds(start, K_BLOCK)]
    ck = ki_ref[1:2, pl.ds(start, K_BLOCK)]
    sk = ki_ref[2:3, pl.ds(start, K_BLOCK)]
    dr = rq - rk
    dc = cq - ck
    return jnp.where(sq == sk, jnp.sqrt(dr * dr + dc * dc), jnp.inf)


def fwd_kernel(heads, lo_ref, hi_ref, slope_ref, q_ref, k_ref, v_ref, qi_ref, ki_ref, o_ref, lse_ref):
    i = pl.program_id(0)
    queries = [q_ref[h] for h in range(heads)]
    width = q_ref.shape[2]

    def body(kb, carry):
        start = pl.multiple_of(kb * K_BLOCK, K_BLOCK)
        dist = block_geometry(qi_ref, ki_ref, start)
        out = []
        for h in range(heads):
            m_old, l_old, acc_old = carry[h]
            keys = k_ref[h, pl.ds(start, K_BLOCK), :]
            vals = v_ref[h, pl.ds(start, K_BLOCK), :]
            s = lax.dot_general(queries[h], keys, (((1,), (1,)), ((), ())),
                                preferred_element_type=jnp.float32) - slope_ref[h] * dist
            m_new = jnp.maximum(m_old, jnp.max(s, axis=1, keepdims=True))
            alpha = jnp.exp(m_old - m_new)
            p = jnp.exp(s - m_new)
            l_new = alpha * l_old + jnp.sum(p, axis=1, keepdims=True)
            acc_new = alpha * acc_old + jnp.dot(p.astype(jnp.bfloat16), vals,
                                                preferred_element_type=jnp.float32)
            out.append((m_new, l_new, acc_new))
        return tuple(out)

    init = tuple(
        (jnp.full((Q_BLOCK, 1), NEG, jnp.float32), jnp.zeros((Q_BLOCK, 1), jnp.float32),
         jnp.zeros((Q_BLOCK, width), jnp.float32))
        for _ in range(heads)
    )
    final = lax.fori_loop(lo_ref[i], hi_ref[i], body, init)
    for h in range(heads):
        m, l, acc = final[h]
        o_ref[h] = acc / l
        lse_ref[h] = m + jnp.log(l)


def bwd_kernel(heads, scale, lo_ref, hi_ref, slope_ref, q_ref, k_ref, v_ref, qi_ref, ki_ref,
               o_ref, do_ref, lse_ref, dq_ref, dk_ref, dv_ref):
    i = pl.program_id(0)

    @pl.when(i == 0)
    def _():
        dk_ref[...] = jnp.zeros_like(dk_ref)
        dv_ref[...] = jnp.zeros_like(dv_ref)

    queries = [q_ref[h] for h in range(heads)]
    grads = [do_ref[h] for h in range(heads)]
    lses = [lse_ref[h] for h in range(heads)]
    deltas = [jnp.sum(grads[h].astype(jnp.float32) * o_ref[h], axis=1, keepdims=True)
              for h in range(heads)]
    width = q_ref.shape[2]

    def body(kb, carry):
        start = pl.multiple_of(kb * K_BLOCK, K_BLOCK)
        dist = block_geometry(qi_ref, ki_ref, start)
        out = []
        for h in range(heads):
            keys = k_ref[h, pl.ds(start, K_BLOCK), :]
            vals = v_ref[h, pl.ds(start, K_BLOCK), :]
            s = lax.dot_general(queries[h], keys, (((1,), (1,)), ((), ())),
                                preferred_element_type=jnp.float32) - slope_ref[h] * dist
            p = jnp.exp(s - lses[h])
            dp = lax.dot_general(grads[h], vals, (((1,), (1,)), ((), ())),
                                 preferred_element_type=jnp.float32)
            ds = (p * (dp - deltas[h])).astype(jnp.bfloat16)
            out.append(carry[h] + jnp.dot(ds, keys, preferred_element_type=jnp.float32))
            dk_ref[h, pl.ds(start, K_BLOCK), :] += lax.dot_general(
                ds, queries[h], (((0,), (0,)), ((), ())), preferred_element_type=jnp.float32)
            dv_ref[h, pl.ds(start, K_BLOCK), :] += lax.dot_general(
                p.astype(jnp.bfloat16), grads[h], (((0,), (0,)), ((), ())),
                preferred_element_type=jnp.float32)
        return tuple(out)

    init = tuple(jnp.zeros((Q_BLOCK, width), jnp.float32) for _ in range(heads))
    final = lax.fori_loop(lo_ref[i], hi_ref[i], body, init)
    for h in range(heads):
        dq_ref[h] = (final[h] * scale).astype(dq_ref.dtype)


def attention_fwd(lo, hi, slopes, q, k, v, qinfo, kinfo):
    heads, tokens, width = q.shape
    grid = (tokens // Q_BLOCK,)
    whole = lambda i, lo, hi: (0, 0, 0)
    rows = lambda i, lo, hi: (0, i, 0)
    return pl.pallas_call(
        functools.partial(fwd_kernel, heads),
        grid_spec=pltpu.PrefetchScalarGridSpec(
            num_scalar_prefetch=2,
            grid=grid,
            in_specs=[
                pl.BlockSpec(memory_space=pltpu.SMEM),
                pl.BlockSpec((heads, Q_BLOCK, width), rows),
                pl.BlockSpec((heads, tokens, width), whole),
                pl.BlockSpec((heads, tokens, width), whole),
                pl.BlockSpec((Q_BLOCK, 3), lambda i, lo, hi: (i, 0)),
                pl.BlockSpec((3, tokens), lambda i, lo, hi: (0, 0)),
            ],
            out_specs=[
                pl.BlockSpec((heads, Q_BLOCK, width), rows),
                pl.BlockSpec((heads, Q_BLOCK, 1), rows),
            ],
        ),
        out_shape=[
            jax.ShapeDtypeStruct((heads, tokens, width), jnp.float32),
            jax.ShapeDtypeStruct((heads, tokens, 1), jnp.float32),
        ],
        compiler_params=pltpu.CompilerParams(dimension_semantics=("arbitrary",)),
    )(lo, hi, slopes, q, k, v, qinfo, kinfo)


def attention_bwd(lo, hi, slopes, q, k, v, qinfo, kinfo, o, do, lse, scale):
    heads, tokens, width = q.shape
    grid = (tokens // Q_BLOCK,)
    whole = lambda i, lo, hi: (0, 0, 0)
    rows = lambda i, lo, hi: (0, i, 0)
    return pl.pallas_call(
        functools.partial(bwd_kernel, heads, scale),
        grid_spec=pltpu.PrefetchScalarGridSpec(
            num_scalar_prefetch=2,
            grid=grid,
            in_specs=[
                pl.BlockSpec(memory_space=pltpu.SMEM),
                pl.BlockSpec((heads, Q_BLOCK, width), rows),
                pl.BlockSpec((heads, tokens, width), whole),
                pl.BlockSpec((heads, tokens, width), whole),
                pl.BlockSpec((Q_BLOCK, 3), lambda i, lo, hi: (i, 0)),
                pl.BlockSpec((3, tokens), lambda i, lo, hi: (0, 0)),
                pl.BlockSpec((heads, Q_BLOCK, width), rows),
                pl.BlockSpec((heads, Q_BLOCK, width), rows),
                pl.BlockSpec((heads, Q_BLOCK, 1), rows),
            ],
            out_specs=[
                pl.BlockSpec((heads, Q_BLOCK, width), rows),
                pl.BlockSpec((heads, tokens, width), whole),
                pl.BlockSpec((heads, tokens, width), whole),
            ],
        ),
        out_shape=[
            jax.ShapeDtypeStruct((heads, tokens, width), jnp.bfloat16),
            jax.ShapeDtypeStruct((heads, tokens, width), jnp.float32),
            jax.ShapeDtypeStruct((heads, tokens, width), jnp.float32),
        ],
        compiler_params=pltpu.CompilerParams(dimension_semantics=("arbitrary",)),
    )(lo, hi, slopes, q, k, v, qinfo, kinfo, o, do, lse)


def scatter_blocks(partial, tensor_size):
    me = lax.axis_index("tensor")
    blocks = partial.reshape(tensor_size, -1, partial.shape[1])
    own = lax.dynamic_index_in_dim(blocks, me, keepdims=False).astype(jnp.float32)
    outgoing = [
        lax.dynamic_index_in_dim(blocks, (me + shift) % tensor_size, keepdims=False).astype(
            jnp.bfloat16
        )
        for shift in range(1, tensor_size)
    ]
    return own, outgoing


def exchange_blocks(own, outgoing, tensor_size):
    total = own
    for shift in range(1, tensor_size):
        pairs = [(i, (i + shift) % tensor_size) for i in range(tensor_size)]
        total = total + lax.ppermute(outgoing[shift - 1], "tensor", pairs).astype(jnp.float32)
    return total


def scatter_tensor(partial, tensor_size):
    return exchange_blocks(*scatter_blocks(partial, tensor_size), tensor_size)


def halving_scatter(blocks, axis_name, wire):
    me = lax.axis_index(axis_name)
    bit = 0
    while blocks.shape[0] > 1:
        pairs = [(i, i ^ (1 << bit)) for i in range(blocks.shape[0] << bit)]
        halves = blocks.reshape((blocks.shape[0] // 2, 2) + blocks.shape[1:])
        mine = (me >> bit) & 1
        keep = lax.dynamic_index_in_dim(halves, mine, axis=1, keepdims=False)
        send = lax.dynamic_index_in_dim(halves, 1 - mine, axis=1, keepdims=False)
        arrived = lax.ppermute(send.astype(wire), axis_name, pairs)
        blocks = keep + arrived.astype(blocks.dtype)
        bit += 1
    return blocks[0]


def doubling_sum(values, axis_name, size):
    bit = 0
    while (1 << bit) < size:
        pairs = [(i, i ^ (1 << bit)) for i in range(size)]
        values = values + lax.ppermute(values, axis_name, pairs)
        bit += 1
    return values


def on_device_body(
    dp_size,
    patches,
    counts,
    norm_gain,
    norm_bias,
    w_qkv,
    b_qv,
    w_out,
    out_bias,
    w_up,
    b_up,
    w_down,
    cotangent,
):
    local_rows = patches.shape[0]
    width_here = w_qkv.shape[2]
    heads_here = width_here // HEAD_DIM
    ff_here = w_up.shape[1]
    tensor_pos = lax.axis_index("tensor")
    tensor_size = D // width_here
    score_scale = HEAD_DIM ** (-0.5)
    segment, grid_row, grid_col, is_valid = layout(counts[0])
    keep_rows = lax.dynamic_slice_in_dim(is_valid, tensor_pos * local_rows, local_rows)[:, None]
    slopes = slopes_of(tensor_pos * heads_here, heads_here)
    inputs = patches.astype(jnp.float32)
    inputs_all = lax.all_gather(patches, "tensor", axis=0, tiled=True).astype(jnp.float32)
    normed = normalize(inputs_all, norm_gain[0], norm_bias[0]).astype(jnp.bfloat16)
    projected = jnp.einsum("td,dsc->tsc", normed, w_qkv, preferred_element_type=jnp.float32)
    queries = (projected[:, 0] + b_qv[0]).astype(jnp.bfloat16)
    keys = projected[:, 1].astype(jnp.bfloat16)
    values = (projected[:, 2] + b_qv[1]).astype(jnp.bfloat16)

    def head_major(rows):
        return rows.reshape(TOK_DEV, heads_here, HEAD_DIM).transpose(1, 0, 2)

    def row_major(heads):
        return heads.transpose(1, 0, 2).reshape(TOK_DEV, width_here)

    key_lo, key_hi = key_ranges(segment, TOK_DEV)
    segment_f = segment.astype(jnp.float32)
    query_info = jnp.stack([grid_row, grid_col, segment_f], axis=1)
    key_info = jnp.stack([grid_row, grid_col, segment_f], axis=0)
    query_heads = head_major(queries) * jnp.asarray(score_scale, jnp.bfloat16)
    key_heads = head_major(keys)
    value_heads = head_major(values)
    mixed_f32, log_totals = attention_fwd(
        key_lo, key_hi, slopes, query_heads, key_heads, value_heads, query_info, key_info
    )
    upstream = cotangent.astype(jnp.float32)
    branch_grad = lax.all_gather(
        (keep_rows * upstream).astype(jnp.bfloat16), "tensor", axis=0, tiled=True
    )
    mixed_f32, log_totals, branch_grad = lax.optimization_barrier(
        (mixed_f32, log_totals, branch_grad)
    )
    mixed_rows = row_major(mixed_f32).astype(jnp.bfloat16)
    mixed_all = lax.all_gather(mixed_rows, "tensor", axis=1, tiled=True)
    w_out_all = lax.all_gather(w_out, "tensor", axis=0, tiled=True)
    attended = jnp.dot(mixed_all, w_out_all, preferred_element_type=jnp.float32)
    after_attn_all = inputs_all + is_valid[:, None] * (attended + out_bias[0])
    after_attn = lax.dynamic_slice_in_dim(after_attn_all, tensor_pos * local_rows, local_rows)
    normed_two = normalize(after_attn_all, norm_gain[1], norm_bias[1]).astype(jnp.bfloat16)
    hidden_pre = jnp.dot(normed_two, w_up, preferred_element_type=jnp.float32) + b_up
    hidden = jax.nn.gelu(hidden_pre, approximate=False).astype(jnp.bfloat16)
    branch_partial = jnp.dot(hidden, w_down, preferred_element_type=jnp.float32)
    down_bias_grad = jnp.sum(keep_rows * upstream, axis=0)
    w_down_grad_t = jnp.einsum(
        "td,tf->df", branch_grad, hidden, preferred_element_type=jnp.float32
    )
    hidden_grad = jnp.einsum("td,fd->tf", branch_grad, w_down, preferred_element_type=jnp.float32)
    _, gelu_back = jax.vjp(lambda pre_act: jax.nn.gelu(pre_act, approximate=False), hidden_pre)
    pre_grad = gelu_back(hidden_grad)[0].astype(jnp.bfloat16)
    up_bias_grad = jnp.sum(pre_grad, axis=0, dtype=jnp.float32)
    w_up_grad = jnp.einsum("td,tf->df", normed_two, pre_grad, preferred_element_type=jnp.float32)
    normed_two_grad = lax.psum_scatter(
        jnp.einsum("tf,df->td", pre_grad, w_up, preferred_element_type=jnp.float32).astype(
            jnp.bfloat16
        ),
        "tensor",
        scatter_dimension=0,
        tiled=True,
    ).astype(jnp.float32)
    branch_own, branch_out = scatter_blocks(branch_partial, tensor_size)
    normed_two_grad, branch_own, branch_out = lax.optimization_barrier(
        (normed_two_grad, branch_own, branch_out)
    )
    _, norm_two_back = jax.vjp(normalize, after_attn, norm_gain[1], norm_bias[1])
    through_two, gain_two_grad, shift_two_grad = norm_two_back(normed_two_grad)
    after_grad = upstream + through_two
    attn_bias_grad = jnp.sum(keep_rows * after_grad, axis=0)
    attn_local = (keep_rows * after_grad).astype(jnp.bfloat16)
    attn_grad = lax.all_gather(attn_local, "tensor", axis=0, tiled=True)
    w_out_grad_t = jnp.einsum(
        "td,tc->dc", attn_grad, mixed_rows, preferred_element_type=jnp.float32
    )
    mixed_grad = jnp.einsum(
        "td,cd->tc", attn_grad, w_out, preferred_element_type=jnp.float32
    ).astype(jnp.bfloat16)
    early_parts = jnp.concatenate([w_down_grad_t, w_up_grad, w_out_grad_t], axis=1).astype(
        jnp.bfloat16
    )
    early_parts, mixed_grad, branch_own, branch_out = lax.optimization_barrier(
        (early_parts, mixed_grad, branch_own, branch_out)
    )
    branch = exchange_blocks(branch_own, branch_out, tensor_size)
    result = (after_attn + keep_rows * (branch + out_bias[1])).astype(jnp.bfloat16)
    early_sum = lax.psum_scatter(early_parts, "dp", scatter_dimension=0, tiled=True).astype(
        jnp.float32
    )
    query_acc, key_acc, value_acc = attention_bwd(
        key_lo, key_hi, slopes, query_heads, key_heads, value_heads, query_info, key_info,
        mixed_f32, head_major(mixed_grad), log_totals, score_scale,
    )
    query_acc, key_acc, value_acc, result = lax.optimization_barrier(
        (query_acc, key_acc, value_acc, result)
    )
    query_grad = row_major(query_acc)
    key_grad = row_major(key_acc).astype(jnp.bfloat16)
    value_grad = row_major(value_acc).astype(jnp.bfloat16)
    projected_grad = jnp.concatenate([query_grad, key_grad, value_grad], axis=1)
    projected_grad, early_sum = lax.optimization_barrier((projected_grad, early_sum))
    qv_bias_grad = jnp.stack(
        [
            jnp.sum(query_grad, axis=0, dtype=jnp.float32),
            jnp.sum(value_grad, axis=0, dtype=jnp.float32),
        ]
    )
    w_qkv_grad = jnp.einsum("td,tc->dc", normed, projected_grad, preferred_element_type=jnp.float32)
    normed_grad_partial = jnp.einsum(
        "tc,dc->td",
        projected_grad,
        w_qkv.reshape(D, 3 * width_here),
        preferred_element_type=jnp.float32,
    )
    centred_all = inputs_all - jnp.mean(inputs_all, axis=-1, keepdims=True)
    unit_all = centred_all * lax.rsqrt(
        jnp.mean(centred_all * centred_all, axis=-1, keepdims=True) + EPSILON
    )
    gain_one_grad = jnp.sum(normed_grad_partial * unit_all, axis=0)
    shift_one_grad = jnp.sum(normed_grad_partial, axis=0)
    normed_grad = scatter_tensor(normed_grad_partial, tensor_size)
    _, norm_one_back = jax.vjp(normalize, inputs, norm_gain[0], norm_bias[0])
    through_one = norm_one_back(normed_grad)[0]
    input_grad = (after_grad + through_one).astype(jnp.bfloat16)
    qv_full = lax.dynamic_update_slice_in_dim(
        jnp.zeros((2, D), jnp.float32), qv_bias_grad, tensor_pos * width_here, 1
    )
    up_full = lax.dynamic_update_slice_in_dim(
        jnp.zeros((FF,), jnp.float32), up_bias_grad, tensor_pos * ff_here, 0
    )
    small = jnp.concatenate(
        [
            jnp.stack([gain_one_grad, gain_two_grad]).reshape(-1),
            jnp.stack([shift_one_grad, shift_two_grad]).reshape(-1),
            jnp.stack([attn_bias_grad, down_bias_grad]).reshape(-1),
            qv_full.reshape(-1),
            up_full,
        ]
    )
    qkv_sum = halving_scatter(
        w_qkv_grad.reshape(dp_size, D // dp_size, -1), "dp", jnp.bfloat16
    )
    qkv_part = qkv_sum.reshape(-1, 3, width_here)
    summed = doubling_sum(doubling_sum(small, "dp", dp_size), "tensor", tensor_size)
    gains_grad = summed[: 2 * D].reshape(2, D)
    shifts_grad = summed[2 * D : 4 * D].reshape(2, D)
    outer_grad = summed[4 * D : 6 * D].reshape(2, D)
    qv_sum = summed[6 * D : 8 * D].reshape(2, D)
    up_sum = summed[8 * D :]
    down_part = early_sum[:, :ff_here].T
    up_part = early_sum[:, ff_here : 2 * ff_here]
    out_part = early_sum[:, 2 * ff_here :].T
    return (
        result,
        input_grad,
        gains_grad,
        shifts_grad,
        qkv_part,
        qv_sum,
        out_part,
        outer_grad,
        up_part,
        up_sum,
        down_part,
    )


def solution(mesh):
    placed = (
        P(("dp", "tensor"), None),
        P("dp", None),
        P(),
        P(),
        P(None, None, "tensor"),
        P(None, "tensor"),
        P("tensor", None),
        P(),
        P(None, "tensor"),
        P("tensor"),
        P("tensor", None),
        P(("dp", "tensor"), None),
    )
    return jax.shard_map(
        functools.partial(on_device_body, mesh.shape["dp"]),
        mesh=mesh,
        in_specs=placed,
        out_specs=(
            P(("dp", "tensor"), None),
            P(("dp", "tensor"), None),
            P(),
            P(),
            P("dp", None, "tensor"),
            P(),
            P("tensor", "dp"),
            P(),
            P("dp", "tensor"),
            P(),
            P("tensor", "dp"),
        ),
        check_vma=False,
    )
```

```python
import functools

import jax
import jax.numpy as jnp
from jax import lax
from jax.experimental import pallas as pl
from jax.experimental.pallas import tpu as pltpu
from jax.sharding import PartitionSpec as P


D = 768
HEADS = 12
HEAD_DIM = 64
FF = 3072
SIDE_S = 12
SIDE_M = 15
SIDE_L = 20
TOK_DEV = 2048


EPSILON = 1e-06


def layout(group_counts):
    positions = jnp.arange(TOK_DEV, dtype=jnp.int32)
    area_small = SIDE_S * SIDE_S
    area_middle = SIDE_M * SIDE_M
    area_large = SIDE_L * SIDE_L
    end_small = group_counts[0] * area_small
    end_middle = end_small + group_counts[1] * area_middle
    end_large = end_middle + group_counts[2] * area_large
    size_class = (positions >= end_small).astype(jnp.int32) + (positions >= end_middle).astype(
        jnp.int32
    )
    begins = jnp.where(size_class == 0, 0, jnp.where(size_class == 1, end_small, end_middle))
    area_len = jnp.where(
        size_class == 0, area_small, jnp.where(size_class == 1, area_middle, area_large)
    )
    side_len = jnp.where(size_class == 0, SIDE_S, jnp.where(size_class == 1, SIDE_M, SIDE_L))
    within = positions - begins
    picture_index = within // area_len
    within_image = within % area_len
    is_valid = positions < end_large
    segment = jnp.where(is_valid, size_class * 16 + picture_index, 255)
    grid_row = (within_image // side_len).astype(jnp.float32)
    grid_col = (within_image % side_len).astype(jnp.float32)
    return (segment, grid_row, grid_col, is_valid.astype(jnp.float32))


def normalize(values, gain_row, shift_row):
    centred = values - jnp.mean(values, axis=-1, keepdims=True)
    spread = jnp.mean(centred * centred, axis=-1, keepdims=True)
    return centred * lax.rsqrt(spread + EPSILON) * gain_row + shift_row


def slopes_of(first_head, count_heads):
    head_number = (first_head + jnp.arange(count_heads, dtype=jnp.int32)).astype(jnp.float32) + 1.0
    return jnp.exp2(-8.0 * head_number / HEADS)


Q_BLOCK = 256
K_BLOCK = 256
NEG = -1e30


def key_ranges(segment, tokens):
    starts = jnp.arange(0, tokens, Q_BLOCK)
    first = segment[starts]
    last = segment[starts + Q_BLOCK - 1]
    key_lo = jnp.sum(segment[None, :] < first[:, None], axis=1)
    key_hi = jnp.sum(segment[None, :] <= last[:, None], axis=1)
    return (key_lo // K_BLOCK).astype(jnp.int32), ((key_hi + K_BLOCK - 1) // K_BLOCK).astype(jnp.int32)


def block_geometry(qi_ref, ki_ref, start):
    rq = qi_ref[:, 0:1]
    cq = qi_ref[:, 1:2]
    sq = qi_ref[:, 2:3]
    rk = ki_ref[0:1, pl.ds(start, K_BLOCK)]
    ck = ki_ref[1:2, pl.ds(start, K_BLOCK)]
    sk = ki_ref[2:3, pl.ds(start, K_BLOCK)]
    dr = rq - rk
    dc = cq - ck
    return jnp.where(sq == sk, jnp.sqrt(dr * dr + dc * dc), jnp.inf)


def fwd_kernel(heads, lo_ref, hi_ref, slope_ref, q_ref, k_ref, v_ref, qi_ref, ki_ref, o_ref, lse_ref):
    i = pl.program_id(0)
    queries = [q_ref[h] for h in range(heads)]
    width = q_ref.shape[2]

    def body(kb, carry):
        start = pl.multiple_of(kb * K_BLOCK, K_BLOCK)
        dist = block_geometry(qi_ref, ki_ref, start)
        out = []
        for h in range(heads):
            m_old, l_old, acc_old = carry[h]
            keys = k_ref[h, pl.ds(start, K_BLOCK), :]
            vals = v_ref[h, pl.ds(start, K_BLOCK), :]
            s = lax.dot_general(queries[h], keys, (((1,), (1,)), ((), ())),
                                preferred_element_type=jnp.float32) - slope_ref[h] * dist
            m_new = jnp.maximum(m_old, jnp.max(s, axis=1, keepdims=True))
            alpha = jnp.exp(m_old - m_new)
            p = jnp.exp(s - m_new)
            l_new = alpha * l_old + jnp.sum(p, axis=1, keepdims=True)
            acc_new = alpha * acc_old + jnp.dot(p.astype(jnp.bfloat16), vals,
                                                preferred_element_type=jnp.float32)
            out.append((m_new, l_new, acc_new))
        return tuple(out)

    init = tuple(
        (jnp.full((Q_BLOCK, 1), NEG, jnp.float32), jnp.zeros((Q_BLOCK, 1), jnp.float32),
         jnp.zeros((Q_BLOCK, width), jnp.float32))
        for _ in range(heads)
    )
    final = lax.fori_loop(lo_ref[i], hi_ref[i], body, init)
    for h in range(heads):
        m, l, acc = final[h]
        o_ref[h] = acc / l
        lse_ref[h] = m + jnp.log(l)


def bwd_kernel(heads, lo_ref, hi_ref, slope_ref, q_ref, k_ref, v_ref, qi_ref, ki_ref,
               o_ref, do_ref, lse_ref, dq_ref, dk_ref, dv_ref):
    i = pl.program_id(0)

    @pl.when(i == 0)
    def _():
        dk_ref[...] = jnp.zeros_like(dk_ref)
        dv_ref[...] = jnp.zeros_like(dv_ref)

    queries = [q_ref[h] for h in range(heads)]
    grads = [do_ref[h] for h in range(heads)]
    lses = [lse_ref[h] for h in range(heads)]
    deltas = [jnp.sum(grads[h].astype(jnp.float32) * o_ref[h], axis=1, keepdims=True)
              for h in range(heads)]
    width = q_ref.shape[2]

    def body(kb, carry):
        start = pl.multiple_of(kb * K_BLOCK, K_BLOCK)
        dist = block_geometry(qi_ref, ki_ref, start)
        out = []
        for h in range(heads):
            keys = k_ref[h, pl.ds(start, K_BLOCK), :]
            vals = v_ref[h, pl.ds(start, K_BLOCK), :]
            s = lax.dot_general(queries[h], keys, (((1,), (1,)), ((), ())),
                                preferred_element_type=jnp.float32) - slope_ref[h] * dist
            p = jnp.exp(s - lses[h])
            dp = lax.dot_general(grads[h], vals, (((1,), (1,)), ((), ())),
                                 preferred_element_type=jnp.float32)
            ds = (p * (dp - deltas[h])).astype(jnp.bfloat16)
            out.append(carry[h] + jnp.dot(ds, keys, preferred_element_type=jnp.float32))
            dk_ref[h, pl.ds(start, K_BLOCK), :] += lax.dot_general(
                ds, queries[h], (((0,), (0,)), ((), ())), preferred_element_type=jnp.float32)
            dv_ref[h, pl.ds(start, K_BLOCK), :] += lax.dot_general(
                p.astype(jnp.bfloat16), grads[h], (((0,), (0,)), ((), ())),
                preferred_element_type=jnp.float32)
        return tuple(out)

    init = tuple(jnp.zeros((Q_BLOCK, width), jnp.float32) for _ in range(heads))
    final = lax.fori_loop(lo_ref[i], hi_ref[i], body, init)
    for h in range(heads):
        dq_ref[h] = final[h]


def attention_fwd(lo, hi, slopes, q, k, v, qinfo, kinfo):
    heads, tokens, width = q.shape
    grid = (tokens // Q_BLOCK,)
    whole = lambda i, lo, hi: (0, 0, 0)
    rows = lambda i, lo, hi: (0, i, 0)
    return pl.pallas_call(
        functools.partial(fwd_kernel, heads),
        grid_spec=pltpu.PrefetchScalarGridSpec(
            num_scalar_prefetch=2,
            grid=grid,
            in_specs=[
                pl.BlockSpec(memory_space=pltpu.SMEM),
                pl.BlockSpec((heads, Q_BLOCK, width), rows),
                pl.BlockSpec((heads, tokens, width), whole),
                pl.BlockSpec((heads, tokens, width), whole),
                pl.BlockSpec((Q_BLOCK, 3), lambda i, lo, hi: (i, 0)),
                pl.BlockSpec((3, tokens), lambda i, lo, hi: (0, 0)),
            ],
            out_specs=[
                pl.BlockSpec((heads, Q_BLOCK, width), rows),
                pl.BlockSpec((heads, Q_BLOCK, 1), rows),
            ],
        ),
        out_shape=[
            jax.ShapeDtypeStruct((heads, tokens, width), jnp.float32),
            jax.ShapeDtypeStruct((heads, tokens, 1), jnp.float32),
        ],
        compiler_params=pltpu.CompilerParams(dimension_semantics=("arbitrary",)),
    )(lo, hi, slopes, q, k, v, qinfo, kinfo)


def attention_bwd(lo, hi, slopes, q, k, v, qinfo, kinfo, o, do, lse):
    heads, tokens, width = q.shape
    grid = (tokens // Q_BLOCK,)
    whole = lambda i, lo, hi: (0, 0, 0)
    rows = lambda i, lo, hi: (0, i, 0)
    return pl.pallas_call(
        functools.partial(bwd_kernel, heads),
        grid_spec=pltpu.PrefetchScalarGridSpec(
            num_scalar_prefetch=2,
            grid=grid,
            in_specs=[
                pl.BlockSpec(memory_space=pltpu.SMEM),
                pl.BlockSpec((heads, Q_BLOCK, width), rows),
                pl.BlockSpec((heads, tokens, width), whole),
                pl.BlockSpec((heads, tokens, width), whole),
                pl.BlockSpec((Q_BLOCK, 3), lambda i, lo, hi: (i, 0)),
                pl.BlockSpec((3, tokens), lambda i, lo, hi: (0, 0)),
                pl.BlockSpec((heads, Q_BLOCK, width), rows),
                pl.BlockSpec((heads, Q_BLOCK, width), rows),
                pl.BlockSpec((heads, Q_BLOCK, 1), rows),
            ],
            out_specs=[
                pl.BlockSpec((heads, Q_BLOCK, width), rows),
                pl.BlockSpec((heads, tokens, width), whole),
                pl.BlockSpec((heads, tokens, width), whole),
            ],
        ),
        out_shape=[
            jax.ShapeDtypeStruct((heads, tokens, width), jnp.float32),
            jax.ShapeDtypeStruct((heads, tokens, width), jnp.float32),
            jax.ShapeDtypeStruct((heads, tokens, width), jnp.float32),
        ],
        compiler_params=pltpu.CompilerParams(dimension_semantics=("arbitrary",)),
    )(lo, hi, slopes, q, k, v, qinfo, kinfo, o, do, lse)


def scatter_blocks(partial, tensor_size):
    me = lax.axis_index("tensor")
    blocks = partial.reshape(tensor_size, -1, partial.shape[1])
    own = lax.dynamic_index_in_dim(blocks, me, keepdims=False).astype(jnp.float32)
    outgoing = [
        lax.dynamic_index_in_dim(blocks, (me + shift) % tensor_size, keepdims=False).astype(
            jnp.bfloat16
        )
        for shift in range(1, tensor_size)
    ]
    return own, outgoing


def exchange_blocks(own, outgoing, tensor_size):
    total = own
    for shift in range(1, tensor_size):
        pairs = [(i, (i + shift) % tensor_size) for i in range(tensor_size)]
        total = total + lax.ppermute(outgoing[shift - 1], "tensor", pairs).astype(jnp.float32)
    return total


def scatter_tensor(partial, tensor_size):
    return exchange_blocks(*scatter_blocks(partial, tensor_size), tensor_size)


def halving_scatter(blocks, axis_name, wire):
    me = lax.axis_index(axis_name)
    bit = 0
    while blocks.shape[0] > 1:
        pairs = [(i, i ^ (1 << bit)) for i in range(blocks.shape[0] << bit)]
        halves = blocks.reshape((blocks.shape[0] // 2, 2) + blocks.shape[1:])
        mine = (me >> bit) & 1
        keep = lax.dynamic_index_in_dim(halves, mine, axis=1, keepdims=False)
        send = lax.dynamic_index_in_dim(halves, 1 - mine, axis=1, keepdims=False)
        arrived = lax.ppermute(send.astype(wire), axis_name, pairs)
        blocks = keep + arrived.astype(blocks.dtype)
        bit += 1
    return blocks[0]


def doubling_sum(values, axis_name, size):
    bit = 0
    while (1 << bit) < size:
        pairs = [(i, i ^ (1 << bit)) for i in range(size)]
        values = values + lax.ppermute(values, axis_name, pairs)
        bit += 1
    return values


def on_device_body(
    dp_size,
    patches,
    counts,
    norm_gain,
    norm_bias,
    w_qkv,
    b_qv,
    w_out,
    out_bias,
    w_up,
    b_up,
    w_down,
    cotangent,
):
    local_rows = patches.shape[0]
    width_here = w_qkv.shape[2]
    heads_here = width_here // HEAD_DIM
    ff_here = w_up.shape[1]
    tensor_pos = lax.axis_index("tensor")
    tensor_size = D // width_here
    score_scale = HEAD_DIM ** (-0.5)
    segment, grid_row, grid_col, is_valid = layout(counts[0])
    keep_rows = lax.dynamic_slice_in_dim(is_valid, tensor_pos * local_rows, local_rows)[:, None]
    slopes = slopes_of(tensor_pos * heads_here, heads_here)
    inputs = patches.astype(jnp.float32)
    inputs_all = lax.all_gather(patches, "tensor", axis=0, tiled=True).astype(jnp.float32)
    normed = normalize(inputs_all, norm_gain[0], norm_bias[0]).astype(jnp.bfloat16)
    projected = jnp.einsum("td,dsc->tsc", normed, w_qkv, preferred_element_type=jnp.float32)
    queries = (projected[:, 0] + b_qv[0]).astype(jnp.bfloat16)
    keys = projected[:, 1].astype(jnp.bfloat16)
    values = (projected[:, 2] + b_qv[1]).astype(jnp.bfloat16)

    def head_major(rows):
        return rows.reshape(TOK_DEV, heads_here, HEAD_DIM).transpose(1, 0, 2)

    def row_major(heads):
        return heads.transpose(1, 0, 2).reshape(TOK_DEV, width_here)

    key_lo, key_hi = key_ranges(segment, TOK_DEV)
    segment_f = segment.astype(jnp.float32)
    query_info = jnp.stack([grid_row, grid_col, segment_f], axis=1)
    key_info = jnp.stack([grid_row, grid_col, segment_f], axis=0)
    query_heads = head_major(queries) * jnp.asarray(score_scale, jnp.bfloat16)
    key_heads = head_major(keys)
    value_heads = head_major(values)
    mixed_f32, log_totals = attention_fwd(
        key_lo, key_hi, slopes, query_heads, key_heads, value_heads, query_info, key_info
    )
    upstream = cotangent.astype(jnp.float32)
    branch_grad = lax.all_gather(
        (keep_rows * upstream).astype(jnp.bfloat16), "tensor", axis=0, tiled=True
    )
    mixed_f32, log_totals, branch_grad = lax.optimization_barrier(
        (mixed_f32, log_totals, branch_grad)
    )
    mixed_rows = row_major(mixed_f32).astype(jnp.bfloat16)
    mixed_all = lax.all_gather(mixed_rows, "tensor", axis=1, tiled=True)
    w_out_all = lax.all_gather(w_out, "tensor", axis=0, tiled=True)
    attended = jnp.dot(mixed_all, w_out_all, preferred_element_type=jnp.float32)
    after_attn_all = inputs_all + is_valid[:, None] * (attended + out_bias[0])
    after_attn = lax.dynamic_slice_in_dim(after_attn_all, tensor_pos * local_rows, local_rows)
    normed_two = normalize(after_attn_all, norm_gain[1], norm_bias[1]).astype(jnp.bfloat16)
    hidden_pre = jnp.dot(normed_two, w_up, preferred_element_type=jnp.float32) + b_up
    normal_cdf = 0.5 * (1.0 + lax.erf(hidden_pre * (2.0 ** -0.5)))
    hidden = (hidden_pre * normal_cdf).astype(jnp.bfloat16)
    branch_partial = jnp.dot(hidden, w_down, preferred_element_type=jnp.float32)
    down_bias_grad = jnp.sum(keep_rows * upstream, axis=0)
    w_down_grad_t = jnp.einsum(
        "td,tf->df", branch_grad, hidden, preferred_element_type=jnp.float32
    )
    hidden_grad = jnp.einsum("td,fd->tf", branch_grad, w_down, preferred_element_type=jnp.float32)
    normal_pdf = jnp.exp(-0.5 * hidden_pre * hidden_pre) * ((2.0 * jnp.pi) ** -0.5)
    pre_grad = (hidden_grad * (normal_cdf + hidden_pre * normal_pdf)).astype(jnp.bfloat16)
    up_bias_grad = jnp.sum(pre_grad, axis=0, dtype=jnp.float32)
    w_up_grad = jnp.einsum("td,tf->df", normed_two, pre_grad, preferred_element_type=jnp.float32)
    normed_two_grad = lax.psum_scatter(
        jnp.einsum("tf,df->td", pre_grad, w_up, preferred_element_type=jnp.float32).astype(
            jnp.bfloat16
        ),
        "tensor",
        scatter_dimension=0,
        tiled=True,
    ).astype(jnp.float32)
    branch_own, branch_out = scatter_blocks(branch_partial, tensor_size)
    normed_two_grad, branch_own, branch_out = lax.optimization_barrier(
        (normed_two_grad, branch_own, branch_out)
    )
    _, norm_two_back = jax.vjp(normalize, after_attn, norm_gain[1], norm_bias[1])
    through_two, gain_two_grad, shift_two_grad = norm_two_back(normed_two_grad)
    after_grad = upstream + through_two
    attn_bias_grad = jnp.sum(keep_rows * after_grad, axis=0)
    attn_local = (keep_rows * after_grad).astype(jnp.bfloat16)
    attn_grad = lax.all_gather(attn_local, "tensor", axis=0, tiled=True)
    w_out_grad_t = jnp.einsum(
        "td,tc->dc", attn_grad, mixed_rows, preferred_element_type=jnp.float32
    )
    mixed_grad = jnp.einsum(
        "td,cd->tc", attn_grad, w_out, preferred_element_type=jnp.float32
    ).astype(jnp.bfloat16)
    early_parts = jnp.concatenate([w_down_grad_t, w_up_grad, w_out_grad_t], axis=1).astype(
        jnp.bfloat16
    )
    early_parts, mixed_grad, branch_own, branch_out = lax.optimization_barrier(
        (early_parts, mixed_grad, branch_own, branch_out)
    )
    branch = exchange_blocks(branch_own, branch_out, tensor_size)
    result = (after_attn + keep_rows * (branch + out_bias[1])).astype(jnp.bfloat16)
    early_sum = lax.psum_scatter(early_parts, "dp", scatter_dimension=0, tiled=True).astype(
        jnp.float32
    )
    query_acc, key_acc, value_acc = attention_bwd(
        key_lo, key_hi, slopes, query_heads, key_heads, value_heads, query_info, key_info,
        mixed_f32, head_major(mixed_grad), log_totals,
    )
    query_acc, key_acc, value_acc, result = lax.optimization_barrier(
        (query_acc, key_acc, value_acc, result)
    )
    query_grad = row_major(query_acc * score_scale).astype(jnp.bfloat16)
    key_grad = row_major(key_acc).astype(jnp.bfloat16)
    value_grad = row_major(value_acc).astype(jnp.bfloat16)
    projected_grad = jnp.concatenate([query_grad, key_grad, value_grad], axis=1)
    projected_grad, early_sum = lax.optimization_barrier((projected_grad, early_sum))
    qv_bias_grad = jnp.stack(
        [
            jnp.sum(query_grad, axis=0, dtype=jnp.float32),
            jnp.sum(value_grad, axis=0, dtype=jnp.float32),
        ]
    )
    w_qkv_grad = jnp.einsum("td,tc->dc", normed, projected_grad, preferred_element_type=jnp.float32)
    normed_grad_partial = jnp.einsum(
        "tc,dc->td",
        projected_grad,
        w_qkv.reshape(D, 3 * width_here),
        preferred_element_type=jnp.float32,
    )
    centred_all = inputs_all - jnp.mean(inputs_all, axis=-1, keepdims=True)
    unit_all = centred_all * lax.rsqrt(
        jnp.mean(centred_all * centred_all, axis=-1, keepdims=True) + EPSILON
    )
    gain_one_grad = jnp.sum(normed_grad_partial * unit_all, axis=0)
    shift_one_grad = jnp.sum(normed_grad_partial, axis=0)
    normed_grad = scatter_tensor(normed_grad_partial, tensor_size)
    _, norm_one_back = jax.vjp(normalize, inputs, norm_gain[0], norm_bias[0])
    through_one = norm_one_back(normed_grad)[0]
    input_grad = (after_grad + through_one).astype(jnp.bfloat16)
    qv_full = lax.dynamic_update_slice_in_dim(
        jnp.zeros((2, D), jnp.float32), qv_bias_grad, tensor_pos * width_here, 1
    )
    up_full = lax.dynamic_update_slice_in_dim(
        jnp.zeros((FF,), jnp.float32), up_bias_grad, tensor_pos * ff_here, 0
    )
    small = jnp.concatenate(
        [
            jnp.stack([gain_one_grad, gain_two_grad]).reshape(-1),
            jnp.stack([shift_one_grad, shift_two_grad]).reshape(-1),
            jnp.stack([attn_bias_grad, down_bias_grad]).reshape(-1),
            qv_full.reshape(-1),
            up_full,
        ]
    )
    qkv_sum = halving_scatter(
        w_qkv_grad.reshape(dp_size, D // dp_size, -1), "dp", jnp.bfloat16
    )
    qkv_part = qkv_sum.reshape(-1, 3, width_here)
    summed = doubling_sum(doubling_sum(small, "dp", dp_size), "tensor", tensor_size)
    gains_grad = summed[: 2 * D].reshape(2, D)
    shifts_grad = summed[2 * D : 4 * D].reshape(2, D)
    outer_grad = summed[4 * D : 6 * D].reshape(2, D)
    qv_sum = summed[6 * D : 8 * D].reshape(2, D)
    up_sum = summed[8 * D :]
    down_part = early_sum[:, :ff_here].T
    up_part = early_sum[:, ff_here : 2 * ff_here]
    out_part = early_sum[:, 2 * ff_here :].T
    return (
        result,
        input_grad,
        gains_grad,
        shifts_grad,
        qkv_part,
        qv_sum,
        out_part,
        outer_grad,
        up_part,
        up_sum,
        down_part,
    )


def solution(mesh):
    placed = (
        P(("dp", "tensor"), None),
        P("dp", None),
        P(),
        P(),
        P(None, None, "tensor"),
        P(None, "tensor"),
        P("tensor", None),
        P(),
        P(None, "tensor"),
        P("tensor"),
        P("tensor", None),
        P(("dp", "tensor"), None),
    )
    return jax.shard_map(
        functools.partial(on_device_body, mesh.shape["dp"]),
        mesh=mesh,
        in_specs=placed,
        out_specs=(
            P(("dp", "tensor"), None),
            P(("dp", "tensor"), None),
            P(),
            P(),
            P("dp", None, "tensor"),
            P(),
            P("tensor", "dp"),
            P(),
            P("dp", "tensor"),
            P(),
            P("tensor", "dp"),
        ),
        check_vma=False,
    )
```

```python
import functools

import jax
import jax.numpy as jnp
from jax import lax
from jax.experimental import pallas as pl
from jax.experimental.pallas import tpu as pltpu
from jax.sharding import PartitionSpec as P


D = 768
HEADS = 12
HEAD_DIM = 64
FF = 3072
SIDE_S = 12
SIDE_M = 15
SIDE_L = 20
TOK_DEV = 2048


EPSILON = 1e-06


def layout(group_counts):
    positions = jnp.arange(TOK_DEV, dtype=jnp.int32)
    area_small = SIDE_S * SIDE_S
    area_middle = SIDE_M * SIDE_M
    area_large = SIDE_L * SIDE_L
    end_small = group_counts[0] * area_small
    end_middle = end_small + group_counts[1] * area_middle
    end_large = end_middle + group_counts[2] * area_large
    size_class = (positions >= end_small).astype(jnp.int32) + (positions >= end_middle).astype(
        jnp.int32
    )
    begins = jnp.where(size_class == 0, 0, jnp.where(size_class == 1, end_small, end_middle))
    area_len = jnp.where(
        size_class == 0, area_small, jnp.where(size_class == 1, area_middle, area_large)
    )
    side_len = jnp.where(size_class == 0, SIDE_S, jnp.where(size_class == 1, SIDE_M, SIDE_L))
    within = positions - begins
    picture_index = within // area_len
    within_image = within % area_len
    is_valid = positions < end_large
    segment = jnp.where(is_valid, size_class * 16 + picture_index, 255)
    grid_row = (within_image // side_len).astype(jnp.float32)
    grid_col = (within_image % side_len).astype(jnp.float32)
    return (segment, grid_row, grid_col, is_valid.astype(jnp.float32))


def normalize(values, gain_row, shift_row):
    centred = values - jnp.mean(values, axis=-1, keepdims=True)
    spread = jnp.mean(centred * centred, axis=-1, keepdims=True)
    return centred * lax.rsqrt(spread + EPSILON) * gain_row + shift_row


def normalize_backward(values, gain_row, grad):
    centred = values - jnp.mean(values, axis=-1, keepdims=True)
    scale = lax.rsqrt(jnp.mean(centred * centred, axis=-1, keepdims=True) + EPSILON)
    unit = centred * scale
    scaled = grad * gain_row
    through = scale * (
        scaled
        - jnp.mean(scaled, axis=-1, keepdims=True)
        - unit * jnp.mean(scaled * unit, axis=-1, keepdims=True)
    )
    return through, jnp.sum(grad * unit, axis=0), jnp.sum(grad, axis=0)


def slopes_of(first_head, count_heads):
    head_number = (first_head + jnp.arange(count_heads, dtype=jnp.int32)).astype(jnp.float32) + 1.0
    return jnp.exp2(-8.0 * head_number / HEADS)


Q_BLOCK = 256
K_BLOCK = 256
NEG = -1e30


def key_ranges(segment, tokens):
    starts = jnp.arange(0, tokens, Q_BLOCK)
    first = segment[starts]
    last = segment[starts + Q_BLOCK - 1]
    key_lo = jnp.sum(segment[None, :] < first[:, None], axis=1)
    key_hi = jnp.sum(segment[None, :] <= last[:, None], axis=1)
    return (key_lo // K_BLOCK).astype(jnp.int32), ((key_hi + K_BLOCK - 1) // K_BLOCK).astype(jnp.int32)


def block_geometry(qi_ref, ki_ref, start):
    rq = qi_ref[:, 0:1]
    cq = qi_ref[:, 1:2]
    sq = qi_ref[:, 2:3]
    rk = ki_ref[0:1, pl.ds(start, K_BLOCK)]
    ck = ki_ref[1:2, pl.ds(start, K_BLOCK)]
    sk = ki_ref[2:3, pl.ds(start, K_BLOCK)]
    dr = rq - rk
    dc = cq - ck
    return jnp.where(sq == sk, jnp.sqrt(dr * dr + dc * dc), jnp.inf)


def fwd_kernel(heads, lo_ref, hi_ref, slope_ref, q_ref, k_ref, v_ref, qi_ref, ki_ref, o_ref, lse_ref):
    i = pl.program_id(0)
    queries = [q_ref[h] for h in range(heads)]
    width = q_ref.shape[2]

    def body(kb, carry):
        start = pl.multiple_of(kb * K_BLOCK, K_BLOCK)
        dist = block_geometry(qi_ref, ki_ref, start)
        out = []
        for h in range(heads):
            m_old, l_old, acc_old = carry[h]
            keys = k_ref[h, pl.ds(start, K_BLOCK), :]
            vals = v_ref[h, pl.ds(start, K_BLOCK), :]
            s = lax.dot_general(queries[h], keys, (((1,), (1,)), ((), ())),
                                preferred_element_type=jnp.float32) - slope_ref[h] * dist
            m_new = jnp.maximum(m_old, jnp.max(s, axis=1, keepdims=True))
            alpha = jnp.exp(m_old - m_new)
            p = jnp.exp(s - m_new)
            l_new = alpha * l_old + jnp.sum(p, axis=1, keepdims=True)
            acc_new = alpha * acc_old + jnp.dot(p.astype(jnp.bfloat16), vals,
                                                preferred_element_type=jnp.float32)
            out.append((m_new, l_new, acc_new))
        return tuple(out)

    init = tuple(
        (jnp.full((Q_BLOCK, 1), NEG, jnp.float32), jnp.zeros((Q_BLOCK, 1), jnp.float32),
         jnp.zeros((Q_BLOCK, width), jnp.float32))
        for _ in range(heads)
    )
    final = lax.fori_loop(lo_ref[i], hi_ref[i], body, init)
    for h in range(heads):
        m, l, acc = final[h]
        o_ref[h] = acc / l
        lse_ref[h] = m + jnp.log(l)


def bwd_kernel(heads, lo_ref, hi_ref, slope_ref, q_ref, k_ref, v_ref, qi_ref, ki_ref,
               o_ref, do_ref, lse_ref, dq_ref, dk_ref, dv_ref):
    i = pl.program_id(0)

    @pl.when(i == 0)
    def _():
        dk_ref[...] = jnp.zeros_like(dk_ref)
        dv_ref[...] = jnp.zeros_like(dv_ref)

    queries = [q_ref[h] for h in range(heads)]
    grads = [do_ref[h] for h in range(heads)]
    lses = [lse_ref[h] for h in range(heads)]
    deltas = [jnp.sum(grads[h].astype(jnp.float32) * o_ref[h], axis=1, keepdims=True)
              for h in range(heads)]
    width = q_ref.shape[2]

    def body(kb, carry):
        start = pl.multiple_of(kb * K_BLOCK, K_BLOCK)
        dist = block_geometry(qi_ref, ki_ref, start)
        out = []
        for h in range(heads):
            keys = k_ref[h, pl.ds(start, K_BLOCK), :]
            vals = v_ref[h, pl.ds(start, K_BLOCK), :]
            s = lax.dot_general(queries[h], keys, (((1,), (1,)), ((), ())),
                                preferred_element_type=jnp.float32) - slope_ref[h] * dist
            p = jnp.exp(s - lses[h])
            dp = lax.dot_general(grads[h], vals, (((1,), (1,)), ((), ())),
                                 preferred_element_type=jnp.float32)
            ds = (p * (dp - deltas[h])).astype(jnp.bfloat16)
            out.append(carry[h] + jnp.dot(ds, keys, preferred_element_type=jnp.float32))
            dk_ref[h, pl.ds(start, K_BLOCK), :] += lax.dot_general(
                ds, queries[h], (((0,), (0,)), ((), ())), preferred_element_type=jnp.float32)
            dv_ref[h, pl.ds(start, K_BLOCK), :] += lax.dot_general(
                p.astype(jnp.bfloat16), grads[h], (((0,), (0,)), ((), ())),
                preferred_element_type=jnp.float32)
        return tuple(out)

    init = tuple(jnp.zeros((Q_BLOCK, width), jnp.float32) for _ in range(heads))
    final = lax.fori_loop(lo_ref[i], hi_ref[i], body, init)
    for h in range(heads):
        dq_ref[h] = final[h]


def attention_fwd(lo, hi, slopes, q, k, v, qinfo, kinfo):
    heads, tokens, width = q.shape
    grid = (tokens // Q_BLOCK,)
    whole = lambda i, lo, hi: (0, 0, 0)
    rows = lambda i, lo, hi: (0, i, 0)
    return pl.pallas_call(
        functools.partial(fwd_kernel, heads),
        grid_spec=pltpu.PrefetchScalarGridSpec(
            num_scalar_prefetch=2,
            grid=grid,
            in_specs=[
                pl.BlockSpec(memory_space=pltpu.SMEM),
                pl.BlockSpec((heads, Q_BLOCK, width), rows),
                pl.BlockSpec((heads, tokens, width), whole),
                pl.BlockSpec((heads, tokens, width), whole),
                pl.BlockSpec((Q_BLOCK, 3), lambda i, lo, hi: (i, 0)),
                pl.BlockSpec((3, tokens), lambda i, lo, hi: (0, 0)),
            ],
            out_specs=[
                pl.BlockSpec((heads, Q_BLOCK, width), rows),
                pl.BlockSpec((heads, Q_BLOCK, 1), rows),
            ],
        ),
        out_shape=[
            jax.ShapeDtypeStruct((heads, tokens, width), jnp.float32),
            jax.ShapeDtypeStruct((heads, tokens, 1), jnp.float32),
        ],
        compiler_params=pltpu.CompilerParams(dimension_semantics=("arbitrary",)),
    )(lo, hi, slopes, q, k, v, qinfo, kinfo)


def attention_bwd(lo, hi, slopes, q, k, v, qinfo, kinfo, o, do, lse):
    heads, tokens, width = q.shape
    grid = (tokens // Q_BLOCK,)
    whole = lambda i, lo, hi: (0, 0, 0)
    rows = lambda i, lo, hi: (0, i, 0)
    return pl.pallas_call(
        functools.partial(bwd_kernel, heads),
        grid_spec=pltpu.PrefetchScalarGridSpec(
            num_scalar_prefetch=2,
            grid=grid,
            in_specs=[
                pl.BlockSpec(memory_space=pltpu.SMEM),
                pl.BlockSpec((heads, Q_BLOCK, width), rows),
                pl.BlockSpec((heads, tokens, width), whole),
                pl.BlockSpec((heads, tokens, width), whole),
                pl.BlockSpec((Q_BLOCK, 3), lambda i, lo, hi: (i, 0)),
                pl.BlockSpec((3, tokens), lambda i, lo, hi: (0, 0)),
                pl.BlockSpec((heads, Q_BLOCK, width), rows),
                pl.BlockSpec((heads, Q_BLOCK, width), rows),
                pl.BlockSpec((heads, Q_BLOCK, 1), rows),
            ],
            out_specs=[
                pl.BlockSpec((heads, Q_BLOCK, width), rows),
                pl.BlockSpec((heads, tokens, width), whole),
                pl.BlockSpec((heads, tokens, width), whole),
            ],
        ),
        out_shape=[
            jax.ShapeDtypeStruct((heads, tokens, width), jnp.float32),
            jax.ShapeDtypeStruct((heads, tokens, width), jnp.float32),
            jax.ShapeDtypeStruct((heads, tokens, width), jnp.float32),
        ],
        compiler_params=pltpu.CompilerParams(dimension_semantics=("arbitrary",)),
    )(lo, hi, slopes, q, k, v, qinfo, kinfo, o, do, lse)


def scatter_blocks(partial, tensor_size):
    me = lax.axis_index("tensor")
    blocks = partial.reshape(tensor_size, -1, partial.shape[1])
    own = lax.dynamic_index_in_dim(blocks, me, keepdims=False).astype(jnp.float32)
    outgoing = [
        lax.dynamic_index_in_dim(blocks, (me + shift) % tensor_size, keepdims=False).astype(
            jnp.bfloat16
        )
        for shift in range(1, tensor_size)
    ]
    return own, outgoing


def exchange_blocks(own, outgoing, tensor_size):
    total = own
    for shift in range(1, tensor_size):
        pairs = [(i, (i + shift) % tensor_size) for i in range(tensor_size)]
        total = total + lax.ppermute(outgoing[shift - 1], "tensor", pairs).astype(jnp.float32)
    return total


def scatter_tensor(partial, tensor_size):
    return exchange_blocks(*scatter_blocks(partial, tensor_size), tensor_size)


def halving_scatter(blocks, axis_name, wire):
    me = lax.axis_index(axis_name)
    bit = 0
    while blocks.shape[0] > 1:
        pairs = [(i, i ^ (1 << bit)) for i in range(blocks.shape[0] << bit)]
        halves = blocks.reshape((blocks.shape[0] // 2, 2) + blocks.shape[1:])
        mine = (me >> bit) & 1
        keep = lax.dynamic_index_in_dim(halves, mine, axis=1, keepdims=False)
        send = lax.dynamic_index_in_dim(halves, 1 - mine, axis=1, keepdims=False)
        arrived = lax.ppermute(send.astype(wire), axis_name, pairs)
        blocks = keep + arrived.astype(blocks.dtype)
        bit += 1
    return blocks[0]


def doubling_sum(values, axis_name, size):
    bit = 0
    while (1 << bit) < size:
        pairs = [(i, i ^ (1 << bit)) for i in range(size)]
        values = values + lax.ppermute(values, axis_name, pairs)
        bit += 1
    return values


def on_device_body(
    dp_size,
    patches,
    counts,
    norm_gain,
    norm_bias,
    w_qkv,
    b_qv,
    w_out,
    out_bias,
    w_up,
    b_up,
    w_down,
    cotangent,
):
    local_rows = patches.shape[0]
    width_here = w_qkv.shape[2]
    heads_here = width_here // HEAD_DIM
    ff_here = w_up.shape[1]
    tensor_pos = lax.axis_index("tensor")
    tensor_size = D // width_here
    score_scale = HEAD_DIM ** (-0.5)
    segment, grid_row, grid_col, is_valid = layout(counts[0])
    keep_rows = lax.dynamic_slice_in_dim(is_valid, tensor_pos * local_rows, local_rows)[:, None]
    slopes = slopes_of(tensor_pos * heads_here, heads_here)
    inputs = patches.astype(jnp.float32)
    inputs_all = lax.all_gather(patches, "tensor", axis=0, tiled=True).astype(jnp.float32)
    normed = normalize(inputs_all, norm_gain[0], norm_bias[0]).astype(jnp.bfloat16)
    projected = jnp.einsum("td,dsc->tsc", normed, w_qkv, preferred_element_type=jnp.float32)
    queries = (projected[:, 0] + b_qv[0]).astype(jnp.bfloat16)
    keys = projected[:, 1].astype(jnp.bfloat16)
    values = (projected[:, 2] + b_qv[1]).astype(jnp.bfloat16)

    def head_major(rows):
        return rows.reshape(TOK_DEV, heads_here, HEAD_DIM).transpose(1, 0, 2)

    def row_major(heads):
        return heads.transpose(1, 0, 2).reshape(TOK_DEV, width_here)

    key_lo, key_hi = key_ranges(segment, TOK_DEV)
    segment_f = segment.astype(jnp.float32)
    query_info = jnp.stack([grid_row, grid_col, segment_f], axis=1)
    key_info = jnp.stack([grid_row, grid_col, segment_f], axis=0)
    query_heads = head_major(queries) * jnp.asarray(score_scale, jnp.bfloat16)
    key_heads = head_major(keys)
    value_heads = head_major(values)
    mixed_f32, log_totals = attention_fwd(
        key_lo, key_hi, slopes, query_heads, key_heads, value_heads, query_info, key_info
    )
    upstream = cotangent.astype(jnp.float32)
    branch_grad = lax.all_gather(
        (keep_rows * upstream).astype(jnp.bfloat16), "tensor", axis=0, tiled=True
    )
    mixed_f32, log_totals, branch_grad = lax.optimization_barrier(
        (mixed_f32, log_totals, branch_grad)
    )
    mixed_rows = row_major(mixed_f32).astype(jnp.bfloat16)
    mixed_all = lax.all_gather(mixed_rows, "tensor", axis=1, tiled=True)
    w_out_all = lax.all_gather(w_out, "tensor", axis=0, tiled=True)
    attended = jnp.dot(mixed_all, w_out_all, preferred_element_type=jnp.float32)
    after_attn_all = inputs_all + is_valid[:, None] * (attended + out_bias[0])
    after_attn = lax.dynamic_slice_in_dim(after_attn_all, tensor_pos * local_rows, local_rows)
    normed_two = normalize(after_attn_all, norm_gain[1], norm_bias[1]).astype(jnp.bfloat16)
    hidden_pre = jnp.dot(normed_two, w_up, preferred_element_type=jnp.float32) + b_up
    normal_cdf = 0.5 * (1.0 + lax.erf(hidden_pre * (2.0 ** -0.5)))
    hidden = (hidden_pre * normal_cdf).astype(jnp.bfloat16)
    branch_partial = jnp.dot(hidden, w_down, preferred_element_type=jnp.float32)
    down_bias_grad = jnp.sum(keep_rows * upstream, axis=0)
    w_down_grad_t = jnp.einsum(
        "td,tf->df", branch_grad, hidden, preferred_element_type=jnp.float32
    )
    hidden_grad = jnp.einsum("td,fd->tf", branch_grad, w_down, preferred_element_type=jnp.float32)
    normal_pdf = jnp.exp(-0.5 * hidden_pre * hidden_pre) * ((2.0 * jnp.pi) ** -0.5)
    pre_grad = (hidden_grad * (normal_cdf + hidden_pre * normal_pdf)).astype(jnp.bfloat16)
    up_bias_grad = jnp.sum(pre_grad, axis=0, dtype=jnp.float32)
    w_up_grad = jnp.einsum("td,tf->df", normed_two, pre_grad, preferred_element_type=jnp.float32)
    normed_two_grad = lax.psum_scatter(
        jnp.einsum("tf,df->td", pre_grad, w_up, preferred_element_type=jnp.float32).astype(
            jnp.bfloat16
        ),
        "tensor",
        scatter_dimension=0,
        tiled=True,
    ).astype(jnp.float32)
    branch_own, branch_out = scatter_blocks(branch_partial, tensor_size)
    normed_two_grad, branch_own, branch_out = lax.optimization_barrier(
        (normed_two_grad, branch_own, branch_out)
    )
    through_two, gain_two_grad, shift_two_grad = normalize_backward(
        after_attn, norm_gain[1], normed_two_grad
    )
    after_grad = upstream + through_two
    attn_bias_grad = jnp.sum(keep_rows * after_grad, axis=0)
    attn_local = (keep_rows * after_grad).astype(jnp.bfloat16)
    attn_grad = lax.all_gather(attn_local, "tensor", axis=0, tiled=True)
    w_out_grad_t = jnp.einsum(
        "td,tc->dc", attn_grad, mixed_rows, preferred_element_type=jnp.float32
    )
    mixed_grad = jnp.einsum(
        "td,cd->tc", attn_grad, w_out, preferred_element_type=jnp.float32
    ).astype(jnp.bfloat16)
    early_parts = jnp.concatenate([w_down_grad_t, w_up_grad], axis=1).astype(
        jnp.bfloat16
    )
    early_parts, mixed_grad, branch_own, branch_out = lax.optimization_barrier(
        (early_parts, mixed_grad, branch_own, branch_out)
    )
    branch = exchange_blocks(branch_own, branch_out, tensor_size)
    result = (after_attn + keep_rows * (branch + out_bias[1])).astype(jnp.bfloat16)
    early_sum = lax.psum_scatter(early_parts, "dp", scatter_dimension=0, tiled=True).astype(
        jnp.float32
    )
    query_acc, key_acc, value_acc = attention_bwd(
        key_lo, key_hi, slopes, query_heads, key_heads, value_heads, query_info, key_info,
        mixed_f32, head_major(mixed_grad), log_totals,
    )
    query_acc, key_acc, value_acc, result = lax.optimization_barrier(
        (query_acc, key_acc, value_acc, result)
    )
    query_grad = row_major(query_acc * score_scale).astype(jnp.bfloat16)
    key_grad = row_major(key_acc).astype(jnp.bfloat16)
    value_grad = row_major(value_acc).astype(jnp.bfloat16)
    projected_grad = jnp.concatenate([query_grad, key_grad, value_grad], axis=1)
    projected_grad, early_sum = lax.optimization_barrier((projected_grad, early_sum))
    qv_bias_grad = jnp.stack(
        [
            jnp.sum(query_grad, axis=0, dtype=jnp.float32),
            jnp.sum(value_grad, axis=0, dtype=jnp.float32),
        ]
    )
    w_qkv_grad = jnp.einsum("td,tc->dc", normed, projected_grad, preferred_element_type=jnp.float32)
    normed_grad_partial = jnp.einsum(
        "tc,dc->td",
        projected_grad,
        w_qkv.reshape(D, 3 * width_here),
        preferred_element_type=jnp.float32,
    )
    centred_all = inputs_all - jnp.mean(inputs_all, axis=-1, keepdims=True)
    unit_all = centred_all * lax.rsqrt(
        jnp.mean(centred_all * centred_all, axis=-1, keepdims=True) + EPSILON
    )
    gain_one_grad = jnp.sum(normed_grad_partial * unit_all, axis=0)
    shift_one_grad = jnp.sum(normed_grad_partial, axis=0)
    normed_grad = scatter_tensor(normed_grad_partial, tensor_size)
    through_one = normalize_backward(inputs, norm_gain[0], normed_grad)[0]
    input_grad = (after_grad + through_one).astype(jnp.bfloat16)
    qv_full = lax.dynamic_update_slice_in_dim(
        jnp.zeros((2, D), jnp.float32), qv_bias_grad, tensor_pos * width_here, 1
    )
    up_full = lax.dynamic_update_slice_in_dim(
        jnp.zeros((FF,), jnp.float32), up_bias_grad, tensor_pos * ff_here, 0
    )
    small = jnp.concatenate(
        [
            jnp.stack([gain_one_grad, gain_two_grad]).reshape(-1),
            jnp.stack([shift_one_grad, shift_two_grad]).reshape(-1),
            jnp.stack([attn_bias_grad, down_bias_grad]).reshape(-1),
            qv_full.reshape(-1),
            up_full,
        ]
    )
    qkv_sum = halving_scatter(
        jnp.concatenate([w_qkv_grad, w_out_grad_t], axis=1).reshape(
            dp_size, D // dp_size, -1
        ),
        "dp",
        jnp.bfloat16,
    )
    qkv_part = qkv_sum[:, : 3 * width_here].reshape(-1, 3, width_here)
    summed = doubling_sum(doubling_sum(small, "dp", dp_size), "tensor", tensor_size)
    gains_grad = summed[: 2 * D].reshape(2, D)
    shifts_grad = summed[2 * D : 4 * D].reshape(2, D)
    outer_grad = summed[4 * D : 6 * D].reshape(2, D)
    qv_sum = summed[6 * D : 8 * D].reshape(2, D)
    up_sum = summed[8 * D :]
    down_part = early_sum[:, :ff_here].T
    up_part = early_sum[:, ff_here : 2 * ff_here]
    out_part = qkv_sum[:, 3 * width_here :].T
    return (
        result,
        input_grad,
        gains_grad,
        shifts_grad,
        qkv_part,
        qv_sum,
        out_part,
        outer_grad,
        up_part,
        up_sum,
        down_part,
    )


def solution(mesh):
    placed = (
        P(("dp", "tensor"), None),
        P("dp", None),
        P(),
        P(),
        P(None, None, "tensor"),
        P(None, "tensor"),
        P("tensor", None),
        P(),
        P(None, "tensor"),
        P("tensor"),
        P("tensor", None),
        P(("dp", "tensor"), None),
    )
    return jax.shard_map(
        functools.partial(on_device_body, mesh.shape["dp"]),
        mesh=mesh,
        in_specs=placed,
        out_specs=(
            P(("dp", "tensor"), None),
            P(("dp", "tensor"), None),
            P(),
            P(),
            P("dp", None, "tensor"),
            P(),
            P("tensor", "dp"),
            P(),
            P("dp", "tensor"),
            P(),
            P("tensor", "dp"),
        ),
        check_vma=False,
    )
```

```python
import functools

import jax
import jax.numpy as jnp
from jax import lax
from jax.experimental import pallas as pl
from jax.experimental.pallas import tpu as pltpu
from jax.sharding import PartitionSpec as P


D = 768
HEADS = 12
HEAD_DIM = 64
FF = 3072
SIDE_S = 12
SIDE_M = 15
SIDE_L = 20
TOK_DEV = 2048


EPSILON = 1e-06


def layout(group_counts):
    positions = jnp.arange(TOK_DEV, dtype=jnp.int32)
    area_small = SIDE_S * SIDE_S
    area_middle = SIDE_M * SIDE_M
    area_large = SIDE_L * SIDE_L
    end_small = group_counts[0] * area_small
    end_middle = end_small + group_counts[1] * area_middle
    end_large = end_middle + group_counts[2] * area_large
    size_class = (positions >= end_small).astype(jnp.int32) + (positions >= end_middle).astype(
        jnp.int32
    )
    begins = jnp.where(size_class == 0, 0, jnp.where(size_class == 1, end_small, end_middle))
    area_len = jnp.where(
        size_class == 0, area_small, jnp.where(size_class == 1, area_middle, area_large)
    )
    side_len = jnp.where(size_class == 0, SIDE_S, jnp.where(size_class == 1, SIDE_M, SIDE_L))
    within = positions - begins
    picture_index = within // area_len
    within_image = within % area_len
    is_valid = positions < end_large
    segment = jnp.where(is_valid, size_class * 16 + picture_index, 255)
    grid_row = (within_image // side_len).astype(jnp.float32)
    grid_col = (within_image % side_len).astype(jnp.float32)
    return (segment, grid_row, grid_col, is_valid.astype(jnp.float32))


def normalize(values, gain_row, shift_row):
    centred = values - jnp.mean(values, axis=-1, keepdims=True)
    spread = jnp.mean(centred * centred, axis=-1, keepdims=True)
    return centred * lax.rsqrt(spread + EPSILON) * gain_row + shift_row


def normalize_backward(values, gain_row, grad):
    centred = values - jnp.mean(values, axis=-1, keepdims=True)
    scale = lax.rsqrt(jnp.mean(centred * centred, axis=-1, keepdims=True) + EPSILON)
    unit = centred * scale
    scaled = grad * gain_row
    through = scale * (
        scaled
        - jnp.mean(scaled, axis=-1, keepdims=True)
        - unit * jnp.mean(scaled * unit, axis=-1, keepdims=True)
    )
    return through, jnp.sum(grad * unit, axis=0), jnp.sum(grad, axis=0)


def slopes_of(first_head, count_heads):
    head_number = (first_head + jnp.arange(count_heads, dtype=jnp.int32)).astype(jnp.float32) + 1.0
    return jnp.exp2(-8.0 * head_number / HEADS)


Q_BLOCK = 256
K_BLOCK = 256
NEG = -1e30


def key_ranges(segment, tokens):
    starts = jnp.arange(0, tokens, Q_BLOCK)
    first = segment[starts]
    last = segment[starts + Q_BLOCK - 1]
    key_lo = jnp.sum(segment[None, :] < first[:, None], axis=1)
    key_hi = jnp.sum(segment[None, :] <= last[:, None], axis=1)
    return (key_lo // K_BLOCK).astype(jnp.int32), ((key_hi + K_BLOCK - 1) // K_BLOCK).astype(jnp.int32)


def block_geometry(qi_ref, ki_ref, start):
    rq = qi_ref[:, 0:1]
    cq = qi_ref[:, 1:2]
    sq = qi_ref[:, 2:3]
    rk = ki_ref[0:1, pl.ds(start, K_BLOCK)]
    ck = ki_ref[1:2, pl.ds(start, K_BLOCK)]
    sk = ki_ref[2:3, pl.ds(start, K_BLOCK)]
    dr = rq - rk
    dc = cq - ck
    return jnp.where(sq == sk, jnp.sqrt(dr * dr + dc * dc), jnp.inf)


def fwd_kernel(heads, lo_ref, hi_ref, slope_ref, q_ref, k_ref, v_ref, qi_ref, ki_ref, o_ref, lse_ref):
    i = pl.program_id(0)
    queries = [q_ref[h] for h in range(heads)]
    width = q_ref.shape[2]

    def body(kb, carry):
        start = pl.multiple_of(kb * K_BLOCK, K_BLOCK)
        dist = block_geometry(qi_ref, ki_ref, start)
        out = []
        for h in range(heads):
            m_old, l_old, acc_old = carry[h]
            keys = k_ref[h, pl.ds(start, K_BLOCK), :]
            vals = v_ref[h, pl.ds(start, K_BLOCK), :]
            s = lax.dot_general(queries[h], keys, (((1,), (1,)), ((), ())),
                                preferred_element_type=jnp.float32) - slope_ref[h] * dist
            m_new = jnp.maximum(m_old, jnp.max(s, axis=1, keepdims=True))
            alpha = jnp.exp(m_old - m_new)
            p = jnp.exp(s - m_new)
            l_new = alpha * l_old + jnp.sum(p, axis=1, keepdims=True)
            acc_new = alpha * acc_old + jnp.dot(p.astype(jnp.bfloat16), vals,
                                                preferred_element_type=jnp.float32)
            out.append((m_new, l_new, acc_new))
        return tuple(out)

    init = tuple(
        (jnp.full((Q_BLOCK, 1), NEG, jnp.float32), jnp.zeros((Q_BLOCK, 1), jnp.float32),
         jnp.zeros((Q_BLOCK, width), jnp.float32))
        for _ in range(heads)
    )
    final = lax.fori_loop(lo_ref[i], hi_ref[i], body, init)
    for h in range(heads):
        m, l, acc = final[h]
        o_ref[h] = acc / l
        lse_ref[h] = m + jnp.log(l)


def bwd_kernel(heads, lo_ref, hi_ref, slope_ref, q_ref, k_ref, v_ref, qi_ref, ki_ref,
               o_ref, do_ref, lse_ref, dq_ref, dk_ref, dv_ref):
    i = pl.program_id(0)

    @pl.when(i == 0)
    def _():
        dk_ref[...] = jnp.zeros_like(dk_ref)
        dv_ref[...] = jnp.zeros_like(dv_ref)

    queries = [q_ref[h] for h in range(heads)]
    grads = [do_ref[h] for h in range(heads)]
    lses = [lse_ref[h] for h in range(heads)]
    deltas = [jnp.sum(grads[h].astype(jnp.float32) * o_ref[h], axis=1, keepdims=True)
              for h in range(heads)]
    width = q_ref.shape[2]

    def body(kb, carry):
        start = pl.multiple_of(kb * K_BLOCK, K_BLOCK)
        dist = block_geometry(qi_ref, ki_ref, start)
        out = []
        for h in range(heads):
            keys = k_ref[h, pl.ds(start, K_BLOCK), :]
            vals = v_ref[h, pl.ds(start, K_BLOCK), :]
            s = lax.dot_general(queries[h], keys, (((1,), (1,)), ((), ())),
                                preferred_element_type=jnp.float32) - slope_ref[h] * dist
            p = jnp.exp(s - lses[h])
            dp = lax.dot_general(grads[h], vals, (((1,), (1,)), ((), ())),
                                 preferred_element_type=jnp.float32)
            ds = (p * (dp - deltas[h])).astype(jnp.bfloat16)
            out.append(carry[h] + jnp.dot(ds, keys, preferred_element_type=jnp.float32))
            dk_ref[h, pl.ds(start, K_BLOCK), :] += lax.dot_general(
                ds, queries[h], (((0,), (0,)), ((), ())), preferred_element_type=jnp.float32)
            dv_ref[h, pl.ds(start, K_BLOCK), :] += lax.dot_general(
                p.astype(jnp.bfloat16), grads[h], (((0,), (0,)), ((), ())),
                preferred_element_type=jnp.float32)
        return tuple(out)

    init = tuple(jnp.zeros((Q_BLOCK, width), jnp.float32) for _ in range(heads))
    final = lax.fori_loop(lo_ref[i], hi_ref[i], body, init)
    for h in range(heads):
        dq_ref[h] = final[h]


def attention_fwd(lo, hi, slopes, q, k, v, qinfo, kinfo):
    heads, tokens, width = q.shape
    grid = (tokens // Q_BLOCK,)
    whole = lambda i, lo, hi: (0, 0, 0)
    rows = lambda i, lo, hi: (0, i, 0)
    return pl.pallas_call(
        functools.partial(fwd_kernel, heads),
        grid_spec=pltpu.PrefetchScalarGridSpec(
            num_scalar_prefetch=2,
            grid=grid,
            in_specs=[
                pl.BlockSpec(memory_space=pltpu.SMEM),
                pl.BlockSpec((heads, Q_BLOCK, width), rows),
                pl.BlockSpec((heads, tokens, width), whole),
                pl.BlockSpec((heads, tokens, width), whole),
                pl.BlockSpec((Q_BLOCK, 3), lambda i, lo, hi: (i, 0)),
                pl.BlockSpec((3, tokens), lambda i, lo, hi: (0, 0)),
            ],
            out_specs=[
                pl.BlockSpec((heads, Q_BLOCK, width), rows),
                pl.BlockSpec((heads, Q_BLOCK, 1), rows),
            ],
        ),
        out_shape=[
            jax.ShapeDtypeStruct((heads, tokens, width), jnp.float32),
            jax.ShapeDtypeStruct((heads, tokens, 1), jnp.float32),
        ],
        compiler_params=pltpu.CompilerParams(dimension_semantics=("arbitrary",)),
    )(lo, hi, slopes, q, k, v, qinfo, kinfo)


def attention_bwd(lo, hi, slopes, q, k, v, qinfo, kinfo, o, do, lse):
    heads, tokens, width = q.shape
    grid = (tokens // Q_BLOCK,)
    whole = lambda i, lo, hi: (0, 0, 0)
    rows = lambda i, lo, hi: (0, i, 0)
    return pl.pallas_call(
        functools.partial(bwd_kernel, heads),
        grid_spec=pltpu.PrefetchScalarGridSpec(
            num_scalar_prefetch=2,
            grid=grid,
            in_specs=[
                pl.BlockSpec(memory_space=pltpu.SMEM),
                pl.BlockSpec((heads, Q_BLOCK, width), rows),
                pl.BlockSpec((heads, tokens, width), whole),
                pl.BlockSpec((heads, tokens, width), whole),
                pl.BlockSpec((Q_BLOCK, 3), lambda i, lo, hi: (i, 0)),
                pl.BlockSpec((3, tokens), lambda i, lo, hi: (0, 0)),
                pl.BlockSpec((heads, Q_BLOCK, width), rows),
                pl.BlockSpec((heads, Q_BLOCK, width), rows),
                pl.BlockSpec((heads, Q_BLOCK, 1), rows),
            ],
            out_specs=[
                pl.BlockSpec((heads, Q_BLOCK, width), rows),
                pl.BlockSpec((heads, tokens, width), whole),
                pl.BlockSpec((heads, tokens, width), whole),
            ],
        ),
        out_shape=[
            jax.ShapeDtypeStruct((heads, tokens, width), jnp.float32),
            jax.ShapeDtypeStruct((heads, tokens, width), jnp.float32),
            jax.ShapeDtypeStruct((heads, tokens, width), jnp.float32),
        ],
        compiler_params=pltpu.CompilerParams(dimension_semantics=("arbitrary",)),
    )(lo, hi, slopes, q, k, v, qinfo, kinfo, o, do, lse)


def scatter_blocks(partial, tensor_size):
    me = lax.axis_index("tensor")
    blocks = partial.reshape(tensor_size, -1, partial.shape[1])
    own = lax.dynamic_index_in_dim(blocks, me, keepdims=False).astype(jnp.float32)
    outgoing = [
        lax.dynamic_index_in_dim(blocks, (me + shift) % tensor_size, keepdims=False).astype(
            jnp.bfloat16
        )
        for shift in range(1, tensor_size)
    ]
    return own, outgoing


def exchange_blocks(own, outgoing, tensor_size):
    total = own
    for shift in range(1, tensor_size):
        pairs = [(i, (i + shift) % tensor_size) for i in range(tensor_size)]
        total = total + lax.ppermute(outgoing[shift - 1], "tensor", pairs).astype(jnp.float32)
    return total


def scatter_tensor(partial, tensor_size):
    return exchange_blocks(*scatter_blocks(partial, tensor_size), tensor_size)


def halving_scatter(blocks, axis_name, wire):
    me = lax.axis_index(axis_name)
    bit = 0
    while blocks.shape[0] > 1:
        pairs = [(i, i ^ (1 << bit)) for i in range(blocks.shape[0] << bit)]
        halves = blocks.reshape((blocks.shape[0] // 2, 2) + blocks.shape[1:])
        mine = (me >> bit) & 1
        keep = lax.dynamic_index_in_dim(halves, mine, axis=1, keepdims=False)
        send = lax.dynamic_index_in_dim(halves, 1 - mine, axis=1, keepdims=False)
        arrived = lax.ppermute(send.astype(wire), axis_name, pairs)
        blocks = keep + arrived.astype(blocks.dtype)
        bit += 1
    return blocks[0]


def doubling_sum(values, axis_name, size):
    bit = 0
    while (1 << bit) < size:
        pairs = [(i, i ^ (1 << bit)) for i in range(size)]
        values = values + lax.ppermute(values, axis_name, pairs)
        bit += 1
    return values


def on_device_body(
    dp_size,
    patches,
    counts,
    norm_gain,
    norm_bias,
    w_qkv,
    b_qv,
    w_out,
    out_bias,
    w_up,
    b_up,
    w_down,
    cotangent,
):
    local_rows = patches.shape[0]
    width_here = w_qkv.shape[2]
    heads_here = width_here // HEAD_DIM
    ff_here = w_up.shape[1]
    tensor_pos = lax.axis_index("tensor")
    tensor_size = D // width_here
    score_scale = HEAD_DIM ** (-0.5)
    segment, grid_row, grid_col, is_valid = layout(counts[0])
    keep_rows = lax.dynamic_slice_in_dim(is_valid, tensor_pos * local_rows, local_rows)[:, None]
    slopes = slopes_of(tensor_pos * heads_here, heads_here)
    inputs = patches.astype(jnp.float32)
    inputs_all = lax.all_gather(patches, "tensor", axis=0, tiled=True).astype(jnp.float32)
    normed = normalize(inputs_all, norm_gain[0], norm_bias[0]).astype(jnp.bfloat16)
    projected = jnp.einsum("td,dsc->tsc", normed, w_qkv, preferred_element_type=jnp.float32)
    queries = (projected[:, 0] + b_qv[0]).astype(jnp.bfloat16)
    keys = projected[:, 1].astype(jnp.bfloat16)
    values = (projected[:, 2] + b_qv[1]).astype(jnp.bfloat16)

    def head_major(rows):
        return rows.reshape(TOK_DEV, heads_here, HEAD_DIM).transpose(1, 0, 2)

    def row_major(heads):
        return heads.transpose(1, 0, 2).reshape(TOK_DEV, width_here)

    key_lo, key_hi = key_ranges(segment, TOK_DEV)
    segment_f = segment.astype(jnp.float32)
    query_info = jnp.stack([grid_row, grid_col, segment_f], axis=1)
    key_info = jnp.stack([grid_row, grid_col, segment_f], axis=0)
    query_heads = head_major(queries) * jnp.asarray(score_scale, jnp.bfloat16)
    key_heads = head_major(keys)
    value_heads = head_major(values)
    mixed_f32, log_totals = attention_fwd(
        key_lo, key_hi, slopes, query_heads, key_heads, value_heads, query_info, key_info
    )
    upstream = cotangent.astype(jnp.float32)
    branch_grad = lax.all_gather(
        (keep_rows * upstream).astype(jnp.bfloat16), "tensor", axis=0, tiled=True
    )
    mixed_f32, log_totals, branch_grad = lax.optimization_barrier(
        (mixed_f32, log_totals, branch_grad)
    )
    mixed_rows = row_major(mixed_f32).astype(jnp.bfloat16)
    mixed_all = lax.all_gather(mixed_rows, "tensor", axis=1, tiled=True)
    w_out_all = lax.all_gather(w_out, "tensor", axis=0, tiled=True)
    attended = jnp.dot(mixed_all, w_out_all, preferred_element_type=jnp.float32)
    after_attn_all = inputs_all + is_valid[:, None] * (attended + out_bias[0])
    after_attn = lax.dynamic_slice_in_dim(after_attn_all, tensor_pos * local_rows, local_rows)
    normed_two = normalize(after_attn_all, norm_gain[1], norm_bias[1]).astype(jnp.bfloat16)
    hidden_pre = jnp.dot(normed_two, w_up, preferred_element_type=jnp.float32) + b_up
    normal_cdf = 0.5 * (1.0 + lax.erf(hidden_pre * (2.0 ** -0.5)))
    hidden = (hidden_pre * normal_cdf).astype(jnp.bfloat16)
    branch_partial = jnp.dot(hidden, w_down, preferred_element_type=jnp.float32)
    down_bias_grad = jnp.sum(keep_rows * upstream, axis=0)
    w_down_grad_t = jnp.einsum(
        "td,tf->df", branch_grad, hidden, preferred_element_type=jnp.float32
    )
    hidden_grad = jnp.einsum("td,fd->tf", branch_grad, w_down, preferred_element_type=jnp.float32)
    normal_pdf = jnp.exp(-0.5 * hidden_pre * hidden_pre) * ((2.0 * jnp.pi) ** -0.5)
    pre_grad = (hidden_grad * (normal_cdf + hidden_pre * normal_pdf)).astype(jnp.bfloat16)
    up_bias_grad = jnp.sum(pre_grad, axis=0, dtype=jnp.float32)
    w_up_grad = jnp.einsum("td,tf->df", normed_two, pre_grad, preferred_element_type=jnp.float32)
    normed_two_grad = lax.psum_scatter(
        jnp.einsum("tf,df->td", pre_grad, w_up, preferred_element_type=jnp.float32).astype(
            jnp.bfloat16
        ),
        "tensor",
        scatter_dimension=0,
        tiled=True,
    ).astype(jnp.float32)
    branch_own, branch_out = scatter_blocks(branch_partial, tensor_size)
    normed_two_grad, branch_own, branch_out = lax.optimization_barrier(
        (normed_two_grad, branch_own, branch_out)
    )
    through_two, gain_two_grad, shift_two_grad = normalize_backward(
        after_attn, norm_gain[1], normed_two_grad
    )
    after_grad = upstream + through_two
    attn_bias_grad = jnp.sum(keep_rows * after_grad, axis=0)
    attn_local = (keep_rows * after_grad).astype(jnp.bfloat16)
    attn_grad = lax.all_gather(attn_local, "tensor", axis=0, tiled=True)
    w_out_grad_t = jnp.einsum(
        "td,tc->dc", attn_grad, mixed_rows, preferred_element_type=jnp.float32
    )
    mixed_grad = jnp.einsum(
        "td,cd->tc", attn_grad, w_out, preferred_element_type=jnp.float32
    ).astype(jnp.bfloat16)
    early_parts = jnp.concatenate([w_down_grad_t, w_up_grad, w_out_grad_t], axis=1).astype(
        jnp.bfloat16
    )
    early_parts, mixed_grad, branch_own, branch_out = lax.optimization_barrier(
        (early_parts, mixed_grad, branch_own, branch_out)
    )
    branch = exchange_blocks(branch_own, branch_out, tensor_size)
    result = (after_attn + keep_rows * (branch + out_bias[1])).astype(jnp.bfloat16)
    early_sum = lax.psum_scatter(early_parts, "dp", scatter_dimension=0, tiled=True).astype(
        jnp.float32
    )
    query_acc, key_acc, value_acc = attention_bwd(
        key_lo, key_hi, slopes, query_heads, key_heads, value_heads, query_info, key_info,
        mixed_f32, head_major(mixed_grad), log_totals,
    )
    query_acc, key_acc, value_acc, result = lax.optimization_barrier(
        (query_acc, key_acc, value_acc, result)
    )
    query_grad = row_major(query_acc * score_scale).astype(jnp.bfloat16)
    key_grad = row_major(key_acc).astype(jnp.bfloat16)
    value_grad = row_major(value_acc).astype(jnp.bfloat16)
    projected_grad = jnp.concatenate([query_grad, key_grad, value_grad], axis=1)
    qv_bias_grad = jnp.stack(
        [
            jnp.sum(query_grad, axis=0, dtype=jnp.float32),
            jnp.sum(value_grad, axis=0, dtype=jnp.float32),
        ]
    )
    w_qkv_grad = jnp.einsum("td,tc->dc", normed, projected_grad, preferred_element_type=jnp.float32)
    normed_grad_partial = jnp.einsum(
        "tc,dc->td",
        projected_grad,
        w_qkv.reshape(D, 3 * width_here),
        preferred_element_type=jnp.float32,
    )
    normed_grad_partial, early_sum = lax.optimization_barrier((normed_grad_partial, early_sum))
    centred_all = inputs_all - jnp.mean(inputs_all, axis=-1, keepdims=True)
    unit_all = centred_all * lax.rsqrt(
        jnp.mean(centred_all * centred_all, axis=-1, keepdims=True) + EPSILON
    )
    gain_one_grad = jnp.sum(normed_grad_partial * unit_all, axis=0)
    shift_one_grad = jnp.sum(normed_grad_partial, axis=0)
    normed_grad = scatter_tensor(normed_grad_partial, tensor_size)
    through_one = normalize_backward(inputs, norm_gain[0], normed_grad)[0]
    input_grad = (after_grad + through_one).astype(jnp.bfloat16)
    qv_full = lax.dynamic_update_slice_in_dim(
        jnp.zeros((2, D), jnp.float32), qv_bias_grad, tensor_pos * width_here, 1
    )
    up_full = lax.dynamic_update_slice_in_dim(
        jnp.zeros((FF,), jnp.float32), up_bias_grad, tensor_pos * ff_here, 0
    )
    small = jnp.concatenate(
        [
            jnp.stack([gain_one_grad, gain_two_grad]).reshape(-1),
            jnp.stack([shift_one_grad, shift_two_grad]).reshape(-1),
            jnp.stack([attn_bias_grad, down_bias_grad]).reshape(-1),
            qv_full.reshape(-1),
            up_full,
        ]
    )
    qkv_sum = halving_scatter(
        w_qkv_grad.reshape(dp_size, D // dp_size, -1), "dp", jnp.bfloat16
    )
    qkv_part = qkv_sum.reshape(-1, 3, width_here)
    summed = doubling_sum(doubling_sum(small, "dp", dp_size), "tensor", tensor_size)
    gains_grad = summed[: 2 * D].reshape(2, D)
    shifts_grad = summed[2 * D : 4 * D].reshape(2, D)
    outer_grad = summed[4 * D : 6 * D].reshape(2, D)
    qv_sum = summed[6 * D : 8 * D].reshape(2, D)
    up_sum = summed[8 * D :]
    down_part = early_sum[:, :ff_here].T
    up_part = early_sum[:, ff_here : 2 * ff_here]
    out_part = early_sum[:, 2 * ff_here :].T
    return (
        result,
        input_grad,
        gains_grad,
        shifts_grad,
        qkv_part,
        qv_sum,
        out_part,
        outer_grad,
        up_part,
        up_sum,
        down_part,
    )


def solution(mesh):
    placed = (
        P(("dp", "tensor"), None),
        P("dp", None),
        P(),
        P(),
        P(None, None, "tensor"),
        P(None, "tensor"),
        P("tensor", None),
        P(),
        P(None, "tensor"),
        P("tensor"),
        P("tensor", None),
        P(("dp", "tensor"), None),
    )
    return jax.shard_map(
        functools.partial(on_device_body, mesh.shape["dp"]),
        mesh=mesh,
        in_specs=placed,
        out_specs=(
            P(("dp", "tensor"), None),
            P(("dp", "tensor"), None),
            P(),
            P(),
            P("dp", None, "tensor"),
            P(),
            P("tensor", "dp"),
            P(),
            P("dp", "tensor"),
            P(),
            P("tensor", "dp"),
        ),
        check_vma=False,
    )
```

```python
import functools

import jax
import jax.numpy as jnp
from jax import lax
from jax.experimental import pallas as pl
from jax.experimental.pallas import tpu as pltpu
from jax.sharding import PartitionSpec as P


D = 768
HEADS = 12
HEAD_DIM = 64
FF = 3072
SIDE_S = 12
SIDE_M = 15
SIDE_L = 20
TOK_DEV = 2048


EPSILON = 1e-06


def layout(group_counts):
    positions = jnp.arange(TOK_DEV, dtype=jnp.int32)
    area_small = SIDE_S * SIDE_S
    area_middle = SIDE_M * SIDE_M
    area_large = SIDE_L * SIDE_L
    end_small = group_counts[0] * area_small
    end_middle = end_small + group_counts[1] * area_middle
    end_large = end_middle + group_counts[2] * area_large
    size_class = (positions >= end_small).astype(jnp.int32) + (positions >= end_middle).astype(
        jnp.int32
    )
    begins = jnp.where(size_class == 0, 0, jnp.where(size_class == 1, end_small, end_middle))
    area_len = jnp.where(
        size_class == 0, area_small, jnp.where(size_class == 1, area_middle, area_large)
    )
    side_len = jnp.where(size_class == 0, SIDE_S, jnp.where(size_class == 1, SIDE_M, SIDE_L))
    within = positions - begins
    picture_index = within // area_len
    within_image = within % area_len
    is_valid = positions < end_large
    segment = jnp.where(is_valid, size_class * 16 + picture_index, 255)
    grid_row = (within_image // side_len).astype(jnp.float32)
    grid_col = (within_image % side_len).astype(jnp.float32)
    return (segment, grid_row, grid_col, is_valid.astype(jnp.float32))


def normalize(values, gain_row, shift_row):
    centred = values - jnp.mean(values, axis=-1, keepdims=True)
    spread = jnp.mean(centred * centred, axis=-1, keepdims=True)
    return centred * lax.rsqrt(spread + EPSILON) * gain_row + shift_row


def normalize_backward(values, gain_row, grad):
    centred = values - jnp.mean(values, axis=-1, keepdims=True)
    scale = lax.rsqrt(jnp.mean(centred * centred, axis=-1, keepdims=True) + EPSILON)
    unit = centred * scale
    scaled = grad * gain_row
    through = scale * (
        scaled
        - jnp.mean(scaled, axis=-1, keepdims=True)
        - unit * jnp.mean(scaled * unit, axis=-1, keepdims=True)
    )
    return through, jnp.sum(grad * unit, axis=0), jnp.sum(grad, axis=0)


def slopes_of(first_head, count_heads):
    head_number = (first_head + jnp.arange(count_heads, dtype=jnp.int32)).astype(jnp.float32) + 1.0
    return jnp.exp2(-8.0 * head_number / HEADS)


Q_BLOCK = 256
K_BLOCK = 256
NEG = -1e30


def key_ranges(segment, tokens):
    starts = jnp.arange(0, tokens, Q_BLOCK)
    first = segment[starts]
    last = segment[starts + Q_BLOCK - 1]
    key_lo = jnp.sum(segment[None, :] < first[:, None], axis=1)
    key_hi = jnp.sum(segment[None, :] <= last[:, None], axis=1)
    return (key_lo // K_BLOCK).astype(jnp.int32), ((key_hi + K_BLOCK - 1) // K_BLOCK).astype(jnp.int32)


def block_geometry(qi_ref, ki_ref, start):
    rq = qi_ref[:, 0:1]
    cq = qi_ref[:, 1:2]
    sq = qi_ref[:, 2:3]
    rk = ki_ref[0:1, pl.ds(start, K_BLOCK)]
    ck = ki_ref[1:2, pl.ds(start, K_BLOCK)]
    sk = ki_ref[2:3, pl.ds(start, K_BLOCK)]
    dr = rq - rk
    dc = cq - ck
    return jnp.where(sq == sk, jnp.sqrt(dr * dr + dc * dc), jnp.inf)


def fwd_kernel(heads, lo_ref, hi_ref, slope_ref, q_ref, k_ref, v_ref, qi_ref, ki_ref, o_ref, lse_ref):
    i = pl.program_id(0)
    queries = [q_ref[h] for h in range(heads)]
    width = q_ref.shape[2]

    def body(kb, carry):
        start = pl.multiple_of(kb * K_BLOCK, K_BLOCK)
        dist = block_geometry(qi_ref, ki_ref, start)
        out = []
        for h in range(heads):
            m_old, l_old, acc_old = carry[h]
            keys = k_ref[h, pl.ds(start, K_BLOCK), :]
            vals = v_ref[h, pl.ds(start, K_BLOCK), :]
            s = lax.dot_general(queries[h], keys, (((1,), (1,)), ((), ())),
                                preferred_element_type=jnp.float32) - slope_ref[h] * dist
            m_new = jnp.maximum(m_old, jnp.max(s, axis=1, keepdims=True))
            alpha = jnp.exp(m_old - m_new)
            p = jnp.exp(s - m_new)
            l_new = alpha * l_old + jnp.sum(p, axis=1, keepdims=True)
            acc_new = alpha * acc_old + jnp.dot(p.astype(jnp.bfloat16), vals,
                                                preferred_element_type=jnp.float32)
            out.append((m_new, l_new, acc_new))
        return tuple(out)

    init = tuple(
        (jnp.full((Q_BLOCK, 1), NEG, jnp.float32), jnp.zeros((Q_BLOCK, 1), jnp.float32),
         jnp.zeros((Q_BLOCK, width), jnp.float32))
        for _ in range(heads)
    )
    final = lax.fori_loop(lo_ref[i], hi_ref[i], body, init)
    for h in range(heads):
        m, l, acc = final[h]
        o_ref[h] = acc / l
        lse_ref[h] = m + jnp.log(l)


def bwd_kernel(heads, lo_ref, hi_ref, slope_ref, q_ref, k_ref, v_ref, qi_ref, ki_ref,
               o_ref, do_ref, lse_ref, dq_ref, dk_ref, dv_ref):
    i = pl.program_id(0)

    @pl.when(i == 0)
    def _():
        dk_ref[...] = jnp.zeros_like(dk_ref)
        dv_ref[...] = jnp.zeros_like(dv_ref)

    queries = [q_ref[h] for h in range(heads)]
    grads = [do_ref[h] for h in range(heads)]
    lses = [lse_ref[h] for h in range(heads)]
    deltas = [jnp.sum(grads[h].astype(jnp.float32) * o_ref[h], axis=1, keepdims=True)
              for h in range(heads)]
    width = q_ref.shape[2]

    def body(kb, carry):
        start = pl.multiple_of(kb * K_BLOCK, K_BLOCK)
        dist = block_geometry(qi_ref, ki_ref, start)
        out = []
        for h in range(heads):
            keys = k_ref[h, pl.ds(start, K_BLOCK), :]
            vals = v_ref[h, pl.ds(start, K_BLOCK), :]
            s = lax.dot_general(queries[h], keys, (((1,), (1,)), ((), ())),
                                preferred_element_type=jnp.float32) - slope_ref[h] * dist
            p = jnp.exp(s - lses[h])
            dp = lax.dot_general(grads[h], vals, (((1,), (1,)), ((), ())),
                                 preferred_element_type=jnp.float32)
            ds = (p * (dp - deltas[h])).astype(jnp.bfloat16)
            out.append(carry[h] + jnp.dot(ds, keys, preferred_element_type=jnp.float32))
            dk_ref[h, pl.ds(start, K_BLOCK), :] += lax.dot_general(
                ds, queries[h], (((0,), (0,)), ((), ())), preferred_element_type=jnp.float32)
            dv_ref[h, pl.ds(start, K_BLOCK), :] += lax.dot_general(
                p.astype(jnp.bfloat16), grads[h], (((0,), (0,)), ((), ())),
                preferred_element_type=jnp.float32)
        return tuple(out)

    init = tuple(jnp.zeros((Q_BLOCK, width), jnp.float32) for _ in range(heads))
    final = lax.fori_loop(lo_ref[i], hi_ref[i], body, init)
    for h in range(heads):
        dq_ref[h] = final[h]


def attention_fwd(lo, hi, slopes, q, k, v, qinfo, kinfo):
    heads, tokens, width = q.shape
    grid = (tokens // Q_BLOCK,)
    whole = lambda i, lo, hi: (0, 0, 0)
    rows = lambda i, lo, hi: (0, i, 0)
    return pl.pallas_call(
        functools.partial(fwd_kernel, heads),
        grid_spec=pltpu.PrefetchScalarGridSpec(
            num_scalar_prefetch=2,
            grid=grid,
            in_specs=[
                pl.BlockSpec(memory_space=pltpu.SMEM),
                pl.BlockSpec((heads, Q_BLOCK, width), rows),
                pl.BlockSpec((heads, tokens, width), whole),
                pl.BlockSpec((heads, tokens, width), whole),
                pl.BlockSpec((Q_BLOCK, 3), lambda i, lo, hi: (i, 0)),
                pl.BlockSpec((3, tokens), lambda i, lo, hi: (0, 0)),
            ],
            out_specs=[
                pl.BlockSpec((heads, Q_BLOCK, width), rows),
                pl.BlockSpec((heads, Q_BLOCK, 1), rows),
            ],
        ),
        out_shape=[
            jax.ShapeDtypeStruct((heads, tokens, width), jnp.float32),
            jax.ShapeDtypeStruct((heads, tokens, 1), jnp.float32),
        ],
        compiler_params=pltpu.CompilerParams(dimension_semantics=("arbitrary",)),
    )(lo, hi, slopes, q, k, v, qinfo, kinfo)


def attention_bwd(lo, hi, slopes, q, k, v, qinfo, kinfo, o, do, lse):
    heads, tokens, width = q.shape
    grid = (tokens // Q_BLOCK,)
    whole = lambda i, lo, hi: (0, 0, 0)
    rows = lambda i, lo, hi: (0, i, 0)
    return pl.pallas_call(
        functools.partial(bwd_kernel, heads),
        grid_spec=pltpu.PrefetchScalarGridSpec(
            num_scalar_prefetch=2,
            grid=grid,
            in_specs=[
                pl.BlockSpec(memory_space=pltpu.SMEM),
                pl.BlockSpec((heads, Q_BLOCK, width), rows),
                pl.BlockSpec((heads, tokens, width), whole),
                pl.BlockSpec((heads, tokens, width), whole),
                pl.BlockSpec((Q_BLOCK, 3), lambda i, lo, hi: (i, 0)),
                pl.BlockSpec((3, tokens), lambda i, lo, hi: (0, 0)),
                pl.BlockSpec((heads, Q_BLOCK, width), rows),
                pl.BlockSpec((heads, Q_BLOCK, width), rows),
                pl.BlockSpec((heads, Q_BLOCK, 1), rows),
            ],
            out_specs=[
                pl.BlockSpec((heads, Q_BLOCK, width), rows),
                pl.BlockSpec((heads, tokens, width), whole),
                pl.BlockSpec((heads, tokens, width), whole),
            ],
        ),
        out_shape=[
            jax.ShapeDtypeStruct((heads, tokens, width), jnp.float32),
            jax.ShapeDtypeStruct((heads, tokens, width), jnp.float32),
            jax.ShapeDtypeStruct((heads, tokens, width), jnp.float32),
        ],
        compiler_params=pltpu.CompilerParams(dimension_semantics=("arbitrary",)),
    )(lo, hi, slopes, q, k, v, qinfo, kinfo, o, do, lse)


def scatter_blocks(partial, tensor_size):
    me = lax.axis_index("tensor")
    blocks = partial.reshape(tensor_size, -1, partial.shape[1])
    own = lax.dynamic_index_in_dim(blocks, me, keepdims=False).astype(jnp.float32)
    outgoing = [
        lax.dynamic_index_in_dim(blocks, (me + shift) % tensor_size, keepdims=False).astype(
            jnp.bfloat16
        )
        for shift in range(1, tensor_size)
    ]
    return own, outgoing


def exchange_blocks(own, outgoing, tensor_size):
    total = own
    for shift in range(1, tensor_size):
        pairs = [(i, (i + shift) % tensor_size) for i in range(tensor_size)]
        total = total + lax.ppermute(outgoing[shift - 1], "tensor", pairs).astype(jnp.float32)
    return total


def scatter_tensor(partial, tensor_size):
    return exchange_blocks(*scatter_blocks(partial, tensor_size), tensor_size)


def direct_sum(values, axis_name, size):
    total = values
    for shift in range(1, size):
        pairs = [(i, (i + shift) % size) for i in range(size)]
        total = total + lax.ppermute(values, axis_name, pairs)
    return total


def halving_scatter(blocks, axis_name, wire):
    me = lax.axis_index(axis_name)
    bit = 0
    while blocks.shape[0] > 1:
        pairs = [(i, i ^ (1 << bit)) for i in range(blocks.shape[0] << bit)]
        halves = blocks.reshape((blocks.shape[0] // 2, 2) + blocks.shape[1:])
        mine = (me >> bit) & 1
        keep = lax.dynamic_index_in_dim(halves, mine, axis=1, keepdims=False)
        send = lax.dynamic_index_in_dim(halves, 1 - mine, axis=1, keepdims=False)
        arrived = lax.ppermute(send.astype(wire), axis_name, pairs)
        blocks = keep + arrived.astype(blocks.dtype)
        bit += 1
    return blocks[0]


def doubling_sum(values, axis_name, size):
    bit = 0
    while (1 << bit) < size:
        pairs = [(i, i ^ (1 << bit)) for i in range(size)]
        values = values + lax.ppermute(values, axis_name, pairs)
        bit += 1
    return values


def on_device_body(
    dp_size,
    patches,
    counts,
    norm_gain,
    norm_bias,
    w_qkv,
    b_qv,
    w_out,
    out_bias,
    w_up,
    b_up,
    w_down,
    cotangent,
):
    local_rows = patches.shape[0]
    width_here = w_qkv.shape[2]
    heads_here = width_here // HEAD_DIM
    ff_here = w_up.shape[1]
    tensor_pos = lax.axis_index("tensor")
    tensor_size = D // width_here
    score_scale = HEAD_DIM ** (-0.5)
    segment, grid_row, grid_col, is_valid = layout(counts[0])
    keep_rows = lax.dynamic_slice_in_dim(is_valid, tensor_pos * local_rows, local_rows)[:, None]
    slopes = slopes_of(tensor_pos * heads_here, heads_here)
    inputs = patches.astype(jnp.float32)
    inputs_all = lax.all_gather(patches, "tensor", axis=0, tiled=True).astype(jnp.float32)
    normed = normalize(inputs_all, norm_gain[0], norm_bias[0]).astype(jnp.bfloat16)
    projected = jnp.einsum("td,dsc->tsc", normed, w_qkv, preferred_element_type=jnp.float32)
    queries = (projected[:, 0] + b_qv[0]).astype(jnp.bfloat16)
    keys = projected[:, 1].astype(jnp.bfloat16)
    values = (projected[:, 2] + b_qv[1]).astype(jnp.bfloat16)

    def head_major(rows):
        return rows.reshape(TOK_DEV, heads_here, HEAD_DIM).transpose(1, 0, 2)

    def row_major(heads):
        return heads.transpose(1, 0, 2).reshape(TOK_DEV, width_here)

    key_lo, key_hi = key_ranges(segment, TOK_DEV)
    segment_f = segment.astype(jnp.float32)
    query_info = jnp.stack([grid_row, grid_col, segment_f], axis=1)
    key_info = jnp.stack([grid_row, grid_col, segment_f], axis=0)
    query_heads = head_major(queries) * jnp.asarray(score_scale, jnp.bfloat16)
    key_heads = head_major(keys)
    value_heads = head_major(values)
    mixed_f32, log_totals = attention_fwd(
        key_lo, key_hi, slopes, query_heads, key_heads, value_heads, query_info, key_info
    )
    upstream = cotangent.astype(jnp.float32)
    branch_grad = lax.all_gather(
        (keep_rows * upstream).astype(jnp.bfloat16), "tensor", axis=0, tiled=True
    )
    mixed_f32, log_totals, branch_grad = lax.optimization_barrier(
        (mixed_f32, log_totals, branch_grad)
    )
    mixed_rows = row_major(mixed_f32).astype(jnp.bfloat16)
    mixed_all = lax.all_gather(mixed_rows, "tensor", axis=1, tiled=True)
    w_out_all = lax.all_gather(w_out, "tensor", axis=0, tiled=True)
    attended = jnp.dot(mixed_all, w_out_all, preferred_element_type=jnp.float32)
    after_attn_all = inputs_all + is_valid[:, None] * (attended + out_bias[0])
    after_attn = lax.dynamic_slice_in_dim(after_attn_all, tensor_pos * local_rows, local_rows)
    normed_two = normalize(after_attn_all, norm_gain[1], norm_bias[1]).astype(jnp.bfloat16)
    hidden_pre = jnp.dot(normed_two, w_up, preferred_element_type=jnp.float32) + b_up
    normal_cdf = 0.5 * (1.0 + lax.erf(hidden_pre * (2.0 ** -0.5)))
    hidden = (hidden_pre * normal_cdf).astype(jnp.bfloat16)
    branch_partial = jnp.dot(hidden, w_down, preferred_element_type=jnp.float32)
    down_bias_grad = jnp.sum(keep_rows * upstream, axis=0)
    w_down_grad_t = jnp.einsum(
        "td,tf->df", branch_grad, hidden, preferred_element_type=jnp.float32
    )
    hidden_grad = jnp.einsum("td,fd->tf", branch_grad, w_down, preferred_element_type=jnp.float32)
    normal_pdf = jnp.exp(-0.5 * hidden_pre * hidden_pre) * ((2.0 * jnp.pi) ** -0.5)
    pre_grad = (hidden_grad * (normal_cdf + hidden_pre * normal_pdf)).astype(jnp.bfloat16)
    up_bias_grad = jnp.sum(pre_grad, axis=0, dtype=jnp.float32)
    w_up_grad = jnp.einsum("td,tf->df", normed_two, pre_grad, preferred_element_type=jnp.float32)
    normed_two_grad = lax.psum_scatter(
        jnp.einsum("tf,df->td", pre_grad, w_up, preferred_element_type=jnp.float32).astype(
            jnp.bfloat16
        ),
        "tensor",
        scatter_dimension=0,
        tiled=True,
    ).astype(jnp.float32)
    branch_own, branch_out = scatter_blocks(branch_partial, tensor_size)
    normed_two_grad, branch_own, branch_out = lax.optimization_barrier(
        (normed_two_grad, branch_own, branch_out)
    )
    through_two, gain_two_grad, shift_two_grad = normalize_backward(
        after_attn, norm_gain[1], normed_two_grad
    )
    after_grad = upstream + through_two
    attn_bias_grad = jnp.sum(keep_rows * after_grad, axis=0)
    attn_local = (keep_rows * after_grad).astype(jnp.bfloat16)
    attn_grad = lax.all_gather(attn_local, "tensor", axis=0, tiled=True)
    w_out_grad_t = jnp.einsum(
        "td,tc->dc", attn_grad, mixed_rows, preferred_element_type=jnp.float32
    )
    mixed_grad = jnp.einsum(
        "td,cd->tc", attn_grad, w_out, preferred_element_type=jnp.float32
    ).astype(jnp.bfloat16)
    early_parts = jnp.concatenate([w_down_grad_t, w_up_grad, w_out_grad_t], axis=1).astype(
        jnp.bfloat16
    )
    early_parts, mixed_grad, branch_own, branch_out = lax.optimization_barrier(
        (early_parts, mixed_grad, branch_own, branch_out)
    )
    branch = exchange_blocks(branch_own, branch_out, tensor_size)
    result = (after_attn + keep_rows * (branch + out_bias[1])).astype(jnp.bfloat16)
    early_sum = lax.psum_scatter(early_parts, "dp", scatter_dimension=0, tiled=True).astype(
        jnp.float32
    )
    query_acc, key_acc, value_acc = attention_bwd(
        key_lo, key_hi, slopes, query_heads, key_heads, value_heads, query_info, key_info,
        mixed_f32, head_major(mixed_grad), log_totals,
    )
    query_acc, key_acc, value_acc, result = lax.optimization_barrier(
        (query_acc, key_acc, value_acc, result)
    )
    query_grad = row_major(query_acc * score_scale).astype(jnp.bfloat16)
    key_grad = row_major(key_acc).astype(jnp.bfloat16)
    value_grad = row_major(value_acc).astype(jnp.bfloat16)
    projected_grad = jnp.concatenate([query_grad, key_grad, value_grad], axis=1)
    qv_bias_grad = jnp.stack(
        [
            jnp.sum(query_grad, axis=0, dtype=jnp.float32),
            jnp.sum(value_grad, axis=0, dtype=jnp.float32),
        ]
    )
    w_qkv_grad = jnp.einsum("td,tc->dc", normed, projected_grad, preferred_element_type=jnp.float32)
    normed_grad_partial = jnp.einsum(
        "tc,dc->td",
        projected_grad,
        w_qkv.reshape(D, 3 * width_here),
        preferred_element_type=jnp.float32,
    )
    normed_grad_partial, early_sum = lax.optimization_barrier(
        (normed_grad_partial, early_sum)
    )
    centred_all = inputs_all - jnp.mean(inputs_all, axis=-1, keepdims=True)
    unit_all = centred_all * lax.rsqrt(
        jnp.mean(centred_all * centred_all, axis=-1, keepdims=True) + EPSILON
    )
    gain_one_grad = jnp.sum(normed_grad_partial * unit_all, axis=0)
    shift_one_grad = jnp.sum(normed_grad_partial, axis=0)
    normed_grad = scatter_tensor(normed_grad_partial, tensor_size)
    through_one = normalize_backward(inputs, norm_gain[0], normed_grad)[0]
    input_grad = (after_grad + through_one).astype(jnp.bfloat16)
    qv_full = lax.dynamic_update_slice_in_dim(
        jnp.zeros((2, D), jnp.float32), qv_bias_grad, tensor_pos * width_here, 1
    )
    up_full = lax.dynamic_update_slice_in_dim(
        jnp.zeros((FF,), jnp.float32), up_bias_grad, tensor_pos * ff_here, 0
    )
    small = jnp.concatenate(
        [
            jnp.stack([gain_one_grad, gain_two_grad]).reshape(-1),
            jnp.stack([shift_one_grad, shift_two_grad]).reshape(-1),
            jnp.stack([attn_bias_grad, down_bias_grad]).reshape(-1),
            qv_full.reshape(-1),
            up_full,
        ]
    )
    qkv_sum = halving_scatter(
        w_qkv_grad.reshape(dp_size, D // dp_size, -1), "dp", jnp.bfloat16
    )
    qkv_part = qkv_sum.reshape(-1, 3, width_here)
    summed = direct_sum(doubling_sum(small, "dp", dp_size), "tensor", tensor_size)
    gains_grad = summed[: 2 * D].reshape(2, D)
    shifts_grad = summed[2 * D : 4 * D].reshape(2, D)
    outer_grad = summed[4 * D : 6 * D].reshape(2, D)
    qv_sum = summed[6 * D : 8 * D].reshape(2, D)
    up_sum = summed[8 * D :]
    down_part = early_sum[:, :ff_here].T
    up_part = early_sum[:, ff_here : 2 * ff_here]
    out_part = early_sum[:, 2 * ff_here :].T
    return (
        result,
        input_grad,
        gains_grad,
        shifts_grad,
        qkv_part,
        qv_sum,
        out_part,
        outer_grad,
        up_part,
        up_sum,
        down_part,
    )


def solution(mesh):
    placed = (
        P(("dp", "tensor"), None),
        P("dp", None),
        P(),
        P(),
        P(None, None, "tensor"),
        P(None, "tensor"),
        P("tensor", None),
        P(),
        P(None, "tensor"),
        P("tensor"),
        P("tensor", None),
        P(("dp", "tensor"), None),
    )
    return jax.shard_map(
        functools.partial(on_device_body, mesh.shape["dp"]),
        mesh=mesh,
        in_specs=placed,
        out_specs=(
            P(("dp", "tensor"), None),
            P(("dp", "tensor"), None),
            P(),
            P(),
            P("dp", None, "tensor"),
            P(),
            P("tensor", "dp"),
            P(),
            P("dp", "tensor"),
            P(),
            P("tensor", "dp"),
        ),
        check_vma=False,
    )
```

```python
import functools

import jax
import jax.numpy as jnp
from jax import lax
from jax.experimental import pallas as pl
from jax.experimental.pallas import tpu as pltpu
from jax.sharding import PartitionSpec as P


D = 768
HEADS = 12
HEAD_DIM = 64
FF = 3072
SIDE_S = 12
SIDE_M = 15
SIDE_L = 20
TOK_DEV = 2048


EPSILON = 1e-06


def layout(group_counts):
    positions = jnp.arange(TOK_DEV, dtype=jnp.int32)
    area_small = SIDE_S * SIDE_S
    area_middle = SIDE_M * SIDE_M
    area_large = SIDE_L * SIDE_L
    end_small = group_counts[0] * area_small
    end_middle = end_small + group_counts[1] * area_middle
    end_large = end_middle + group_counts[2] * area_large
    size_class = (positions >= end_small).astype(jnp.int32) + (positions >= end_middle).astype(
        jnp.int32
    )
    begins = jnp.where(size_class == 0, 0, jnp.where(size_class == 1, end_small, end_middle))
    area_len = jnp.where(
        size_class == 0, area_small, jnp.where(size_class == 1, area_middle, area_large)
    )
    side_len = jnp.where(size_class == 0, SIDE_S, jnp.where(size_class == 1, SIDE_M, SIDE_L))
    within = positions - begins
    picture_index = within // area_len
    within_image = within % area_len
    is_valid = positions < end_large
    segment = jnp.where(is_valid, size_class * 16 + picture_index, 255)
    grid_row = (within_image // side_len).astype(jnp.float32)
    grid_col = (within_image % side_len).astype(jnp.float32)
    return (segment, grid_row, grid_col, is_valid.astype(jnp.float32))


def normalize(values, gain_row, shift_row):
    centred = values - jnp.mean(values, axis=-1, keepdims=True)
    spread = jnp.mean(centred * centred, axis=-1, keepdims=True)
    return centred * lax.rsqrt(spread + EPSILON) * gain_row + shift_row


def normalize_backward(values, gain_row, grad):
    centred = values - jnp.mean(values, axis=-1, keepdims=True)
    scale = lax.rsqrt(jnp.mean(centred * centred, axis=-1, keepdims=True) + EPSILON)
    unit = centred * scale
    scaled = grad * gain_row
    through = scale * (
        scaled
        - jnp.mean(scaled, axis=-1, keepdims=True)
        - unit * jnp.mean(scaled * unit, axis=-1, keepdims=True)
    )
    return through, jnp.sum(grad * unit, axis=0), jnp.sum(grad, axis=0)


def slopes_of(first_head, count_heads):
    head_number = (first_head + jnp.arange(count_heads, dtype=jnp.int32)).astype(jnp.float32) + 1.0
    return jnp.exp2(-8.0 * head_number / HEADS)


Q_BLOCK = 256
K_BLOCK = 256
NEG = -1e30


def key_ranges(segment, tokens):
    starts = jnp.arange(0, tokens, Q_BLOCK)
    first = segment[starts]
    last = segment[starts + Q_BLOCK - 1]
    key_lo = jnp.sum(segment[None, :] < first[:, None], axis=1)
    key_hi = jnp.sum(segment[None, :] <= last[:, None], axis=1)
    return (key_lo // K_BLOCK).astype(jnp.int32), ((key_hi + K_BLOCK - 1) // K_BLOCK).astype(jnp.int32)


def block_geometry(qi_ref, ki_ref, start):
    rq = qi_ref[:, 0:1]
    cq = qi_ref[:, 1:2]
    sq = qi_ref[:, 2:3]
    rk = ki_ref[0:1, pl.ds(start, K_BLOCK)]
    ck = ki_ref[1:2, pl.ds(start, K_BLOCK)]
    sk = ki_ref[2:3, pl.ds(start, K_BLOCK)]
    dr = rq - rk
    dc = cq - ck
    return jnp.where(sq == sk, jnp.sqrt(dr * dr + dc * dc), jnp.inf)


def fwd_kernel(heads, lo_ref, hi_ref, slope_ref, q_ref, k_ref, v_ref, qi_ref, ki_ref, o_ref, lse_ref):
    i = pl.program_id(0)
    queries = [q_ref[h] for h in range(heads)]
    width = q_ref.shape[2]

    def body(kb, carry):
        start = pl.multiple_of(kb * K_BLOCK, K_BLOCK)
        dist = block_geometry(qi_ref, ki_ref, start)
        out = []
        for h in range(heads):
            m_old, l_old, acc_old = carry[h]
            keys = k_ref[h, pl.ds(start, K_BLOCK), :]
            vals = v_ref[h, pl.ds(start, K_BLOCK), :]
            s = lax.dot_general(queries[h], keys, (((1,), (1,)), ((), ())),
                                preferred_element_type=jnp.float32) - slope_ref[h] * dist
            m_new = jnp.maximum(m_old, jnp.max(s, axis=1, keepdims=True))
            alpha = jnp.exp(m_old - m_new)
            p = jnp.exp(s - m_new)
            l_new = alpha * l_old + jnp.sum(p, axis=1, keepdims=True)
            acc_new = alpha * acc_old + jnp.dot(p.astype(jnp.bfloat16), vals,
                                                preferred_element_type=jnp.float32)
            out.append((m_new, l_new, acc_new))
        return tuple(out)

    init = tuple(
        (jnp.full((Q_BLOCK, 1), NEG, jnp.float32), jnp.zeros((Q_BLOCK, 1), jnp.float32),
         jnp.zeros((Q_BLOCK, width), jnp.float32))
        for _ in range(heads)
    )
    final = lax.fori_loop(lo_ref[i], hi_ref[i], body, init)
    for h in range(heads):
        m, l, acc = final[h]
        o_ref[h] = acc * (1.0 / l)
        lse_ref[h] = m + jnp.log(l)


def bwd_kernel(heads, lo_ref, hi_ref, slope_ref, q_ref, k_ref, v_ref, qi_ref, ki_ref,
               o_ref, do_ref, lse_ref, dq_ref, dk_ref, dv_ref):
    i = pl.program_id(0)

    @pl.when(i == 0)
    def _():
        dk_ref[...] = jnp.zeros_like(dk_ref)
        dv_ref[...] = jnp.zeros_like(dv_ref)

    queries = [q_ref[h] for h in range(heads)]
    grads = [do_ref[h] for h in range(heads)]
    lses = [lse_ref[h] for h in range(heads)]
    deltas = [jnp.sum(grads[h].astype(jnp.float32) * o_ref[h], axis=1, keepdims=True)
              for h in range(heads)]
    width = q_ref.shape[2]

    def body(kb, carry):
        start = pl.multiple_of(kb * K_BLOCK, K_BLOCK)
        dist = block_geometry(qi_ref, ki_ref, start)
        out = []
        for h in range(heads):
            keys = k_ref[h, pl.ds(start, K_BLOCK), :]
            vals = v_ref[h, pl.ds(start, K_BLOCK), :]
            s = lax.dot_general(queries[h], keys, (((1,), (1,)), ((), ())),
                                preferred_element_type=jnp.float32) - slope_ref[h] * dist
            p = jnp.exp(s - lses[h])
            dp = lax.dot_general(grads[h], vals, (((1,), (1,)), ((), ())),
                                 preferred_element_type=jnp.float32)
            ds = (p * (dp - deltas[h])).astype(jnp.bfloat16)
            out.append(carry[h] + jnp.dot(ds, keys, preferred_element_type=jnp.float32))
            dk_ref[h, pl.ds(start, K_BLOCK), :] += lax.dot_general(
                ds, queries[h], (((0,), (0,)), ((), ())), preferred_element_type=jnp.float32)
            dv_ref[h, pl.ds(start, K_BLOCK), :] += lax.dot_general(
                p.astype(jnp.bfloat16), grads[h], (((0,), (0,)), ((), ())),
                preferred_element_type=jnp.float32)
        return tuple(out)

    init = tuple(jnp.zeros((Q_BLOCK, width), jnp.float32) for _ in range(heads))
    final = lax.fori_loop(lo_ref[i], hi_ref[i], body, init)
    for h in range(heads):
        dq_ref[h] = final[h]


def attention_fwd(lo, hi, slopes, q, k, v, qinfo, kinfo):
    heads, tokens, width = q.shape
    grid = (tokens // Q_BLOCK,)
    whole = lambda i, lo, hi: (0, 0, 0)
    rows = lambda i, lo, hi: (0, i, 0)
    return pl.pallas_call(
        functools.partial(fwd_kernel, heads),
        grid_spec=pltpu.PrefetchScalarGridSpec(
            num_scalar_prefetch=2,
            grid=grid,
            in_specs=[
                pl.BlockSpec(memory_space=pltpu.SMEM),
                pl.BlockSpec((heads, Q_BLOCK, width), rows),
                pl.BlockSpec((heads, tokens, width), whole),
                pl.BlockSpec((heads, tokens, width), whole),
                pl.BlockSpec((Q_BLOCK, 3), lambda i, lo, hi: (i, 0)),
                pl.BlockSpec((3, tokens), lambda i, lo, hi: (0, 0)),
            ],
            out_specs=[
                pl.BlockSpec((heads, Q_BLOCK, width), rows),
                pl.BlockSpec((heads, Q_BLOCK, 1), rows),
            ],
        ),
        out_shape=[
            jax.ShapeDtypeStruct((heads, tokens, width), jnp.float32),
            jax.ShapeDtypeStruct((heads, tokens, 1), jnp.float32),
        ],
        compiler_params=pltpu.CompilerParams(dimension_semantics=("arbitrary",)),
    )(lo, hi, slopes, q, k, v, qinfo, kinfo)


def attention_bwd(lo, hi, slopes, q, k, v, qinfo, kinfo, o, do, lse):
    heads, tokens, width = q.shape
    grid = (tokens // Q_BLOCK,)
    whole = lambda i, lo, hi: (0, 0, 0)
    rows = lambda i, lo, hi: (0, i, 0)
    return pl.pallas_call(
        functools.partial(bwd_kernel, heads),
        grid_spec=pltpu.PrefetchScalarGridSpec(
            num_scalar_prefetch=2,
            grid=grid,
            in_specs=[
                pl.BlockSpec(memory_space=pltpu.SMEM),
                pl.BlockSpec((heads, Q_BLOCK, width), rows),
                pl.BlockSpec((heads, tokens, width), whole),
                pl.BlockSpec((heads, tokens, width), whole),
                pl.BlockSpec((Q_BLOCK, 3), lambda i, lo, hi: (i, 0)),
                pl.BlockSpec((3, tokens), lambda i, lo, hi: (0, 0)),
                pl.BlockSpec((heads, Q_BLOCK, width), rows),
                pl.BlockSpec((heads, Q_BLOCK, width), rows),
                pl.BlockSpec((heads, Q_BLOCK, 1), rows),
            ],
            out_specs=[
                pl.BlockSpec((heads, Q_BLOCK, width), rows),
                pl.BlockSpec((heads, tokens, width), whole),
                pl.BlockSpec((heads, tokens, width), whole),
            ],
        ),
        out_shape=[
            jax.ShapeDtypeStruct((heads, tokens, width), jnp.float32),
            jax.ShapeDtypeStruct((heads, tokens, width), jnp.float32),
            jax.ShapeDtypeStruct((heads, tokens, width), jnp.float32),
        ],
        compiler_params=pltpu.CompilerParams(dimension_semantics=("arbitrary",)),
    )(lo, hi, slopes, q, k, v, qinfo, kinfo, o, do, lse)


def scatter_blocks(partial, tensor_size):
    me = lax.axis_index("tensor")
    blocks = partial.reshape(tensor_size, -1, partial.shape[1])
    own = lax.dynamic_index_in_dim(blocks, me, keepdims=False).astype(jnp.float32)
    outgoing = [
        lax.dynamic_index_in_dim(blocks, (me + shift) % tensor_size, keepdims=False).astype(
            jnp.bfloat16
        )
        for shift in range(1, tensor_size)
    ]
    return own, outgoing


def exchange_blocks(own, outgoing, tensor_size):
    total = own
    for shift in range(1, tensor_size):
        pairs = [(i, (i + shift) % tensor_size) for i in range(tensor_size)]
        total = total + lax.ppermute(outgoing[shift - 1], "tensor", pairs).astype(jnp.float32)
    return total


def scatter_tensor(partial, tensor_size):
    return exchange_blocks(*scatter_blocks(partial, tensor_size), tensor_size)


def halving_scatter(blocks, axis_name, wire):
    me = lax.axis_index(axis_name)
    bit = 0
    while blocks.shape[0] > 1:
        pairs = [(i, i ^ (1 << bit)) for i in range(blocks.shape[0] << bit)]
        halves = blocks.reshape((blocks.shape[0] // 2, 2) + blocks.shape[1:])
        mine = (me >> bit) & 1
        keep = lax.dynamic_index_in_dim(halves, mine, axis=1, keepdims=False)
        send = lax.dynamic_index_in_dim(halves, 1 - mine, axis=1, keepdims=False)
        arrived = lax.ppermute(send.astype(wire), axis_name, pairs)
        blocks = keep + arrived.astype(blocks.dtype)
        bit += 1
    return blocks[0]


def doubling_sum(values, axis_name, size):
    bit = 0
    while (1 << bit) < size:
        pairs = [(i, i ^ (1 << bit)) for i in range(size)]
        values = values + lax.ppermute(values, axis_name, pairs)
        bit += 1
    return values


def on_device_body(
    dp_size,
    patches,
    counts,
    norm_gain,
    norm_bias,
    w_qkv,
    b_qv,
    w_out,
    out_bias,
    w_up,
    b_up,
    w_down,
    cotangent,
):
    local_rows = patches.shape[0]
    width_here = w_qkv.shape[2]
    heads_here = width_here // HEAD_DIM
    ff_here = w_up.shape[1]
    tensor_pos = lax.axis_index("tensor")
    tensor_size = D // width_here
    score_scale = HEAD_DIM ** (-0.5)
    segment, grid_row, grid_col, is_valid = layout(counts[0])
    keep_rows = lax.dynamic_slice_in_dim(is_valid, tensor_pos * local_rows, local_rows)[:, None]
    slopes = slopes_of(tensor_pos * heads_here, heads_here)
    inputs = patches.astype(jnp.float32)
    inputs_all = lax.all_gather(patches, "tensor", axis=0, tiled=True).astype(jnp.float32)
    normed = normalize(inputs_all, norm_gain[0], norm_bias[0]).astype(jnp.bfloat16)
    projected = jnp.einsum("td,dsc->tsc", normed, w_qkv, preferred_element_type=jnp.float32)
    queries = (projected[:, 0] + b_qv[0]).astype(jnp.bfloat16)
    keys = projected[:, 1].astype(jnp.bfloat16)
    values = (projected[:, 2] + b_qv[1]).astype(jnp.bfloat16)

    def head_major(rows):
        return rows.reshape(TOK_DEV, heads_here, HEAD_DIM).transpose(1, 0, 2)

    def row_major(heads):
        return heads.transpose(1, 0, 2).reshape(TOK_DEV, width_here)

    key_lo, key_hi = key_ranges(segment, TOK_DEV)
    segment_f = segment.astype(jnp.float32)
    query_info = jnp.stack([grid_row, grid_col, segment_f], axis=1)
    key_info = jnp.stack([grid_row, grid_col, segment_f], axis=0)
    query_heads = head_major(queries) * jnp.asarray(score_scale, jnp.bfloat16)
    key_heads = head_major(keys)
    value_heads = head_major(values)
    mixed_f32, log_totals = attention_fwd(
        key_lo, key_hi, slopes, query_heads, key_heads, value_heads, query_info, key_info
    )
    upstream = cotangent.astype(jnp.float32)
    branch_grad = lax.all_gather(
        (keep_rows * upstream).astype(jnp.bfloat16), "tensor", axis=0, tiled=True
    )
    mixed_f32, log_totals, branch_grad = lax.optimization_barrier(
        (mixed_f32, log_totals, branch_grad)
    )
    mixed_rows = row_major(mixed_f32).astype(jnp.bfloat16)
    mixed_all = lax.all_gather(mixed_rows, "tensor", axis=1, tiled=True)
    w_out_all = lax.all_gather(w_out, "tensor", axis=0, tiled=True)
    attended = jnp.dot(mixed_all, w_out_all, preferred_element_type=jnp.float32)
    after_attn_all = inputs_all + is_valid[:, None] * (attended + out_bias[0])
    after_attn = lax.dynamic_slice_in_dim(after_attn_all, tensor_pos * local_rows, local_rows)
    normed_two = normalize(after_attn_all, norm_gain[1], norm_bias[1]).astype(jnp.bfloat16)
    hidden_pre = jnp.dot(normed_two, w_up, preferred_element_type=jnp.float32) + b_up
    normal_cdf = 0.5 * (1.0 + lax.erf(hidden_pre * (2.0 ** -0.5)))
    hidden = (hidden_pre * normal_cdf).astype(jnp.bfloat16)
    branch_partial = jnp.dot(hidden, w_down, preferred_element_type=jnp.float32)
    down_bias_grad = jnp.sum(keep_rows * upstream, axis=0)
    w_down_grad_t = jnp.einsum(
        "td,tf->df", branch_grad, hidden, preferred_element_type=jnp.float32
    )
    hidden_grad = jnp.einsum("td,fd->tf", branch_grad, w_down, preferred_element_type=jnp.float32)
    normal_pdf = jnp.exp(-0.5 * hidden_pre * hidden_pre) * ((2.0 * jnp.pi) ** -0.5)
    pre_grad = (hidden_grad * (normal_cdf + hidden_pre * normal_pdf)).astype(jnp.bfloat16)
    up_bias_grad = jnp.sum(pre_grad, axis=0, dtype=jnp.float32)
    w_up_grad = jnp.einsum("td,tf->df", normed_two, pre_grad, preferred_element_type=jnp.float32)
    normed_two_grad = lax.psum_scatter(
        jnp.einsum("tf,df->td", pre_grad, w_up, preferred_element_type=jnp.float32).astype(
            jnp.bfloat16
        ),
        "tensor",
        scatter_dimension=0,
        tiled=True,
    ).astype(jnp.float32)
    branch_own, branch_out = scatter_blocks(branch_partial, tensor_size)
    normed_two_grad, branch_own, branch_out = lax.optimization_barrier(
        (normed_two_grad, branch_own, branch_out)
    )
    through_two, gain_two_grad, shift_two_grad = normalize_backward(
        after_attn, norm_gain[1], normed_two_grad
    )
    after_grad = upstream + through_two
    attn_bias_grad = jnp.sum(keep_rows * after_grad, axis=0)
    attn_local = (keep_rows * after_grad).astype(jnp.bfloat16)
    attn_grad = lax.all_gather(attn_local, "tensor", axis=0, tiled=True)
    w_out_grad_t = jnp.einsum(
        "td,tc->dc", attn_grad, mixed_rows, preferred_element_type=jnp.float32
    )
    mixed_grad = jnp.einsum(
        "td,cd->tc", attn_grad, w_out, preferred_element_type=jnp.float32
    ).astype(jnp.bfloat16)
    early_parts = jnp.concatenate([w_down_grad_t, w_up_grad, w_out_grad_t], axis=1).astype(
        jnp.bfloat16
    )
    early_parts, mixed_grad, branch_own, branch_out = lax.optimization_barrier(
        (early_parts, mixed_grad, branch_own, branch_out)
    )
    branch = exchange_blocks(branch_own, branch_out, tensor_size)
    result = (after_attn + keep_rows * (branch + out_bias[1])).astype(jnp.bfloat16)
    early_sum = lax.psum_scatter(early_parts, "dp", scatter_dimension=0, tiled=True).astype(
        jnp.float32
    )
    query_acc, key_acc, value_acc = attention_bwd(
        key_lo, key_hi, slopes, query_heads, key_heads, value_heads, query_info, key_info,
        mixed_f32, head_major(mixed_grad), log_totals,
    )
    query_acc, key_acc, value_acc, result = lax.optimization_barrier(
        (query_acc, key_acc, value_acc, result)
    )
    query_grad = row_major(query_acc * score_scale).astype(jnp.bfloat16)
    key_grad = row_major(key_acc).astype(jnp.bfloat16)
    value_grad = row_major(value_acc).astype(jnp.bfloat16)
    projected_grad = jnp.concatenate([query_grad, key_grad, value_grad], axis=1)
    qv_bias_grad = jnp.stack(
        [
            jnp.sum(query_grad, axis=0, dtype=jnp.float32),
            jnp.sum(value_grad, axis=0, dtype=jnp.float32),
        ]
    )
    w_qkv_grad = jnp.einsum("td,tc->dc", normed, projected_grad, preferred_element_type=jnp.float32)
    normed_grad_partial = jnp.einsum(
        "tc,dc->td",
        projected_grad,
        w_qkv.reshape(D, 3 * width_here),
        preferred_element_type=jnp.float32,
    )
    normed_grad_partial, early_sum = lax.optimization_barrier(
        (normed_grad_partial, early_sum)
    )
    centred_all = inputs_all - jnp.mean(inputs_all, axis=-1, keepdims=True)
    unit_all = centred_all * lax.rsqrt(
        jnp.mean(centred_all * centred_all, axis=-1, keepdims=True) + EPSILON
    )
    gain_one_grad = jnp.sum(normed_grad_partial * unit_all, axis=0)
    shift_one_grad = jnp.sum(normed_grad_partial, axis=0)
    normed_grad = scatter_tensor(normed_grad_partial, tensor_size)
    through_one = normalize_backward(inputs, norm_gain[0], normed_grad)[0]
    input_grad = (after_grad + through_one).astype(jnp.bfloat16)
    qv_full = lax.dynamic_update_slice_in_dim(
        jnp.zeros((2, D), jnp.float32), qv_bias_grad, tensor_pos * width_here, 1
    )
    up_full = lax.dynamic_update_slice_in_dim(
        jnp.zeros((FF,), jnp.float32), up_bias_grad, tensor_pos * ff_here, 0
    )
    small = jnp.concatenate(
        [
            jnp.stack([gain_one_grad, gain_two_grad]).reshape(-1),
            jnp.stack([shift_one_grad, shift_two_grad]).reshape(-1),
            jnp.stack([attn_bias_grad, down_bias_grad]).reshape(-1),
            qv_full.reshape(-1),
            up_full,
        ]
    )
    qkv_sum = halving_scatter(
        w_qkv_grad.reshape(dp_size, D // dp_size, -1), "dp", jnp.bfloat16
    )
    qkv_part = qkv_sum.reshape(-1, 3, width_here)
    summed = doubling_sum(doubling_sum(small, "dp", dp_size), "tensor", tensor_size)
    gains_grad = summed[: 2 * D].reshape(2, D)
    shifts_grad = summed[2 * D : 4 * D].reshape(2, D)
    outer_grad = summed[4 * D : 6 * D].reshape(2, D)
    qv_sum = summed[6 * D : 8 * D].reshape(2, D)
    up_sum = summed[8 * D :]
    down_part = early_sum[:, :ff_here].T
    up_part = early_sum[:, ff_here : 2 * ff_here]
    out_part = early_sum[:, 2 * ff_here :].T
    return (
        result,
        input_grad,
        gains_grad,
        shifts_grad,
        qkv_part,
        qv_sum,
        out_part,
        outer_grad,
        up_part,
        up_sum,
        down_part,
    )


def solution(mesh):
    placed = (
        P(("dp", "tensor"), None),
        P("dp", None),
        P(),
        P(),
        P(None, None, "tensor"),
        P(None, "tensor"),
        P("tensor", None),
        P(),
        P(None, "tensor"),
        P("tensor"),
        P("tensor", None),
        P(("dp", "tensor"), None),
    )
    return jax.shard_map(
        functools.partial(on_device_body, mesh.shape["dp"]),
        mesh=mesh,
        in_specs=placed,
        out_specs=(
            P(("dp", "tensor"), None),
            P(("dp", "tensor"), None),
            P(),
            P(),
            P("dp", None, "tensor"),
            P(),
            P("tensor", "dp"),
            P(),
            P("dp", "tensor"),
            P(),
            P("tensor", "dp"),
        ),
        check_vma=False,
    )
```
